32 devices in a mesh: tok: 8 (over z, core), mdl: 4 (over y, x).
Axes of the slice: x: 2, y: 2, z: 4, core: 2. Of those that a mesh axis runs over, the one named last changes fastest.
Arguments:
- inputs: bfloat16 [8192, 2560], P('tok', 'mdl'), may hold values from -6 to 6
- positions: int32 [8192], P(('tok', 'mdl')), may hold values from 0 to 1023, as said below
- norm1_gain: bfloat16 [2560], P('tok'), may hold values from 0.099609375 to 1.8984375
- qkv_weight: bfloat16 [2560, 3072], P('tok', 'mdl'), as said below
- out_weight: bfloat16 [2560, 2560], P('mdl', 'tok'), may hold values from -0.5 to 0.5
- norm2_gain: bfloat16 [2560], P('tok'), may hold values from 0.099609375 to 1.8984375
- gate_weight: bfloat16 [2560, 7680], P('tok', 'mdl'), may hold values from -0.125 to 0.125
- up_weight: bfloat16 [2560, 7680], P('tok', 'mdl'), may hold values from -0.125 to 0.125
- down_weight: bfloat16 [7680, 2560], P('mdl', 'tok'), may hold values from -0.0625 to 0.0625
- cotangent: bfloat16 [8192, 2560], P('tok'), may hold values from -6 to 6
Outputs:
- block_out: bfloat16 [8192, 2560], P('tok', 'mdl')
- input_grad: float32 [8192, 2560], P('tok', 'mdl')
- norm1_gain_grad: float32 [2560], P('tok')
- qkv_grad: float32 [2560, 3072], P('tok', 'mdl')
- out_grad: float32 [2560, 2560], P('mdl', 'tok')
- norm2_gain_grad: float32 [2560], P('tok')
- gate_grad: float32 [2560, 7680], P('tok', 'mdl')
- up_grad: float32 [2560, 7680], P('tok', 'mdl')
- down_grad: float32 [7680, 2560], P('mdl', 'tok')
The draws below stay inside these ranges and needn't reach their ends.
Inputs may be any that keep to these rules, and one draw needn't show every extreme that they name: positions[t] is 0 where a packed sequence begins and positions[t-1] + 1 otherwise; every sequence lies inside one aligned block of 1024 tokens. `qkv_weight`: projection weights, columns in the order of the query heads, the key head and the value head.
All inputs are finite; a program needn't handle non-finite values.
Results may differ from the reference program's by a relative error of at most 0.023.
Values may be sent and summed in bfloat16 or wider, within the bound.
A program may use at most 320 MiB of HBM per device.

```python
import math
import jax
import jax.numpy as jnp
from jax import lax

D = 2560
HEADS = 10
HEAD = 256
FF = 7680
SEG_MAX = 1024
TOKENS = 8192
HEAD_COLS = 2560
QKV = 3072
N_MDL = 4


def draw_positions(key, part):
    blocks = TOKENS // SEG_MAX
    cut_points = jax.random.randint(key, (blocks, 2), 0, SEG_MAX)
    cut_points = cut_points.at[0].set(0)
    offset = jnp.arange(SEG_MAX, dtype=jnp.int32)
    starts = (offset[None, :] == 0) | (offset[None, :] == cut_points[:, 0:1]) | (offset[None, :] == cut_points[:, 1:2])
    token_index = jnp.arange(TOKENS, dtype=jnp.int32)
    seg_start = lax.cummax(jnp.where(starts.reshape(-1), token_index, 0), axis=0)
    return (token_index - seg_start).astype(jnp.int32)


def draw_qkv_weight(key, part):
    base_key = jax.random.fold_in(key, 11)
    matrix = jax.random.normal(base_key, (D, QKV), jnp.float32) * D ** (-0.5)
    return matrix.astype(jnp.bfloat16)


def levels(key, extent, cuts, smallest, largest):
    loudness = 1.0
    for dim, shards_of in cuts:
        steps = jax.random.uniform(jax.random.fold_in(jax.random.fold_in(key, 6), dim), (shards_of,), jnp.float32, smallest / len(cuts), largest / len(cuts))
        loudness = loudness * jnp.repeat(jnp.exp(steps), extent[dim] // shards_of).reshape((-1,) + (1,) * (len(extent) - 1 - dim))
    return loudness


def centred(rng, shape, scale, bound, shards=(), held_as=jnp.bfloat16):
    loudness = levels(rng, shape, shards, -0.22, 0.18) if shards else 1.0
    values = jax.random.normal(rng, shape, jnp.float32) * scale * loudness
    return jnp.minimum(jnp.maximum(values, -bound), bound).astype(held_as)


def setup_inputs(seed: int = 0) -> dict:
    keys = jax.random.split(jax.random.key(seed), 11)
    return {
        "inputs": centred(keys[0], (TOKENS, D), 1.0, 6.0, ((0, 8), (1, 4))),
        "positions": draw_positions(jax.random.fold_in(keys[10], 71), 0),
        "norm1_gain": jnp.clip(1.0 + 0.18 * jax.random.normal(keys[2], (D,), jnp.float32), 0.099609375, 1.8984375).astype(jnp.bfloat16),
        "qkv_weight": draw_qkv_weight(jax.random.fold_in(keys[10], 71), 0),
        "out_weight": centred(keys[4], (HEAD_COLS, D), (HEAD_COLS // 16) ** -0.5, 0.5, ((0, 4), (1, 8))),
        "norm2_gain": jnp.clip(1.0 + 0.18 * jax.random.normal(keys[5], (D,), jnp.float32), 0.099609375, 1.8984375).astype(jnp.bfloat16),
        "gate_weight": centred(keys[6], (D, FF), D ** -0.5, 0.125, ((0, 8), (1, 4))),
        "up_weight": centred(keys[7], (D, FF), D ** -0.5, 0.125, ((0, 8), (1, 4))),
        "down_weight": centred(keys[8], (FF, D), FF ** -0.5, 0.0625, ((0, 4), (1, 8))),
        "cotangent": centred(keys[9], (TOKENS, D), 1.0, 6.0, ((0, 8),)),
    }


norm_eps = 1e-06

def normalize(vector_rows, gain_row):
    return vector_rows * lax.rsqrt(lax.optimization_barrier(jnp.mean(vector_rows * vector_rows, axis=-1, keepdims=True)) + norm_eps) * gain_row

def gated_gelu(gate_in, up_in):
    return jax.nn.gelu(gate_in, approximate=True) * up_in

def rotary_tables(position_ids, head_width):
    half_width = head_width // 2
    frequency = jnp.exp(jnp.arange(half_width, dtype=jnp.float32) * (-2.0 * math.log(10000.0) / head_width))
    angles = position_ids.astype(jnp.float32)[:, None] * frequency[None, :]
    return (jnp.cos(angles), jnp.sin(angles))

def rotate(vector, cos_table, sin_table):
    half_width = vector.shape[-1] // 2
    lower_half = vector[..., :half_width]
    upper_half = vector[..., half_width:]
    return jnp.concatenate([lower_half * cos_table - upper_half * sin_table, upper_half * cos_table + lower_half * sin_table], axis=-1)

def unrotate(vector, cos_table, sin_table):
    half_width = vector.shape[-1] // 2
    lower_half = vector[..., :half_width]
    upper_half = vector[..., half_width:]
    return jnp.concatenate([lower_half * cos_table + upper_half * sin_table, upper_half * cos_table - lower_half * sin_table], axis=-1)

def contract_last(left_op, right_op):
    return lax.dot_general(left_op, right_op, (((1,), (1,)), ((), ())), preferred_element_type=jnp.float32)

def contract_first(left_op, right_op):
    return lax.dot_general(left_op, right_op, (((0,), (0,)), ((), ())), preferred_element_type=jnp.float32)

def split_sum(operand_pairs, groups):
    group_size = operand_pairs[0][0].shape[1] // groups
    summed = jnp.zeros((operand_pairs[0][0].shape[0], operand_pairs[0][1].shape[1]), jnp.float32)
    for group_idx in range(groups):
        col_start = group_idx * group_size
        group_term = jnp.zeros_like(summed)
        for pair in operand_pairs:
            group_term = group_term + jnp.dot(pair[0][:, col_start:col_start + group_size], pair[1][col_start:col_start + group_size], preferred_element_type=jnp.float32)
        summed = summed + lax.optimization_barrier(group_term.astype(jnp.bfloat16)).astype(jnp.float32)
    return summed

def reference(inputs, positions, norm1_gain, qkv_weight, out_weight, norm2_gain, gate_weight, up_weight, down_weight, cotangent):
    head_cols = HEADS * HEAD
    gain_one = norm1_gain.astype(jnp.float32)
    gain_two = norm2_gain.astype(jnp.float32)
    score_scale = HEAD ** (-0.5)
    blocks = TOKENS // SEG_MAX

    def block_step(carry, block):
        token_rows, position_ids, upstream = block
        length = token_rows.shape[0]
        residual = token_rows.astype(jnp.float32)
        normed_one = normalize(residual, gain_one).astype(jnp.bfloat16)
        qkv_rows = jnp.dot(normed_one, qkv_weight, preferred_element_type=jnp.float32).astype(jnp.bfloat16)
        cos_table, sin_table = rotary_tables(position_ids, HEAD)
        query_rows = rotate(qkv_rows[:, :head_cols].astype(jnp.float32).reshape(length, HEADS, HEAD), cos_table[:, None, :], sin_table[:, None, :])
        query_rows = (query_rows * score_scale).astype(jnp.bfloat16).reshape(length * HEADS, HEAD)
        key_rows = rotate(qkv_rows[:, head_cols:head_cols + HEAD].astype(jnp.float32), cos_table, sin_table).astype(jnp.bfloat16)
        value_rows = qkv_rows[:, head_cols + HEAD:]
        token_index = jnp.arange(length, dtype=jnp.int32)
        distance = token_index[:, None] - token_index[None, :]
        visible = ((distance >= 0) & (distance <= position_ids[:, None]))[:, None, :]
        scores = contract_last(query_rows, key_rows).reshape(length, HEADS, length)
        masked = jnp.where(visible, scores, -jnp.inf)
        row_max = lax.optimization_barrier(jnp.max(masked, axis=-1, keepdims=True))
        weights_exp = jnp.exp(masked - row_max)
        row_sum = lax.optimization_barrier(jnp.sum(weights_exp, axis=-1, keepdims=True))
        log_norm = row_max + jnp.log(row_sum)
        attn_probs = (weights_exp / row_sum).astype(jnp.bfloat16).reshape(length * HEADS, length)
        attended = jnp.dot(attn_probs, value_rows, preferred_element_type=jnp.float32).astype(jnp.bfloat16).reshape(length, head_cols)
        mixed = residual + split_sum([(attended, out_weight)], N_MDL)
        normed_two = normalize(mixed, gain_two).astype(jnp.bfloat16)
        gate_in = jnp.dot(normed_two, gate_weight, preferred_element_type=jnp.float32)
        up_in = jnp.dot(normed_two, up_weight, preferred_element_type=jnp.float32)
        hidden = gated_gelu(gate_in, up_in).astype(jnp.bfloat16)
        block_out = (mixed + split_sum([(hidden, down_weight)], N_MDL)).astype(jnp.bfloat16)
        d_hidden = contract_last(upstream, down_weight)
        unused, gelu_back = jax.vjp(gated_gelu, gate_in, up_in)
        d_gate, d_up = gelu_back(d_hidden)
        d_gate = d_gate.astype(jnp.bfloat16)
        d_up = d_up.astype(jnp.bfloat16)
        down_step = contract_first(hidden, upstream)
        gate_step = contract_first(normed_two, d_gate)
        up_step = contract_first(normed_two, d_up)
        d_normed_two = split_sum([(d_gate, gate_weight.T), (d_up, up_weight.T)], N_MDL)
        unused, norm_back = jax.vjp(normalize, mixed, gain_two)
        d_mixed, gain_two_step = norm_back(d_normed_two)
        d_mixed = d_mixed + upstream.astype(jnp.float32)
        d_mixed_b = d_mixed.astype(jnp.bfloat16)
        out_step = contract_first(attended, d_mixed_b)
        d_attended = contract_last(d_mixed_b, out_weight).astype(jnp.bfloat16)
        d_rows = d_attended.reshape(length * HEADS, HEAD)
        again = jnp.exp(jnp.where(visible, scores, -jnp.inf) - log_norm)
        again_b = again.astype(jnp.bfloat16).reshape(length * HEADS, length)
        d_values = contract_first(again_b, d_rows)
        d_probs = contract_last(d_rows, value_rows).reshape(length, HEADS, length)
        delta = lax.optimization_barrier(jnp.sum(d_attended.astype(jnp.float32).reshape(length, HEADS, HEAD) * attended.astype(jnp.float32).reshape(length, HEADS, HEAD), axis=-1, keepdims=True))
        d_scores = (again * (d_probs - delta)).astype(jnp.bfloat16).reshape(length * HEADS, length)
        d_queries = jnp.dot(d_scores, key_rows, preferred_element_type=jnp.float32).reshape(length, HEADS, HEAD) * score_scale
        d_queries = unrotate(d_queries, cos_table[:, None, :], sin_table[:, None, :]).reshape(length, head_cols)
        d_keys = unrotate(contract_first(d_scores, query_rows), cos_table, sin_table)
        d_qkv = jnp.concatenate([d_queries, d_keys, d_values], axis=1).astype(jnp.bfloat16)
        qkv_step = contract_first(normed_one, d_qkv)
        d_normed_one = split_sum([(d_qkv, qkv_weight.T)], N_MDL)
        unused, norm_one_back = jax.vjp(normalize, residual, gain_one)
        d_residual, gain_one_step = norm_one_back(d_normed_one)
        input_grad = d_mixed + d_residual
        steps_sum = (gain_one_step, qkv_step, out_step, gain_two_step, gate_step, up_step, down_step)
        carry = tuple((total + step_part for total, step_part in zip(carry, steps_sum)))
        return (carry, (block_out, input_grad))
    zero_grads = (jnp.zeros((D,), jnp.float32), jnp.zeros((D, QKV), jnp.float32), jnp.zeros((head_cols, D), jnp.float32), jnp.zeros((D,), jnp.float32), jnp.zeros((D, FF), jnp.float32), jnp.zeros((D, FF), jnp.float32), jnp.zeros((FF, D), jnp.float32))
    stacked = (inputs.reshape(blocks, SEG_MAX, D), positions.reshape(blocks, SEG_MAX), cotangent.reshape(blocks, SEG_MAX, D))
    grads, results = lax.scan(block_step, zero_grads, stacked)
    block_out = results[0].reshape(TOKENS, D)
    input_grad = results[1].reshape(TOKENS, D)
    return (block_out, input_grad, grads[0], grads[1], grads[2], grads[3], grads[4], grads[5], grads[6])
```

```python
import math

import jax
import jax.numpy as jnp
from jax import lax
from jax.experimental import pallas as pl
from jax.experimental.pallas import tpu as pltpu
from jax.sharding import PartitionSpec as P


HEADS = 10
HEAD = 256
NORM_EPS = 1e-06
F32 = jnp.float32
BF16 = jnp.bfloat16
MASKED = -1e30


def nt(left_op, right_op):
    return lax.dot_general(
        left_op, right_op, (((1,), (1,)), ((), ())), preferred_element_type=F32
    )


def tn(left_op, right_op):
    return lax.dot_general(
        left_op, right_op, (((0,), (0,)), ((), ())), preferred_element_type=F32
    )


def nn(left_op, right_op):
    return jnp.dot(left_op, right_op, preferred_element_type=F32)


def swap(block, distance):
    size = lax.axis_size("mdl")
    return lax.ppermute(block, "mdl", [(i, i ^ distance) for i in range(size)])


def gather_mdl(block, dim):
    size = lax.axis_size("mdl")
    if size != 4:
        return lax.all_gather(block, "mdl", axis=dim, tiled=True)
    me = lax.axis_index("mdl")
    half = block.shape[0] // 2
    along_x = swap(block, 1)
    along_y = swap(block, 2)
    top = swap(along_x[:half], 2)
    bottom = swap(along_y[half:], 1)
    width = block.shape[dim]
    shape = list(block.shape)
    shape[dim] = width * size
    whole = jnp.zeros(shape, block.dtype)

    def put(whole, piece, source, row):
        start = [0, 0]
        start[dim] = source * width
        start[0] = start[0] + row
        return lax.dynamic_update_slice(whole, piece, tuple(start))

    whole = put(whole, block, me, 0)
    whole = put(whole, along_x, me ^ 1, 0)
    whole = put(whole, along_y, me ^ 2, 0)
    whole = put(whole, top, me ^ 3, 0)
    whole = put(whole, bottom, me ^ 3, half)
    return whole


def scatter_mdl(part, dim):
    size = lax.axis_size("mdl")
    if size != 4:
        return lax.psum_scatter(part, "mdl", scatter_dimension=dim, tiled=True).astype(F32)
    me = lax.axis_index("mdl")
    shape = list(part.shape)
    shape[dim] //= size
    half = shape[0] // 2

    def piece(block, row):
        start = [0, 0]
        start[dim] = block * shape[dim]
        start[0] = start[0] + row
        return lax.dynamic_slice(part, tuple(start), (half, shape[1]))

    sums = []
    for row, first, second in ((0, 1, 2), (half, 2, 1)):
        sent = jnp.stack([piece(me ^ first, row), piece(me ^ 3, row)])
        sums.append((row, second, swap(sent, first)))
    partial = []
    for row, second, got in sums:
        other = piece(me ^ second, row).astype(F32) + got[1].astype(F32)
        partial.append((row, got[0], swap(other.astype(BF16), second)))
    return jnp.concatenate(
        [
            piece(me, row).astype(F32) + first.astype(F32) + second.astype(F32)
            for row, first, second in partial
        ],
        axis=0,
    )


def sum_mdl(value):
    size = lax.axis_size("mdl")
    distance = 1
    while distance < size:
        value = value + swap(value, distance)
        distance *= 2
    return value


def rows_to_cols(block):
    return lax.all_to_all(block, "mdl", split_axis=0, concat_axis=1, tiled=True)


def cols_to_rows(block):
    return lax.all_to_all(block, "mdl", split_axis=1, concat_axis=0, tiled=True)


def turn(vector, cos, sin):
    half = HEAD // 2
    lower, upper = vector[:, :half], vector[:, half:]
    return jnp.concatenate([lower * cos - upper * sin, upper * cos + lower * sin], axis=1)


def unturn(vector, cos, sin):
    half = HEAD // 2
    lower, upper = vector[:, :half], vector[:, half:]
    return jnp.concatenate([lower * cos + upper * sin, upper * cos - lower * sin], axis=1)


def seen(first_ref, position_ref, queries, keys):
    row = lax.broadcasted_iota(jnp.int32, (queries, keys), 0) + first_ref[0]
    distance = row - lax.broadcasted_iota(jnp.int32, (queries, keys), 1)
    return (distance >= 0) & (distance <= position_ref[...])


def forward_kernel(first_ref, q_ref, kv_ref, cos_ref, sin_ref, pos_ref, out_ref, norm_ref):
    query = turn(q_ref[...].astype(F32), cos_ref[...], sin_ref[...])
    query = (query * HEAD ** (-0.5)).astype(BF16)
    keys, values = kv_ref[:, :HEAD], kv_ref[:, HEAD:]
    scores = nt(query, keys)
    scores = jnp.where(seen(first_ref, pos_ref, *scores.shape), scores, MASKED)
    top = jnp.max(scores, axis=1, keepdims=True)
    weights = jnp.exp(scores - top)
    total = jnp.sum(weights, axis=1, keepdims=True)
    out_ref[...] = (nn(weights.astype(BF16), values) / total).astype(BF16)
    norm_ref[0] = top + jnp.log(total)


def backward_kernel(
    first_ref, q_ref, kv_ref, cos_ref, sin_ref, pos_ref, att_ref, datt_ref, norm_ref,
    dq_ref, dkv_ref,
):
    head = pl.program_id(0)
    scale = HEAD ** (-0.5)
    cos, sin = cos_ref[...], sin_ref[...]
    query = (turn(q_ref[...].astype(F32), cos, sin) * scale).astype(BF16)
    keys, values = kv_ref[:, :HEAD], kv_ref[:, HEAD:]
    scores = nt(query, keys)
    visible = seen(first_ref, pos_ref, *scores.shape)
    again = jnp.where(visible, jnp.exp(scores - norm_ref[0]), 0.0)
    d_att = datt_ref[...]
    delta = jnp.sum(d_att.astype(F32) * att_ref[...].astype(F32), axis=1, keepdims=True)
    d_scores = (again * (nt(d_att, values) - delta)).astype(BF16)
    d_query = nn(d_scores, keys) * scale
    dq_ref[...] = unturn(d_query, cos, sin).astype(BF16)

    @pl.when(head == 0)
    def _():
        dkv_ref[...] = jnp.zeros_like(dkv_ref)

    dkv_ref[:, :HEAD] += tn(d_scores, query)
    dkv_ref[:, HEAD:] += tn(again.astype(BF16), d_att)


def whole_spec(shape):
    return pl.BlockSpec(shape, lambda head: (0,) * len(shape))


def attention_forward(first, qkv, kv, cos, sin, pos):
    rows, keys = qkv.shape[0], kv.shape[0]
    head_spec = pl.BlockSpec((rows, HEAD), lambda head: (0, head))
    return pl.pallas_call(
        forward_kernel,
        grid=(HEADS,),
        out_shape=(
            jax.ShapeDtypeStruct((rows, HEADS * HEAD), BF16),
            jax.ShapeDtypeStruct((HEADS, rows, 1), F32),
        ),
        in_specs=[
            pl.BlockSpec(memory_space=pltpu.SMEM),
            head_spec,
            whole_spec((keys, 2 * HEAD)),
            whole_spec((rows, HEAD // 2)),
            whole_spec((rows, HEAD // 2)),
            whole_spec((rows, 1)),
        ],
        out_specs=(head_spec, pl.BlockSpec((1, rows, 1), lambda head: (head, 0, 0))),
        compiler_params=pltpu.CompilerParams(
            dimension_semantics=("arbitrary",), vmem_limit_bytes=32 << 20
        ),
        cost_estimate=pl.CostEstimate(
            flops=4 * rows * keys * HEADS * HEAD,
            bytes_accessed=4 * rows * HEADS * HEAD + 4 * keys * HEAD,
            transcendentals=rows * keys * HEADS,
        ),
        name="attention_forward",
    )(first, qkv, kv, cos, sin, pos)


def attention_backward(first, qkv, kv, cos, sin, pos, att, d_att, norm):
    rows, keys = qkv.shape[0], kv.shape[0]
    head_spec = pl.BlockSpec((rows, HEAD), lambda head: (0, head))
    return pl.pallas_call(
        backward_kernel,
        grid=(HEADS,),
        out_shape=(
            jax.ShapeDtypeStruct((rows, HEADS * HEAD), BF16),
            jax.ShapeDtypeStruct((keys, 2 * HEAD), F32),
        ),
        in_specs=[
            pl.BlockSpec(memory_space=pltpu.SMEM),
            head_spec,
            whole_spec((keys, 2 * HEAD)),
            whole_spec((rows, HEAD // 2)),
            whole_spec((rows, HEAD // 2)),
            whole_spec((rows, 1)),
            head_spec,
            head_spec,
            pl.BlockSpec((1, rows, 1), lambda head: (head, 0, 0)),
        ],
        out_specs=(head_spec, whole_spec((keys, 2 * HEAD))),
        compiler_params=pltpu.CompilerParams(
            dimension_semantics=("arbitrary",), vmem_limit_bytes=40 << 20
        ),
        cost_estimate=pl.CostEstimate(
            flops=10 * rows * keys * HEADS * HEAD,
            bytes_accessed=8 * rows * HEADS * HEAD + 12 * keys * HEAD,
            transcendentals=rows * keys * HEADS,
        ),
        name="attention_backward",
    )(first, qkv, kv, cos, sin, pos, att, d_att, norm)


def after(value, *earlier):
    return lax.optimization_barrier((value, *earlier))[0]


def row_scale(rows_b, axis=-1):
    rows = rows_b.astype(F32)
    return lax.rsqrt(jnp.mean(rows * rows, axis=axis, keepdims=True) + NORM_EPS)


def gelu_parts(value):
    root = math.sqrt(2.0 / math.pi)
    square = value * value
    tanh = jnp.tanh(root * (value + 0.044715 * value * square))
    cdf = 0.5 * (1.0 + tanh)
    slope = cdf + 0.5 * value * (1.0 - tanh * tanh) * root * (1.0 + 3 * 0.044715 * square)
    return value * cdf, slope


def scaled(weight, gain):
    return (weight.astype(F32) * gain.astype(F32)[:, None]).astype(BF16)


def on_device(
    inputs, positions, norm1_gain, qkv_weight, out_weight, norm2_gain, gate_weight,
    up_weight, down_weight, cotangent,
):
    me = lax.axis_index("mdl")
    size = lax.axis_size("mdl")
    head_cols = HEADS * HEAD
    width = inputs.shape[1]
    features = width * size

    def from_tok(weight, dim):
        return lax.all_gather(weight, "tok", axis=dim, tiled=True)

    def to_tok(grad, dim):
        total = lax.psum_scatter(grad, "tok", scatter_dimension=dim, tiled=True)
        return total.astype(F32)

    w_qkv = from_tok(scaled(qkv_weight, norm1_gain), 0)
    w_out = from_tok(out_weight, 1)
    w_gate = from_tok(scaled(gate_weight, norm2_gain), 0)
    w_up = from_tok(scaled(up_weight, norm2_gain), 0)
    w_down = from_tok(down_weight, 1)

    rows_in = gather_mdl(inputs, 1)
    scale_one = row_scale(rows_in)
    qkv_part = (nn(rows_in, w_qkv) * scale_one).astype(BF16)
    qkv = rows_to_cols(qkv_part)
    count = qkv.shape[0]
    half = HEAD // 2
    frequency = jnp.exp(jnp.arange(half, dtype=F32) * (-2.0 * math.log(10000.0) / HEAD))
    angles = positions.astype(F32)[:, None] * frequency[None, :]
    cos, sin = jnp.cos(angles), jnp.sin(angles)
    key_rows = turn(qkv[:, head_cols : head_cols + HEAD].astype(F32), cos, sin).astype(BF16)
    kv = gather_mdl(jnp.concatenate([key_rows, qkv[:, head_cols + HEAD :]], axis=1), 0)
    first = (me * count).astype(jnp.int32).reshape(1)
    pos = positions[:, None]
    attended, log_norm = attention_forward(first, qkv, kv, cos, sin, pos)
    head_block = cols_to_rows(attended)
    residual = inputs.astype(F32)
    mixed = residual + scatter_mdl(nn(head_block, w_out).astype(BF16), 1)

    rows_two = gather_mdl(mixed.astype(BF16), 1)
    scale_two = row_scale(rows_two)
    gate_in = nn(rows_two, w_gate) * scale_two
    up_in = nn(rows_two, w_up) * scale_two
    gelu, _ = gelu_parts(gate_in)
    hidden = (gelu * up_in).astype(BF16)
    gate_in, up_in, hidden = lax.optimization_barrier((gate_in, up_in, hidden))
    gelu, slope = gelu_parts(gate_in)

    down_local = tn(hidden, cotangent).astype(BF16)
    down_grad = to_tok(down_local, 1)
    d_hidden = nt(cotangent, w_down)
    d_gate = d_hidden * up_in * slope
    d_up = d_hidden * gelu
    stat_two = jnp.sum(d_gate * gate_in + d_up * up_in, axis=1)
    gate_scaled = (d_gate * scale_two).astype(BF16)
    up_scaled = (d_up * scale_two).astype(BF16)
    d_two_part = (nt(d_gate.astype(BF16), w_gate) + nt(d_up.astype(BF16), w_up)).astype(BF16)
    rows_later = after(rows_two, d_two_part)
    gate_local = tn(rows_later, gate_scaled).astype(BF16)
    gate_sum = to_tok(gate_local, 0)
    rows_later = after(rows_two, gate_local)
    up_local = tn(rows_later, up_scaled).astype(BF16)
    up_sum = to_tok(up_local, 0)
    d_two = scatter_mdl(d_two_part, 1)
    stat_two = sum_mdl(stat_two.reshape(8, -1)).reshape(-1, 1) * (1.0 / features)
    scale_mixed = scale_two * mixed
    cotangent_own = lax.dynamic_slice_in_dim(cotangent, me * width, width, 1).astype(F32)
    d_mixed = cotangent_own + scale_two * (d_two - scale_mixed * stat_two)

    d_mixed_b = after(d_mixed.astype(BF16), up_local)
    d_mixed_rows = gather_mdl(d_mixed_b, 1)
    hidden_later = after(hidden, d_mixed_b)
    ffn_part = nn(hidden_later, w_down).astype(BF16)
    d_head = nt(after(d_mixed_rows, ffn_part), w_out).astype(BF16)
    d_attended = rows_to_cols(d_head)
    out_local = tn(d_mixed_rows, after(head_block, d_head)).astype(BF16)
    out_grad = to_tok(out_local, 0).T
    d_attended = after(d_attended, out_local)
    block_out = (mixed + scatter_mdl(ffn_part, 1)).astype(BF16)
    d_query, d_kv = attention_backward(
        first, qkv, kv, cos, sin, pos, attended, d_attended, log_norm
    )
    d_kv = scatter_mdl(d_kv.astype(BF16), 0)
    d_key = unturn(d_kv[:, :HEAD], cos, sin).astype(BF16)
    d_qkv = jnp.concatenate([d_query, d_key, d_kv[:, HEAD:].astype(BF16)], axis=1)
    stat_one = jnp.sum(d_qkv.astype(F32) * qkv.astype(F32), axis=1)
    d_qkv_part = cols_to_rows(d_qkv)
    stat_rows = jnp.zeros((size, count), F32)
    stat_rows = sum_mdl(lax.dynamic_update_slice(stat_rows, stat_one[None], (me, 0)))
    stat_one = stat_rows.reshape(-1, 1) * (1.0 / features)
    qkv_local = tn(rows_in, (d_qkv_part.astype(F32) * scale_one).astype(BF16)).astype(BF16)
    qkv_sum = to_tok(qkv_local, 0)
    d_one = scatter_mdl(nt(d_qkv_part, w_qkv).astype(BF16), 1)
    input_grad = d_mixed + scale_one * (d_one - (scale_one * residual) * stat_one)

    norm1_late, norm2_late, qkv_late, gate_late, up_late, _ = lax.optimization_barrier(
        (norm1_gain, norm2_gain, qkv_weight, gate_weight, up_weight, up_local)
    )

    def unfold(total, gain):
        return total * gain.astype(F32)[:, None]

    def gain_grad(*pairs):
        return sum(jnp.sum(weight.astype(F32) * total, axis=1) for weight, total in pairs)

    gain_two_grad = sum_mdl(gain_grad((gate_late, gate_sum), (up_late, up_sum)))
    gain_one_grad = sum_mdl(gain_grad((qkv_late, qkv_sum)))
    return (
        block_out,
        input_grad,
        gain_one_grad,
        unfold(qkv_sum, norm1_late),
        out_grad,
        gain_two_grad,
        unfold(gate_sum, norm2_late),
        unfold(up_sum, norm2_late),
        down_grad,
    )


def solution(mesh):
    return jax.shard_map(
        on_device,
        mesh=mesh,
        in_specs=(
            P("tok", "mdl"),
            P(("tok", "mdl")),
            P("tok"),
            P("tok", "mdl"),
            P("mdl", "tok"),
            P("tok"),
            P("tok", "mdl"),
            P("tok", "mdl"),
            P("mdl", "tok"),
            P("tok", None),
        ),
        out_specs=(
            P("tok", "mdl"),
            P("tok", "mdl"),
            P("tok"),
            P("tok", "mdl"),
            P("mdl", "tok"),
            P("tok"),
            P("tok", "mdl"),
            P("tok", "mdl"),
            P("mdl", "tok"),
        ),
        check_vma=False,
    )
```

```python
import math

import jax
import jax.numpy as jnp
from jax import lax
from jax.experimental import pallas as pl
from jax.experimental.pallas import tpu as pltpu
from jax.sharding import PartitionSpec as P


HEADS = 10
HEAD = 256
NORM_EPS = 1e-06
F32 = jnp.float32
BF16 = jnp.bfloat16
MASKED = -1e30


def nt(left_op, right_op):
    return lax.dot_general(
        left_op, right_op, (((1,), (1,)), ((), ())), preferred_element_type=F32
    )


def tn(left_op, right_op):
    return lax.dot_general(
        left_op, right_op, (((0,), (0,)), ((), ())), preferred_element_type=F32
    )


def nn(left_op, right_op):
    return jnp.dot(left_op, right_op, preferred_element_type=F32)


def swap(block, distance):
    size = lax.axis_size("mdl")
    return lax.ppermute(block, "mdl", [(i, i ^ distance) for i in range(size)])


def gather_mdl(block, dim):
    size = lax.axis_size("mdl")
    if size != 4:
        return lax.all_gather(block, "mdl", axis=dim, tiled=True)
    me = lax.axis_index("mdl")
    half = block.shape[0] // 2
    along_x = swap(block, 1)
    along_y = swap(block, 2)
    top = swap(along_x[:half], 2)
    bottom = swap(along_y[half:], 1)
    width = block.shape[dim]
    shape = list(block.shape)
    shape[dim] = width * size
    whole = jnp.zeros(shape, block.dtype)

    def put(whole, piece, source, row):
        start = [0, 0]
        start[dim] = source * width
        start[0] = start[0] + row
        return lax.dynamic_update_slice(whole, piece, tuple(start))

    whole = put(whole, block, me, 0)
    whole = put(whole, along_x, me ^ 1, 0)
    whole = put(whole, along_y, me ^ 2, 0)
    whole = put(whole, top, me ^ 3, 0)
    whole = put(whole, bottom, me ^ 3, half)
    return whole


def scatter_mdl(part, dim):
    size = lax.axis_size("mdl")
    if size != 4:
        return lax.psum_scatter(part, "mdl", scatter_dimension=dim, tiled=True).astype(F32)
    me = lax.axis_index("mdl")
    shape = list(part.shape)
    shape[dim] //= size
    half = shape[0] // 2

    def piece(block, row):
        start = [0, 0]
        start[dim] = block * shape[dim]
        start[0] = start[0] + row
        return lax.dynamic_slice(part, tuple(start), (half, shape[1]))

    sums = []
    for row, first, second in ((0, 1, 2), (half, 2, 1)):
        sent = jnp.stack([piece(me ^ first, row), piece(me ^ 3, row)])
        sums.append((row, second, swap(sent, first)))
    partial = []
    for row, second, got in sums:
        other = piece(me ^ second, row).astype(F32) + got[1].astype(F32)
        partial.append((row, got[0], swap(other.astype(BF16), second)))
    return jnp.concatenate(
        [
            piece(me, row).astype(F32) + first.astype(F32) + second.astype(F32)
            for row, first, second in partial
        ],
        axis=0,
    )


def sum_mdl(value):
    size = lax.axis_size("mdl")
    distance = 1
    while distance < size:
        value = value + swap(value, distance)
        distance *= 2
    return value


def rows_to_cols(block):
    return lax.all_to_all(block, "mdl", split_axis=0, concat_axis=1, tiled=True)


def cols_to_rows(block):
    return lax.all_to_all(block, "mdl", split_axis=1, concat_axis=0, tiled=True)


def turn(vector, cos, sin):
    half = HEAD // 2
    lower, upper = vector[:, :half], vector[:, half:]
    return jnp.concatenate([lower * cos - upper * sin, upper * cos + lower * sin], axis=1)


def unturn(vector, cos, sin):
    half = HEAD // 2
    lower, upper = vector[:, :half], vector[:, half:]
    return jnp.concatenate([lower * cos + upper * sin, upper * cos - lower * sin], axis=1)


def seen(first_ref, position_ref, queries, keys):
    row = lax.broadcasted_iota(jnp.int32, (queries, keys), 0) + first_ref[0]
    distance = row - lax.broadcasted_iota(jnp.int32, (queries, keys), 1)
    return (distance >= 0) & (distance <= position_ref[...])


def forward_kernel(first_ref, q_ref, kv_ref, cos_ref, sin_ref, pos_ref, out_ref, norm_ref):
    query = turn(q_ref[...].astype(F32), cos_ref[...], sin_ref[...])
    query = (query * HEAD ** (-0.5)).astype(BF16)
    keys, values = kv_ref[:, :HEAD], kv_ref[:, HEAD:]
    scores = nt(query, keys)
    scores = jnp.where(seen(first_ref, pos_ref, *scores.shape), scores, MASKED)
    top = jnp.max(scores, axis=1, keepdims=True)
    weights = jnp.exp(scores - top)
    total = jnp.sum(weights, axis=1, keepdims=True)
    out_ref[...] = (nn(weights.astype(BF16), values) / total).astype(BF16)
    norm_ref[0] = top + jnp.log(total)


def backward_kernel(
    first_ref, q_ref, kv_ref, cos_ref, sin_ref, pos_ref, att_ref, datt_ref, norm_ref,
    dq_ref, dkv_ref,
):
    head = pl.program_id(0)
    scale = HEAD ** (-0.5)
    cos, sin = cos_ref[...], sin_ref[...]
    query = (turn(q_ref[...].astype(F32), cos, sin) * scale).astype(BF16)
    keys, values = kv_ref[:, :HEAD], kv_ref[:, HEAD:]
    scores = nt(query, keys)
    visible = seen(first_ref, pos_ref, *scores.shape)
    again = jnp.where(visible, jnp.exp(scores - norm_ref[0]), 0.0)
    d_att = datt_ref[...]
    delta = jnp.sum(d_att.astype(F32) * att_ref[...].astype(F32), axis=1, keepdims=True)
    d_scores = (again * (nt(d_att, values) - delta)).astype(BF16)
    d_query = nn(d_scores, keys) * scale
    dq_ref[...] = unturn(d_query, cos, sin).astype(BF16)

    @pl.when(head == 0)
    def _():
        dkv_ref[...] = jnp.zeros_like(dkv_ref)

    dkv_ref[:, :HEAD] += tn(d_scores, query)
    dkv_ref[:, HEAD:] += tn(again.astype(BF16), d_att)


def whole_spec(shape):
    return pl.BlockSpec(shape, lambda head: (0,) * len(shape))


def attention_forward(first, qkv, kv, cos, sin, pos):
    rows, keys = qkv.shape[0], kv.shape[0]
    head_spec = pl.BlockSpec((rows, HEAD), lambda head: (0, head))
    return pl.pallas_call(
        forward_kernel,
        grid=(HEADS,),
        out_shape=(
            jax.ShapeDtypeStruct((rows, HEADS * HEAD), BF16),
            jax.ShapeDtypeStruct((HEADS, rows, 1), F32),
        ),
        in_specs=[
            pl.BlockSpec(memory_space=pltpu.SMEM),
            head_spec,
            whole_spec((keys, 2 * HEAD)),
            whole_spec((rows, HEAD // 2)),
            whole_spec((rows, HEAD // 2)),
            whole_spec((rows, 1)),
        ],
        out_specs=(head_spec, pl.BlockSpec((1, rows, 1), lambda head: (head, 0, 0))),
        compiler_params=pltpu.CompilerParams(
            dimension_semantics=("arbitrary",), vmem_limit_bytes=32 << 20
        ),
        cost_estimate=pl.CostEstimate(
            flops=4 * rows * keys * HEADS * HEAD,
            bytes_accessed=4 * rows * HEADS * HEAD + 4 * keys * HEAD,
            transcendentals=rows * keys * HEADS,
        ),
        name="attention_forward",
    )(first, qkv, kv, cos, sin, pos)


def attention_backward(first, qkv, kv, cos, sin, pos, att, d_att, norm):
    rows, keys = qkv.shape[0], kv.shape[0]
    head_spec = pl.BlockSpec((rows, HEAD), lambda head: (0, head))
    return pl.pallas_call(
        backward_kernel,
        grid=(HEADS,),
        out_shape=(
            jax.ShapeDtypeStruct((rows, HEADS * HEAD), BF16),
            jax.ShapeDtypeStruct((keys, 2 * HEAD), F32),
        ),
        in_specs=[
            pl.BlockSpec(memory_space=pltpu.SMEM),
            head_spec,
            whole_spec((keys, 2 * HEAD)),
            whole_spec((rows, HEAD // 2)),
            whole_spec((rows, HEAD // 2)),
            whole_spec((rows, 1)),
            head_spec,
            head_spec,
            pl.BlockSpec((1, rows, 1), lambda head: (head, 0, 0)),
        ],
        out_specs=(head_spec, whole_spec((keys, 2 * HEAD))),
        compiler_params=pltpu.CompilerParams(
            dimension_semantics=("arbitrary",), vmem_limit_bytes=40 << 20
        ),
        cost_estimate=pl.CostEstimate(
            flops=10 * rows * keys * HEADS * HEAD,
            bytes_accessed=8 * rows * HEADS * HEAD + 12 * keys * HEAD,
            transcendentals=rows * keys * HEADS,
        ),
        name="attention_backward",
    )(first, qkv, kv, cos, sin, pos, att, d_att, norm)


def pair_kernel(core_ref, rows_ref, right_ref, kept_ref, sent_ref):
    total = tn(rows_ref[...], right_ref[...]).astype(BF16)
    half = total.shape[0] // 2

    @pl.when(core_ref[0] == 0)
    def _():
        kept_ref[...] = total[:half]
        sent_ref[...] = total[half:]

    @pl.when(core_ref[0] == 1)
    def _():
        kept_ref[...] = total[half:]
        sent_ref[...] = total[:half]


def pair_grad(left, right):
    tokens, rows = left.shape
    cols = right.shape[1]
    pairs = lax.axis_size("tok") // 2
    core = lax.axis_index("tok") % 2
    step = rows // pairs
    if step % 128:
        total = tn(left, right).astype(BF16).reshape(pairs, 2, step // 2, cols)
        kept, sent = (
            lax.dynamic_index_in_dim(total, index, 1, False).reshape(-1, cols)
            for index in (core, 1 - core)
        )
        return kept, sent
    out = jax.ShapeDtypeStruct((rows // 2, cols), BF16)
    out_spec = pl.BlockSpec((step // 2, cols), lambda pair: (pair, 0))
    return pl.pallas_call(
        pair_kernel,
        grid=(pairs,),
        out_shape=(out, out),
        in_specs=[
            pl.BlockSpec(memory_space=pltpu.SMEM),
            pl.BlockSpec((tokens, step), lambda pair: (0, pair)),
            pl.BlockSpec((tokens, cols), lambda pair: (0, 0)),
        ],
        out_specs=(out_spec, out_spec),
        compiler_params=pltpu.CompilerParams(
            dimension_semantics=("arbitrary",), vmem_limit_bytes=48 << 20
        ),
        cost_estimate=pl.CostEstimate(
            flops=2 * tokens * rows * cols,
            bytes_accessed=2 * (tokens * rows + tokens * cols + rows * cols),
            transcendentals=0,
        ),
        name="pair_grad",
    )(core.astype(jnp.int32).reshape(1), left, right)


def two_kernel(gate_ref, up_ref, weight_ref, out_ref):
    cols = gate_ref.shape[1]
    out_ref[...] = (
        nt(gate_ref[...], weight_ref[:, :cols]) + nt(up_ref[...], weight_ref[:, cols:])
    ).astype(BF16)


def two_products(d_gate, d_up, weight):
    tokens, cols = d_gate.shape
    rows = weight.shape[0]
    if cols % 128:
        return (nt(d_gate, weight[:, :cols]) + nt(d_up, weight[:, cols:])).astype(BF16)
    step = 512
    whole = pl.BlockSpec((tokens, cols), lambda row: (0, 0))
    return pl.pallas_call(
        two_kernel,
        grid=(rows // step,),
        out_shape=jax.ShapeDtypeStruct((tokens, rows), BF16),
        in_specs=[whole, whole, pl.BlockSpec((step, 2 * cols), lambda row: (row, 0))],
        out_specs=pl.BlockSpec((tokens, step), lambda row: (0, row)),
        compiler_params=pltpu.CompilerParams(
            dimension_semantics=("arbitrary",), vmem_limit_bytes=48 << 20
        ),
        cost_estimate=pl.CostEstimate(
            flops=4 * tokens * rows * cols,
            bytes_accessed=4 * tokens * cols + 4 * rows * cols + 2 * tokens * rows,
            transcendentals=0,
        ),
        name="two_products",
    )(d_gate, d_up, weight)


def after(value, *earlier):
    return lax.optimization_barrier((value, *earlier))[0]


def row_scale(rows_b, axis=-1):
    rows = rows_b.astype(F32)
    return lax.rsqrt(jnp.mean(rows * rows, axis=axis, keepdims=True) + NORM_EPS)


def gelu_parts(value):
    root = math.sqrt(2.0 / math.pi)
    square = value * value
    tanh = jnp.tanh(root * (value + 0.044715 * value * square))
    cdf = 0.5 * (1.0 + tanh)
    slope = cdf + 0.5 * value * (1.0 - tanh * tanh) * root * (1.0 + 3 * 0.044715 * square)
    return value * cdf, slope


def scaled(weight, gain):
    return (weight.astype(F32) * gain.astype(F32)[:, None]).astype(BF16)


def on_device(
    inputs, positions, norm1_gain, qkv_weight, out_weight, norm2_gain, gate_weight,
    up_weight, down_weight, cotangent,
):
    me = lax.axis_index("mdl")
    size = lax.axis_size("mdl")
    head_cols = HEADS * HEAD
    width = inputs.shape[1]
    features = width * size

    def from_tok(weight, dim):
        return lax.all_gather(weight, "tok", axis=dim, tiled=True)

    def to_tok(grad, dim):
        total = lax.psum_scatter(grad, "tok", scatter_dimension=dim, tiled=True)
        return total.astype(F32)

    def pair_to_tok(local):
        kept, sent = local
        count = lax.axis_size("tok")
        got = lax.ppermute(sent, "tok", [(i, i ^ 1) for i in range(count)])
        both = (kept.astype(F32) + got.astype(F32)).astype(BF16)
        groups = [list(range(core, count, 2)) for core in range(2)]
        total = lax.psum_scatter(
            both, "tok", scatter_dimension=0, tiled=True, axis_index_groups=groups
        )
        return total.astype(F32)

    qkv_cols, ff_cols = qkv_weight.shape[1], gate_weight.shape[1]
    w_attn = from_tok(jnp.concatenate([scaled(qkv_weight, norm1_gain), out_weight.T], axis=1), 0)
    w_qkv, w_out_t = w_attn[:, :qkv_cols], w_attn[:, qkv_cols:]
    gu_local = jnp.concatenate([scaled(w, norm2_gain) for w in (gate_weight, up_weight)], 1)
    w_gu = from_tok(gu_local, 0)
    w_down = from_tok(down_weight, 1)

    rows_in = gather_mdl(inputs, 1)
    scale_one = row_scale(rows_in)
    qkv_part = (nn(rows_in, w_qkv) * scale_one).astype(BF16)
    qkv = rows_to_cols(qkv_part)
    count = qkv.shape[0]
    half = HEAD // 2
    frequency = jnp.exp(jnp.arange(half, dtype=F32) * (-2.0 * math.log(10000.0) / HEAD))
    angles = positions.astype(F32)[:, None] * frequency[None, :]
    cos, sin = jnp.cos(angles), jnp.sin(angles)
    key_rows = turn(qkv[:, head_cols : head_cols + HEAD].astype(F32), cos, sin).astype(BF16)
    kv = gather_mdl(jnp.concatenate([key_rows, qkv[:, head_cols + HEAD :]], axis=1), 0)
    first = (me * count).astype(jnp.int32).reshape(1)
    pos = positions[:, None]
    attended, log_norm = attention_forward(first, qkv, kv, cos, sin, pos)
    head_block = cols_to_rows(attended)
    residual = inputs.astype(F32)
    mixed = residual + scatter_mdl(nt(head_block, w_out_t).astype(BF16), 1)

    rows_two = gather_mdl(mixed.astype(BF16), 1)
    scale_two = row_scale(rows_two)
    rows_hat = (rows_two.astype(F32) * scale_two).astype(BF16)
    gate_in = nn(rows_hat, w_gu[:, :ff_cols])
    up_in = nn(rows_hat, w_gu[:, ff_cols:])
    gelu, _ = gelu_parts(gate_in)
    hidden = (gelu * up_in).astype(BF16)
    gate_in, up_in, hidden = lax.optimization_barrier((gate_in, up_in, hidden))
    gelu, slope = gelu_parts(gate_in)

    down_local = pair_grad(cotangent, hidden)
    down_grad = pair_to_tok(down_local).T
    d_hidden = nt(cotangent, w_down)
    d_gate_f = d_hidden * up_in * slope
    d_up_f = d_hidden * gelu
    stat_two = jnp.sum(d_gate_f * gate_in + d_up_f * up_in, axis=1)
    d_gate, d_up = d_gate_f.astype(BF16), d_up_f.astype(BF16)
    gate_local = pair_grad(rows_hat, d_gate)
    gate_sum = pair_to_tok(gate_local)
    d_two_part = two_products(d_gate, d_up, w_gu)
    rows_later = after(rows_hat, d_two_part)
    up_local = pair_grad(rows_later, d_up)
    up_sum = pair_to_tok(up_local)
    d_two = scatter_mdl(d_two_part, 1)
    stat_two = sum_mdl(stat_two.reshape(8, -1)).reshape(-1, 1) * (1.0 / features)
    scale_mixed = scale_two * mixed
    cotangent_own = lax.dynamic_slice_in_dim(cotangent, me * width, width, 1).astype(F32)
    d_mixed = cotangent_own + scale_two * (d_two - scale_mixed * stat_two)

    d_mixed_b = after(d_mixed.astype(BF16), up_local[0])
    d_mixed_rows = gather_mdl(d_mixed_b, 1)
    hidden_later = after(hidden, d_mixed_b)
    ffn_part = nn(hidden_later, w_down).astype(BF16)
    d_head = nn(after(d_mixed_rows, ffn_part), w_out_t).astype(BF16)
    d_attended = rows_to_cols(d_head)
    out_local = tn(d_mixed_rows, after(head_block, d_head)).astype(BF16)
    out_grad = to_tok(out_local, 0).T
    d_attended = after(d_attended, out_local)
    block_out = (mixed + scatter_mdl(ffn_part, 1)).astype(BF16)
    d_query, d_kv = attention_backward(
        first, qkv, kv, cos, sin, pos, attended, d_attended, log_norm
    )
    d_kv = scatter_mdl(d_kv.astype(BF16), 0)
    d_key = unturn(d_kv[:, :HEAD], cos, sin).astype(BF16)
    d_qkv = jnp.concatenate([d_query, d_key, d_kv[:, HEAD:].astype(BF16)], axis=1)
    stat_one = jnp.sum(d_qkv.astype(F32) * qkv.astype(F32), axis=1)
    d_qkv_part = cols_to_rows(d_qkv)
    stat_rows = jnp.zeros((size, count), F32)
    stat_rows = sum_mdl(lax.dynamic_update_slice(stat_rows, stat_one[None], (me, 0)))
    stat_one = stat_rows.reshape(-1, 1) * (1.0 / features)
    qkv_local = tn(rows_in, (d_qkv_part.astype(F32) * scale_one).astype(BF16)).astype(BF16)
    qkv_sum = to_tok(qkv_local, 0)
    d_one = scatter_mdl(nt(d_qkv_part, w_qkv).astype(BF16), 1)
    input_grad = d_mixed + scale_one * (d_one - (scale_one * residual) * stat_one)

    norm1_late, norm2_late, qkv_late, gate_late, up_late, _ = lax.optimization_barrier(
        (norm1_gain, norm2_gain, qkv_weight, gate_weight, up_weight, up_local[0])
    )

    def unfold(total, gain):
        return total * gain.astype(F32)[:, None]

    def gain_grad(*pairs):
        return sum(jnp.sum(weight.astype(F32) * total, axis=1) for weight, total in pairs)

    gain_two_grad = sum_mdl(gain_grad((gate_late, gate_sum), (up_late, up_sum)))
    gain_one_grad = sum_mdl(gain_grad((qkv_late, qkv_sum)))
    return (
        block_out,
        input_grad,
        gain_one_grad,
        unfold(qkv_sum, norm1_late),
        out_grad,
        gain_two_grad,
        unfold(gate_sum, norm2_late),
        unfold(up_sum, norm2_late),
        down_grad,
    )


def solution(mesh):
    return jax.shard_map(
        on_device,
        mesh=mesh,
        in_specs=(
            P("tok", "mdl"),
            P(("tok", "mdl")),
            P("tok"),
            P("tok", "mdl"),
            P("mdl", "tok"),
            P("tok"),
            P("tok", "mdl"),
            P("tok", "mdl"),
            P("mdl", "tok"),
            P("tok", None),
        ),
        out_specs=(
            P("tok", "mdl"),
            P("tok", "mdl"),
            P("tok"),
            P("tok", "mdl"),
            P("mdl", "tok"),
            P("tok"),
            P("tok", "mdl"),
            P("tok", "mdl"),
            P("mdl", "tok"),
        ),
        check_vma=False,
    )
```

```python
import functools
import math

import jax
import jax.numpy as jnp
from jax import lax
from jax.experimental import pallas as pl
from jax.experimental.pallas import tpu as pltpu
from jax.sharding import PartitionSpec as P


HEADS = 10
HEAD = 256
NORM_EPS = 1e-06
F32 = jnp.float32
BF16 = jnp.bfloat16
MASKED = -1e30


def nt(left_op, right_op):
    return lax.dot_general(
        left_op, right_op, (((1,), (1,)), ((), ())), preferred_element_type=F32
    )


def tn(left_op, right_op):
    return lax.dot_general(
        left_op, right_op, (((0,), (0,)), ((), ())), preferred_element_type=F32
    )


def nn(left_op, right_op):
    return jnp.dot(left_op, right_op, preferred_element_type=F32)


def swap(block, distance):
    size = lax.axis_size("mdl")
    return lax.ppermute(block, "mdl", [(i, i ^ distance) for i in range(size)])


def gather_mdl(block, dim):
    size = lax.axis_size("mdl")
    if size != 4:
        return lax.all_gather(block, "mdl", axis=dim, tiled=True)
    me = lax.axis_index("mdl")
    half = block.shape[0] // 2
    along_x = swap(block, 1)
    along_y = swap(block, 2)
    top = swap(along_x[:half], 2)
    bottom = swap(along_y[half:], 1)
    width = block.shape[dim]
    shape = list(block.shape)
    shape[dim] = width * size
    whole = jnp.zeros(shape, block.dtype)

    def put(whole, piece, source, row):
        start = [0, 0]
        start[dim] = source * width
        start[0] = start[0] + row
        return lax.dynamic_update_slice(whole, piece, tuple(start))

    whole = put(whole, block, me, 0)
    whole = put(whole, along_x, me ^ 1, 0)
    whole = put(whole, along_y, me ^ 2, 0)
    whole = put(whole, top, me ^ 3, 0)
    whole = put(whole, bottom, me ^ 3, half)
    return whole


def scatter_mdl(part, dim):
    size = lax.axis_size("mdl")
    if size != 4:
        return lax.psum_scatter(part, "mdl", scatter_dimension=dim, tiled=True).astype(F32)
    me = lax.axis_index("mdl")
    shape = list(part.shape)
    shape[dim] //= size
    half = shape[0] // 2

    def piece(block, row):
        start = [0, 0]
        start[dim] = block * shape[dim]
        start[0] = start[0] + row
        return lax.dynamic_slice(part, tuple(start), (half, shape[1]))

    sums = []
    for row, first, second in ((0, 1, 2), (half, 2, 1)):
        sent = jnp.stack([piece(me ^ first, row), piece(me ^ 3, row)])
        sums.append((row, second, swap(sent, first)))
    partial = []
    for row, second, got in sums:
        other = piece(me ^ second, row).astype(F32) + got[1].astype(F32)
        partial.append((row, got[0], swap(other.astype(BF16), second)))
    return jnp.concatenate(
        [
            piece(me, row).astype(F32) + first.astype(F32) + second.astype(F32)
            for row, first, second in partial
        ],
        axis=0,
    )


def gather_pieces(block):
    half = block.shape[0] // 2
    along_x = swap(block, 1)
    along_y = swap(block, 2)
    top = swap(along_x[:half], 2)
    bottom = swap(along_y[half:], 1)
    return block, along_x, along_y, top, bottom


def assemble(pieces):
    me = lax.axis_index("mdl")
    own, along_x, along_y, top, bottom = pieces
    rows, width = own.shape
    whole = jnp.zeros((rows, 4 * width), own.dtype)
    for piece, source, row in (
        (own, me, 0),
        (along_x, me ^ 1, 0),
        (along_y, me ^ 2, 0),
        (top, me ^ 3, 0),
        (bottom, me ^ 3, rows // 2),
    ):
        whole = lax.dynamic_update_slice(whole, piece, (row, source * width))
    return whole


def scatter_payload(payload):
    top_sent, bottom_sent, top_kept, bottom_kept = payload
    got_top = swap(top_sent, 1)
    got_bottom = swap(bottom_sent, 2)
    halves = []
    for kept, got, second in ((top_kept, got_top, 2), (bottom_kept, got_bottom, 1)):
        passed = (kept[1].astype(F32) + got[1].astype(F32)).astype(BF16)
        last = swap(passed, second)
        halves.append(kept[0].astype(F32) + got[0].astype(F32) + last.astype(F32))
    return jnp.concatenate(halves, axis=0)


def sum_mdl(value):
    size = lax.axis_size("mdl")
    distance = 1
    while distance < size:
        value = value + swap(value, distance)
        distance *= 2
    return value


def sum_tok(value):
    size = lax.axis_size("tok")
    distance = 1
    while distance < size:
        value = value + lax.ppermute(value, "tok", [(i, i ^ distance) for i in range(size)])
        distance *= 2
    return value


def rows_to_cols(block):
    return lax.all_to_all(block, "mdl", split_axis=0, concat_axis=1, tiled=True)


def cols_to_rows(block):
    return lax.all_to_all(block, "mdl", split_axis=1, concat_axis=0, tiled=True)


def turn(vector, cos, sin):
    half = HEAD // 2
    lower, upper = vector[:, :half], vector[:, half:]
    return jnp.concatenate([lower * cos - upper * sin, upper * cos + lower * sin], axis=1)


def unturn(vector, cos, sin):
    half = HEAD // 2
    lower, upper = vector[:, :half], vector[:, half:]
    return jnp.concatenate([lower * cos + upper * sin, upper * cos - lower * sin], axis=1)


def seen(first_ref, position_ref, queries, keys):
    row = lax.broadcasted_iota(jnp.int32, (queries, keys), 0) + first_ref[0]
    distance = row - lax.broadcasted_iota(jnp.int32, (queries, keys), 1)
    return (distance >= 0) & (distance <= position_ref[...])


def forward_kernel(first_ref, q_ref, kv_ref, cos_ref, sin_ref, pos_ref, out_ref, norm_ref):
    query = turn(q_ref[...].astype(F32), cos_ref[...], sin_ref[...])
    query = (query * HEAD ** (-0.5)).astype(BF16)
    keys, values = kv_ref[:, :HEAD], kv_ref[:, HEAD:]
    scores = nt(query, keys)
    scores = jnp.where(seen(first_ref, pos_ref, *scores.shape), scores, MASKED)
    top = jnp.max(scores, axis=1, keepdims=True)
    weights = jnp.exp(scores - top)
    total = jnp.sum(weights, axis=1, keepdims=True)
    out_ref[...] = (nn(weights.astype(BF16), values) / total).astype(BF16)
    norm_ref[0] = top + jnp.log(total)


def backward_kernel(
    first_ref, q_ref, kv_ref, cos_ref, sin_ref, pos_ref, att_ref, datt_ref, norm_ref,
    dq_ref, dkv_ref,
):
    head = pl.program_id(0)
    scale = HEAD ** (-0.5)
    cos, sin = cos_ref[...], sin_ref[...]
    query = (turn(q_ref[...].astype(F32), cos, sin) * scale).astype(BF16)
    keys, values = kv_ref[:, :HEAD], kv_ref[:, HEAD:]
    scores = nt(query, keys)
    visible = seen(first_ref, pos_ref, *scores.shape)
    again = jnp.where(visible, jnp.exp(scores - norm_ref[0]), 0.0)
    d_att = datt_ref[...]
    delta = jnp.sum(d_att.astype(F32) * att_ref[...].astype(F32), axis=1, keepdims=True)
    d_scores = (again * (nt(d_att, values) - delta)).astype(BF16)
    d_query = nn(d_scores, keys) * scale
    dq_ref[...] = unturn(d_query, cos, sin).astype(BF16)

    @pl.when(head == 0)
    def _():
        dkv_ref[...] = jnp.zeros_like(dkv_ref)

    dkv_ref[:, :HEAD] += tn(d_scores, query)
    dkv_ref[:, HEAD:] += tn(again.astype(BF16), d_att)


def whole_spec(shape):
    return pl.BlockSpec(shape, lambda head: (0,) * len(shape))


def attention_forward(first, qkv, kv, cos, sin, pos):
    rows, keys = qkv.shape[0], kv.shape[0]
    head_spec = pl.BlockSpec((rows, HEAD), lambda head: (0, head))
    return pl.pallas_call(
        forward_kernel,
        grid=(HEADS,),
        out_shape=(
            jax.ShapeDtypeStruct((rows, HEADS * HEAD), BF16),
            jax.ShapeDtypeStruct((HEADS, rows, 1), F32),
        ),
        in_specs=[
            pl.BlockSpec(memory_space=pltpu.SMEM),
            head_spec,
            whole_spec((keys, 2 * HEAD)),
            whole_spec((rows, HEAD // 2)),
            whole_spec((rows, HEAD // 2)),
            whole_spec((rows, 1)),
        ],
        out_specs=(head_spec, pl.BlockSpec((1, rows, 1), lambda head: (head, 0, 0))),
        compiler_params=pltpu.CompilerParams(
            dimension_semantics=("arbitrary",), vmem_limit_bytes=32 << 20
        ),
        cost_estimate=pl.CostEstimate(
            flops=4 * rows * keys * HEADS * HEAD,
            bytes_accessed=4 * rows * HEADS * HEAD + 4 * keys * HEAD,
            transcendentals=rows * keys * HEADS,
        ),
        name="attention_forward",
    )(first, qkv, kv, cos, sin, pos)


def attention_backward(first, qkv, kv, cos, sin, pos, att, d_att, norm):
    rows, keys = qkv.shape[0], kv.shape[0]
    head_spec = pl.BlockSpec((rows, HEAD), lambda head: (0, head))
    return pl.pallas_call(
        backward_kernel,
        grid=(HEADS,),
        out_shape=(
            jax.ShapeDtypeStruct((rows, HEADS * HEAD), BF16),
            jax.ShapeDtypeStruct((keys, 2 * HEAD), F32),
        ),
        in_specs=[
            pl.BlockSpec(memory_space=pltpu.SMEM),
            head_spec,
            whole_spec((keys, 2 * HEAD)),
            whole_spec((rows, HEAD // 2)),
            whole_spec((rows, HEAD // 2)),
            whole_spec((rows, 1)),
            head_spec,
            head_spec,
            pl.BlockSpec((1, rows, 1), lambda head: (head, 0, 0)),
        ],
        out_specs=(head_spec, whole_spec((keys, 2 * HEAD))),
        compiler_params=pltpu.CompilerParams(
            dimension_semantics=("arbitrary",), vmem_limit_bytes=40 << 20
        ),
        cost_estimate=pl.CostEstimate(
            flops=10 * rows * keys * HEADS * HEAD,
            bytes_accessed=8 * rows * HEADS * HEAD + 12 * keys * HEAD,
            transcendentals=rows * keys * HEADS,
        ),
        name="attention_backward",
    )(first, qkv, kv, cos, sin, pos, att, d_att, norm)


def pair_kernel(core_ref, rows_ref, right_ref, kept_ref, sent_ref):
    total = tn(rows_ref[...], right_ref[...]).astype(BF16)
    half = total.shape[0] // 2

    @pl.when(core_ref[0] == 0)
    def _():
        kept_ref[...] = total[:half]
        sent_ref[...] = total[half:]

    @pl.when(core_ref[0] == 1)
    def _():
        kept_ref[...] = total[half:]
        sent_ref[...] = total[:half]


def split_pairs(total, pairs, core):
    rows, cols = total.shape
    total = total.reshape(pairs, 2, rows // pairs // 2, cols)
    return tuple(
        lax.dynamic_index_in_dim(total, index, 1, False).reshape(-1, cols)
        for index in (core, 1 - core)
    )


def pair_grad(left, right):
    tokens, rows = left.shape
    cols = right.shape[1]
    pairs = lax.axis_size("tok") // 2
    core = lax.axis_index("tok") % 2
    step = rows // pairs
    if step % 128:
        return split_pairs(tn(left, right).astype(BF16), pairs, core)
    out = jax.ShapeDtypeStruct((rows // 2, cols), BF16)
    out_spec = pl.BlockSpec((step // 2, cols), lambda pair: (pair, 0))
    return pl.pallas_call(
        pair_kernel,
        grid=(pairs,),
        out_shape=(out, out),
        in_specs=[
            pl.BlockSpec(memory_space=pltpu.SMEM),
            pl.BlockSpec((tokens, step), lambda pair: (0, pair)),
            pl.BlockSpec((tokens, cols), lambda pair: (0, 0)),
        ],
        out_specs=(out_spec, out_spec),
        compiler_params=pltpu.CompilerParams(
            dimension_semantics=("arbitrary",), vmem_limit_bytes=48 << 20
        ),
        cost_estimate=pl.CostEstimate(
            flops=2 * tokens * rows * cols,
            bytes_accessed=2 * (tokens * rows + tokens * cols + rows * cols),
            transcendentals=0,
        ),
        name="pair_grad",
    )(core.astype(jnp.int32).reshape(1), left, right)


def payload_kernel(starts, me_ref, *refs):
    lefts, weight_ref = refs[: len(starts)], refs[len(starts)]
    top_sent, bottom_sent, top_kept, bottom_kept = refs[len(starts) + 1 :]
    total = 0.0
    for left_ref, start in zip(lefts, starts):
        total += nt(left_ref[...], weight_ref[:, start : start + left_ref.shape[1]])
    total = total.astype(BF16)
    half = total.shape[0] // 2
    places = (
        ((top_kept, 0), (bottom_kept, 0)),
        ((top_sent, 0), (bottom_kept, 1)),
        ((top_kept, 1), (bottom_sent, 0)),
        ((top_sent, 1), (bottom_sent, 1)),
    )
    for distance, ((top, top_at), (bottom, bottom_at)) in enumerate(places):

        @pl.when(pl.program_id(0) == 3 - distance)
        def _(top=top, top_at=top_at, bottom=bottom, bottom_at=bottom_at):
            top[top_at] = total[:half]
            bottom[bottom_at] = total[half:]


def scatter_product(lefts, weight, starts):
    tokens = lefts[0].shape[0]
    rows, cols = weight.shape
    step = rows // 4
    me = lax.axis_index("mdl").astype(jnp.int32).reshape(1)
    out = jax.ShapeDtypeStruct((2, tokens // 2, step), BF16)
    depth = sum(left.shape[1] for left in lefts)
    return pl.pallas_call(
        functools.partial(payload_kernel, starts),
        grid_spec=pltpu.PrefetchScalarGridSpec(
            num_scalar_prefetch=1,
            grid=(4,),
            in_specs=[pl.BlockSpec(left.shape, lambda at, me_ref: (0, 0)) for left in lefts]
            + [pl.BlockSpec((step, cols), lambda at, me_ref: (me_ref[0] ^ (3 - at), 0))],
            out_specs=[pl.BlockSpec(out.shape, lambda at, me_ref: (0, 0, 0))] * 4,
        ),
        out_shape=(out,) * 4,
        compiler_params=pltpu.CompilerParams(
            dimension_semantics=("arbitrary",), vmem_limit_bytes=48 << 20
        ),
        cost_estimate=pl.CostEstimate(
            flops=2 * tokens * rows * depth,
            bytes_accessed=2 * (tokens * depth + rows * cols + tokens * rows),
            transcendentals=0,
        ),
        name="scatter_product",
    )(me, *lefts, weight)


def pieces_kernel(start, me_ref, own, along_x, along_y, top, bottom, weight_ref, out_ref, total):
    at = pl.program_id(0)
    width = out_ref.shape[1]
    half = top.shape[0]
    for index, piece in enumerate((own, along_x, along_y)):

        @pl.when(at == index)
        def _(index=index, piece=piece):
            part = nn(piece[...], weight_ref[:, start : start + width])
            if index:
                total[...] += part
            else:
                total[...] = part

    @pl.when(at == 3)
    def _():
        weight = weight_ref[:, start : start + width]
        out_ref[:half] = (total[:half] + nn(top[...], weight)).astype(BF16)
        out_ref[half:] = (total[half:] + nn(bottom[...], weight)).astype(BF16)


def pieces_product(pieces, weight, start, width):
    tokens, step = pieces[0].shape
    rows, cols = weight.shape
    me = lax.axis_index("mdl").astype(jnp.int32).reshape(1)
    return pl.pallas_call(
        functools.partial(pieces_kernel, start),
        grid_spec=pltpu.PrefetchScalarGridSpec(
            num_scalar_prefetch=1,
            grid=(4,),
            in_specs=[pl.BlockSpec(piece.shape, lambda at, me_ref: (0, 0)) for piece in pieces]
            + [pl.BlockSpec((step, cols), lambda at, me_ref: (me_ref[0] ^ at, 0))],
            out_specs=pl.BlockSpec((tokens, width), lambda at, me_ref: (0, 0)),
            scratch_shapes=[pltpu.VMEM((tokens, width), F32)],
        ),
        out_shape=jax.ShapeDtypeStruct((tokens, width), BF16),
        compiler_params=pltpu.CompilerParams(
            dimension_semantics=("arbitrary",), vmem_limit_bytes=40 << 20
        ),
        cost_estimate=pl.CostEstimate(
            flops=2 * tokens * rows * width,
            bytes_accessed=2 * (tokens * rows + rows * cols + tokens * width),
            transcendentals=0,
        ),
        name="pieces_product",
    )(me, *pieces, weight)


def attn_kernel(core_ref, rows_ref, d_qkv_ref, mixed_ref, heads_ref, weight_ref, kept, sent, gain):
    cols = d_qkv_ref.shape[1]
    d_weight = tn(rows_ref[...], d_qkv_ref[...])
    gain[...] = jnp.sum(d_weight * weight_ref[:, :cols].astype(F32), axis=1, keepdims=True)
    left = d_weight.astype(BF16)
    right = tn(mixed_ref[...], heads_ref[...]).astype(BF16)
    half = left.shape[0] // 2
    for core, (first, second) in enumerate(((kept, sent), (sent, kept))):

        @pl.when(core_ref[0] == core)
        def _(first=first, second=second):
            first[:, :cols] = left[:half]
            first[:, cols:] = right[:half]
            second[:, :cols] = left[half:]
            second[:, cols:] = right[half:]


def attn_grad(rows_in, d_qkv, d_mixed, head_block, weight):
    tokens, rows = rows_in.shape
    qkv_cols, cols = d_qkv.shape[1], weight.shape[1]
    pairs = lax.axis_size("tok") // 2
    core = lax.axis_index("tok") % 2
    step = rows // pairs
    if step % 128 or qkv_cols % 128:
        d_weight = tn(rows_in, d_qkv)
        gain = jnp.sum(d_weight * weight[:, :qkv_cols].astype(F32), axis=1, keepdims=True)
        total = jnp.concatenate([d_weight, tn(d_mixed, head_block)], axis=1).astype(BF16)
        return split_pairs(total, pairs, core), gain
    out = jax.ShapeDtypeStruct((rows // 2, cols), BF16)
    out_spec = pl.BlockSpec((step // 2, cols), lambda pair: (pair, 0))
    left_spec = pl.BlockSpec((tokens, step), lambda pair: (0, pair))
    kept, sent, gain = pl.pallas_call(
        attn_kernel,
        grid=(pairs,),
        out_shape=(out, out, jax.ShapeDtypeStruct((rows, 1), F32)),
        in_specs=[
            pl.BlockSpec(memory_space=pltpu.SMEM),
            left_spec,
            pl.BlockSpec(d_qkv.shape, lambda pair: (0, 0)),
            left_spec,
            pl.BlockSpec(head_block.shape, lambda pair: (0, 0)),
            pl.BlockSpec((step, cols), lambda pair: (pair, 0)),
        ],
        out_specs=(out_spec, out_spec, pl.BlockSpec((step, 1), lambda pair: (pair, 0))),
        compiler_params=pltpu.CompilerParams(
            dimension_semantics=("arbitrary",), vmem_limit_bytes=40 << 20
        ),
        cost_estimate=pl.CostEstimate(
            flops=2 * tokens * rows * cols,
            bytes_accessed=4 * tokens * rows + 2 * tokens * cols + 4 * rows * cols,
            transcendentals=0,
        ),
        name="attn_grad",
    )(core.astype(jnp.int32).reshape(1), rows_in, d_qkv, d_mixed, head_block, weight)
    return (kept, sent), gain


def product_to_mdl(lefts, weight, starts):
    if lax.axis_size("mdl") == 4:
        payload = scatter_product(lefts, weight, starts)
        return payload, lambda payload: scatter_payload(payload)
    part = sum(
        nt(left, weight[:, start : start + left.shape[1]]) for left, start in zip(lefts, starts)
    )
    return (part.astype(BF16),), lambda payload: scatter_mdl(payload[0], 1)


def after(value, *earlier):
    return lax.optimization_barrier((value, *earlier))[0]


def row_scale(rows_b, axis=-1):
    rows = rows_b.astype(F32)
    return lax.rsqrt(jnp.mean(rows * rows, axis=axis, keepdims=True) + NORM_EPS)


def gelu_parts(value):
    root = math.sqrt(2.0 / math.pi)
    square = value * value
    tanh = jnp.tanh(root * (value + 0.044715 * value * square))
    cdf = 0.5 * (1.0 + tanh)
    slope = cdf + 0.5 * value * (1.0 - tanh * tanh) * root * (1.0 + 3 * 0.044715 * square)
    return value * cdf, slope


def scaled(weight, gain):
    return (weight.astype(F32) * gain.astype(F32)[:, None]).astype(BF16)


def on_device(
    inputs, positions, norm1_gain, qkv_weight, out_weight, norm2_gain, gate_weight,
    up_weight, down_weight, cotangent,
):
    me = lax.axis_index("mdl")
    size = lax.axis_size("mdl")
    head_cols = HEADS * HEAD
    width = inputs.shape[1]
    features = width * size

    def from_tok(weight, dim):
        return lax.all_gather(weight, "tok", axis=dim, tiled=True)

    def pair_to_tok(local):
        kept, sent = local
        count = lax.axis_size("tok")
        got = lax.ppermute(sent, "tok", [(i, i ^ 1) for i in range(count)])
        both = (kept.astype(F32) + got.astype(F32)).astype(BF16)
        groups = [list(range(core, count, 2)) for core in range(2)]
        total = lax.psum_scatter(
            both, "tok", scatter_dimension=0, tiled=True, axis_index_groups=groups
        )
        return total.astype(F32)

    qkv_cols, ff_cols = qkv_weight.shape[1], gate_weight.shape[1]
    attn_local = jnp.concatenate([scaled(qkv_weight, norm1_gain), out_weight.T], axis=1)
    w_attn = from_tok(attn_local, 0)
    w_qkv = w_attn[:, :qkv_cols]
    gu_local = jnp.concatenate([scaled(w, norm2_gain) for w in (gate_weight, up_weight)], 1)
    w_gu = from_tok(gu_local, 0)
    w_down_t = from_tok(down_weight.T, 0)

    rows_in = gather_mdl(inputs, 1)
    scale_one = row_scale(rows_in)
    qkv_part = (nn(rows_in, w_qkv) * scale_one).astype(BF16)
    qkv = rows_to_cols(qkv_part)
    count = qkv.shape[0]
    half = HEAD // 2
    frequency = jnp.exp(jnp.arange(half, dtype=F32) * (-2.0 * math.log(10000.0) / HEAD))
    angles = positions.astype(F32)[:, None] * frequency[None, :]
    cos, sin = jnp.cos(angles), jnp.sin(angles)
    key_rows = turn(qkv[:, head_cols : head_cols + HEAD].astype(F32), cos, sin).astype(BF16)
    kv = gather_mdl(jnp.concatenate([key_rows, qkv[:, head_cols + HEAD :]], axis=1), 0)
    first = (me * count).astype(jnp.int32).reshape(1)
    pos = positions[:, None]
    attended, log_norm = attention_forward(first, qkv, kv, cos, sin, pos)
    head_block = cols_to_rows(attended)
    residual = inputs.astype(F32)
    payload, scatter = product_to_mdl((head_block,), w_attn, (qkv_cols,))
    mixed = residual + scatter(payload)

    rows_two = gather_mdl(mixed.astype(BF16), 1)
    scale_two = row_scale(rows_two)
    rows_hat = (rows_two.astype(F32) * scale_two).astype(BF16)
    gate_in = nn(rows_hat, w_gu[:, :ff_cols])
    up_in = nn(rows_hat, w_gu[:, ff_cols:])
    gelu, _ = gelu_parts(gate_in)
    hidden = (gelu * up_in).astype(BF16)
    gate_in, up_in, hidden = lax.optimization_barrier((gate_in, up_in, hidden))
    gelu, slope = gelu_parts(gate_in)

    down_local = pair_grad(cotangent, hidden)
    down_grad = pair_to_tok(down_local).T
    d_hidden = nn(cotangent, w_down_t)
    d_gate_f = d_hidden * up_in * slope
    d_up_f = d_hidden * gelu
    stat_two = jnp.sum(d_gate_f * gate_in + d_up_f * up_in, axis=1)
    d_gate, d_up = d_gate_f.astype(BF16), d_up_f.astype(BF16)
    gate_local = pair_grad(rows_hat, d_gate)
    gate_sum = pair_to_tok(gate_local)
    payload, scatter = product_to_mdl((d_gate, d_up), w_gu, (0, ff_cols))
    rows_later = after(rows_hat, payload[0])
    up_local = pair_grad(rows_later, d_up)
    up_sum = pair_to_tok(up_local)
    d_two = scatter(payload)
    stat_two = sum_mdl(stat_two.reshape(8, -1)).reshape(-1, 1) * (1.0 / features)
    scale_mixed = scale_two * mixed
    cotangent_own = lax.dynamic_slice_in_dim(cotangent, me * width, width, 1).astype(F32)
    d_mixed = cotangent_own + scale_two * (d_two - scale_mixed * stat_two)

    d_mixed_b = after(d_mixed.astype(BF16), up_local[0])
    hidden_later = after(hidden, d_mixed_b)
    ffn_payload, ffn_scatter = product_to_mdl((hidden_later,), w_down_t, (0,))
    out_cols = head_block.shape[1]
    if size == 4:
        pieces = gather_pieces(d_mixed_b)
        d_head = pieces_product(pieces, w_attn, qkv_cols, out_cols)
        d_mixed_rows = assemble(tuple(after(piece, d_head) for piece in pieces))
    else:
        d_mixed_rows = gather_mdl(d_mixed_b, 1)
        d_head = nn(d_mixed_rows, w_attn[:, qkv_cols:]).astype(BF16)
    d_attended = rows_to_cols(d_head)
    block_out = (mixed + ffn_scatter(ffn_payload)).astype(BF16)
    d_query, d_kv = attention_backward(
        first, qkv, kv, cos, sin, pos, attended, d_attended, log_norm
    )
    d_kv = scatter_mdl(d_kv.astype(BF16), 0)
    d_key = unturn(d_kv[:, :HEAD], cos, sin).astype(BF16)
    d_qkv = jnp.concatenate([d_query, d_key, d_kv[:, HEAD:].astype(BF16)], axis=1)
    stat_one = jnp.sum(d_qkv.astype(F32) * qkv.astype(F32), axis=1)
    d_qkv_part = cols_to_rows(d_qkv)
    stat_rows = jnp.zeros((size, count), F32)
    stat_rows = sum_mdl(lax.dynamic_update_slice(stat_rows, stat_one[None], (me, 0)))
    stat_one = stat_rows.reshape(-1, 1) * (1.0 / features)
    d_scaled = (d_qkv_part.astype(F32) * scale_one).astype(BF16)
    attn_local, gain_one = attn_grad(rows_in, d_scaled, d_mixed_rows, head_block, w_attn)
    attn_sum = pair_to_tok(attn_local)
    qkv_sum, out_grad = attn_sum[:, :qkv_cols], attn_sum[:, qkv_cols:].T
    d_later = after(d_qkv_part, attn_local[0])
    payload, scatter = product_to_mdl((d_later,), w_attn, (0,))
    d_one = scatter(payload)
    input_grad = d_mixed + scale_one * (d_one - (scale_one * residual) * stat_one)

    norm1_late, norm2_late, gate_late, up_late, _ = lax.optimization_barrier(
        (norm1_gain, norm2_gain, gate_weight, up_weight, up_local[0])
    )

    def unfold(total, gain):
        return total * gain.astype(F32)[:, None]

    gain_two = jnp.sum(
        gate_late.astype(F32) * gate_sum + up_late.astype(F32) * up_sum, axis=1
    )
    gate_grad, up_grad = unfold(gate_sum, norm2_late), unfold(up_sum, norm2_late)
    gain_two_grad = sum_mdl(gain_two)
    gain_one = sum_tok(sum_mdl(gain_one.reshape(8, -1))).reshape(-1)
    shard = norm1_gain.shape[0]
    gain_one = lax.dynamic_slice_in_dim(gain_one, lax.axis_index("tok") * shard, shard, 0)
    gain_one_grad = gain_one / norm1_late.astype(F32)
    return (
        block_out,
        input_grad,
        gain_one_grad,
        unfold(qkv_sum, norm1_late),
        out_grad,
        gain_two_grad,
        gate_grad,
        up_grad,
        down_grad,
    )


def solution(mesh):
    return jax.shard_map(
        on_device,
        mesh=mesh,
        in_specs=(
            P("tok", "mdl"),
            P(("tok", "mdl")),
            P("tok"),
            P("tok", "mdl"),
            P("mdl", "tok"),
            P("tok"),
            P("tok", "mdl"),
            P("tok", "mdl"),
            P("mdl", "tok"),
            P("tok", None),
        ),
        out_specs=(
            P("tok", "mdl"),
            P("tok", "mdl"),
            P("tok"),
            P("tok", "mdl"),
            P("mdl", "tok"),
            P("tok"),
            P("tok", "mdl"),
            P("tok", "mdl"),
            P("mdl", "tok"),
        ),
        check_vma=False,
    )
```

```python
import functools
import math

import jax
import jax.numpy as jnp
from jax import lax
from jax.experimental import pallas as pl
from jax.experimental.pallas import tpu as pltpu
from jax.sharding import PartitionSpec as P


HEADS = 10
HEAD = 256
NORM_EPS = 1e-06
F32 = jnp.float32
BF16 = jnp.bfloat16
MASKED = -1e30


def nt(left_op, right_op):
    return lax.dot_general(
        left_op, right_op, (((1,), (1,)), ((), ())), preferred_element_type=F32
    )


def tn(left_op, right_op):
    return lax.dot_general(
        left_op, right_op, (((0,), (0,)), ((), ())), preferred_element_type=F32
    )


def nn(left_op, right_op):
    return jnp.dot(left_op, right_op, preferred_element_type=F32)


def swap(block, distance):
    size = lax.axis_size("mdl")
    return lax.ppermute(block, "mdl", [(i, i ^ distance) for i in range(size)])


def gather_mdl(block, dim):
    size = lax.axis_size("mdl")
    if size != 4:
        return lax.all_gather(block, "mdl", axis=dim, tiled=True)
    me = lax.axis_index("mdl")
    half = block.shape[0] // 2
    along_x = swap(block, 1)
    along_y = swap(block, 2)
    top = swap(along_x[:half], 2)
    bottom = swap(along_y[half:], 1)
    width = block.shape[dim]
    shape = list(block.shape)
    shape[dim] = width * size
    whole = jnp.zeros(shape, block.dtype)

    def put(whole, piece, source, row):
        start = [0, 0]
        start[dim] = source * width
        start[0] = start[0] + row
        return lax.dynamic_update_slice(whole, piece, tuple(start))

    whole = put(whole, block, me, 0)
    whole = put(whole, along_x, me ^ 1, 0)
    whole = put(whole, along_y, me ^ 2, 0)
    whole = put(whole, top, me ^ 3, 0)
    whole = put(whole, bottom, me ^ 3, half)
    return whole


def scatter_mdl(part, dim):
    size = lax.axis_size("mdl")
    if size != 4:
        return lax.psum_scatter(part, "mdl", scatter_dimension=dim, tiled=True).astype(F32)
    me = lax.axis_index("mdl")
    shape = list(part.shape)
    shape[dim] //= size
    half = shape[0] // 2

    def piece(block, row):
        start = [0, 0]
        start[dim] = block * shape[dim]
        start[0] = start[0] + row
        return lax.dynamic_slice(part, tuple(start), (half, shape[1]))

    sums = []
    for row, first, second in ((0, 1, 2), (half, 2, 1)):
        sent = jnp.stack([piece(me ^ first, row), piece(me ^ 3, row)])
        sums.append((row, second, swap(sent, first)))
    partial = []
    for row, second, got in sums:
        other = piece(me ^ second, row).astype(F32) + got[1].astype(F32)
        partial.append((row, got[0], swap(other.astype(BF16), second)))
    return jnp.concatenate(
        [
            piece(me, row).astype(F32) + first.astype(F32) + second.astype(F32)
            for row, first, second in partial
        ],
        axis=0,
    )


def gather_pieces(block):
    half = block.shape[0] // 2
    along_x = swap(block, 1)
    along_y = swap(block, 2)
    top = swap(along_x[:half], 2)
    bottom = swap(along_y[half:], 1)
    return block, along_x, along_y, top, bottom


def scatter_payload(payload):
    top_sent, bottom_sent, top_kept, bottom_kept = payload
    got_top = swap(top_sent, 1)
    got_bottom = swap(bottom_sent, 2)
    halves = []
    for kept, got, second in ((top_kept, got_top, 2), (bottom_kept, got_bottom, 1)):
        passed = (kept[1].astype(F32) + got[1].astype(F32)).astype(BF16)
        last = swap(passed, second)
        halves.append(kept[0].astype(F32) + got[0].astype(F32) + last.astype(F32))
    return jnp.concatenate(halves, axis=0)


def sum_mdl(value):
    size = lax.axis_size("mdl")
    distance = 1
    while distance < size:
        value = value + swap(value, distance)
        distance *= 2
    return value


def sum_tok(value):
    size = lax.axis_size("tok")
    distance = 1
    while distance < size:
        value = value + lax.ppermute(value, "tok", [(i, i ^ distance) for i in range(size)])
        distance *= 2
    return value


def rows_to_cols(block):
    return lax.all_to_all(block, "mdl", split_axis=0, concat_axis=1, tiled=True)


def cols_to_rows(block):
    return lax.all_to_all(block, "mdl", split_axis=1, concat_axis=0, tiled=True)


def in_order(mebibytes):
    return pltpu.CompilerParams(
        dimension_semantics=(pltpu.ARBITRARY,), vmem_limit_bytes=mebibytes << 20
    )


def cost(flops, bytes_accessed, transcendentals=0):
    return pl.CostEstimate(
        flops=flops, bytes_accessed=bytes_accessed, transcendentals=transcendentals
    )


def turn(vector, cos, sin):
    half = HEAD // 2
    lower, upper = vector[:, :half], vector[:, half:]
    return jnp.concatenate([lower * cos - upper * sin, upper * cos + lower * sin], axis=1)


def unturn(vector, cos, sin):
    half = HEAD // 2
    lower, upper = vector[:, :half], vector[:, half:]
    return jnp.concatenate([lower * cos + upper * sin, upper * cos - lower * sin], axis=1)


def seen(first_ref, position_ref, queries, keys):
    row = lax.broadcasted_iota(jnp.int32, (queries, keys), 0) + first_ref[0]
    distance = row - lax.broadcasted_iota(jnp.int32, (queries, keys), 1)
    return (distance >= 0) & (distance <= position_ref[...])


def forward_kernel(first_ref, q_ref, kv_ref, cos_ref, sin_ref, pos_ref, out_ref, norm_ref):
    query = turn(q_ref[...].astype(F32), cos_ref[...], sin_ref[...])
    query = (query * HEAD ** (-0.5)).astype(BF16)
    keys, values = kv_ref[:, :HEAD], kv_ref[:, HEAD:]
    scores = nt(query, keys)
    scores = jnp.where(seen(first_ref, pos_ref, *scores.shape), scores, MASKED)
    top = jnp.max(scores, axis=1, keepdims=True)
    weights = jnp.exp(scores - top)
    total = jnp.sum(weights, axis=1, keepdims=True)
    out_ref[...] = (nn(weights.astype(BF16), values) / total).astype(BF16)
    norm_ref[0] = top + jnp.log(total)


def backward_kernel(
    first_ref, q_ref, kv_ref, cos_ref, sin_ref, pos_ref, att_ref, datt_ref, norm_ref,
    dq_ref, dkv_ref,
):
    head = pl.program_id(0)
    scale = HEAD ** (-0.5)
    cos, sin = cos_ref[...], sin_ref[...]
    query = (turn(q_ref[...].astype(F32), cos, sin) * scale).astype(BF16)
    keys, values = kv_ref[:, :HEAD], kv_ref[:, HEAD:]
    scores = nt(query, keys)
    visible = seen(first_ref, pos_ref, *scores.shape)
    again = jnp.where(visible, jnp.exp(scores - norm_ref[0]), 0.0)
    d_att = datt_ref[...]
    delta = jnp.sum(d_att.astype(F32) * att_ref[...].astype(F32), axis=1, keepdims=True)
    d_scores = (again * (nt(d_att, values) - delta)).astype(BF16)
    d_query = nn(d_scores, keys) * scale
    dq_ref[...] = unturn(d_query, cos, sin).astype(BF16)

    @pl.when(head == 0)
    def _():
        dkv_ref[...] = jnp.zeros_like(dkv_ref)

    dkv_ref[:, :HEAD] += tn(d_scores, query)
    dkv_ref[:, HEAD:] += tn(again.astype(BF16), d_att)


def whole_spec(shape):
    return pl.BlockSpec(shape, lambda head: (0,) * len(shape))


def attention_forward(first, qkv, kv, cos, sin, pos):
    rows, keys = qkv.shape[0], kv.shape[0]
    head_spec = pl.BlockSpec((rows, HEAD), lambda head: (0, head))
    return pl.pallas_call(
        forward_kernel,
        grid=(HEADS,),
        out_shape=(
            jax.ShapeDtypeStruct((rows, HEADS * HEAD), BF16),
            jax.ShapeDtypeStruct((HEADS, rows, 1), F32),
        ),
        in_specs=[
            pl.BlockSpec(memory_space=pltpu.SMEM),
            head_spec,
            whole_spec((keys, 2 * HEAD)),
            whole_spec((rows, HEAD // 2)),
            whole_spec((rows, HEAD // 2)),
            whole_spec((rows, 1)),
        ],
        out_specs=(head_spec, pl.BlockSpec((1, rows, 1), lambda head: (head, 0, 0))),
        compiler_params=in_order(32),
        cost_estimate=cost(4 * rows * keys * HEADS * HEAD, 4 * rows * HEADS * HEAD + 4 * keys * HEAD, rows * keys * HEADS),
        name="attention_forward",
    )(first, qkv, kv, cos, sin, pos)


def attention_backward(first, qkv, kv, cos, sin, pos, att, d_att, norm):
    rows, keys = qkv.shape[0], kv.shape[0]
    head_spec = pl.BlockSpec((rows, HEAD), lambda head: (0, head))
    return pl.pallas_call(
        backward_kernel,
        grid=(HEADS,),
        out_shape=(
            jax.ShapeDtypeStruct((rows, HEADS * HEAD), BF16),
            jax.ShapeDtypeStruct((keys, 2 * HEAD), F32),
        ),
        in_specs=[
            pl.BlockSpec(memory_space=pltpu.SMEM),
            head_spec,
            whole_spec((keys, 2 * HEAD)),
            whole_spec((rows, HEAD // 2)),
            whole_spec((rows, HEAD // 2)),
            whole_spec((rows, 1)),
            head_spec,
            head_spec,
            pl.BlockSpec((1, rows, 1), lambda head: (head, 0, 0)),
        ],
        out_specs=(head_spec, whole_spec((keys, 2 * HEAD))),
        compiler_params=in_order(40),
        cost_estimate=cost(10 * rows * keys * HEADS * HEAD, 8 * rows * HEADS * HEAD + 12 * keys * HEAD, rows * keys * HEADS),
        name="attention_backward",
    )(first, qkv, kv, cos, sin, pos, att, d_att, norm)


def keep_half(core_ref, total, kept, sent):
    half = total.shape[0] // 2
    for core, (first, second) in enumerate(((kept, sent), (sent, kept))):

        @pl.when(core_ref[0] == core)
        def _(first=first, second=second):
            first[...] = total[:half]
            second[...] = total[half:]


def pair_kernel(core_ref, left_ref, right_ref, *refs):
    total = tn(left_ref[...], right_ref[...])
    if len(refs) == 4:
        weight = refs[0][:, : total.shape[1]].astype(F32)
        refs[3][...] = jnp.sum(total * weight, axis=1, keepdims=True)
    keep_half(core_ref, total.astype(BF16), *refs[-3:-1] if len(refs) == 4 else refs)


def split_pairs(total, pairs, core):
    rows, cols = total.shape
    total = total.reshape(pairs, 2, rows // pairs // 2, cols)
    return tuple(
        lax.dynamic_index_in_dim(total, index, 1, False).reshape(-1, cols)
        for index in (core, 1 - core)
    )


def core_index():
    return (lax.axis_index("tok") % 2).astype(jnp.int32).reshape(1)


def pair_grad(left, right, weight=None):
    tokens, rows = left.shape
    cols = right.shape[1]
    pairs = lax.axis_size("tok") // 2
    step = rows // pairs
    if step % 128 or cols % 128:
        total = tn(left, right)
        halves = split_pairs(total.astype(BF16), pairs, lax.axis_index("tok") % 2)
        if weight is None:
            return halves
        return *halves, jnp.sum(total * weight[:, :cols].astype(F32), axis=1, keepdims=True)
    out_shape = [jax.ShapeDtypeStruct((rows // 2, cols), BF16)] * 2
    out_specs = [pl.BlockSpec((step // 2, cols), lambda pair: (pair, 0))] * 2
    in_specs = [
        pl.BlockSpec(memory_space=pltpu.SMEM),
        pl.BlockSpec((tokens, step), lambda pair: (0, pair)),
        pl.BlockSpec((tokens, cols), lambda pair: (0, 0)),
    ]
    operands = [core_index(), left, right]
    if weight is not None:
        operands.append(weight)
        in_specs.append(pl.BlockSpec((step, weight.shape[1]), lambda pair: (pair, 0)))
        out_shape.append(jax.ShapeDtypeStruct((rows, 1), F32))
        out_specs.append(pl.BlockSpec((step, 1), lambda pair: (pair, 0)))
    return pl.pallas_call(
        pair_kernel,
        grid=(pairs,),
        out_shape=out_shape,
        in_specs=in_specs,
        out_specs=out_specs,
        compiler_params=in_order(48),
        cost_estimate=cost(2 * tokens * rows * cols, 2 * (tokens * (rows + cols) + rows * cols)),
    )(*operands)


def pieces_grad_kernel(me_ref, core_ref, own, along_x, along_y, top, bottom, right_ref, kept, sent):
    at = pl.program_id(0)
    half = top.shape[0]
    for index, piece in enumerate((own, along_x, along_y)):

        @pl.when(at == index)
        def _(piece=piece):
            keep_half(core_ref, tn(piece[...], right_ref[...]).astype(BF16), kept, sent)

    @pl.when(at == 3)
    def _():
        total = tn(top[...], right_ref[:half]) + tn(bottom[...], right_ref[half:])
        keep_half(core_ref, total.astype(BF16), kept, sent)


def pieces_grad(pieces, right):
    tokens, step = pieces[0].shape
    cols = right.shape[1]
    me = lax.axis_index("mdl").astype(jnp.int32).reshape(1)
    out = jax.ShapeDtypeStruct((2 * step, cols), BF16)
    return pl.pallas_call(
        pieces_grad_kernel,
        grid_spec=pltpu.PrefetchScalarGridSpec(
            num_scalar_prefetch=2,
            grid=(4,),
            in_specs=[
                pl.BlockSpec(array.shape, lambda at, me_ref, core_ref: (0, 0))
                for array in (*pieces, right)
            ],
            out_specs=[
                pl.BlockSpec((step // 2, cols), lambda at, me_ref, core_ref: (me_ref[0] ^ at, 0))
            ]
            * 2,
        ),
        out_shape=(out, out),
        compiler_params=in_order(48),
        cost_estimate=cost(8 * tokens * step * cols, 2 * (4 * tokens * step + 5 * step * cols)),
    )(me, core_index(), *pieces, right)


def payload_kernel(starts, me_ref, *refs):
    lefts, weight_ref = refs[: len(starts)], refs[len(starts)]
    top_sent, bottom_sent, top_kept, bottom_kept = refs[len(starts) + 1 :]
    total = 0.0
    for left_ref, start in zip(lefts, starts):
        total += nt(left_ref[...], weight_ref[:, start : start + left_ref.shape[1]])
    total = total.astype(BF16)
    half = total.shape[0] // 2
    places = (
        ((top_kept, 0), (bottom_kept, 0)),
        ((top_sent, 0), (bottom_kept, 1)),
        ((top_kept, 1), (bottom_sent, 0)),
        ((top_sent, 1), (bottom_sent, 1)),
    )
    for distance, ((top, top_at), (bottom, bottom_at)) in enumerate(places):

        @pl.when(pl.program_id(0) == 3 - distance)
        def _(top=top, top_at=top_at, bottom=bottom, bottom_at=bottom_at):
            top[top_at] = total[:half]
            bottom[bottom_at] = total[half:]


def scatter_product(lefts, weight, starts):
    tokens = lefts[0].shape[0]
    rows, cols = weight.shape
    step = rows // 4
    me = lax.axis_index("mdl").astype(jnp.int32).reshape(1)
    out = jax.ShapeDtypeStruct((2, tokens // 2, step), BF16)
    depth = sum(left.shape[1] for left in lefts)
    return pl.pallas_call(
        functools.partial(payload_kernel, starts),
        grid_spec=pltpu.PrefetchScalarGridSpec(
            num_scalar_prefetch=1,
            grid=(4,),
            in_specs=[pl.BlockSpec(left.shape, lambda at, me_ref: (0, 0)) for left in lefts]
            + [pl.BlockSpec((step, cols), lambda at, me_ref: (me_ref[0] ^ (3 - at), 0))],
            out_specs=[pl.BlockSpec(out.shape, lambda at, me_ref: (0, 0, 0))] * 4,
        ),
        out_shape=(out,) * 4,
        compiler_params=in_order(48),
        cost_estimate=cost(2 * tokens * rows * depth, 2 * (tokens * depth + rows * cols + tokens * rows)),
    )(me, *lefts, weight)


def pieces_kernel(start, me_ref, own, along_x, along_y, top, bottom, weight_ref, out_ref, total):
    at = pl.program_id(0)
    width = out_ref.shape[1]
    half = top.shape[0]
    for index, piece in enumerate((own, along_x, along_y)):

        @pl.when(at == index)
        def _(index=index, piece=piece):
            part = nn(piece[...], weight_ref[:, start : start + width])
            if index:
                total[...] += part
            else:
                total[...] = part

    @pl.when(at == 3)
    def _():
        weight = weight_ref[:, start : start + width]
        out_ref[:half] = (total[:half] + nn(top[...], weight)).astype(BF16)
        out_ref[half:] = (total[half:] + nn(bottom[...], weight)).astype(BF16)


def pieces_product(pieces, weight, start, width):
    tokens, step = pieces[0].shape
    rows, cols = weight.shape
    me = lax.axis_index("mdl").astype(jnp.int32).reshape(1)
    return pl.pallas_call(
        functools.partial(pieces_kernel, start),
        grid_spec=pltpu.PrefetchScalarGridSpec(
            num_scalar_prefetch=1,
            grid=(4,),
            in_specs=[pl.BlockSpec(piece.shape, lambda at, me_ref: (0, 0)) for piece in pieces]
            + [pl.BlockSpec((step, cols), lambda at, me_ref: (me_ref[0] ^ at, 0))],
            out_specs=pl.BlockSpec((tokens, width), lambda at, me_ref: (0, 0)),
            scratch_shapes=[pltpu.VMEM((tokens, width), F32)],
        ),
        out_shape=jax.ShapeDtypeStruct((tokens, width), BF16),
        compiler_params=in_order(40),
        cost_estimate=cost(2 * tokens * rows * width, 2 * (tokens * rows + rows * cols + tokens * width)),
    )(me, *pieces, weight)


def product_to_mdl(lefts, weight, starts):
    if lax.axis_size("mdl") == 4:
        payload = scatter_product(lefts, weight, starts)
        return payload, lambda payload: scatter_payload(payload)
    part = sum(
        nt(left, weight[:, start : start + left.shape[1]]) for left, start in zip(lefts, starts)
    )
    return (part.astype(BF16),), lambda payload: scatter_mdl(payload[0], 1)


def after(value, *earlier):
    return lax.optimization_barrier((value, *earlier))[0]


def row_scale(rows_b, axis=-1):
    rows = rows_b.astype(F32)
    return lax.rsqrt(jnp.mean(rows * rows, axis=axis, keepdims=True) + NORM_EPS)


def gelu_parts(value):
    root = math.sqrt(2.0 / math.pi)
    square = value * value
    tanh = jnp.tanh(root * (value + 0.044715 * value * square))
    cdf = 0.5 * (1.0 + tanh)
    slope = cdf + 0.5 * value * (1.0 - tanh * tanh) * root * (1.0 + 3 * 0.044715 * square)
    return value * cdf, slope


def scaled(weight, gain):
    return (weight.astype(F32) * gain.astype(F32)[:, None]).astype(BF16)


def on_device(
    inputs, positions, norm1_gain, qkv_weight, out_weight, norm2_gain, gate_weight,
    up_weight, down_weight, cotangent,
):
    me = lax.axis_index("mdl")
    size = lax.axis_size("mdl")
    head_cols = HEADS * HEAD
    width = inputs.shape[1]
    features = width * size

    def from_tok(weight, dim):
        return lax.all_gather(weight, "tok", axis=dim, tiled=True)

    def pair_to_tok(local):
        kept, sent = local
        count = lax.axis_size("tok")
        got = lax.ppermute(sent, "tok", [(i, i ^ 1) for i in range(count)])
        both = (kept.astype(F32) + got.astype(F32)).astype(BF16)
        groups = [list(range(core, count, 2)) for core in range(2)]
        total = lax.psum_scatter(
            both, "tok", scatter_dimension=0, tiled=True, axis_index_groups=groups
        )
        return total.astype(F32)

    qkv_cols, ff_cols = qkv_weight.shape[1], gate_weight.shape[1]
    attn_local = jnp.concatenate([scaled(qkv_weight, norm1_gain), out_weight.T], axis=1)
    w_attn = from_tok(attn_local, 0)
    w_qkv = w_attn[:, :qkv_cols]
    gu_local = jnp.concatenate([scaled(w, norm2_gain) for w in (gate_weight, up_weight)], 1)
    w_gu = from_tok(gu_local, 0)
    w_down_t = from_tok(down_weight.T, 0)

    rows_in = gather_mdl(inputs, 1)
    scale_one = row_scale(rows_in)
    qkv_part = (nn(rows_in, w_qkv) * scale_one).astype(BF16)
    qkv = rows_to_cols(qkv_part)
    count = qkv.shape[0]
    half = HEAD // 2
    frequency = jnp.exp(jnp.arange(half, dtype=F32) * (-2.0 * math.log(10000.0) / HEAD))
    angles = positions.astype(F32)[:, None] * frequency[None, :]
    cos, sin = jnp.cos(angles), jnp.sin(angles)
    key_rows = turn(qkv[:, head_cols : head_cols + HEAD].astype(F32), cos, sin).astype(BF16)
    kv = gather_mdl(jnp.concatenate([key_rows, qkv[:, head_cols + HEAD :]], axis=1), 0)
    first = (me * count).astype(jnp.int32).reshape(1)
    pos = positions[:, None]
    attended, log_norm = attention_forward(first, qkv, kv, cos, sin, pos)
    head_block = cols_to_rows(attended)
    residual = inputs.astype(F32)
    payload, scatter = product_to_mdl((head_block,), w_attn, (qkv_cols,))
    mixed = residual + scatter(payload)

    rows_two = gather_mdl(mixed.astype(BF16), 1)
    scale_two = row_scale(rows_two)
    rows_hat = (rows_two.astype(F32) * scale_two).astype(BF16)
    gate_in = nn(rows_hat, w_gu[:, :ff_cols])
    up_in = nn(rows_hat, w_gu[:, ff_cols:])
    gelu, _ = gelu_parts(gate_in)
    hidden = (gelu * up_in).astype(BF16)
    gate_in, up_in, hidden = lax.optimization_barrier((gate_in, up_in, hidden))
    gelu, slope = gelu_parts(gate_in)

    down_local = pair_grad(cotangent, hidden)
    down_grad = pair_to_tok(down_local).T
    d_hidden = nn(cotangent, w_down_t)
    d_gate_f = d_hidden * up_in * slope
    d_up_f = d_hidden * gelu
    stat_two = jnp.sum(d_gate_f * gate_in + d_up_f * up_in, axis=1)
    d_gate, d_up = d_gate_f.astype(BF16), d_up_f.astype(BF16)
    gate_local = pair_grad(rows_hat, d_gate)
    gate_sum = pair_to_tok(gate_local)
    payload, scatter = product_to_mdl((d_gate, d_up), w_gu, (0, ff_cols))
    rows_later = after(rows_hat, payload[0])
    up_local = pair_grad(rows_later, d_up)
    up_sum = pair_to_tok(up_local)
    d_two = scatter(payload)
    stat_two = sum_mdl(stat_two.reshape(8, -1)).reshape(-1, 1) * (1.0 / features)
    scale_mixed = scale_two * mixed
    cotangent_own = lax.dynamic_slice_in_dim(cotangent, me * width, width, 1).astype(F32)
    d_mixed = cotangent_own + scale_two * (d_two - scale_mixed * stat_two)

    d_mixed_b = after(d_mixed.astype(BF16), up_local[0])
    hidden_later = after(hidden, d_mixed_b)
    ffn_payload, ffn_scatter = product_to_mdl((hidden_later,), w_down_t, (0,))
    if size == 4 and lax.axis_size("tok") == 8:
        pieces = gather_pieces(d_mixed_b)
        d_head = pieces_product(pieces, w_attn, qkv_cols, head_block.shape[1])
        heads_later = after(head_block, d_head)
        out_local = pieces_grad(pieces, heads_later)
    else:
        d_mixed_rows = gather_mdl(d_mixed_b, 1)
        d_head = nn(d_mixed_rows, w_attn[:, qkv_cols:]).astype(BF16)
        out_local = pair_grad(d_mixed_rows, head_block)
    out_grad = pair_to_tok(out_local).T
    d_attended = rows_to_cols(d_head)
    block_out = (mixed + ffn_scatter(ffn_payload)).astype(BF16)
    d_query, d_kv = attention_backward(
        first, qkv, kv, cos, sin, pos, attended, d_attended, log_norm
    )
    d_kv = scatter_mdl(d_kv.astype(BF16), 0)
    d_key = unturn(d_kv[:, :HEAD], cos, sin).astype(BF16)
    d_qkv = jnp.concatenate([d_query, d_key, d_kv[:, HEAD:].astype(BF16)], axis=1)
    stat_one = jnp.sum(d_qkv.astype(F32) * qkv.astype(F32), axis=1)
    d_qkv_part = cols_to_rows(d_qkv)
    stat_rows = jnp.zeros((size, count), F32)
    stat_rows = sum_mdl(lax.dynamic_update_slice(stat_rows, stat_one[None], (me, 0)))
    stat_one = stat_rows.reshape(-1, 1) * (1.0 / features)
    payload, scatter = product_to_mdl((d_qkv_part,), w_attn, (0,))
    d_scaled = (after(d_qkv_part, payload[0]).astype(F32) * scale_one).astype(BF16)
    *qkv_local, gain_one = pair_grad(rows_in, d_scaled, w_attn)
    qkv_sum = pair_to_tok(qkv_local)
    d_one = scatter(payload)
    input_grad = d_mixed + scale_one * (d_one - (scale_one * residual) * stat_one)

    norm1_late, norm2_late, gate_late, up_late, _ = lax.optimization_barrier(
        (norm1_gain, norm2_gain, gate_weight, up_weight, up_local[0])
    )

    def unfold(total, gain):
        return total * gain.astype(F32)[:, None]

    gain_two = jnp.sum(
        gate_late.astype(F32) * gate_sum + up_late.astype(F32) * up_sum, axis=1
    )
    gate_grad, up_grad = unfold(gate_sum, norm2_late), unfold(up_sum, norm2_late)
    gain_two_grad = sum_mdl(gain_two)
    gain_one = sum_mdl(sum_tok(gain_one.reshape(8, -1))).reshape(-1)
    shard = norm1_gain.shape[0]
    gain_one = lax.dynamic_slice_in_dim(gain_one, lax.axis_index("tok") * shard, shard, 0)
    gain_one_grad = gain_one / norm1_late.astype(F32)
    return (
        block_out,
        input_grad,
        gain_one_grad,
        unfold(qkv_sum, norm1_late),
        out_grad,
        gain_two_grad,
        gate_grad,
        up_grad,
        down_grad,
    )


def solution(mesh):
    return jax.shard_map(
        on_device,
        mesh=mesh,
        in_specs=(
            P("tok", "mdl"),
            P(("tok", "mdl")),
            P("tok"),
            P("tok", "mdl"),
            P("mdl", "tok"),
            P("tok"),
            P("tok", "mdl"),
            P("tok", "mdl"),
            P("mdl", "tok"),
            P("tok", None),
        ),
        out_specs=(
            P("tok", "mdl"),
            P("tok", "mdl"),
            P("tok"),
            P("tok", "mdl"),
            P("mdl", "tok"),
            P("tok"),
            P("tok", "mdl"),
            P("tok", "mdl"),
            P("mdl", "tok"),
        ),
        check_vma=False,
    )
```

```python
import functools
import math

import jax
import jax.numpy as jnp
from jax import lax
from jax.experimental import pallas as pl
from jax.experimental.pallas import tpu as pltpu
from jax.sharding import PartitionSpec as P


HEADS = 10
HEAD = 256
NORM_EPS = 1e-06
F32 = jnp.float32
BF16 = jnp.bfloat16
MASKED = -1e30


def nt(left_op, right_op):
    return lax.dot_general(
        left_op, right_op, (((1,), (1,)), ((), ())), preferred_element_type=F32
    )


def tn(left_op, right_op):
    return lax.dot_general(
        left_op, right_op, (((0,), (0,)), ((), ())), preferred_element_type=F32
    )


def nn(left_op, right_op):
    return jnp.dot(left_op, right_op, preferred_element_type=F32)


def swap(block, distance):
    size = lax.axis_size("mdl")
    return lax.ppermute(block, "mdl", [(i, i ^ distance) for i in range(size)])


def gather_mdl(block, dim):
    size = lax.axis_size("mdl")
    if size != 4:
        return lax.all_gather(block, "mdl", axis=dim, tiled=True)
    me = lax.axis_index("mdl")
    half = block.shape[0] // 2
    along_x = swap(block, 1)
    along_y = swap(block, 2)
    top = swap(along_x[:half], 2)
    bottom = swap(along_y[half:], 1)
    width = block.shape[dim]
    shape = list(block.shape)
    shape[dim] = width * size
    whole = jnp.zeros(shape, block.dtype)

    def put(whole, piece, source, row):
        start = [0, 0]
        start[dim] = source * width
        start[0] = start[0] + row
        return lax.dynamic_update_slice(whole, piece, tuple(start))

    whole = put(whole, block, me, 0)
    whole = put(whole, along_x, me ^ 1, 0)
    whole = put(whole, along_y, me ^ 2, 0)
    whole = put(whole, top, me ^ 3, 0)
    whole = put(whole, bottom, me ^ 3, half)
    return whole


def scatter_mdl(part, dim):
    size = lax.axis_size("mdl")
    if size != 4:
        return lax.psum_scatter(part, "mdl", scatter_dimension=dim, tiled=True).astype(F32)
    me = lax.axis_index("mdl")
    shape = list(part.shape)
    shape[dim] //= size
    half = shape[0] // 2

    def piece(block, row):
        start = [0, 0]
        start[dim] = block * shape[dim]
        start[0] = start[0] + row
        return lax.dynamic_slice(part, tuple(start), (half, shape[1]))

    sums = []
    for row, first, second in ((0, 1, 2), (half, 2, 1)):
        sent = jnp.stack([piece(me ^ first, row), piece(me ^ 3, row)])
        sums.append((row, second, swap(sent, first)))
    partial = []
    for row, second, got in sums:
        other = piece(me ^ second, row).astype(F32) + got[1].astype(F32)
        partial.append((row, got[0], swap(other.astype(BF16), second)))
    return jnp.concatenate(
        [
            piece(me, row).astype(F32) + first.astype(F32) + second.astype(F32)
            for row, first, second in partial
        ],
        axis=0,
    )


def gather_pieces(block):
    half = block.shape[0] // 2
    along_x = swap(block, 1)
    along_y = swap(block, 2)
    top = swap(along_x[:half], 2)
    bottom = swap(along_y[half:], 1)
    return block, along_x, along_y, top, bottom


def scatter_payload(payload):
    top_sent, bottom_sent, top_kept, bottom_kept = payload
    got_top = swap(top_sent, 1)
    got_bottom = swap(bottom_sent, 2)
    halves = []
    for kept, got, second in ((top_kept, got_top, 2), (bottom_kept, got_bottom, 1)):
        passed = (kept[1].astype(F32) + got[1].astype(F32)).astype(BF16)
        last = swap(passed, second)
        halves.append(kept[0].astype(F32) + got[0].astype(F32) + last.astype(F32))
    return jnp.concatenate(halves, axis=0)


def sum_mdl(value):
    size = lax.axis_size("mdl")
    distance = 1
    while distance < size:
        value = value + swap(value, distance)
        distance *= 2
    return value


def sum_tok(value):
    size = lax.axis_size("tok")
    distance = 1
    while distance < size:
        value = value + lax.ppermute(value, "tok", [(i, i ^ distance) for i in range(size)])
        distance *= 2
    return value


def rows_to_cols(block):
    return lax.all_to_all(block, "mdl", split_axis=0, concat_axis=1, tiled=True)


def cols_to_rows(block):
    return lax.all_to_all(block, "mdl", split_axis=1, concat_axis=0, tiled=True)


def in_order(mebibytes):
    return pltpu.CompilerParams(
        dimension_semantics=(pltpu.ARBITRARY,), vmem_limit_bytes=mebibytes << 20
    )


def cost(flops, bytes_accessed, transcendentals=0):
    return pl.CostEstimate(
        flops=flops, bytes_accessed=bytes_accessed, transcendentals=transcendentals
    )


def turn(vector, cos, sin):
    half = HEAD // 2
    lower, upper = vector[:, :half], vector[:, half:]
    return jnp.concatenate([lower * cos - upper * sin, upper * cos + lower * sin], axis=1)


def unturn(vector, cos, sin):
    half = HEAD // 2
    lower, upper = vector[:, :half], vector[:, half:]
    return jnp.concatenate([lower * cos + upper * sin, upper * cos - lower * sin], axis=1)


def seen(first_ref, position_ref, queries, keys):
    row = lax.broadcasted_iota(jnp.int32, (queries, keys), 0) + first_ref[0]
    distance = row - lax.broadcasted_iota(jnp.int32, (queries, keys), 1)
    return (distance >= 0) & (distance <= position_ref[...])


def forward_kernel(first_ref, q_ref, kv_ref, cos_ref, sin_ref, pos_ref, out_ref, norm_ref):
    query = turn(q_ref[...].astype(F32), cos_ref[...], sin_ref[...])
    query = (query * HEAD ** (-0.5)).astype(BF16)
    keys, values = kv_ref[:, :HEAD], kv_ref[:, HEAD:]
    scores = nt(query, keys)
    scores = jnp.where(seen(first_ref, pos_ref, *scores.shape), scores, MASKED)
    top = jnp.max(scores, axis=1, keepdims=True)
    weights = jnp.exp(scores - top)
    total = jnp.sum(weights, axis=1, keepdims=True)
    out_ref[...] = (nn(weights.astype(BF16), values) / total).astype(BF16)
    norm_ref[0] = top + jnp.log(total)


def backward_kernel(
    first_ref, q_ref, kv_ref, cos_ref, sin_ref, pos_ref, att_ref, datt_ref, norm_ref,
    dq_ref, dkv_ref,
):
    head = pl.program_id(0)
    scale = HEAD ** (-0.5)
    cos, sin = cos_ref[...], sin_ref[...]
    query = (turn(q_ref[...].astype(F32), cos, sin) * scale).astype(BF16)
    keys, values = kv_ref[:, :HEAD], kv_ref[:, HEAD:]
    scores = nt(query, keys)
    visible = seen(first_ref, pos_ref, *scores.shape)
    again = jnp.where(visible, jnp.exp(scores - norm_ref[0]), 0.0)
    d_att = datt_ref[...]
    delta = jnp.sum(d_att.astype(F32) * att_ref[...].astype(F32), axis=1, keepdims=True)
    d_scores = (again * (nt(d_att, values) - delta)).astype(BF16)
    d_query = nn(d_scores, keys) * scale
    dq_ref[...] = unturn(d_query, cos, sin).astype(BF16)

    @pl.when(head == 0)
    def _():
        dkv_ref[...] = jnp.zeros_like(dkv_ref)

    dkv_ref[:, :HEAD] += tn(d_scores, query)
    dkv_ref[:, HEAD:] += tn(again.astype(BF16), d_att)


def whole_spec(shape):
    return pl.BlockSpec(shape, lambda head: (0,) * len(shape))


def attention_forward(first, qkv, kv, cos, sin, pos):
    rows, keys = qkv.shape[0], kv.shape[0]
    head_spec = pl.BlockSpec((rows, HEAD), lambda head: (0, head))
    return pl.pallas_call(
        forward_kernel,
        grid=(HEADS,),
        out_shape=(
            jax.ShapeDtypeStruct((rows, HEADS * HEAD), BF16),
            jax.ShapeDtypeStruct((HEADS, rows, 1), F32),
        ),
        in_specs=[
            pl.BlockSpec(memory_space=pltpu.SMEM),
            head_spec,
            whole_spec((keys, 2 * HEAD)),
            whole_spec((rows, HEAD // 2)),
            whole_spec((rows, HEAD // 2)),
            whole_spec((rows, 1)),
        ],
        out_specs=(head_spec, pl.BlockSpec((1, rows, 1), lambda head: (head, 0, 0))),
        compiler_params=in_order(32),
        cost_estimate=cost(4 * rows * keys * HEADS * HEAD, 4 * rows * HEADS * HEAD + 4 * keys * HEAD, rows * keys * HEADS),
        name="attention_forward",
    )(first, qkv, kv, cos, sin, pos)


def attention_backward(first, qkv, kv, cos, sin, pos, att, d_att, norm):
    rows, keys = qkv.shape[0], kv.shape[0]
    head_spec = pl.BlockSpec((rows, HEAD), lambda head: (0, head))
    return pl.pallas_call(
        backward_kernel,
        grid=(HEADS,),
        out_shape=(
            jax.ShapeDtypeStruct((rows, HEADS * HEAD), BF16),
            jax.ShapeDtypeStruct((keys, 2 * HEAD), F32),
        ),
        in_specs=[
            pl.BlockSpec(memory_space=pltpu.SMEM),
            head_spec,
            whole_spec((keys, 2 * HEAD)),
            whole_spec((rows, HEAD // 2)),
            whole_spec((rows, HEAD // 2)),
            whole_spec((rows, 1)),
            head_spec,
            head_spec,
            pl.BlockSpec((1, rows, 1), lambda head: (head, 0, 0)),
        ],
        out_specs=(head_spec, whole_spec((keys, 2 * HEAD))),
        compiler_params=in_order(40),
        cost_estimate=cost(10 * rows * keys * HEADS * HEAD, 8 * rows * HEADS * HEAD + 12 * keys * HEAD, rows * keys * HEADS),
        name="attention_backward",
    )(first, qkv, kv, cos, sin, pos, att, d_att, norm)


def keep_half(core_ref, total, kept, sent):
    half = total.shape[0] // 2
    for core, (first, second) in enumerate(((kept, sent), (sent, kept))):

        @pl.when(core_ref[0] == core)
        def _(first=first, second=second):
            first[...] = total[:half]
            second[...] = total[half:]


def pair_kernel(core_ref, left_ref, right_ref, *refs):
    total = tn(left_ref[...], right_ref[...])
    if len(refs) == 4:
        weight = refs[0][:, : total.shape[1]].astype(F32)
        refs[3][...] = jnp.sum(total * weight, axis=1, keepdims=True)
    keep_half(core_ref, total.astype(BF16), *refs[-3:-1] if len(refs) == 4 else refs)


def split_pairs(total, pairs, core):
    rows, cols = total.shape
    total = total.reshape(pairs, 2, rows // pairs // 2, cols)
    return tuple(
        lax.dynamic_index_in_dim(total, index, 1, False).reshape(-1, cols)
        for index in (core, 1 - core)
    )


def core_index():
    return (lax.axis_index("tok") % 2).astype(jnp.int32).reshape(1)


def pair_grad(left, right, weight=None):
    tokens, rows = left.shape
    cols = right.shape[1]
    pairs = lax.axis_size("tok") // 2
    step = rows // pairs
    if step % 128 or cols % 128:
        total = tn(left, right)
        halves = split_pairs(total.astype(BF16), pairs, lax.axis_index("tok") % 2)
        if weight is None:
            return halves
        return *halves, jnp.sum(total * weight[:, :cols].astype(F32), axis=1, keepdims=True)
    out_shape = [jax.ShapeDtypeStruct((rows // 2, cols), BF16)] * 2
    out_specs = [pl.BlockSpec((step // 2, cols), lambda pair: (pair, 0))] * 2
    in_specs = [
        pl.BlockSpec(memory_space=pltpu.SMEM),
        pl.BlockSpec((tokens, step), lambda pair: (0, pair)),
        pl.BlockSpec((tokens, cols), lambda pair: (0, 0)),
    ]
    operands = [core_index(), left, right]
    if weight is not None:
        operands.append(weight)
        in_specs.append(pl.BlockSpec((step, weight.shape[1]), lambda pair: (pair, 0)))
        out_shape.append(jax.ShapeDtypeStruct((rows, 1), F32))
        out_specs.append(pl.BlockSpec((step, 1), lambda pair: (pair, 0)))
    return pl.pallas_call(
        pair_kernel,
        grid=(pairs,),
        out_shape=out_shape,
        in_specs=in_specs,
        out_specs=out_specs,
        compiler_params=in_order(48),
        cost_estimate=cost(2 * tokens * rows * cols, 2 * (tokens * (rows + cols) + rows * cols)),
    )(*operands)


def pieces_grad_kernel(me_ref, core_ref, own, along_x, along_y, top, bottom, right_ref, kept, sent):
    at = pl.program_id(0)
    half = top.shape[0]
    for index, piece in enumerate((own, along_x, along_y)):

        @pl.when(at == index)
        def _(piece=piece):
            keep_half(core_ref, tn(piece[...], right_ref[...]).astype(BF16), kept, sent)

    @pl.when(at == 3)
    def _():
        total = tn(top[...], right_ref[:half]) + tn(bottom[...], right_ref[half:])
        keep_half(core_ref, total.astype(BF16), kept, sent)


def pieces_grad(pieces, right):
    tokens, step = pieces[0].shape
    cols = right.shape[1]
    me = lax.axis_index("mdl").astype(jnp.int32).reshape(1)
    out = jax.ShapeDtypeStruct((2 * step, cols), BF16)
    return pl.pallas_call(
        pieces_grad_kernel,
        grid_spec=pltpu.PrefetchScalarGridSpec(
            num_scalar_prefetch=2,
            grid=(4,),
            in_specs=[
                pl.BlockSpec(array.shape, lambda at, me_ref, core_ref: (0, 0))
                for array in (*pieces, right)
            ],
            out_specs=[
                pl.BlockSpec((step // 2, cols), lambda at, me_ref, core_ref: (me_ref[0] ^ at, 0))
            ]
            * 2,
        ),
        out_shape=(out, out),
        compiler_params=in_order(48),
        cost_estimate=cost(8 * tokens * step * cols, 2 * (4 * tokens * step + 5 * step * cols)),
    )(me, core_index(), *pieces, right)


def payload_kernel(starts, me_ref, *refs):
    lefts, weight_ref = refs[: len(starts)], refs[len(starts)]
    top_sent, bottom_sent, top_kept, bottom_kept = refs[len(starts) + 1 :]
    total = 0.0
    for left_ref, start in zip(lefts, starts):
        total += nt(left_ref[...], weight_ref[:, start : start + left_ref.shape[1]])
    total = total.astype(BF16)
    half = total.shape[0] // 2
    places = (
        ((top_kept, 0), (bottom_kept, 0)),
        ((top_sent, 0), (bottom_kept, 1)),
        ((top_kept, 1), (bottom_sent, 0)),
        ((top_sent, 1), (bottom_sent, 1)),
    )
    for distance, ((top, top_at), (bottom, bottom_at)) in enumerate(places):

        @pl.when(pl.program_id(0) == 3 - distance)
        def _(top=top, top_at=top_at, bottom=bottom, bottom_at=bottom_at):
            top[top_at] = total[:half]
            bottom[bottom_at] = total[half:]


def scatter_product(lefts, weight, starts):
    tokens = lefts[0].shape[0]
    rows, cols = weight.shape
    step = rows // 4
    me = lax.axis_index("mdl").astype(jnp.int32).reshape(1)
    out = jax.ShapeDtypeStruct((2, tokens // 2, step), BF16)
    depth = sum(left.shape[1] for left in lefts)
    return pl.pallas_call(
        functools.partial(payload_kernel, starts),
        grid_spec=pltpu.PrefetchScalarGridSpec(
            num_scalar_prefetch=1,
            grid=(4,),
            in_specs=[pl.BlockSpec(left.shape, lambda at, me_ref: (0, 0)) for left in lefts]
            + [pl.BlockSpec((step, cols), lambda at, me_ref: (me_ref[0] ^ (3 - at), 0))],
            out_specs=[pl.BlockSpec(out.shape, lambda at, me_ref: (0, 0, 0))] * 4,
        ),
        out_shape=(out,) * 4,
        compiler_params=in_order(48),
        cost_estimate=cost(2 * tokens * rows * depth, 2 * (tokens * depth + rows * cols + tokens * rows)),
    )(me, *lefts, weight)


def pieces_kernel(start, me_ref, own, along_x, along_y, top, bottom, weight_ref, out_ref, total):
    at = pl.program_id(0)
    width = out_ref.shape[1]
    half = top.shape[0]
    for index, piece in enumerate((own, along_x, along_y)):

        @pl.when(at == index)
        def _(index=index, piece=piece):
            part = nn(piece[...], weight_ref[:, start : start + width])
            if index:
                total[...] += part
            else:
                total[...] = part

    @pl.when(at == 3)
    def _():
        weight = weight_ref[:, start : start + width]
        out_ref[:half] = (total[:half] + nn(top[...], weight)).astype(BF16)
        out_ref[half:] = (total[half:] + nn(bottom[...], weight)).astype(BF16)


def pieces_product(pieces, weight, start, width):
    tokens, step = pieces[0].shape
    rows, cols = weight.shape
    me = lax.axis_index("mdl").astype(jnp.int32).reshape(1)
    return pl.pallas_call(
        functools.partial(pieces_kernel, start),
        grid_spec=pltpu.PrefetchScalarGridSpec(
            num_scalar_prefetch=1,
            grid=(4,),
            in_specs=[pl.BlockSpec(piece.shape, lambda at, me_ref: (0, 0)) for piece in pieces]
            + [pl.BlockSpec((step, cols), lambda at, me_ref: (me_ref[0] ^ at, 0))],
            out_specs=pl.BlockSpec((tokens, width), lambda at, me_ref: (0, 0)),
            scratch_shapes=[pltpu.VMEM((tokens, width), F32)],
        ),
        out_shape=jax.ShapeDtypeStruct((tokens, width), BF16),
        compiler_params=in_order(40),
        cost_estimate=cost(2 * tokens * rows * width, 2 * (tokens * rows + rows * cols + tokens * width)),
    )(me, *pieces, weight)


def product_to_mdl(lefts, weight, starts):
    if lax.axis_size("mdl") == 4:
        payload = scatter_product(lefts, weight, starts)
        return payload, lambda payload: scatter_payload(payload)
    part = sum(
        nt(left, weight[:, start : start + left.shape[1]]) for left, start in zip(lefts, starts)
    )
    return (part.astype(BF16),), lambda payload: scatter_mdl(payload[0], 1)


def after(value, *earlier):
    return lax.optimization_barrier((value, *earlier))[0]


def row_scale(rows_b, axis=-1):
    rows = rows_b.astype(F32)
    return lax.rsqrt(jnp.mean(rows * rows, axis=axis, keepdims=True) + NORM_EPS)


def gelu_parts(value):
    root = math.sqrt(2.0 / math.pi)
    square = value * value
    tanh = jnp.tanh(root * (value + 0.044715 * value * square))
    cdf = 0.5 * (1.0 + tanh)
    slope = cdf + 0.5 * value * (1.0 - tanh * tanh) * root * (1.0 + 3 * 0.044715 * square)
    return value * cdf, slope


def scaled(weight, gain):
    return (weight.astype(F32) * gain.astype(F32)[:, None]).astype(BF16)


def on_device(
    inputs, positions, norm1_gain, qkv_weight, out_weight, norm2_gain, gate_weight,
    up_weight, down_weight, cotangent,
):
    me = lax.axis_index("mdl")
    size = lax.axis_size("mdl")
    head_cols = HEADS * HEAD
    width = inputs.shape[1]
    features = width * size

    def from_tok(weight, dim):
        return lax.all_gather(weight, "tok", axis=dim, tiled=True)

    def pair_to_tok(local):
        kept, sent = local
        count = lax.axis_size("tok")
        got = lax.ppermute(sent, "tok", [(i, i ^ 1) for i in range(count)])
        both = (kept.astype(F32) + got.astype(F32)).astype(BF16)
        groups = [list(range(core, count, 2)) for core in range(2)]
        total = lax.psum_scatter(
            both, "tok", scatter_dimension=0, tiled=True, axis_index_groups=groups
        )
        return total.astype(F32)

    qkv_cols, ff_cols = qkv_weight.shape[1], gate_weight.shape[1]
    attn_local = jnp.concatenate([scaled(qkv_weight, norm1_gain), out_weight.T], axis=1)
    w_attn = from_tok(attn_local, 0)
    w_qkv = w_attn[:, :qkv_cols]
    gu_local = jnp.concatenate([scaled(w, norm2_gain) for w in (gate_weight, up_weight)], 1)
    w_gu = from_tok(gu_local, 0)
    w_down_t = from_tok(down_weight.T, 0)

    rows_in = gather_mdl(inputs, 1)
    scale_one = row_scale(rows_in)
    qkv_part = (nn(rows_in, w_qkv) * scale_one).astype(BF16)
    qkv = rows_to_cols(qkv_part)
    count = qkv.shape[0]
    half = HEAD // 2
    frequency = jnp.exp(jnp.arange(half, dtype=F32) * (-2.0 * math.log(10000.0) / HEAD))
    angles = positions.astype(F32)[:, None] * frequency[None, :]
    cos, sin = jnp.cos(angles), jnp.sin(angles)
    key_rows = turn(qkv[:, head_cols : head_cols + HEAD].astype(F32), cos, sin).astype(BF16)
    kv = gather_mdl(jnp.concatenate([key_rows, qkv[:, head_cols + HEAD :]], axis=1), 0)
    first = (me * count).astype(jnp.int32).reshape(1)
    pos = positions[:, None]
    attended, log_norm = attention_forward(first, qkv, kv, cos, sin, pos)
    head_block = cols_to_rows(attended)
    residual = inputs.astype(F32)
    payload, scatter = product_to_mdl((head_block,), w_attn, (qkv_cols,))
    mixed = residual + scatter(payload)

    rows_two = gather_mdl(mixed.astype(BF16), 1)
    scale_two = row_scale(rows_two)
    rows_hat = (rows_two.astype(F32) * scale_two).astype(BF16)
    gate_in = nn(rows_hat, w_gu[:, :ff_cols])
    up_in = nn(rows_hat, w_gu[:, ff_cols:])
    gelu, _ = gelu_parts(gate_in)
    hidden = (gelu * up_in).astype(BF16)
    gate_in, up_in, hidden = lax.optimization_barrier((gate_in, up_in, hidden))
    gelu, slope = gelu_parts(gate_in)

    down_local = pair_grad(cotangent, hidden)
    down_grad = pair_to_tok(down_local)
    d_hidden = nn(cotangent, w_down_t)
    d_gate_f = d_hidden * up_in * slope
    d_up_f = d_hidden * gelu
    stat_two = jnp.sum(d_gate_f * gate_in + d_up_f * up_in, axis=1)
    d_gate, d_up = d_gate_f.astype(BF16), d_up_f.astype(BF16)
    gate_local = pair_grad(rows_hat, d_gate)
    gate_sum = pair_to_tok(gate_local)
    payload, scatter = product_to_mdl((d_gate, d_up), w_gu, (0, ff_cols))
    rows_later = after(rows_hat, payload[0])
    up_local = pair_grad(rows_later, d_up)
    up_sum = pair_to_tok(up_local)
    d_two = scatter(payload)
    stat_two = sum_mdl(stat_two.reshape(8, -1)).reshape(-1, 1) * (1.0 / features)
    scale_mixed = scale_two * mixed
    cotangent_own = lax.dynamic_slice_in_dim(cotangent, me * width, width, 1).astype(F32)
    d_mixed = cotangent_own + scale_two * (d_two - scale_mixed * stat_two)

    d_mixed_b = after(d_mixed.astype(BF16), up_local[0])
    hidden_later = after(hidden, d_mixed_b)
    ffn_payload, ffn_scatter = product_to_mdl((hidden_later,), w_down_t, (0,))
    if size == 4 and lax.axis_size("tok") == 8:
        pieces = gather_pieces(d_mixed_b)
        d_head = pieces_product(pieces, w_attn, qkv_cols, head_block.shape[1])
        heads_later = after(head_block, d_head)
        out_local = pieces_grad(pieces, heads_later)
    else:
        d_mixed_rows = gather_mdl(d_mixed_b, 1)
        d_head = nn(d_mixed_rows, w_attn[:, qkv_cols:]).astype(BF16)
        out_local = pair_grad(d_mixed_rows, head_block)
    out_grad = pair_to_tok(out_local)
    d_attended = rows_to_cols(d_head)
    block_out = (mixed + ffn_scatter(ffn_payload)).astype(BF16)
    d_query, d_kv = attention_backward(
        first, qkv, kv, cos, sin, pos, attended, d_attended, log_norm
    )
    d_kv = scatter_mdl(d_kv.astype(BF16), 0)
    d_key = unturn(d_kv[:, :HEAD], cos, sin).astype(BF16)
    d_qkv = jnp.concatenate([d_query, d_key, d_kv[:, HEAD:].astype(BF16)], axis=1)
    stat_one = jnp.sum(d_qkv.astype(F32) * qkv.astype(F32), axis=1)
    d_qkv_part = cols_to_rows(d_qkv)
    stat_rows = jnp.zeros((size, count), F32)
    stat_rows = sum_mdl(lax.dynamic_update_slice(stat_rows, stat_one[None], (me, 0)))
    stat_one = stat_rows.reshape(-1, 1) * (1.0 / features)
    payload, scatter = product_to_mdl((d_qkv_part,), w_attn, (0,))
    d_scaled = (after(d_qkv_part, payload[0]).astype(F32) * scale_one).astype(BF16)
    *qkv_local, gain_one = pair_grad(rows_in, d_scaled, w_attn)
    qkv_sum = pair_to_tok(qkv_local)
    d_one = scatter(payload)
    input_grad = d_mixed + scale_one * (d_one - (scale_one * residual) * stat_one)

    norm1_late, norm2_late, gate_late, up_late, _ = lax.optimization_barrier(
        (norm1_gain, norm2_gain, gate_weight, up_weight, up_local[0])
    )

    def unfold(total, gain):
        return total * gain.astype(F32)[:, None]

    gain_two = jnp.sum(
        gate_late.astype(F32) * gate_sum + up_late.astype(F32) * up_sum, axis=1
    )
    gate_grad, up_grad = unfold(gate_sum, norm2_late), unfold(up_sum, norm2_late)
    down_grad = down_grad.T
    out_grad = out_grad.T
    gain_two_grad = sum_mdl(gain_two)
    gain_one = sum_mdl(sum_tok(gain_one.reshape(8, -1))).reshape(-1)
    shard = norm1_gain.shape[0]
    gain_one = lax.dynamic_slice_in_dim(gain_one, lax.axis_index("tok") * shard, shard, 0)
    gain_one_grad = gain_one / norm1_late.astype(F32)
    return (
        block_out,
        input_grad,
        gain_one_grad,
        unfold(qkv_sum, norm1_late),
        out_grad,
        gain_two_grad,
        gate_grad,
        up_grad,
        down_grad,
    )


def solution(mesh):
    return jax.shard_map(
        on_device,
        mesh=mesh,
        in_specs=(
            P("tok", "mdl"),
            P(("tok", "mdl")),
            P("tok"),
            P("tok", "mdl"),
            P("mdl", "tok"),
            P("tok"),
            P("tok", "mdl"),
            P("tok", "mdl"),
            P("mdl", "tok"),
            P("tok", None),
        ),
        out_specs=(
            P("tok", "mdl"),
            P("tok", "mdl"),
            P("tok"),
            P("tok", "mdl"),
            P("mdl", "tok"),
            P("tok"),
            P("tok", "mdl"),
            P("tok", "mdl"),
            P("mdl", "tok"),
        ),
        check_vma=False,
    )
```

```python
import functools
import math

import jax
import jax.numpy as jnp
from jax import lax
from jax.experimental import pallas as pl
from jax.experimental.pallas import tpu as pltpu
from jax.sharding import PartitionSpec as P


HEADS = 10
HEAD = 256
NORM_EPS = 1e-06
F32 = jnp.float32
BF16 = jnp.bfloat16
MASKED = -1e30


def nt(left_op, right_op):
    return lax.dot_general(
        left_op, right_op, (((1,), (1,)), ((), ())), preferred_element_type=F32
    )


def tn(left_op, right_op):
    return lax.dot_general(
        left_op, right_op, (((0,), (0,)), ((), ())), preferred_element_type=F32
    )


def nn(left_op, right_op):
    return jnp.dot(left_op, right_op, preferred_element_type=F32)


def swap(block, distance):
    size = lax.axis_size("mdl")
    return lax.ppermute(block, "mdl", [(i, i ^ distance) for i in range(size)])


def gather_mdl(block, dim):
    size = lax.axis_size("mdl")
    if size != 4:
        return lax.all_gather(block, "mdl", axis=dim, tiled=True)
    me = lax.axis_index("mdl")
    half = block.shape[0] // 2
    along_x = swap(block, 1)
    along_y = swap(block, 2)
    top = swap(along_x[:half], 2)
    bottom = swap(along_y[half:], 1)
    width = block.shape[dim]
    shape = list(block.shape)
    shape[dim] = width * size
    whole = jnp.zeros(shape, block.dtype)

    def put(whole, piece, source, row):
        start = [0, 0]
        start[dim] = source * width
        start[0] = start[0] + row
        return lax.dynamic_update_slice(whole, piece, tuple(start))

    whole = put(whole, block, me, 0)
    whole = put(whole, along_x, me ^ 1, 0)
    whole = put(whole, along_y, me ^ 2, 0)
    whole = put(whole, top, me ^ 3, 0)
    whole = put(whole, bottom, me ^ 3, half)
    return whole


def scatter_mdl(part, dim):
    size = lax.axis_size("mdl")
    if size != 4:
        return lax.psum_scatter(part, "mdl", scatter_dimension=dim, tiled=True).astype(F32)
    me = lax.axis_index("mdl")
    shape = list(part.shape)
    shape[dim] //= size
    half = shape[0] // 2

    def piece(block, row):
        start = [0, 0]
        start[dim] = block * shape[dim]
        start[0] = start[0] + row
        return lax.dynamic_slice(part, tuple(start), (half, shape[1]))

    sums = []
    for row, first, second in ((0, 1, 2), (half, 2, 1)):
        sent = jnp.stack([piece(me ^ first, row), piece(me ^ 3, row)])
        sums.append((row, second, swap(sent, first)))
    partial = []
    for row, second, got in sums:
        other = piece(me ^ second, row).astype(F32) + got[1].astype(F32)
        partial.append((row, got[0], swap(other.astype(BF16), second)))
    return jnp.concatenate(
        [
            piece(me, row).astype(F32) + first.astype(F32) + second.astype(F32)
            for row, first, second in partial
        ],
        axis=0,
    )


def gather_pieces(block):
    half = block.shape[0] // 2
    along_x = swap(block, 1)
    along_y = swap(block, 2)
    top = swap(along_x[:half], 2)
    bottom = swap(along_y[half:], 1)
    return block, along_x, along_y, top, bottom


def scatter_payload(payload):
    top_sent, bottom_sent, top_kept, bottom_kept = payload
    got_top = swap(top_sent, 1)
    got_bottom = swap(bottom_sent, 2)
    halves = []
    for kept, got, second in ((top_kept, got_top, 2), (bottom_kept, got_bottom, 1)):
        passed = (kept[1].astype(F32) + got[1].astype(F32)).astype(BF16)
        last = swap(passed, second)
        halves.append(kept[0].astype(F32) + got[0].astype(F32) + last.astype(F32))
    return jnp.concatenate(halves, axis=0)


def sum_mdl(value):
    size = lax.axis_size("mdl")
    distance = 1
    while distance < size:
        value = value + swap(value, distance)
        distance *= 2
    return value


def sum_tok(value):
    size = lax.axis_size("tok")
    distance = 1
    while distance < size:
        value = value + lax.ppermute(value, "tok", [(i, i ^ distance) for i in range(size)])
        distance *= 2
    return value


def rows_to_cols(block):
    return lax.all_to_all(block, "mdl", split_axis=0, concat_axis=1, tiled=True)


def cols_to_rows(block):
    return lax.all_to_all(block, "mdl", split_axis=1, concat_axis=0, tiled=True)


def in_order(mebibytes):
    return pltpu.CompilerParams(
        dimension_semantics=(pltpu.ARBITRARY,), vmem_limit_bytes=mebibytes << 20
    )


def cost(flops, bytes_accessed, transcendentals=0):
    return pl.CostEstimate(
        flops=flops, bytes_accessed=bytes_accessed, transcendentals=transcendentals
    )


def turn(vector, cos, sin):
    half = HEAD // 2
    lower, upper = vector[:, :half], vector[:, half:]
    return jnp.concatenate([lower * cos - upper * sin, upper * cos + lower * sin], axis=1)


def unturn(vector, cos, sin):
    half = HEAD // 2
    lower, upper = vector[:, :half], vector[:, half:]
    return jnp.concatenate([lower * cos + upper * sin, upper * cos - lower * sin], axis=1)


def seen(first_ref, position_ref, queries, keys):
    row = lax.broadcasted_iota(jnp.int32, (queries, keys), 0) + first_ref[0]
    distance = row - lax.broadcasted_iota(jnp.int32, (queries, keys), 1)
    return (distance >= 0) & (distance <= position_ref[...])


def forward_kernel(first_ref, q_ref, kv_ref, cos_ref, sin_ref, pos_ref, out_ref, norm_ref):
    query = turn(q_ref[...].astype(F32), cos_ref[...], sin_ref[...])
    query = (query * HEAD ** (-0.5)).astype(BF16)
    keys, values = kv_ref[:, :HEAD], kv_ref[:, HEAD:]
    scores = nt(query, keys)
    scores = jnp.where(seen(first_ref, pos_ref, *scores.shape), scores, MASKED)
    top = jnp.max(scores, axis=1, keepdims=True)
    weights = jnp.exp(scores - top)
    total = jnp.sum(weights, axis=1, keepdims=True)
    out_ref[...] = (nn(weights.astype(BF16), values) / total).astype(BF16)
    norm_ref[0] = top + jnp.log(total)


def backward_kernel(
    first_ref, q_ref, kv_ref, cos_ref, sin_ref, pos_ref, att_ref, datt_ref, norm_ref,
    dq_ref, dkv_ref,
):
    head = pl.program_id(0)
    scale = HEAD ** (-0.5)
    cos, sin = cos_ref[...], sin_ref[...]
    query = (turn(q_ref[...].astype(F32), cos, sin) * scale).astype(BF16)
    keys, values = kv_ref[:, :HEAD], kv_ref[:, HEAD:]
    scores = nt(query, keys)
    visible = seen(first_ref, pos_ref, *scores.shape)
    again = jnp.where(visible, jnp.exp(scores - norm_ref[0]), 0.0)
    d_att = datt_ref[...]
    delta = jnp.sum(d_att.astype(F32) * att_ref[...].astype(F32), axis=1, keepdims=True)
    d_scores = (again * (nt(d_att, values) - delta)).astype(BF16)
    d_query = nn(d_scores, keys) * scale
    dq_ref[...] = unturn(d_query, cos, sin).astype(BF16)

    @pl.when(head == 0)
    def _():
        dkv_ref[...] = jnp.zeros_like(dkv_ref)

    dkv_ref[:, :HEAD] += tn(d_scores, query)
    dkv_ref[:, HEAD:] += tn(again.astype(BF16), d_att)


def whole_spec(shape):
    return pl.BlockSpec(shape, lambda head: (0,) * len(shape))


def attention_forward(first, qkv, kv, cos, sin, pos):
    rows, keys = qkv.shape[0], kv.shape[0]
    head_spec = pl.BlockSpec((rows, HEAD), lambda head: (0, head))
    return pl.pallas_call(
        forward_kernel,
        grid=(HEADS,),
        out_shape=(
            jax.ShapeDtypeStruct((rows, HEADS * HEAD), BF16),
            jax.ShapeDtypeStruct((HEADS, rows, 1), F32),
        ),
        in_specs=[
            pl.BlockSpec(memory_space=pltpu.SMEM),
            head_spec,
            whole_spec((keys, 2 * HEAD)),
            whole_spec((rows, HEAD // 2)),
            whole_spec((rows, HEAD // 2)),
            whole_spec((rows, 1)),
        ],
        out_specs=(head_spec, pl.BlockSpec((1, rows, 1), lambda head: (head, 0, 0))),
        compiler_params=in_order(32),
        cost_estimate=cost(4 * rows * keys * HEADS * HEAD, 4 * rows * HEADS * HEAD + 4 * keys * HEAD, rows * keys * HEADS),
        name="attention_forward",
    )(first, qkv, kv, cos, sin, pos)


def attention_backward(first, qkv, kv, cos, sin, pos, att, d_att, norm):
    rows, keys = qkv.shape[0], kv.shape[0]
    head_spec = pl.BlockSpec((rows, HEAD), lambda head: (0, head))
    return pl.pallas_call(
        backward_kernel,
        grid=(HEADS,),
        out_shape=(
            jax.ShapeDtypeStruct((rows, HEADS * HEAD), BF16),
            jax.ShapeDtypeStruct((keys, 2 * HEAD), F32),
        ),
        in_specs=[
            pl.BlockSpec(memory_space=pltpu.SMEM),
            head_spec,
            whole_spec((keys, 2 * HEAD)),
            whole_spec((rows, HEAD // 2)),
            whole_spec((rows, HEAD // 2)),
            whole_spec((rows, 1)),
            head_spec,
            head_spec,
            pl.BlockSpec((1, rows, 1), lambda head: (head, 0, 0)),
        ],
        out_specs=(head_spec, whole_spec((keys, 2 * HEAD))),
        compiler_params=in_order(40),
        cost_estimate=cost(10 * rows * keys * HEADS * HEAD, 8 * rows * HEADS * HEAD + 12 * keys * HEAD, rows * keys * HEADS),
        name="attention_backward",
    )(first, qkv, kv, cos, sin, pos, att, d_att, norm)


def keep_half(core_ref, total, kept, sent):
    half = total.shape[0] // 2
    for core, (first, second) in enumerate(((kept, sent), (sent, kept))):

        @pl.when(core_ref[0] == core)
        def _(first=first, second=second):
            first[...] = total[:half]
            second[...] = total[half:]


def pair_kernel(core_ref, left_ref, right_ref, *refs):
    total = tn(left_ref[...], right_ref[...])
    if len(refs) == 4:
        weight = refs[0][:, : total.shape[1]].astype(F32)
        refs[3][...] = jnp.sum(total * weight, axis=1, keepdims=True)
    keep_half(core_ref, total.astype(BF16), *refs[-3:-1] if len(refs) == 4 else refs)


def split_pairs(total, pairs, core):
    rows, cols = total.shape
    total = total.reshape(pairs, 2, rows // pairs // 2, cols)
    return tuple(
        lax.dynamic_index_in_dim(total, index, 1, False).reshape(-1, cols)
        for index in (core, 1 - core)
    )


def core_index():
    return (lax.axis_index("tok") % 2).astype(jnp.int32).reshape(1)


def pair_grad(left, right, weight=None):
    tokens, rows = left.shape
    cols = right.shape[1]
    pairs = lax.axis_size("tok") // 2
    step = rows // pairs
    if step % 128 or cols % 128:
        total = tn(left, right)
        halves = split_pairs(total.astype(BF16), pairs, lax.axis_index("tok") % 2)
        if weight is None:
            return halves
        return *halves, jnp.sum(total * weight[:, :cols].astype(F32), axis=1, keepdims=True)
    out_shape = [jax.ShapeDtypeStruct((rows // 2, cols), BF16)] * 2
    out_specs = [pl.BlockSpec((step // 2, cols), lambda pair: (pair, 0))] * 2
    in_specs = [
        pl.BlockSpec(memory_space=pltpu.SMEM),
        pl.BlockSpec((tokens, step), lambda pair: (0, pair)),
        pl.BlockSpec((tokens, cols), lambda pair: (0, 0)),
    ]
    operands = [core_index(), left, right]
    if weight is not None:
        operands.append(weight)
        in_specs.append(pl.BlockSpec((step, weight.shape[1]), lambda pair: (pair, 0)))
        out_shape.append(jax.ShapeDtypeStruct((rows, 1), F32))
        out_specs.append(pl.BlockSpec((step, 1), lambda pair: (pair, 0)))
    return pl.pallas_call(
        pair_kernel,
        grid=(pairs,),
        out_shape=out_shape,
        in_specs=in_specs,
        out_specs=out_specs,
        compiler_params=in_order(48),
        cost_estimate=cost(2 * tokens * rows * cols, 2 * (tokens * (rows + cols) + rows * cols)),
    )(*operands)


def part_kernel(core_ref, rows_ref, above_ref, d_gate_ref, d_up_ref, hidden_ref, kept, sent):
    cols = hidden_ref.shape[1]
    for at, (left_ref, right_ref) in enumerate(
        ((rows_ref, d_gate_ref), (rows_ref, d_up_ref), (above_ref, hidden_ref))
    ):
        total = tn(left_ref[...], right_ref[...]).astype(BF16)
        window = (slice(None), pl.ds(at * cols, cols))
        keep_half(core_ref, total, kept.at[window], sent.at[window])


def part_grad(rows, above, d_gate, d_up, hidden):
    tokens, features = rows.shape
    cols = hidden.shape[1]
    pairs = lax.axis_size("tok") // 2
    step = features // pairs
    if step % 128 or cols % 128:
        total = [tn(rows, d_gate), tn(rows, d_up), tn(above, hidden)]
        total = jnp.concatenate(total, axis=1).astype(BF16)
        return split_pairs(total, pairs, lax.axis_index("tok") % 2)
    out = jax.ShapeDtypeStruct((features // 2, 3 * cols), BF16)
    left_spec = pl.BlockSpec((tokens, step), lambda pair: (0, pair))
    right_spec = pl.BlockSpec((tokens, cols), lambda pair: (0, 0))
    return pl.pallas_call(
        part_kernel,
        grid=(pairs,),
        out_shape=(out, out),
        in_specs=[pl.BlockSpec(memory_space=pltpu.SMEM)] + [left_spec] * 2 + [right_spec] * 3,
        out_specs=[pl.BlockSpec((step // 2, 3 * cols), lambda pair: (pair, 0))] * 2,
        compiler_params=in_order(48),
        cost_estimate=cost(
            6 * tokens * features * cols,
            2 * (2 * tokens * features + 3 * cols * (tokens + features)),
        ),
    )(core_index(), rows, above, d_gate, d_up, hidden)


def pieces_grad_kernel(me_ref, core_ref, own, along_x, along_y, top, bottom, right_ref, kept, sent):
    at = pl.program_id(0)
    half = top.shape[0]
    for index, piece in enumerate((own, along_x, along_y)):

        @pl.when(at == index)
        def _(piece=piece):
            keep_half(core_ref, tn(piece[...], right_ref[...]).astype(BF16), kept, sent)

    @pl.when(at == 3)
    def _():
        total = tn(top[...], right_ref[:half]) + tn(bottom[...], right_ref[half:])
        keep_half(core_ref, total.astype(BF16), kept, sent)


def pieces_grad(pieces, right):
    tokens, step = pieces[0].shape
    cols = right.shape[1]
    me = lax.axis_index("mdl").astype(jnp.int32).reshape(1)
    out = jax.ShapeDtypeStruct((2 * step, cols), BF16)
    return pl.pallas_call(
        pieces_grad_kernel,
        grid_spec=pltpu.PrefetchScalarGridSpec(
            num_scalar_prefetch=2,
            grid=(4,),
            in_specs=[
                pl.BlockSpec(array.shape, lambda at, me_ref, core_ref: (0, 0))
                for array in (*pieces, right)
            ],
            out_specs=[
                pl.BlockSpec((step // 2, cols), lambda at, me_ref, core_ref: (me_ref[0] ^ at, 0))
            ]
            * 2,
        ),
        out_shape=(out, out),
        compiler_params=in_order(48),
        cost_estimate=cost(8 * tokens * step * cols, 2 * (4 * tokens * step + 5 * step * cols)),
    )(me, core_index(), *pieces, right)


def sum_kernel(starts, *refs):
    *lefts, weight_ref, out_ref = refs
    total = 0.0
    for left_ref, start in zip(lefts, starts):
        total += nt(left_ref[...], weight_ref[:, start : start + left_ref.shape[1]])
    out_ref[...] = total


def sum_products(lefts, weight, starts):
    tokens = lefts[0].shape[0]
    rows, cols = weight.shape
    if lefts[0].shape[1] % 128:
        return sum(
            nt(left, weight[:, start : start + left.shape[1]])
            for left, start in zip(lefts, starts)
        )
    step = 512
    depth = sum(left.shape[1] for left in lefts)
    return pl.pallas_call(
        functools.partial(sum_kernel, starts),
        grid=(rows // step,),
        out_shape=jax.ShapeDtypeStruct((tokens, rows), F32),
        in_specs=[pl.BlockSpec(left.shape, lambda row: (0, 0)) for left in lefts]
        + [pl.BlockSpec((step, cols), lambda row: (row, 0))],
        out_specs=pl.BlockSpec((tokens, step), lambda row: (0, row)),
        compiler_params=in_order(48),
        cost_estimate=cost(2 * tokens * rows * depth, 2 * rows * cols + 4 * tokens * rows),
    )(*lefts, weight)


def payload_kernel(starts, me_ref, *refs):
    lefts, weight_ref = refs[: len(starts)], refs[len(starts)]
    top_sent, bottom_sent, top_kept, bottom_kept = refs[-4:]
    total = refs[-5][...] if len(refs) == len(starts) + 6 else 0.0
    for left_ref, start in zip(lefts, starts):
        total += nt(left_ref[...], weight_ref[:, start : start + left_ref.shape[1]])
    total = total.astype(BF16)
    half = total.shape[0] // 2
    places = (
        ((top_kept, 0), (bottom_kept, 0)),
        ((top_sent, 0), (bottom_kept, 1)),
        ((top_kept, 1), (bottom_sent, 0)),
        ((top_sent, 1), (bottom_sent, 1)),
    )
    for distance, ((top, top_at), (bottom, bottom_at)) in enumerate(places):

        @pl.when(pl.program_id(0) == 3 - distance)
        def _(top=top, top_at=top_at, bottom=bottom, bottom_at=bottom_at):
            top[top_at] = total[:half]
            bottom[bottom_at] = total[half:]


def scatter_product(lefts, weight, starts, partial=()):
    tokens = lefts[0].shape[0]
    rows, cols = weight.shape
    step = rows // 4
    me = lax.axis_index("mdl").astype(jnp.int32).reshape(1)
    out = jax.ShapeDtypeStruct((2, tokens // 2, step), BF16)
    depth = sum(left.shape[1] for left in lefts)
    return pl.pallas_call(
        functools.partial(payload_kernel, starts),
        grid_spec=pltpu.PrefetchScalarGridSpec(
            num_scalar_prefetch=1,
            grid=(4,),
            in_specs=[pl.BlockSpec(left.shape, lambda at, me_ref: (0, 0)) for left in lefts]
            + [pl.BlockSpec((step, cols), lambda at, me_ref: (me_ref[0] ^ (3 - at), 0))]
            + [pl.BlockSpec((tokens, step), lambda at, me_ref: (0, me_ref[0] ^ (3 - at)))]
            * len(partial),
            out_specs=[pl.BlockSpec(out.shape, lambda at, me_ref: (0, 0, 0))] * 4,
        ),
        out_shape=(out,) * 4,
        compiler_params=in_order(48),
        cost_estimate=cost(2 * tokens * rows * depth, 2 * (tokens * depth + rows * cols + tokens * rows)),
    )(me, *lefts, weight, *partial)


def pieces_kernel(start, me_ref, own, along_x, along_y, top, bottom, weight_ref, out_ref, total):
    at = pl.program_id(0)
    width = out_ref.shape[1]
    half = top.shape[0]
    for index, piece in enumerate((own, along_x, along_y)):

        @pl.when(at == index)
        def _(index=index, piece=piece):
            part = nn(piece[...], weight_ref[:, start : start + width])
            if index:
                total[...] += part
            else:
                total[...] = part

    @pl.when(at == 3)
    def _():
        weight = weight_ref[:, start : start + width]
        out_ref[:half] = (total[:half] + nn(top[...], weight)).astype(BF16)
        out_ref[half:] = (total[half:] + nn(bottom[...], weight)).astype(BF16)


def pieces_product(pieces, weight, start, width):
    tokens, step = pieces[0].shape
    rows, cols = weight.shape
    me = lax.axis_index("mdl").astype(jnp.int32).reshape(1)
    return pl.pallas_call(
        functools.partial(pieces_kernel, start),
        grid_spec=pltpu.PrefetchScalarGridSpec(
            num_scalar_prefetch=1,
            grid=(4,),
            in_specs=[pl.BlockSpec(piece.shape, lambda at, me_ref: (0, 0)) for piece in pieces]
            + [pl.BlockSpec((step, cols), lambda at, me_ref: (me_ref[0] ^ at, 0))],
            out_specs=pl.BlockSpec((tokens, width), lambda at, me_ref: (0, 0)),
            scratch_shapes=[pltpu.VMEM((tokens, width), F32)],
        ),
        out_shape=jax.ShapeDtypeStruct((tokens, width), BF16),
        compiler_params=in_order(40),
        cost_estimate=cost(2 * tokens * rows * width, 2 * (tokens * rows + rows * cols + tokens * width)),
    )(me, *pieces, weight)


def product_to_mdl(lefts, weight, starts, partial=()):
    if lax.axis_size("mdl") == 4:
        payload = scatter_product(lefts, weight, starts, partial)
        return payload, lambda payload: scatter_payload(payload)
    part = sum((sum_products(lefts, weight, starts), *partial))
    return (part.astype(BF16),), lambda payload: scatter_mdl(payload[0], 1)


def after(value, *earlier):
    return lax.optimization_barrier((value, *earlier))[0]


def row_scale(rows_b, axis=-1):
    rows = rows_b.astype(F32)
    return lax.rsqrt(jnp.mean(rows * rows, axis=axis, keepdims=True) + NORM_EPS)


def gelu_parts(value):
    root = math.sqrt(2.0 / math.pi)
    square = value * value
    tanh = jnp.tanh(root * (value + 0.044715 * value * square))
    cdf = 0.5 * (1.0 + tanh)
    slope = cdf + 0.5 * value * (1.0 - tanh * tanh) * root * (1.0 + 3 * 0.044715 * square)
    return value * cdf, slope


def scaled(weight, gain):
    return (weight.astype(F32) * gain.astype(F32)[:, None]).astype(BF16)


def on_device(
    inputs, positions, norm1_gain, qkv_weight, out_weight, norm2_gain, gate_weight,
    up_weight, down_weight, cotangent,
):
    me = lax.axis_index("mdl")
    size = lax.axis_size("mdl")
    head_cols = HEADS * HEAD
    width = inputs.shape[1]
    features = width * size

    def from_tok(weight, dim):
        return lax.all_gather(weight, "tok", axis=dim, tiled=True)

    def pair_to_tok(local):
        kept, sent = local
        count = lax.axis_size("tok")
        got = lax.ppermute(sent, "tok", [(i, i ^ 1) for i in range(count)])
        both = (kept.astype(F32) + got.astype(F32)).astype(BF16)
        groups = [list(range(core, count, 2)) for core in range(2)]
        total = lax.psum_scatter(
            both, "tok", scatter_dimension=0, tiled=True, axis_index_groups=groups
        )
        return total.astype(F32)

    qkv_cols, ff_cols = qkv_weight.shape[1], gate_weight.shape[1]
    attn_local = jnp.concatenate([scaled(qkv_weight, norm1_gain), out_weight.T], axis=1)
    w_attn = from_tok(attn_local, 0)
    w_qkv = w_attn[:, :qkv_cols]
    middle = -(-ff_cols // 256) * 128
    parts = ((0, middle), (middle, ff_cols))
    w_parts = []
    for start, stop in parts:
        local = [scaled(w[:, start:stop], norm2_gain) for w in (gate_weight, up_weight)]
        local = jnp.concatenate([*local, down_weight[start:stop].T], axis=1)
        w_parts.append(from_tok(local, 0))

    rows_in = gather_mdl(inputs, 1)
    scale_one = row_scale(rows_in)
    qkv_part = (nn(rows_in, w_qkv) * scale_one).astype(BF16)
    qkv = rows_to_cols(qkv_part)
    count = qkv.shape[0]
    half = HEAD // 2
    frequency = jnp.exp(jnp.arange(half, dtype=F32) * (-2.0 * math.log(10000.0) / HEAD))
    angles = positions.astype(F32)[:, None] * frequency[None, :]
    cos, sin = jnp.cos(angles), jnp.sin(angles)
    key_rows = turn(qkv[:, head_cols : head_cols + HEAD].astype(F32), cos, sin).astype(BF16)
    kv = gather_mdl(jnp.concatenate([key_rows, qkv[:, head_cols + HEAD :]], axis=1), 0)
    first = (me * count).astype(jnp.int32).reshape(1)
    pos = positions[:, None]
    attended, log_norm = attention_forward(first, qkv, kv, cos, sin, pos)
    head_block = cols_to_rows(attended)
    residual = inputs.astype(F32)
    payload, scatter = product_to_mdl((head_block,), w_attn, (qkv_cols,))
    mixed = residual + scatter(payload)

    rows_two = gather_mdl(mixed.astype(BF16), 1)
    scale_two = row_scale(rows_two)
    rows_hat = (rows_two.astype(F32) * scale_two).astype(BF16)
    rows, above, stat_two, partial, hiddens, sums = rows_hat, cotangent, 0.0, (), [], []
    for index, (weight, (start, stop)) in enumerate(zip(w_parts, parts)):
        cols = stop - start
        last = index == len(parts) - 1
        gate_in = nn(rows, weight[:, :cols])
        up_in = nn(rows, weight[:, cols : 2 * cols])
        d_hidden = nn(above, weight[:, 2 * cols :])
        gelu, slope = gelu_parts(gate_in)
        hidden = (gelu * up_in).astype(BF16)
        d_gate = d_hidden * up_in * slope
        d_up = d_hidden * gelu
        stat_two += jnp.sum(d_gate * gate_in + d_up * up_in, axis=1)
        d_gate, d_up = d_gate.astype(BF16), d_up.astype(BF16)
        hiddens.append(hidden)
        lefts, starts = (d_gate, d_up), (0, cols)
        if last:
            payload, scatter = product_to_mdl(lefts, weight, starts, partial)
            rows, above, _ = lax.optimization_barrier((rows, above, payload[0]))
        local = part_grad(rows, above, d_gate, d_up, hidden)
        if not last:
            d_gate = after(d_gate, local[0])
            partial = (sum_products((d_gate, d_up), weight, starts),)
            rows, above, _ = lax.optimization_barrier((rows, above, local[0]))
        sums.append(pair_to_tok(local))
    d_two = scatter(payload)
    stat_two = sum_mdl(stat_two.reshape(8, -1)).reshape(-1, 1) * (1.0 / features)
    scale_mixed = scale_two * mixed
    cotangent_own = lax.dynamic_slice_in_dim(cotangent, me * width, width, 1).astype(F32)
    d_mixed = cotangent_own + scale_two * (d_two - scale_mixed * stat_two)

    d_mixed_b = after(d_mixed.astype(BF16), local[0])
    down_starts = tuple(2 * (stop - start) for start, stop in parts)
    ffn = (sum_products((after(hiddens[0], d_mixed_b),), w_parts[0], down_starts[:1]),)
    ffn_payload, ffn_scatter = product_to_mdl(
        (after(hiddens[1], d_mixed_b),), w_parts[1], down_starts[1:], ffn
    )
    if size == 4 and lax.axis_size("tok") == 8:
        pieces = gather_pieces(d_mixed_b)
        d_head = pieces_product(pieces, w_attn, qkv_cols, head_block.shape[1])
        heads_later = after(head_block, d_head)
        out_local = pieces_grad(pieces, heads_later)
    else:
        d_mixed_rows = gather_mdl(d_mixed_b, 1)
        d_head = nn(d_mixed_rows, w_attn[:, qkv_cols:]).astype(BF16)
        out_local = pair_grad(d_mixed_rows, head_block)
    out_grad = pair_to_tok(out_local)
    d_attended = rows_to_cols(d_head)
    d_query, d_kv = attention_backward(
        first, qkv, kv, cos, sin, pos, attended, d_attended, log_norm
    )
    d_kv = scatter_mdl(d_kv.astype(BF16), 0)
    d_key = unturn(d_kv[:, :HEAD], cos, sin).astype(BF16)
    d_qkv = jnp.concatenate([d_query, d_key, d_kv[:, HEAD:].astype(BF16)], axis=1)
    stat_one = jnp.sum(d_qkv.astype(F32) * qkv.astype(F32), axis=1)
    d_qkv_part = cols_to_rows(d_qkv)
    stat_rows = jnp.zeros((size, count), F32)
    stat_rows = sum_mdl(lax.dynamic_update_slice(stat_rows, stat_one[None], (me, 0)))
    stat_one = stat_rows.reshape(-1, 1) * (1.0 / features)
    payload, scatter = product_to_mdl((d_qkv_part,), w_attn, (0,))
    d_scaled = (after(d_qkv_part, payload[0]).astype(F32) * scale_one).astype(BF16)
    *qkv_local, gain_one = pair_grad(rows_in, d_scaled, w_attn)
    qkv_sum = pair_to_tok(qkv_local)
    d_one = scatter(payload)
    ffn_sum = ffn_scatter(ffn_payload)
    block_out = (mixed + ffn_sum).astype(BF16)
    input_grad = d_mixed + scale_one * (d_one - (scale_one * residual) * stat_one)

    norm1_late, norm2_late, gate_late, up_late, _ = lax.optimization_barrier(
        (norm1_gain, norm2_gain, gate_weight, up_weight, local[0])
    )

    def unfold(total, gain):
        return total * gain.astype(F32)[:, None]

    def joined(at):
        widths = [total.shape[1] // 3 for total in sums]
        pieces = [total[:, at * cols :][:, :cols] for total, cols in zip(sums, widths)]
        return jnp.concatenate(pieces, axis=1)

    gate_sum, up_sum, down_grad = joined(0), joined(1), joined(2).T
    gain_two = jnp.sum(
        gate_late.astype(F32) * gate_sum + up_late.astype(F32) * up_sum, axis=1
    )
    gate_grad, up_grad = unfold(gate_sum, norm2_late), unfold(up_sum, norm2_late)
    out_grad = out_grad.T
    gain_two_grad = sum_mdl(gain_two)
    gain_one = sum_mdl(sum_tok(gain_one.reshape(8, -1))).reshape(-1)
    shard = norm1_gain.shape[0]
    gain_one = lax.dynamic_slice_in_dim(gain_one, lax.axis_index("tok") * shard, shard, 0)
    gain_one_grad = gain_one / norm1_late.astype(F32)
    return (
        block_out,
        input_grad,
        gain_one_grad,
        unfold(qkv_sum, norm1_late),
        out_grad,
        gain_two_grad,
        gate_grad,
        up_grad,
        down_grad,
    )


def solution(mesh):
    return jax.shard_map(
        on_device,
        mesh=mesh,
        in_specs=(
            P("tok", "mdl"),
            P(("tok", "mdl")),
            P("tok"),
            P("tok", "mdl"),
            P("mdl", "tok"),
            P("tok"),
            P("tok", "mdl"),
            P("tok", "mdl"),
            P("mdl", "tok"),
            P("tok", None),
        ),
        out_specs=(
            P("tok", "mdl"),
            P("tok", "mdl"),
            P("tok"),
            P("tok", "mdl"),
            P("mdl", "tok"),
            P("tok"),
            P("tok", "mdl"),
            P("tok", "mdl"),
            P("mdl", "tok"),
        ),
        check_vma=False,
    )
```

```python
import functools
import math

import jax
import jax.numpy as jnp
from jax import lax
from jax.experimental import pallas as pl
from jax.experimental.pallas import tpu as pltpu
from jax.sharding import PartitionSpec as P


HEADS = 10
HEAD = 256
NORM_EPS = 1e-06
F32 = jnp.float32
BF16 = jnp.bfloat16
MASKED = -1e30


def nt(left_op, right_op):
    return lax.dot_general(
        left_op, right_op, (((1,), (1,)), ((), ())), preferred_element_type=F32
    )


def tn(left_op, right_op):
    return lax.dot_general(
        left_op, right_op, (((0,), (0,)), ((), ())), preferred_element_type=F32
    )


def nn(left_op, right_op):
    return jnp.dot(left_op, right_op, preferred_element_type=F32)


def swap(block, distance):
    size = lax.axis_size("mdl")
    return lax.ppermute(block, "mdl", [(i, i ^ distance) for i in range(size)])


def gather_mdl(block, dim):
    size = lax.axis_size("mdl")
    if size != 4:
        return lax.all_gather(block, "mdl", axis=dim, tiled=True)
    me = lax.axis_index("mdl")
    half = block.shape[0] // 2
    along_x = swap(block, 1)
    along_y = swap(block, 2)
    top = swap(along_x[:half], 2)
    bottom = swap(along_y[half:], 1)
    width = block.shape[dim]
    shape = list(block.shape)
    shape[dim] = width * size
    whole = jnp.zeros(shape, block.dtype)

    def put(whole, piece, source, row):
        start = [0, 0]
        start[dim] = source * width
        start[0] = start[0] + row
        return lax.dynamic_update_slice(whole, piece, tuple(start))

    whole = put(whole, block, me, 0)
    whole = put(whole, along_x, me ^ 1, 0)
    whole = put(whole, along_y, me ^ 2, 0)
    whole = put(whole, top, me ^ 3, 0)
    whole = put(whole, bottom, me ^ 3, half)
    return whole


def scatter_mdl(part, dim):
    size = lax.axis_size("mdl")
    if size != 4:
        return lax.psum_scatter(part, "mdl", scatter_dimension=dim, tiled=True).astype(F32)
    me = lax.axis_index("mdl")
    shape = list(part.shape)
    shape[dim] //= size
    half = shape[0] // 2

    def piece(block, row):
        start = [0, 0]
        start[dim] = block * shape[dim]
        start[0] = start[0] + row
        return lax.dynamic_slice(part, tuple(start), (half, shape[1]))

    sums = []
    for row, first, second in ((0, 1, 2), (half, 2, 1)):
        sent = jnp.stack([piece(me ^ first, row), piece(me ^ 3, row)])
        sums.append((row, second, swap(sent, first)))
    partial = []
    for row, second, got in sums:
        other = piece(me ^ second, row).astype(F32) + got[1].astype(F32)
        partial.append((row, got[0], swap(other.astype(BF16), second)))
    return jnp.concatenate(
        [
            piece(me, row).astype(F32) + first.astype(F32) + second.astype(F32)
            for row, first, second in partial
        ],
        axis=0,
    )


def gather_pieces(block):
    half = block.shape[0] // 2
    along_x = swap(block, 1)
    along_y = swap(block, 2)
    top = swap(along_x[:half], 2)
    bottom = swap(along_y[half:], 1)
    return block, along_x, along_y, top, bottom


def scatter_payload(payload, *earlier):
    top_sent, bottom_sent, top_kept, bottom_kept = payload
    got_top = swap(top_sent, 1)
    got_bottom = swap(bottom_sent, 2)
    halves = []
    for kept, got, second in ((top_kept, got_top, 2), (bottom_kept, got_bottom, 1)):
        passed = (kept[1].astype(F32) + got[1].astype(F32)).astype(BF16)
        if earlier:
            passed = after(passed, *earlier)
        last = swap(passed, second)
        halves.append(kept[0].astype(F32) + got[0].astype(F32) + last.astype(F32))
    return jnp.concatenate(halves, axis=0)


def sum_mdl(value):
    size = lax.axis_size("mdl")
    distance = 1
    while distance < size:
        value = value + swap(value, distance)
        distance *= 2
    return value


def sum_tok(value):
    size = lax.axis_size("tok")
    distance = 1
    while distance < size:
        value = value + lax.ppermute(value, "tok", [(i, i ^ distance) for i in range(size)])
        distance *= 2
    return value


def rows_to_cols(block):
    return lax.all_to_all(block, "mdl", split_axis=0, concat_axis=1, tiled=True)


def cols_to_rows(block):
    return lax.all_to_all(block, "mdl", split_axis=1, concat_axis=0, tiled=True)


def first_kernel(
    x_ref, w_ref, rows_ref, weight_ref, own, x_sent, x_got, w_up, w_down, w_core, w_got
):
    me, tok = lax.axis_index("mdl"), lax.axis_index("tok")
    pairs = lax.axis_size("tok") // 2
    level, last = tok // 2, pairs - 1
    half, width, shard = x_ref.shape[0] // 2, x_ref.shape[1], w_ref.shape[0]
    below, above = level > 0, level < last

    barrier = pltpu.get_barrier_semaphore()
    pl.semaphore_signal(barrier, inc=1, device_id={"mdl": me ^ 1})
    pl.semaphore_signal(barrier, inc=1, device_id={"mdl": me ^ 2})
    pl.semaphore_signal(barrier, inc=1, device_id={"tok": tok ^ 1})

    @pl.when(below)
    def _():
        pl.semaphore_signal(barrier, inc=1, device_id={"tok": tok - 2})

    @pl.when(above)
    def _():
        pl.semaphore_signal(barrier, inc=1, device_id={"tok": tok + 2})

    pl.semaphore_wait(barrier, 3 + below.astype(jnp.int32) + above.astype(jnp.int32))

    def cols(block):
        return pl.ds(pl.multiple_of(block * width, 128), width)

    def block(index):
        return weight_ref.at[pl.ds(pl.multiple_of(index * shard, 16), shard)]

    def x_copy(source, target, at, to):
        return pltpu.make_async_remote_copy(
            source, target, x_sent.at[at], x_got.at[at], device_id={"mdl": me ^ to}
        )

    def w_copy(source, index, sent, to):
        return pltpu.make_async_remote_copy(
            source, block(index), sent, w_got.at[index], device_id={"tok": to}
        )

    mine = rows_ref.at[:, cols(me)]
    to_x, to_y = x_copy(x_ref, mine, 0, 1), x_copy(x_ref, mine, 1, 2)

    @pl.when(above)
    def _():
        w_copy(w_ref, tok, w_up.at[0], tok + 2).start()

    @pl.when(below)
    def _():
        w_copy(w_ref, tok, w_down.at[0], tok - 2).start()

    to_x.start()
    to_y.start()
    w_copy(w_ref, tok, w_core.at[tok], tok ^ 1).start()
    keep_x = pltpu.make_async_copy(x_ref, mine, own.at[0])
    keep_w = pltpu.make_async_copy(w_ref, block(tok), own.at[1])
    keep_x.start()
    keep_w.start()

    def relay(distance):
        low, high = tok - 2 * distance, tok + 2 * distance

        @pl.when(level >= distance)
        def _():
            w_copy(block(low), low, w_core.at[low], tok ^ 1).wait_recv()

            @pl.when(above)
            def _():
                w_copy(block(low), low, w_up.at[distance], tok + 2).start()

            w_copy(block(low), low, w_core.at[low], tok ^ 1).start()

        @pl.when(level + distance <= last)
        def _():
            w_copy(block(high), high, w_core.at[high], tok ^ 1).wait_recv()

            @pl.when(below)
            def _():
                w_copy(block(high), high, w_down.at[distance], tok - 2).start()

            w_copy(block(high), high, w_core.at[high], tok ^ 1).start()

    relay(1)
    from_x = rows_ref.at[pl.ds(0, half), cols(me ^ 1)]
    from_y = rows_ref.at[pl.ds(half, half), cols(me ^ 2)]
    top, bottom = x_copy(from_x, from_x, 2, 2), x_copy(from_y, from_y, 3, 1)
    to_x.wait_recv()
    top.start()
    to_y.wait_recv()
    bottom.start()
    for distance in range(2, pairs):
        relay(distance)
    for copy in (keep_x, keep_w):
        copy.wait()
    for copy in (top, bottom):
        copy.wait_recv()
    for copy in (to_x, to_y, top, bottom):
        copy.wait_send()

    for distance in range(pairs):

        @pl.when((level >= distance) & above)
        def _(distance=distance):
            w_copy(block(tok), tok, w_up.at[distance], tok + 2).wait_send()

        @pl.when((level + distance <= last) & below)
        def _(distance=distance):
            w_copy(block(tok), tok, w_down.at[distance], tok - 2).wait_send()

        near, far = 2 * distance + tok % 2, 2 * distance + 1 - tok % 2
        w_copy(block(near), near, w_core.at[near], tok ^ 1).wait_send()
        w_copy(block(far), far, w_core.at[near], tok ^ 1).wait_recv()


def first_gather(inputs, weight):
    tokens, width = inputs.shape
    shard, cols = weight.shape
    pairs = lax.axis_size("tok") // 2
    dma = pltpu.SemaphoreType.DMA
    return pl.pallas_call(
        first_kernel,
        out_shape=(
            jax.ShapeDtypeStruct((tokens, 4 * width), BF16),
            jax.ShapeDtypeStruct((2 * pairs * shard, cols), BF16),
        ),
        in_specs=[pl.BlockSpec(memory_space=pltpu.VMEM)] * 2,
        out_specs=[pl.BlockSpec(memory_space=pl.ANY)] * 2,
        scratch_shapes=[
            dma((2,)), dma((4,)), dma((4,)), dma((pairs,)), dma((pairs,)),
            dma((2 * pairs,)), dma((2 * pairs,)),
        ],
        compiler_params=pltpu.CompilerParams(
            collective_id=0, has_side_effects=True, vmem_limit_bytes=16 << 20
        ),
    )(inputs, weight)


def in_order(mebibytes):
    return pltpu.CompilerParams(
        dimension_semantics=(pltpu.ARBITRARY,), vmem_limit_bytes=mebibytes << 20
    )


def cost(flops, bytes_accessed, transcendentals=0):
    return pl.CostEstimate(
        flops=flops, bytes_accessed=bytes_accessed, transcendentals=transcendentals
    )


def turn(vector, cos, sin):
    half = HEAD // 2
    lower, upper = vector[:, :half], vector[:, half:]
    return jnp.concatenate([lower * cos - upper * sin, upper * cos + lower * sin], axis=1)


def unturn(vector, cos, sin):
    half = HEAD // 2
    lower, upper = vector[:, :half], vector[:, half:]
    return jnp.concatenate([lower * cos + upper * sin, upper * cos - lower * sin], axis=1)


def seen(first_ref, position_ref, queries, keys):
    row = lax.broadcasted_iota(jnp.int32, (queries, keys), 0) + first_ref[0]
    distance = row - lax.broadcasted_iota(jnp.int32, (queries, keys), 1)
    return (distance >= 0) & (distance <= position_ref[...])


def forward_kernel(first_ref, q_ref, kv_ref, cos_ref, sin_ref, pos_ref, out_ref, norm_ref):
    query = turn(q_ref[...].astype(F32), cos_ref[...], sin_ref[...])
    query = (query * HEAD ** (-0.5)).astype(BF16)
    keys, values = kv_ref[:, :HEAD], kv_ref[:, HEAD:]
    scores = nt(query, keys)
    scores = jnp.where(seen(first_ref, pos_ref, *scores.shape), scores, MASKED)
    top = jnp.max(scores, axis=1, keepdims=True)
    weights = jnp.exp(scores - top)
    total = jnp.sum(weights, axis=1, keepdims=True)
    out_ref[...] = (nn(weights.astype(BF16), values) / total).astype(BF16)
    norm_ref[0] = top + jnp.log(total)


def backward_kernel(
    first_ref, q_ref, kv_ref, cos_ref, sin_ref, pos_ref, att_ref, datt_ref, norm_ref,
    dq_ref, dkv_ref,
):
    head = pl.program_id(0)
    scale = HEAD ** (-0.5)
    cos, sin = cos_ref[...], sin_ref[...]
    query = (turn(q_ref[...].astype(F32), cos, sin) * scale).astype(BF16)
    keys, values = kv_ref[:, :HEAD], kv_ref[:, HEAD:]
    scores = nt(query, keys)
    visible = seen(first_ref, pos_ref, *scores.shape)
    again = jnp.where(visible, jnp.exp(scores - norm_ref[0]), 0.0)
    d_att = datt_ref[...]
    delta = jnp.sum(d_att.astype(F32) * att_ref[...].astype(F32), axis=1, keepdims=True)
    d_scores = (again * (nt(d_att, values) - delta)).astype(BF16)
    d_query = nn(d_scores, keys) * scale
    dq_ref[...] = unturn(d_query, cos, sin).astype(BF16)

    @pl.when(head == 0)
    def _():
        dkv_ref[...] = jnp.zeros_like(dkv_ref)

    dkv_ref[:, :HEAD] += tn(d_scores, query)
    dkv_ref[:, HEAD:] += tn(again.astype(BF16), d_att)


def whole_spec(shape):
    return pl.BlockSpec(shape, lambda head: (0,) * len(shape))


def attention_forward(first, qkv, kv, cos, sin, pos):
    rows, keys = qkv.shape[0], kv.shape[0]
    head_spec = pl.BlockSpec((rows, HEAD), lambda head: (0, head))
    return pl.pallas_call(
        forward_kernel,
        grid=(HEADS,),
        out_shape=(
            jax.ShapeDtypeStruct((rows, HEADS * HEAD), BF16),
            jax.ShapeDtypeStruct((HEADS, rows, 1), F32),
        ),
        in_specs=[
            pl.BlockSpec(memory_space=pltpu.SMEM),
            head_spec,
            whole_spec((keys, 2 * HEAD)),
            whole_spec((rows, HEAD // 2)),
            whole_spec((rows, HEAD // 2)),
            whole_spec((rows, 1)),
        ],
        out_specs=(head_spec, pl.BlockSpec((1, rows, 1), lambda head: (head, 0, 0))),
        compiler_params=in_order(32),
        cost_estimate=cost(4 * rows * keys * HEADS * HEAD, 4 * rows * HEADS * HEAD + 4 * keys * HEAD, rows * keys * HEADS),
        name="attention_forward",
    )(first, qkv, kv, cos, sin, pos)


def attention_backward(first, qkv, kv, cos, sin, pos, att, d_att, norm):
    rows, keys = qkv.shape[0], kv.shape[0]
    head_spec = pl.BlockSpec((rows, HEAD), lambda head: (0, head))
    return pl.pallas_call(
        backward_kernel,
        grid=(HEADS,),
        out_shape=(
            jax.ShapeDtypeStruct((rows, HEADS * HEAD), BF16),
            jax.ShapeDtypeStruct((keys, 2 * HEAD), F32),
        ),
        in_specs=[
            pl.BlockSpec(memory_space=pltpu.SMEM),
            head_spec,
            whole_spec((keys, 2 * HEAD)),
            whole_spec((rows, HEAD // 2)),
            whole_spec((rows, HEAD // 2)),
            whole_spec((rows, 1)),
            head_spec,
            head_spec,
            pl.BlockSpec((1, rows, 1), lambda head: (head, 0, 0)),
        ],
        out_specs=(head_spec, whole_spec((keys, 2 * HEAD))),
        compiler_params=in_order(40),
        cost_estimate=cost(10 * rows * keys * HEADS * HEAD, 8 * rows * HEADS * HEAD + 12 * keys * HEAD, rows * keys * HEADS),
        name="attention_backward",
    )(first, qkv, kv, cos, sin, pos, att, d_att, norm)


def keep_half(core_ref, total, kept, sent):
    half = total.shape[0] // 2
    for core, (first, second) in enumerate(((kept, sent), (sent, kept))):

        @pl.when(core_ref[0] == core)
        def _(first=first, second=second):
            first[...] = total[:half]
            second[...] = total[half:]


def pair_kernel(core_ref, left_ref, right_ref, *refs):
    total = tn(left_ref[...], right_ref[...])
    if len(refs) == 4:
        weight = refs[0][:, : total.shape[1]].astype(F32)
        refs[3][...] = jnp.sum(total * weight, axis=1, keepdims=True)
    keep_half(core_ref, total.astype(BF16), *refs[-3:-1] if len(refs) == 4 else refs)


def split_pairs(total, pairs, core):
    rows, cols = total.shape
    total = total.reshape(pairs, 2, rows // pairs // 2, cols)
    return tuple(
        lax.dynamic_index_in_dim(total, index, 1, False).reshape(-1, cols)
        for index in (core, 1 - core)
    )


def core_index():
    return (lax.axis_index("tok") % 2).astype(jnp.int32).reshape(1)


def pair_grad(left, right, weight=None):
    tokens, rows = left.shape
    cols = right.shape[1]
    pairs = lax.axis_size("tok") // 2
    step = rows // pairs
    if step % 128 or cols % 128:
        total = tn(left, right)
        halves = split_pairs(total.astype(BF16), pairs, lax.axis_index("tok") % 2)
        if weight is None:
            return halves
        return *halves, jnp.sum(total * weight[:, :cols].astype(F32), axis=1, keepdims=True)
    out_shape = [jax.ShapeDtypeStruct((rows // 2, cols), BF16)] * 2
    out_specs = [pl.BlockSpec((step // 2, cols), lambda pair: (pair, 0))] * 2
    in_specs = [
        pl.BlockSpec(memory_space=pltpu.SMEM),
        pl.BlockSpec((tokens, step), lambda pair: (0, pair)),
        pl.BlockSpec((tokens, cols), lambda pair: (0, 0)),
    ]
    operands = [core_index(), left, right]
    if weight is not None:
        operands.append(weight)
        in_specs.append(pl.BlockSpec((step, weight.shape[1]), lambda pair: (pair, 0)))
        out_shape.append(jax.ShapeDtypeStruct((rows, 1), F32))
        out_specs.append(pl.BlockSpec((step, 1), lambda pair: (pair, 0)))
    return pl.pallas_call(
        pair_kernel,
        grid=(pairs,),
        out_shape=out_shape,
        in_specs=in_specs,
        out_specs=out_specs,
        compiler_params=in_order(48),
        cost_estimate=cost(2 * tokens * rows * cols, 2 * (tokens * (rows + cols) + rows * cols)),
    )(*operands)


def part_kernel(core_ref, rows_ref, above_ref, d_gate_ref, d_up_ref, hidden_ref, kept, sent):
    cols = hidden_ref.shape[1]
    for at, (left_ref, right_ref) in enumerate(
        ((rows_ref, d_gate_ref), (rows_ref, d_up_ref), (above_ref, hidden_ref))
    ):
        total = tn(left_ref[...], right_ref[...]).astype(BF16)
        window = (slice(None), pl.ds(at * cols, cols))
        keep_half(core_ref, total, kept.at[window], sent.at[window])


def part_grad(rows, above, d_gate, d_up, hidden):
    tokens, features = rows.shape
    cols = hidden.shape[1]
    pairs = lax.axis_size("tok") // 2
    step = features // pairs
    if step % 128 or cols % 128:
        total = [tn(rows, d_gate), tn(rows, d_up), tn(above, hidden)]
        total = jnp.concatenate(total, axis=1).astype(BF16)
        return split_pairs(total, pairs, lax.axis_index("tok") % 2)
    out = jax.ShapeDtypeStruct((features // 2, 3 * cols), BF16)
    left_spec = pl.BlockSpec((tokens, step), lambda pair: (0, pair))
    right_spec = pl.BlockSpec((tokens, cols), lambda pair: (0, 0))
    return pl.pallas_call(
        part_kernel,
        grid=(pairs,),
        out_shape=(out, out),
        in_specs=[pl.BlockSpec(memory_space=pltpu.SMEM)] + [left_spec] * 2 + [right_spec] * 3,
        out_specs=[pl.BlockSpec((step // 2, 3 * cols), lambda pair: (pair, 0))] * 2,
        compiler_params=in_order(48),
        cost_estimate=cost(
            6 * tokens * features * cols,
            2 * (2 * tokens * features + 3 * cols * (tokens + features)),
        ),
    )(core_index(), rows, above, d_gate, d_up, hidden)


def pieces_grad_kernel(me_ref, core_ref, own, along_x, along_y, top, bottom, right_ref, kept, sent):
    at = pl.program_id(0)
    half = top.shape[0]
    for index, piece in enumerate((own, along_x, along_y)):

        @pl.when(at == index)
        def _(piece=piece):
            keep_half(core_ref, tn(piece[...], right_ref[...]).astype(BF16), kept, sent)

    @pl.when(at == 3)
    def _():
        total = tn(top[...], right_ref[:half]) + tn(bottom[...], right_ref[half:])
        keep_half(core_ref, total.astype(BF16), kept, sent)


def pieces_grad(pieces, right):
    tokens, step = pieces[0].shape
    cols = right.shape[1]
    me = lax.axis_index("mdl").astype(jnp.int32).reshape(1)
    out = jax.ShapeDtypeStruct((2 * step, cols), BF16)
    return pl.pallas_call(
        pieces_grad_kernel,
        grid_spec=pltpu.PrefetchScalarGridSpec(
            num_scalar_prefetch=2,
            grid=(4,),
            in_specs=[
                pl.BlockSpec(array.shape, lambda at, me_ref, core_ref: (0, 0))
                for array in (*pieces, right)
            ],
            out_specs=[
                pl.BlockSpec((step // 2, cols), lambda at, me_ref, core_ref: (me_ref[0] ^ at, 0))
            ]
            * 2,
        ),
        out_shape=(out, out),
        compiler_params=in_order(48),
        cost_estimate=cost(8 * tokens * step * cols, 2 * (4 * tokens * step + 5 * step * cols)),
    )(me, core_index(), *pieces, right)


def sum_kernel(starts, *refs):
    *lefts, weight_ref, out_ref = refs
    total = 0.0
    for left_ref, start in zip(lefts, starts):
        total += nt(left_ref[...], weight_ref[:, start : start + left_ref.shape[1]])
    out_ref[...] = total


def sum_products(lefts, weight, starts):
    tokens = lefts[0].shape[0]
    rows, cols = weight.shape
    if lefts[0].shape[1] % 128:
        return sum(
            nt(left, weight[:, start : start + left.shape[1]])
            for left, start in zip(lefts, starts)
        )
    step = 512
    depth = sum(left.shape[1] for left in lefts)
    return pl.pallas_call(
        functools.partial(sum_kernel, starts),
        grid=(rows // step,),
        out_shape=jax.ShapeDtypeStruct((tokens, rows), F32),
        in_specs=[pl.BlockSpec(left.shape, lambda row: (0, 0)) for left in lefts]
        + [pl.BlockSpec((step, cols), lambda row: (row, 0))],
        out_specs=pl.BlockSpec((tokens, step), lambda row: (0, row)),
        compiler_params=in_order(48),
        cost_estimate=cost(2 * tokens * rows * depth, 2 * rows * cols + 4 * tokens * rows),
    )(*lefts, weight)


def payload_kernel(starts, me_ref, *refs):
    lefts, weight_ref = refs[: len(starts)], refs[len(starts)]
    top_sent, bottom_sent, top_kept, bottom_kept = refs[-4:]
    total = refs[-5][...] if len(refs) == len(starts) + 6 else 0.0
    for left_ref, start in zip(lefts, starts):
        total += nt(left_ref[...], weight_ref[:, start : start + left_ref.shape[1]])
    total = total.astype(BF16)
    half = total.shape[0] // 2
    places = (
        ((top_kept, 0), (bottom_kept, 0)),
        ((top_sent, 0), (bottom_kept, 1)),
        ((top_kept, 1), (bottom_sent, 0)),
        ((top_sent, 1), (bottom_sent, 1)),
    )
    for distance, ((top, top_at), (bottom, bottom_at)) in enumerate(places):

        @pl.when(pl.program_id(0) == 3 - distance)
        def _(top=top, top_at=top_at, bottom=bottom, bottom_at=bottom_at):
            top[top_at] = total[:half]
            bottom[bottom_at] = total[half:]


def scatter_product(lefts, weight, starts, partial=()):
    tokens = lefts[0].shape[0]
    rows, cols = weight.shape
    step = rows // 4
    me = lax.axis_index("mdl").astype(jnp.int32).reshape(1)
    out = jax.ShapeDtypeStruct((2, tokens // 2, step), BF16)
    depth = sum(left.shape[1] for left in lefts)
    return pl.pallas_call(
        functools.partial(payload_kernel, starts),
        grid_spec=pltpu.PrefetchScalarGridSpec(
            num_scalar_prefetch=1,
            grid=(4,),
            in_specs=[pl.BlockSpec(left.shape, lambda at, me_ref: (0, 0)) for left in lefts]
            + [pl.BlockSpec((step, cols), lambda at, me_ref: (me_ref[0] ^ (3 - at), 0))]
            + [pl.BlockSpec((tokens, step), lambda at, me_ref: (0, me_ref[0] ^ (3 - at)))]
            * len(partial),
            out_specs=[pl.BlockSpec(out.shape, lambda at, me_ref: (0, 0, 0))] * 4,
        ),
        out_shape=(out,) * 4,
        compiler_params=in_order(48),
        cost_estimate=cost(2 * tokens * rows * depth, 2 * (tokens * depth + rows * cols + tokens * rows)),
    )(me, *lefts, weight, *partial)


def pieces_kernel(start, me_ref, own, along_x, along_y, top, bottom, weight_ref, out_ref, total):
    at = pl.program_id(0)
    width = out_ref.shape[1]
    half = top.shape[0]
    for index, piece in enumerate((own, along_x, along_y)):

        @pl.when(at == index)
        def _(index=index, piece=piece):
            part = nn(piece[...], weight_ref[:, start : start + width])
            if index:
                total[...] += part
            else:
                total[...] = part

    @pl.when(at == 3)
    def _():
        weight = weight_ref[:, start : start + width]
        out_ref[:half] = (total[:half] + nn(top[...], weight)).astype(BF16)
        out_ref[half:] = (total[half:] + nn(bottom[...], weight)).astype(BF16)


def pieces_product(pieces, weight, start, width):
    tokens, step = pieces[0].shape
    rows, cols = weight.shape
    me = lax.axis_index("mdl").astype(jnp.int32).reshape(1)
    return pl.pallas_call(
        functools.partial(pieces_kernel, start),
        grid_spec=pltpu.PrefetchScalarGridSpec(
            num_scalar_prefetch=1,
            grid=(4,),
            in_specs=[pl.BlockSpec(piece.shape, lambda at, me_ref: (0, 0)) for piece in pieces]
            + [pl.BlockSpec((step, cols), lambda at, me_ref: (me_ref[0] ^ at, 0))],
            out_specs=pl.BlockSpec((tokens, width), lambda at, me_ref: (0, 0)),
            scratch_shapes=[pltpu.VMEM((tokens, width), F32)],
        ),
        out_shape=jax.ShapeDtypeStruct((tokens, width), BF16),
        compiler_params=in_order(40),
        cost_estimate=cost(2 * tokens * rows * width, 2 * (tokens * rows + rows * cols + tokens * width)),
    )(me, *pieces, weight)


def product_to_mdl(lefts, weight, starts, partial=()):
    if lax.axis_size("mdl") == 4:
        payload = scatter_product(lefts, weight, starts, partial)
        return payload, lambda payload, *earlier: scatter_payload(payload, *earlier)
    part = sum((sum_products(lefts, weight, starts), *partial))
    return (part.astype(BF16),), lambda payload, *earlier: scatter_mdl(payload[0], 1)


def after(value, *earlier):
    return lax.optimization_barrier((value, *earlier))[0]


def row_scale(rows_b, axis=-1):
    rows = rows_b.astype(F32)
    return lax.rsqrt(jnp.mean(rows * rows, axis=axis, keepdims=True) + NORM_EPS)


def gelu_parts(value):
    root = math.sqrt(2.0 / math.pi)
    square = value * value
    tanh = jnp.tanh(root * (value + 0.044715 * value * square))
    cdf = 0.5 * (1.0 + tanh)
    slope = cdf + 0.5 * value * (1.0 - tanh * tanh) * root * (1.0 + 3 * 0.044715 * square)
    return value * cdf, slope


def scaled(weight, gain):
    return (weight.astype(F32) * gain.astype(F32)[:, None]).astype(BF16)


def on_device(
    inputs, positions, norm1_gain, qkv_weight, out_weight, norm2_gain, gate_weight,
    up_weight, down_weight, cotangent,
):
    me = lax.axis_index("mdl")
    size = lax.axis_size("mdl")
    head_cols = HEADS * HEAD
    width = inputs.shape[1]
    features = width * size

    def from_tok(weight, dim):
        return lax.all_gather(weight, "tok", axis=dim, tiled=True)

    def pair_to_tok(local):
        kept, sent = local
        count = lax.axis_size("tok")
        got = lax.ppermute(sent, "tok", [(i, i ^ 1) for i in range(count)])
        both = (kept.astype(F32) + got.astype(F32)).astype(BF16)
        groups = [list(range(core, count, 2)) for core in range(2)]
        total = lax.psum_scatter(
            both, "tok", scatter_dimension=0, tiled=True, axis_index_groups=groups
        )
        return total.astype(F32)

    qkv_cols, ff_cols = qkv_weight.shape[1], gate_weight.shape[1]
    attn_local = jnp.concatenate([scaled(qkv_weight, norm1_gain), out_weight.T], axis=1)
    middle = -(-ff_cols // 256) * 128
    parts = ((0, middle), (middle, ff_cols))

    def part_local(start, stop):
        local = [scaled(w[:, start:stop], norm2_gain) for w in (gate_weight, up_weight)]
        return jnp.concatenate([*local, down_weight[start:stop].T], axis=1)

    locals_ff = [part_local(*part) for part in parts]
    if size == 4 and lax.axis_size("tok") == 8:
        rows_in, w_attn = first_gather(inputs, after(attn_local, locals_ff[0]))
        locals_ff = lax.optimization_barrier((*locals_ff, w_attn))[:-1]
    else:
        rows_in = gather_mdl(inputs, 1)
        w_attn = from_tok(attn_local, 0)
    w_qkv = w_attn[:, :qkv_cols]
    w_parts = [from_tok(local, 0) for local in locals_ff]

    scale_one = row_scale(rows_in)
    qkv_part = (nn(rows_in, w_qkv) * scale_one).astype(BF16)
    qkv = rows_to_cols(qkv_part)
    count = qkv.shape[0]
    half = HEAD // 2
    frequency = jnp.exp(jnp.arange(half, dtype=F32) * (-2.0 * math.log(10000.0) / HEAD))
    angles = positions.astype(F32)[:, None] * frequency[None, :]
    cos, sin = jnp.cos(angles), jnp.sin(angles)
    key_rows = turn(qkv[:, head_cols : head_cols + HEAD].astype(F32), cos, sin).astype(BF16)
    kv = gather_mdl(jnp.concatenate([key_rows, qkv[:, head_cols + HEAD :]], axis=1), 0)
    first = (me * count).astype(jnp.int32).reshape(1)
    pos = positions[:, None]
    attended, log_norm = attention_forward(first, qkv, kv, cos, sin, pos)
    head_block = cols_to_rows(attended)
    residual = inputs.astype(F32)
    payload, scatter = product_to_mdl((head_block,), w_attn, (qkv_cols,))
    mixed = residual + scatter(payload)

    rows_two = gather_mdl(mixed.astype(BF16), 1)
    scale_two = row_scale(rows_two)
    rows_hat = (rows_two.astype(F32) * scale_two).astype(BF16)
    rows, above, stat_two, partial, hiddens, sums = rows_hat, cotangent, 0.0, (), [], []
    for index, (weight, (start, stop)) in enumerate(zip(w_parts, parts)):
        cols = stop - start
        last = index == len(parts) - 1
        gate_in = nn(rows, weight[:, :cols])
        up_in = nn(rows, weight[:, cols : 2 * cols])
        d_hidden = nn(above, weight[:, 2 * cols :])
        gelu, slope = gelu_parts(gate_in)
        hidden = (gelu * up_in).astype(BF16)
        d_gate = d_hidden * up_in * slope
        d_up = d_hidden * gelu
        stat_two += jnp.sum(d_gate * gate_in + d_up * up_in, axis=1)
        d_gate, d_up = d_gate.astype(BF16), d_up.astype(BF16)
        hiddens.append(hidden)
        lefts, starts = (d_gate, d_up), (0, cols)
        if last:
            payload, scatter = product_to_mdl(lefts, weight, starts, partial)
            rows, above, _ = lax.optimization_barrier((rows, above, payload[0]))
        local = part_grad(rows, above, d_gate, d_up, hidden)
        if not last:
            d_gate = after(d_gate, local[0])
            partial = (sum_products((d_gate, d_up), weight, starts),)
            rows, above, _ = lax.optimization_barrier((rows, above, local[0]))
        sums.append(pair_to_tok(local))
    d_two = scatter(payload)
    stat_two = sum_mdl(stat_two.reshape(8, -1)).reshape(-1, 1) * (1.0 / features)
    scale_mixed = scale_two * mixed
    cotangent_own = lax.dynamic_slice_in_dim(cotangent, me * width, width, 1).astype(F32)
    d_mixed = cotangent_own + scale_two * (d_two - scale_mixed * stat_two)

    d_mixed_b = after(d_mixed.astype(BF16), local[0])
    down_starts = tuple(2 * (stop - start) for start, stop in parts)
    ffn = (sum_products((after(hiddens[0], d_mixed_b),), w_parts[0], down_starts[:1]),)
    ffn_payload, ffn_scatter = product_to_mdl(
        (after(hiddens[1], d_mixed_b),), w_parts[1], down_starts[1:], ffn
    )
    if size == 4 and lax.axis_size("tok") == 8:
        pieces = gather_pieces(d_mixed_b)
        d_head = pieces_product(pieces, w_attn, qkv_cols, head_block.shape[1])
        heads_later = after(head_block, d_head)
        out_local = pieces_grad(pieces, heads_later)
    else:
        d_mixed_rows = gather_mdl(d_mixed_b, 1)
        d_head = nn(d_mixed_rows, w_attn[:, qkv_cols:]).astype(BF16)
        out_local = pair_grad(d_mixed_rows, head_block)
    out_grad = pair_to_tok(out_local)
    d_attended = rows_to_cols(d_head)
    d_query, d_kv = attention_backward(
        first, qkv, kv, cos, sin, pos, attended, d_attended, log_norm
    )
    d_kv = scatter_mdl(d_kv.astype(BF16), 0)
    d_key = unturn(d_kv[:, :HEAD], cos, sin).astype(BF16)
    d_qkv = jnp.concatenate([d_query, d_key, d_kv[:, HEAD:].astype(BF16)], axis=1)
    stat_one = jnp.sum(d_qkv.astype(F32) * qkv.astype(F32), axis=1)
    d_qkv_part = cols_to_rows(d_qkv)
    stat_rows = jnp.zeros((size, count), F32)
    stat_rows = sum_mdl(lax.dynamic_update_slice(stat_rows, stat_one[None], (me, 0)))
    stat_one = stat_rows.reshape(-1, 1) * (1.0 / features)
    payload, scatter = product_to_mdl((d_qkv_part,), w_attn, (0,))
    d_scaled = (after(d_qkv_part, payload[0]).astype(F32) * scale_one).astype(BF16)
    *qkv_local, gain_one = pair_grad(rows_in, d_scaled, w_attn)
    qkv_sum = pair_to_tok(qkv_local)
    d_one = scatter(payload)
    ffn_sum = ffn_scatter(ffn_payload, d_qkv_part)
    block_out = (mixed + ffn_sum).astype(BF16)
    input_grad = d_mixed + scale_one * (d_one - (scale_one * residual) * stat_one)

    norm1_late, norm2_late, gate_late, up_late, _ = lax.optimization_barrier(
        (norm1_gain, norm2_gain, gate_weight, up_weight, local[0])
    )

    def unfold(total, gain):
        return total * gain.astype(F32)[:, None]

    def joined(at):
        widths = [total.shape[1] // 3 for total in sums]
        pieces = [total[:, at * cols :][:, :cols] for total, cols in zip(sums, widths)]
        return jnp.concatenate(pieces, axis=1)

    gate_sum, up_sum, down_grad = joined(0), joined(1), joined(2).T
    gain_two = jnp.sum(
        gate_late.astype(F32) * gate_sum + up_late.astype(F32) * up_sum, axis=1
    )
    gate_grad, up_grad = unfold(gate_sum, norm2_late), unfold(up_sum, norm2_late)
    out_grad = out_grad.T
    gain_two_grad = sum_mdl(gain_two)
    gain_one = sum_mdl(sum_tok(gain_one.reshape(8, -1))).reshape(-1)
    shard = norm1_gain.shape[0]
    gain_one = lax.dynamic_slice_in_dim(gain_one, lax.axis_index("tok") * shard, shard, 0)
    gain_one_grad = gain_one / norm1_late.astype(F32)
    return (
        block_out,
        input_grad,
        gain_one_grad,
        unfold(qkv_sum, norm1_late),
        out_grad,
        gain_two_grad,
        gate_grad,
        up_grad,
        down_grad,
    )


def solution(mesh):
    return jax.shard_map(
        on_device,
        mesh=mesh,
        in_specs=(
            P("tok", "mdl"),
            P(("tok", "mdl")),
            P("tok"),
            P("tok", "mdl"),
            P("mdl", "tok"),
            P("tok"),
            P("tok", "mdl"),
            P("tok", "mdl"),
            P("mdl", "tok"),
            P("tok", None),
        ),
        out_specs=(
            P("tok", "mdl"),
            P("tok", "mdl"),
            P("tok"),
            P("tok", "mdl"),
            P("mdl", "tok"),
            P("tok"),
            P("tok", "mdl"),
            P("tok", "mdl"),
            P("mdl", "tok"),
        ),
        check_vma=False,
    )
```

```python
import functools
import math

import jax
import jax.numpy as jnp
from jax import lax
from jax.experimental import pallas as pl
from jax.experimental.pallas import tpu as pltpu
from jax.sharding import PartitionSpec as P


HEADS = 10
HEAD = 256
NORM_EPS = 1e-06
F32 = jnp.float32
BF16 = jnp.bfloat16
MASKED = -1e30


def nt(left_op, right_op):
    return lax.dot_general(
        left_op, right_op, (((1,), (1,)), ((), ())), preferred_element_type=F32
    )


def tn(left_op, right_op):
    return lax.dot_general(
        left_op, right_op, (((0,), (0,)), ((), ())), preferred_element_type=F32
    )


def nn(left_op, right_op):
    return jnp.dot(left_op, right_op, preferred_element_type=F32)


def swap(block, distance):
    size = lax.axis_size("mdl")
    return lax.ppermute(block, "mdl", [(i, i ^ distance) for i in range(size)])


def gather_mdl(block, dim):
    size = lax.axis_size("mdl")
    if size != 4:
        return lax.all_gather(block, "mdl", axis=dim, tiled=True)
    me = lax.axis_index("mdl")
    half = block.shape[0] // 2
    along_x = swap(block, 1)
    along_y = swap(block, 2)
    top = swap(along_x[:half], 2)
    bottom = swap(along_y[half:], 1)
    width = block.shape[dim]
    shape = list(block.shape)
    shape[dim] = width * size
    whole = jnp.zeros(shape, block.dtype)

    def put(whole, piece, source, row):
        start = [0, 0]
        start[dim] = source * width
        start[0] = start[0] + row
        return lax.dynamic_update_slice(whole, piece, tuple(start))

    whole = put(whole, block, me, 0)
    whole = put(whole, along_x, me ^ 1, 0)
    whole = put(whole, along_y, me ^ 2, 0)
    whole = put(whole, top, me ^ 3, 0)
    whole = put(whole, bottom, me ^ 3, half)
    return whole


def scatter_mdl(part, dim):
    size = lax.axis_size("mdl")
    if size != 4:
        return lax.psum_scatter(part, "mdl", scatter_dimension=dim, tiled=True).astype(F32)
    me = lax.axis_index("mdl")
    shape = list(part.shape)
    shape[dim] //= size
    half = shape[0] // 2

    def piece(block, row):
        start = [0, 0]
        start[dim] = block * shape[dim]
        start[0] = start[0] + row
        return lax.dynamic_slice(part, tuple(start), (half, shape[1]))

    sums = []
    for row, first, second in ((0, 1, 2), (half, 2, 1)):
        sent = jnp.stack([piece(me ^ first, row), piece(me ^ 3, row)])
        sums.append((row, second, swap(sent, first)))
    partial = []
    for row, second, got in sums:
        other = piece(me ^ second, row).astype(F32) + got[1].astype(F32)
        partial.append((row, got[0], swap(other.astype(BF16), second)))
    return jnp.concatenate(
        [
            piece(me, row).astype(F32) + first.astype(F32) + second.astype(F32)
            for row, first, second in partial
        ],
        axis=0,
    )


def gather_pieces(block):
    half = block.shape[0] // 2
    along_x = swap(block, 1)
    along_y = swap(block, 2)
    top = swap(along_x[:half], 2)
    bottom = swap(along_y[half:], 1)
    return block, along_x, along_y, top, bottom


def scatter_payload(payload, *earlier):
    top_sent, bottom_sent, top_kept, bottom_kept = payload
    got_top = swap(top_sent, 1)
    got_bottom = swap(bottom_sent, 2)
    halves = []
    for kept, got, second in ((top_kept, got_top, 2), (bottom_kept, got_bottom, 1)):
        passed = (kept[1].astype(F32) + got[1].astype(F32)).astype(BF16)
        if earlier:
            passed = after(passed, *earlier)
        last = swap(passed, second)
        halves.append(kept[0].astype(F32) + got[0].astype(F32) + last.astype(F32))
    return jnp.concatenate(halves, axis=0)


def sum_mdl(value):
    size = lax.axis_size("mdl")
    distance = 1
    while distance < size:
        value = value + swap(value, distance)
        distance *= 2
    return value


def sum_tok(value):
    size = lax.axis_size("tok")
    distance = 1
    while distance < size:
        value = value + lax.ppermute(value, "tok", [(i, i ^ distance) for i in range(size)])
        distance *= 2
    return value


def rows_to_cols(block):
    return lax.all_to_all(block, "mdl", split_axis=0, concat_axis=1, tiled=True)


def cols_to_rows(block):
    return lax.all_to_all(block, "mdl", split_axis=1, concat_axis=0, tiled=True)


def first_kernel(
    parts, x_ref, w_ref, gain_ref, *refs
):
    weights, (rows_ref, weight_ref), locals_ref = refs[:3], refs[3:5], refs[5:7]
    held, joined = refs[7:10], refs[10:12]
    own, x_sent, x_got, w_up, w_down, w_core, w_got = refs[12:]
    me, tok = lax.axis_index("mdl"), lax.axis_index("tok")
    pairs = lax.axis_size("tok") // 2
    level, last = tok // 2, pairs - 1
    half, width, shard = x_ref.shape[0] // 2, x_ref.shape[1], w_ref.shape[0]
    below, above = level > 0, level < last

    barrier = pltpu.get_barrier_semaphore()
    pl.semaphore_signal(barrier, inc=1, device_id={"mdl": me ^ 1})
    pl.semaphore_signal(barrier, inc=1, device_id={"mdl": me ^ 2})
    pl.semaphore_signal(barrier, inc=1, device_id={"tok": tok ^ 1})

    @pl.when(below)
    def _():
        pl.semaphore_signal(barrier, inc=1, device_id={"tok": tok - 2})

    @pl.when(above)
    def _():
        pl.semaphore_signal(barrier, inc=1, device_id={"tok": tok + 2})

    pl.semaphore_wait(barrier, 3 + below.astype(jnp.int32) + above.astype(jnp.int32))

    def cols(block):
        return pl.ds(pl.multiple_of(block * width, 128), width)

    def block(index):
        return weight_ref.at[pl.ds(pl.multiple_of(index * shard, 16), shard)]

    def x_copy(source, target, at, to):
        return pltpu.make_async_remote_copy(
            source, target, x_sent.at[at], x_got.at[at], device_id={"mdl": me ^ to}
        )

    def w_copy(source, index, sent, to):
        return pltpu.make_async_remote_copy(
            source, block(index), sent, w_got.at[index], device_id={"tok": to}
        )

    mine = rows_ref.at[:, cols(me)]
    to_x, to_y = x_copy(x_ref, mine, 0, 1), x_copy(x_ref, mine, 1, 2)

    @pl.when(above)
    def _():
        w_copy(w_ref, tok, w_up.at[0], tok + 2).start()

    @pl.when(below)
    def _():
        w_copy(w_ref, tok, w_down.at[0], tok - 2).start()

    to_x.start()
    to_y.start()
    w_copy(w_ref, tok, w_core.at[tok], tok ^ 1).start()
    keep_x = pltpu.make_async_copy(x_ref, mine, own.at[0])
    keep_w = pltpu.make_async_copy(w_ref, block(tok), own.at[1])
    keep_x.start()
    keep_w.start()
    loads = [
        pltpu.make_async_copy(weight, to, own.at[2 + at])
        for at, (weight, to) in enumerate(zip(weights, held))
    ]
    for copy in loads:
        copy.start()
    for copy in loads:
        copy.wait()
    for (start, stop), out in zip(parts, joined):
        count = stop - start
        for at, source in enumerate(held):
            value = source[:, start:stop]
            if at < 2:
                value = (value.astype(F32) * gain_ref[...]).astype(BF16)
            out[:, at * count : (at + 1) * count] = value

    def relay(distance):
        low, high = tok - 2 * distance, tok + 2 * distance

        @pl.when(level >= distance)
        def _():
            w_copy(block(low), low, w_core.at[low], tok ^ 1).wait_recv()

            @pl.when(above)
            def _():
                w_copy(block(low), low, w_up.at[distance], tok + 2).start()

            w_copy(block(low), low, w_core.at[low], tok ^ 1).start()

        @pl.when(level + distance <= last)
        def _():
            w_copy(block(high), high, w_core.at[high], tok ^ 1).wait_recv()

            @pl.when(below)
            def _():
                w_copy(block(high), high, w_down.at[distance], tok - 2).start()

            w_copy(block(high), high, w_core.at[high], tok ^ 1).start()

    relay(1)
    stores = [
        pltpu.make_async_copy(out, to, own.at[5 + at])
        for at, (out, to) in enumerate(zip(joined, locals_ref))
    ]
    for copy in stores:
        copy.start()
    from_x = rows_ref.at[pl.ds(0, half), cols(me ^ 1)]
    from_y = rows_ref.at[pl.ds(half, half), cols(me ^ 2)]
    top, bottom = x_copy(from_x, from_x, 2, 2), x_copy(from_y, from_y, 3, 1)
    to_x.wait_recv()
    top.start()
    to_y.wait_recv()
    bottom.start()
    for distance in range(2, pairs):
        relay(distance)
    for copy in (keep_x, keep_w, *stores):
        copy.wait()
    for copy in (top, bottom):
        copy.wait_recv()
    for copy in (to_x, to_y, top, bottom):
        copy.wait_send()

    for distance in range(pairs):

        @pl.when((level >= distance) & above)
        def _(distance=distance):
            w_copy(block(tok), tok, w_up.at[distance], tok + 2).wait_send()

        @pl.when((level + distance <= last) & below)
        def _(distance=distance):
            w_copy(block(tok), tok, w_down.at[distance], tok - 2).wait_send()

        near, far = 2 * distance + tok % 2, 2 * distance + 1 - tok % 2
        w_copy(block(near), near, w_core.at[near], tok ^ 1).wait_send()
        w_copy(block(far), far, w_core.at[near], tok ^ 1).wait_recv()


def first_gather(inputs, weight, gain, weights, parts):
    tokens, width = inputs.shape
    shard, cols = weight.shape
    pairs = lax.axis_size("tok") // 2
    dma = pltpu.SemaphoreType.DMA
    locals_ff = [(shard, 3 * (stop - start)) for start, stop in parts]
    shapes = [(tokens, 4 * width), (2 * pairs * shard, cols), *locals_ff]
    *gathered, first, second = pl.pallas_call(
        functools.partial(first_kernel, parts),
        out_shape=[jax.ShapeDtypeStruct(shape, BF16) for shape in shapes],
        in_specs=[pl.BlockSpec(memory_space=pltpu.VMEM)] * 3
        + [pl.BlockSpec(memory_space=pl.ANY)] * 3,
        out_specs=[pl.BlockSpec(memory_space=pl.ANY)] * 4,
        scratch_shapes=[pltpu.VMEM(array.shape, BF16) for array in weights]
        + [pltpu.VMEM(shape, BF16) for shape in locals_ff]
        + [
            dma((7,)), dma((4,)), dma((4,)), dma((pairs,)), dma((pairs,)),
            dma((2 * pairs,)), dma((2 * pairs,)),
        ],
        compiler_params=pltpu.CompilerParams(
            collective_id=0, has_side_effects=True, vmem_limit_bytes=60 << 20
        ),
    )(inputs, weight, gain, *weights)
    return *gathered, (first, second)


def in_order(mebibytes):
    return pltpu.CompilerParams(
        dimension_semantics=(pltpu.ARBITRARY,), vmem_limit_bytes=mebibytes << 20
    )


def cost(flops, bytes_accessed, transcendentals=0):
    return pl.CostEstimate(
        flops=flops, bytes_accessed=bytes_accessed, transcendentals=transcendentals
    )


def turn(vector, cos, sin):
    half = HEAD // 2
    lower, upper = vector[:, :half], vector[:, half:]
    return jnp.concatenate([lower * cos - upper * sin, upper * cos + lower * sin], axis=1)


def unturn(vector, cos, sin):
    half = HEAD // 2
    lower, upper = vector[:, :half], vector[:, half:]
    return jnp.concatenate([lower * cos + upper * sin, upper * cos - lower * sin], axis=1)


def seen(first_ref, position_ref, queries, keys):
    row = lax.broadcasted_iota(jnp.int32, (queries, keys), 0) + first_ref[0]
    distance = row - lax.broadcasted_iota(jnp.int32, (queries, keys), 1)
    return (distance >= 0) & (distance <= position_ref[...])


def forward_kernel(
    first_ref, q_ref, kv_ref, cos_ref, sin_ref, pos_ref, scale_ref, out_ref, norm_ref
):
    query = turn(q_ref[...].astype(F32) * scale_ref[...], cos_ref[...], sin_ref[...])
    query = (query * HEAD ** (-0.5)).astype(BF16)
    keys, values = kv_ref[:, :HEAD], kv_ref[:, HEAD:]
    scores = nt(query, keys)
    scores = jnp.where(seen(first_ref, pos_ref, *scores.shape), scores, MASKED)
    top = jnp.max(scores, axis=1, keepdims=True)
    weights = jnp.exp(scores - top)
    total = jnp.sum(weights, axis=1, keepdims=True)
    out_ref[...] = (nn(weights.astype(BF16), values) / total).astype(BF16)
    norm_ref[0] = top + jnp.log(total)


def backward_kernel(
    first_ref, q_ref, kv_ref, cos_ref, sin_ref, pos_ref, scale_ref, att_ref, datt_ref, norm_ref,
    dq_ref, dkv_ref,
):
    head = pl.program_id(0)
    scale = HEAD ** (-0.5)
    cos, sin = cos_ref[...], sin_ref[...]
    query = (turn(q_ref[...].astype(F32) * scale_ref[...], cos, sin) * scale).astype(BF16)
    keys, values = kv_ref[:, :HEAD], kv_ref[:, HEAD:]
    scores = nt(query, keys)
    visible = seen(first_ref, pos_ref, *scores.shape)
    again = jnp.where(visible, jnp.exp(scores - norm_ref[0]), 0.0)
    d_att = datt_ref[...]
    delta = jnp.sum(d_att.astype(F32) * att_ref[...].astype(F32), axis=1, keepdims=True)
    d_scores = (again * (nt(d_att, values) - delta)).astype(BF16)
    d_query = nn(d_scores, keys) * scale
    dq_ref[...] = unturn(d_query, cos, sin).astype(BF16)

    @pl.when(head == 0)
    def _():
        dkv_ref[...] = jnp.zeros_like(dkv_ref)

    dkv_ref[:, :HEAD] += tn(d_scores, query)
    dkv_ref[:, HEAD:] += tn(again.astype(BF16), d_att)


def whole_spec(shape):
    return pl.BlockSpec(shape, lambda head: (0,) * len(shape))


def attention_forward(first, qkv, kv, cos, sin, pos, scale):
    rows, keys = qkv.shape[0], kv.shape[0]
    head_spec = pl.BlockSpec((rows, HEAD), lambda head: (0, head))
    return pl.pallas_call(
        forward_kernel,
        grid=(HEADS,),
        out_shape=(
            jax.ShapeDtypeStruct((rows, HEADS * HEAD), BF16),
            jax.ShapeDtypeStruct((HEADS, rows, 1), F32),
        ),
        in_specs=[
            pl.BlockSpec(memory_space=pltpu.SMEM),
            head_spec,
            whole_spec((keys, 2 * HEAD)),
            whole_spec((rows, HEAD // 2)),
            whole_spec((rows, HEAD // 2)),
            whole_spec((rows, 1)),
            whole_spec((rows, 1)),
        ],
        out_specs=(head_spec, pl.BlockSpec((1, rows, 1), lambda head: (head, 0, 0))),
        compiler_params=in_order(32),
        cost_estimate=cost(4 * rows * keys * HEADS * HEAD, 4 * rows * HEADS * HEAD + 4 * keys * HEAD, rows * keys * HEADS),
        name="att_f",
    )(first, qkv, kv, cos, sin, pos, scale)


def attention_backward(first, qkv, kv, cos, sin, pos, scale, att, d_att, norm):
    rows, keys = qkv.shape[0], kv.shape[0]
    head_spec = pl.BlockSpec((rows, HEAD), lambda head: (0, head))
    return pl.pallas_call(
        backward_kernel,
        grid=(HEADS,),
        out_shape=(
            jax.ShapeDtypeStruct((rows, HEADS * HEAD), BF16),
            jax.ShapeDtypeStruct((keys, 2 * HEAD), F32),
        ),
        in_specs=[
            pl.BlockSpec(memory_space=pltpu.SMEM),
            head_spec,
            whole_spec((keys, 2 * HEAD)),
            whole_spec((rows, HEAD // 2)),
            whole_spec((rows, HEAD // 2)),
            whole_spec((rows, 1)),
            whole_spec((rows, 1)),
            head_spec,
            head_spec,
            pl.BlockSpec((1, rows, 1), lambda head: (head, 0, 0)),
        ],
        out_specs=(head_spec, whole_spec((keys, 2 * HEAD))),
        compiler_params=in_order(40),
        cost_estimate=cost(10 * rows * keys * HEADS * HEAD, 8 * rows * HEADS * HEAD + 12 * keys * HEAD, rows * keys * HEADS),
        name="att_b",
    )(first, qkv, kv, cos, sin, pos, scale, att, d_att, norm)


def keep_half(core_ref, total, kept, sent):
    half = total.shape[0] // 2
    for core, (first, second) in enumerate(((kept, sent), (sent, kept))):

        @pl.when(core_ref[0] == core)
        def _(first=first, second=second):
            first[...] = total[:half]
            second[...] = total[half:]


def pair_kernel(core_ref, left_ref, right_ref, *refs):
    total = tn(left_ref[...], right_ref[...])
    if len(refs) == 4:
        weight = refs[0][:, : total.shape[1]].astype(F32)
        refs[3][...] = jnp.sum(total * weight, axis=1, keepdims=True)
    keep_half(core_ref, total.astype(BF16), *refs[-3:-1] if len(refs) == 4 else refs)


def split_pairs(total, pairs, core):
    rows, cols = total.shape
    total = total.reshape(pairs, 2, rows // pairs // 2, cols)
    return tuple(
        lax.dynamic_index_in_dim(total, index, 1, False).reshape(-1, cols)
        for index in (core, 1 - core)
    )


def core_index():
    return (lax.axis_index("tok") % 2).astype(jnp.int32).reshape(1)


def pair_grad(left, right, weight=None):
    tokens, rows = left.shape
    cols = right.shape[1]
    pairs = lax.axis_size("tok") // 2
    step = rows // pairs
    if step % 128 or cols % 128:
        total = tn(left, right)
        halves = split_pairs(total.astype(BF16), pairs, lax.axis_index("tok") % 2)
        if weight is None:
            return halves
        return *halves, jnp.sum(total * weight[:, :cols].astype(F32), axis=1, keepdims=True)
    out_shape = [jax.ShapeDtypeStruct((rows // 2, cols), BF16)] * 2
    out_specs = [pl.BlockSpec((step // 2, cols), lambda pair: (pair, 0))] * 2
    in_specs = [
        pl.BlockSpec(memory_space=pltpu.SMEM),
        pl.BlockSpec((tokens, step), lambda pair: (0, pair)),
        pl.BlockSpec((tokens, cols), lambda pair: (0, 0)),
    ]
    operands = [core_index(), left, right]
    if weight is not None:
        operands.append(weight)
        in_specs.append(pl.BlockSpec((step, weight.shape[1]), lambda pair: (pair, 0)))
        out_shape.append(jax.ShapeDtypeStruct((rows, 1), F32))
        out_specs.append(pl.BlockSpec((step, 1), lambda pair: (pair, 0)))
    return pl.pallas_call(
        pair_kernel,
        grid=(pairs,),
        out_shape=out_shape,
        in_specs=in_specs,
        out_specs=out_specs,
        compiler_params=in_order(48),
        cost_estimate=cost(2 * tokens * rows * cols, 2 * (tokens * (rows + cols) + rows * cols)),
    )(*operands)


def part_kernel(core_ref, rows_ref, above_ref, d_gate_ref, d_up_ref, hidden_ref, kept, sent):
    cols = hidden_ref.shape[1]
    for at, (left_ref, right_ref) in enumerate(
        ((rows_ref, d_gate_ref), (rows_ref, d_up_ref), (above_ref, hidden_ref))
    ):
        total = tn(left_ref[...], right_ref[...]).astype(BF16)
        window = (slice(None), pl.ds(at * cols, cols))
        keep_half(core_ref, total, kept.at[window], sent.at[window])


def part_grad(rows, above, d_gate, d_up, hidden):
    tokens, features = rows.shape
    cols = hidden.shape[1]
    pairs = lax.axis_size("tok") // 2
    step = features // pairs
    if step % 128 or cols % 128:
        total = [tn(rows, d_gate), tn(rows, d_up), tn(above, hidden)]
        total = jnp.concatenate(total, axis=1).astype(BF16)
        return split_pairs(total, pairs, lax.axis_index("tok") % 2)
    out = jax.ShapeDtypeStruct((features // 2, 3 * cols), BF16)
    left_spec = pl.BlockSpec((tokens, step), lambda pair: (0, pair))
    right_spec = pl.BlockSpec((tokens, cols), lambda pair: (0, 0))
    return pl.pallas_call(
        part_kernel,
        grid=(pairs,),
        out_shape=(out, out),
        in_specs=[pl.BlockSpec(memory_space=pltpu.SMEM)] + [left_spec] * 2 + [right_spec] * 3,
        out_specs=[pl.BlockSpec((step // 2, 3 * cols), lambda pair: (pair, 0))] * 2,
        compiler_params=in_order(48),
        cost_estimate=cost(
            6 * tokens * features * cols,
            2 * (2 * tokens * features + 3 * cols * (tokens + features)),
        ),
    )(core_index(), rows, above, d_gate, d_up, hidden)


def pieces_grad_kernel(me_ref, core_ref, own, along_x, along_y, top, bottom, right_ref, kept, sent):
    at = pl.program_id(0)
    half = top.shape[0]
    for index, piece in enumerate((own, along_x, along_y)):

        @pl.when(at == index)
        def _(piece=piece):
            keep_half(core_ref, tn(piece[...], right_ref[...]).astype(BF16), kept, sent)

    @pl.when(at == 3)
    def _():
        total = tn(top[...], right_ref[:half]) + tn(bottom[...], right_ref[half:])
        keep_half(core_ref, total.astype(BF16), kept, sent)


def pieces_grad(pieces, right):
    tokens, step = pieces[0].shape
    cols = right.shape[1]
    me = lax.axis_index("mdl").astype(jnp.int32).reshape(1)
    out = jax.ShapeDtypeStruct((2 * step, cols), BF16)
    return pl.pallas_call(
        pieces_grad_kernel,
        grid_spec=pltpu.PrefetchScalarGridSpec(
            num_scalar_prefetch=2,
            grid=(4,),
            in_specs=[
                pl.BlockSpec(array.shape, lambda at, me_ref, core_ref: (0, 0))
                for array in (*pieces, right)
            ],
            out_specs=[
                pl.BlockSpec((step // 2, cols), lambda at, me_ref, core_ref: (me_ref[0] ^ at, 0))
            ]
            * 2,
        ),
        out_shape=(out, out),
        compiler_params=in_order(48),
        cost_estimate=cost(8 * tokens * step * cols, 2 * (4 * tokens * step + 5 * step * cols)),
    )(me, core_index(), *pieces, right)


def sum_kernel(starts, *refs):
    *lefts, weight_ref, out_ref = refs
    total = 0.0
    for left_ref, start in zip(lefts, starts):
        total += nt(left_ref[...], weight_ref[:, start : start + left_ref.shape[1]])
    out_ref[...] = total


def sum_products(lefts, weight, starts):
    tokens = lefts[0].shape[0]
    rows, cols = weight.shape
    if lefts[0].shape[1] % 128:
        return sum(
            nt(left, weight[:, start : start + left.shape[1]])
            for left, start in zip(lefts, starts)
        )
    step = 512
    depth = sum(left.shape[1] for left in lefts)
    return pl.pallas_call(
        functools.partial(sum_kernel, starts),
        grid=(rows // step,),
        out_shape=jax.ShapeDtypeStruct((tokens, rows), F32),
        in_specs=[pl.BlockSpec(left.shape, lambda row: (0, 0)) for left in lefts]
        + [pl.BlockSpec((step, cols), lambda row: (row, 0))],
        out_specs=pl.BlockSpec((tokens, step), lambda row: (0, row)),
        compiler_params=in_order(48),
        cost_estimate=cost(2 * tokens * rows * depth, 2 * rows * cols + 4 * tokens * rows),
    )(*lefts, weight)


def payload_kernel(starts, me_ref, *refs):
    lefts, weight_ref = refs[: len(starts)], refs[len(starts)]
    top_sent, bottom_sent, top_kept, bottom_kept = refs[-4:]
    total = refs[-5][...] if len(refs) == len(starts) + 6 else 0.0
    for left_ref, start in zip(lefts, starts):
        total += nt(left_ref[...], weight_ref[:, start : start + left_ref.shape[1]])
    total = total.astype(BF16)
    half = total.shape[0] // 2
    places = (
        ((top_kept, 0), (bottom_kept, 0)),
        ((top_sent, 0), (bottom_kept, 1)),
        ((top_kept, 1), (bottom_sent, 0)),
        ((top_sent, 1), (bottom_sent, 1)),
    )
    for distance, ((top, top_at), (bottom, bottom_at)) in enumerate(places):

        @pl.when(pl.program_id(0) == 3 - distance)
        def _(top=top, top_at=top_at, bottom=bottom, bottom_at=bottom_at):
            top[top_at] = total[:half]
            bottom[bottom_at] = total[half:]


def scatter_product(lefts, weight, starts, partial=()):
    tokens = lefts[0].shape[0]
    rows, cols = weight.shape
    step = rows // 4
    me = lax.axis_index("mdl").astype(jnp.int32).reshape(1)
    out = jax.ShapeDtypeStruct((2, tokens // 2, step), BF16)
    depth = sum(left.shape[1] for left in lefts)
    return pl.pallas_call(
        functools.partial(payload_kernel, starts),
        grid_spec=pltpu.PrefetchScalarGridSpec(
            num_scalar_prefetch=1,
            grid=(4,),
            in_specs=[pl.BlockSpec(left.shape, lambda at, me_ref: (0, 0)) for left in lefts]
            + [pl.BlockSpec((step, cols), lambda at, me_ref: (me_ref[0] ^ (3 - at), 0))]
            + [pl.BlockSpec((tokens, step), lambda at, me_ref: (0, me_ref[0] ^ (3 - at)))]
            * len(partial),
            out_specs=[pl.BlockSpec(out.shape, lambda at, me_ref: (0, 0, 0))] * 4,
        ),
        out_shape=(out,) * 4,
        compiler_params=in_order(48),
        cost_estimate=cost(2 * tokens * rows * depth, 2 * (tokens * depth + rows * cols + tokens * rows)),
    )(me, *lefts, weight, *partial)


def pieces_kernel(start, me_ref, own, along_x, along_y, top, bottom, weight_ref, out_ref, total):
    at = pl.program_id(0)
    width = out_ref.shape[1]
    half = top.shape[0]
    for index, piece in enumerate((own, along_x, along_y)):

        @pl.when(at == index)
        def _(index=index, piece=piece):
            part = nn(piece[...], weight_ref[:, start : start + width])
            if index:
                total[...] += part
            else:
                total[...] = part

    @pl.when(at == 3)
    def _():
        weight = weight_ref[:, start : start + width]
        out_ref[:half] = (total[:half] + nn(top[...], weight)).astype(BF16)
        out_ref[half:] = (total[half:] + nn(bottom[...], weight)).astype(BF16)


def pieces_product(pieces, weight, start, width):
    tokens, step = pieces[0].shape
    rows, cols = weight.shape
    me = lax.axis_index("mdl").astype(jnp.int32).reshape(1)
    return pl.pallas_call(
        functools.partial(pieces_kernel, start),
        grid_spec=pltpu.PrefetchScalarGridSpec(
            num_scalar_prefetch=1,
            grid=(4,),
            in_specs=[pl.BlockSpec(piece.shape, lambda at, me_ref: (0, 0)) for piece in pieces]
            + [pl.BlockSpec((step, cols), lambda at, me_ref: (me_ref[0] ^ at, 0))],
            out_specs=pl.BlockSpec((tokens, width), lambda at, me_ref: (0, 0)),
            scratch_shapes=[pltpu.VMEM((tokens, width), F32)],
        ),
        out_shape=jax.ShapeDtypeStruct((tokens, width), BF16),
        compiler_params=in_order(40),
        cost_estimate=cost(2 * tokens * rows * width, 2 * (tokens * rows + rows * cols + tokens * width)),
    )(me, *pieces, weight)


def product_to_mdl(lefts, weight, starts, partial=()):
    if lax.axis_size("mdl") == 4:
        payload = scatter_product(lefts, weight, starts, partial)
        return payload, lambda payload, *earlier: scatter_payload(payload, *earlier)
    part = sum((sum_products(lefts, weight, starts), *partial))
    return (part.astype(BF16),), lambda payload, *earlier: scatter_mdl(payload[0], 1)


def after(value, *earlier):
    return lax.optimization_barrier((value, *earlier))[0]


def row_scale(rows_b, axis=-1):
    rows = rows_b.astype(F32)
    return lax.rsqrt(jnp.mean(rows * rows, axis=axis, keepdims=True) + NORM_EPS)


def gelu_parts(value):
    root = math.sqrt(2.0 / math.pi)
    square = value * value
    tanh = jnp.tanh(root * (value + 0.044715 * value * square))
    cdf = 0.5 * (1.0 + tanh)
    slope = cdf + 0.5 * value * (1.0 - tanh * tanh) * root * (1.0 + 3 * 0.044715 * square)
    return value * cdf, slope


def scaled(weight, gain):
    return (weight.astype(F32) * gain.astype(F32)[:, None]).astype(BF16)


def on_device(
    inputs, positions, norm1_gain, qkv_weight, out_weight, norm2_gain, gate_weight,
    up_weight, down_weight, cotangent,
):
    me = lax.axis_index("mdl")
    size = lax.axis_size("mdl")
    head_cols = HEADS * HEAD
    width = inputs.shape[1]
    features = width * size

    def from_tok(weight, dim):
        return lax.all_gather(weight, "tok", axis=dim, tiled=True)

    def pair_to_tok(local):
        kept, sent = local
        count = lax.axis_size("tok")
        got = lax.ppermute(sent, "tok", [(i, i ^ 1) for i in range(count)])
        both = (kept.astype(F32) + got.astype(F32)).astype(BF16)
        groups = [list(range(core, count, 2)) for core in range(2)]
        total = lax.psum_scatter(
            both, "tok", scatter_dimension=0, tiled=True, axis_index_groups=groups
        )
        return total.astype(F32)

    qkv_cols, ff_cols = qkv_weight.shape[1], gate_weight.shape[1]
    attn_local = jnp.concatenate([scaled(qkv_weight, norm1_gain), out_weight.T], axis=1)
    middle = ff_cols // 256 * 128
    parts = ((0, middle), (middle, ff_cols))
    if size == 4 and lax.axis_size("tok") == 8:
        rows_in, w_attn, locals_ff = first_gather(
            inputs,
            attn_local,
            norm2_gain.astype(F32)[:, None],
            (gate_weight, up_weight, down_weight.T),
            parts,
        )
    else:
        rows_in = gather_mdl(inputs, 1)
        w_attn = from_tok(attn_local, 0)
        scaled_gu = [scaled(weight, norm2_gain) for weight in (gate_weight, up_weight)]
        locals_ff = [
            jnp.concatenate([w[:, start:stop] for w in (*scaled_gu, down_weight.T)], axis=1)
            for start, stop in parts
        ]
    w_qkv = w_attn[:, :qkv_cols]
    w_parts = [from_tok(local, 0) for local in locals_ff]

    qkv = rows_to_cols(nn(rows_in, w_qkv).astype(BF16))
    count = qkv.shape[0]
    scale_own = row_scale(lax.dynamic_slice_in_dim(rows_in, me * count, count, 0))
    scale_one = row_scale(after(rows_in, qkv))
    half = HEAD // 2
    frequency = jnp.exp(jnp.arange(half, dtype=F32) * (-2.0 * math.log(10000.0) / HEAD))
    angles = positions.astype(F32)[:, None] * frequency[None, :]
    cos, sin = jnp.cos(angles), jnp.sin(angles)
    kv_own = qkv[:, head_cols:].astype(F32) * scale_own
    key_rows = turn(kv_own[:, :HEAD], cos, sin)
    kv = gather_mdl(jnp.concatenate([key_rows, kv_own[:, HEAD:]], axis=1).astype(BF16), 0)
    first = (me * count).astype(jnp.int32).reshape(1)
    pos = positions[:, None]
    attended, log_norm = attention_forward(first, qkv, kv, cos, sin, pos, scale_own)
    head_block = cols_to_rows(attended)
    residual = inputs.astype(F32)
    payload, scatter = product_to_mdl((head_block,), w_attn, (qkv_cols,))
    mixed = residual + scatter(payload)

    rows_two = gather_mdl(mixed.astype(BF16), 1)
    scale_two = row_scale(rows_two)
    rows_hat = (rows_two.astype(F32) * scale_two).astype(BF16)
    rows, above, stat_two, partial, hiddens, sums = rows_hat, cotangent, 0.0, (), [], []
    for index, (weight, (start, stop)) in enumerate(zip(w_parts, parts)):
        cols = stop - start
        last = index == len(parts) - 1
        gate_in = nn(rows, weight[:, :cols])
        up_in = nn(rows, weight[:, cols : 2 * cols])
        d_hidden = nn(above, weight[:, 2 * cols :])
        gelu, slope = gelu_parts(gate_in)
        hidden = (gelu * up_in).astype(BF16)
        d_gate = d_hidden * up_in * slope
        d_up = d_hidden * gelu
        stat_two += jnp.sum(d_gate * gate_in + d_up * up_in, axis=1)
        d_gate, d_up = d_gate.astype(BF16), d_up.astype(BF16)
        hiddens.append(hidden)
        lefts, starts = (d_gate, d_up), (0, cols)
        if last:
            payload, scatter = product_to_mdl(lefts, weight, starts, partial)
            rows, above, _ = lax.optimization_barrier((rows, above, payload[0]))
        local = part_grad(rows, above, d_gate, d_up, hidden)
        if not last:
            d_gate = after(d_gate, local[0])
            partial = (sum_products((d_gate, d_up), weight, starts),)
            rows, above, _ = lax.optimization_barrier((rows, above, local[0]))
        sums.append(pair_to_tok(local))
    d_two = scatter(payload)
    stat_two = sum_mdl(stat_two.reshape(8, -1)).reshape(-1, 1) * (1.0 / features)
    scale_mixed = scale_two * mixed
    cotangent_own = lax.dynamic_slice_in_dim(cotangent, me * width, width, 1).astype(F32)
    d_mixed = cotangent_own + scale_two * (d_two - scale_mixed * stat_two)

    d_mixed_b = after(d_mixed.astype(BF16), local[0])
    down_starts = tuple(2 * (stop - start) for start, stop in parts)
    ffn = (sum_products((after(hiddens[0], d_mixed_b),), w_parts[0], down_starts[:1]),)
    ffn_payload, ffn_scatter = product_to_mdl(
        (after(hiddens[1], d_mixed_b),), w_parts[1], down_starts[1:], ffn
    )
    if size == 4 and lax.axis_size("tok") == 8:
        pieces = gather_pieces(d_mixed_b)
        d_head = pieces_product(pieces, w_attn, qkv_cols, head_block.shape[1])
        heads_later = after(head_block, d_head)
        out_local = pieces_grad(pieces, heads_later)
    else:
        d_mixed_rows = gather_mdl(d_mixed_b, 1)
        d_head = nn(d_mixed_rows, w_attn[:, qkv_cols:]).astype(BF16)
        out_local = pair_grad(d_mixed_rows, head_block)
    out_grad = pair_to_tok(out_local)
    d_attended = rows_to_cols(d_head)
    d_query, d_kv = attention_backward(
        first, qkv, kv, cos, sin, pos, scale_own, attended, d_attended, log_norm
    )
    d_kv = scatter_mdl(d_kv.astype(BF16), 0)
    d_key = unturn(d_kv[:, :HEAD], cos, sin).astype(BF16)
    d_qkv = jnp.concatenate([d_query, d_key, d_kv[:, HEAD:].astype(BF16)], axis=1)
    stat_one = jnp.sum(d_qkv.astype(F32) * qkv.astype(F32), axis=1) * scale_own[:, 0]
    d_qkv_part = cols_to_rows(d_qkv)
    stat_rows = jnp.zeros((size, count), F32)
    stat_rows = sum_mdl(lax.dynamic_update_slice(stat_rows, stat_one[None], (me, 0)))
    stat_one = stat_rows.reshape(-1, 1) * (1.0 / features)
    payload, scatter = product_to_mdl((d_qkv_part,), w_attn, (0,))
    d_scaled = (after(d_qkv_part, payload[0]).astype(F32) * scale_one).astype(BF16)
    *qkv_local, gain_one = pair_grad(rows_in, d_scaled, w_attn)
    qkv_sum = pair_to_tok(qkv_local)
    d_one = scatter(payload)
    ffn_sum = ffn_scatter(ffn_payload, d_qkv_part)
    block_out = (mixed + ffn_sum).astype(BF16)
    input_grad = d_mixed + scale_one * (d_one - (scale_one * residual) * stat_one)

    norm1_late, norm2_late, gate_late, up_late, _ = lax.optimization_barrier(
        (norm1_gain, norm2_gain, gate_weight, up_weight, local[0])
    )

    def unfold(total, gain):
        return total * gain.astype(F32)[:, None]

    def joined(at):
        widths = [total.shape[1] // 3 for total in sums]
        pieces = [total[:, at * cols :][:, :cols] for total, cols in zip(sums, widths)]
        return jnp.concatenate(pieces, axis=1)

    gate_sum, up_sum, down_grad = joined(0), joined(1), joined(2).T
    gain_two = jnp.sum(
        gate_late.astype(F32) * gate_sum + up_late.astype(F32) * up_sum, axis=1
    )
    gate_grad, up_grad = unfold(gate_sum, norm2_late), unfold(up_sum, norm2_late)
    out_grad = out_grad.T
    gain_two_grad = sum_mdl(gain_two)
    gain_one = sum_mdl(sum_tok(gain_one.reshape(8, -1))).reshape(-1)
    shard = norm1_gain.shape[0]
    gain_one = lax.dynamic_slice_in_dim(gain_one, lax.axis_index("tok") * shard, shard, 0)
    gain_one_grad = gain_one / norm1_late.astype(F32)
    return (
        block_out,
        input_grad,
        gain_one_grad,
        unfold(qkv_sum, norm1_late),
        out_grad,
        gain_two_grad,
        gate_grad,
        up_grad,
        down_grad,
    )


def solution(mesh):
    return jax.shard_map(
        on_device,
        mesh=mesh,
        in_specs=(
            P("tok", "mdl"),
            P(("tok", "mdl")),
            P("tok"),
            P("tok", "mdl"),
            P("mdl", "tok"),
            P("tok"),
            P("tok", "mdl"),
            P("tok", "mdl"),
            P("mdl", "tok"),
            P("tok", None),
        ),
        out_specs=(
            P("tok", "mdl"),
            P("tok", "mdl"),
            P("tok"),
            P("tok", "mdl"),
            P("mdl", "tok"),
            P("tok"),
            P("tok", "mdl"),
            P("tok", "mdl"),
            P("mdl", "tok"),
        ),
        check_vma=False,
    )
```

```python
import functools
import math

import jax
import jax.numpy as jnp
from jax import lax
from jax.experimental import pallas as pl
from jax.experimental.pallas import tpu as pltpu
from jax.sharding import PartitionSpec as P


HEADS = 10
HEAD = 256
NORM_EPS = 1e-06
F32 = jnp.float32
BF16 = jnp.bfloat16
MASKED = -1e30


def nt(left_op, right_op):
    return lax.dot_general(
        left_op, right_op, (((1,), (1,)), ((), ())), preferred_element_type=F32
    )


def tn(left_op, right_op):
    return lax.dot_general(
        left_op, right_op, (((0,), (0,)), ((), ())), preferred_element_type=F32
    )


def nn(left_op, right_op):
    return jnp.dot(left_op, right_op, preferred_element_type=F32)


def swap(block, distance):
    size = lax.axis_size("mdl")
    return lax.ppermute(block, "mdl", [(i, i ^ distance) for i in range(size)])


def gather_mdl(block, dim):
    size = lax.axis_size("mdl")
    if size != 4:
        return lax.all_gather(block, "mdl", axis=dim, tiled=True)
    me = lax.axis_index("mdl")
    half = block.shape[0] // 2
    along_x = swap(block, 1)
    along_y = swap(block, 2)
    top = swap(along_x[:half], 2)
    bottom = swap(along_y[half:], 1)
    width = block.shape[dim]
    shape = list(block.shape)
    shape[dim] = width * size
    whole = jnp.zeros(shape, block.dtype)

    def put(whole, piece, source, row):
        start = [0, 0]
        start[dim] = source * width
        start[0] = start[0] + row
        return lax.dynamic_update_slice(whole, piece, tuple(start))

    whole = put(whole, block, me, 0)
    whole = put(whole, along_x, me ^ 1, 0)
    whole = put(whole, along_y, me ^ 2, 0)
    whole = put(whole, top, me ^ 3, 0)
    whole = put(whole, bottom, me ^ 3, half)
    return whole


def scatter_mdl(part, dim):
    size = lax.axis_size("mdl")
    if size != 4:
        return lax.psum_scatter(part, "mdl", scatter_dimension=dim, tiled=True).astype(F32)
    me = lax.axis_index("mdl")
    shape = list(part.shape)
    shape[dim] //= size
    half = shape[0] // 2

    def piece(block, row):
        start = [0, 0]
        start[dim] = block * shape[dim]
        start[0] = start[0] + row
        return lax.dynamic_slice(part, tuple(start), (half, shape[1]))

    sums = []
    for row, first, second in ((0, 1, 2), (half, 2, 1)):
        sent = jnp.stack([piece(me ^ first, row), piece(me ^ 3, row)])
        sums.append((row, second, swap(sent, first)))
    partial = []
    for row, second, got in sums:
        other = piece(me ^ second, row).astype(F32) + got[1].astype(F32)
        partial.append((row, got[0], swap(other.astype(BF16), second)))
    return jnp.concatenate(
        [
            piece(me, row).astype(F32) + first.astype(F32) + second.astype(F32)
            for row, first, second in partial
        ],
        axis=0,
    )


def gather_pieces(block):
    half = block.shape[0] // 2
    along_x = swap(block, 1)
    along_y = swap(block, 2)
    top = swap(along_x[:half], 2)
    bottom = swap(along_y[half:], 1)
    return block, along_x, along_y, top, bottom


def scatter_payload(payload, *earlier):
    top_sent, bottom_sent, top_kept, bottom_kept = payload
    got_top = swap(top_sent, 1)
    got_bottom = swap(bottom_sent, 2)
    halves = []
    for kept, got, second in ((top_kept, got_top, 2), (bottom_kept, got_bottom, 1)):
        passed = (kept[1].astype(F32) + got[1].astype(F32)).astype(BF16)
        if earlier:
            passed = after(passed, *earlier)
        last = swap(passed, second)
        halves.append(kept[0].astype(F32) + got[0].astype(F32) + last.astype(F32))
    return jnp.concatenate(halves, axis=0)


def sum_mdl(value):
    size = lax.axis_size("mdl")
    distance = 1
    while distance < size:
        value = value + swap(value, distance)
        distance *= 2
    return value


def sum_tok(value):
    size = lax.axis_size("tok")
    distance = 1
    while distance < size:
        value = value + lax.ppermute(value, "tok", [(i, i ^ distance) for i in range(size)])
        distance *= 2
    return value


def rows_to_cols(block):
    return lax.all_to_all(block, "mdl", split_axis=0, concat_axis=1, tiled=True)


def cols_to_rows(block):
    return lax.all_to_all(block, "mdl", split_axis=1, concat_axis=0, tiled=True)


def first_kernel(
    parts, x_ref, w_ref, gain_ref, *refs
):
    weights, (rows_ref, weight_ref), locals_ref = refs[:3], refs[3:5], refs[5:7]
    held, joined = refs[7:10], refs[10:12]
    own, x_sent, x_got, w_up, w_down, w_core, w_got = refs[12:]
    me, tok = lax.axis_index("mdl"), lax.axis_index("tok")
    pairs = lax.axis_size("tok") // 2
    level, last = tok // 2, pairs - 1
    half, width, shard = x_ref.shape[0] // 2, x_ref.shape[1], w_ref.shape[0]
    below, above = level > 0, level < last

    barrier = pltpu.get_barrier_semaphore()
    pl.semaphore_signal(barrier, inc=1, device_id={"mdl": me ^ 1})
    pl.semaphore_signal(barrier, inc=1, device_id={"mdl": me ^ 2})
    pl.semaphore_signal(barrier, inc=1, device_id={"tok": tok ^ 1})

    @pl.when(below)
    def _():
        pl.semaphore_signal(barrier, inc=1, device_id={"tok": tok - 2})

    @pl.when(above)
    def _():
        pl.semaphore_signal(barrier, inc=1, device_id={"tok": tok + 2})

    pl.semaphore_wait(barrier, 3 + below.astype(jnp.int32) + above.astype(jnp.int32))

    def cols(block):
        return pl.ds(pl.multiple_of(block * width, 128), width)

    def block(index):
        return weight_ref.at[pl.ds(pl.multiple_of(index * shard, 16), shard)]

    def x_copy(source, target, at, to):
        return pltpu.make_async_remote_copy(
            source, target, x_sent.at[at], x_got.at[at], device_id={"mdl": me ^ to}
        )

    def w_copy(source, index, sent, to):
        return pltpu.make_async_remote_copy(
            source, block(index), sent, w_got.at[index], device_id={"tok": to}
        )

    mine = rows_ref.at[:, cols(me)]
    to_x, to_y = x_copy(x_ref, mine, 0, 1), x_copy(x_ref, mine, 1, 2)

    @pl.when(above)
    def _():
        w_copy(w_ref, tok, w_up.at[0], tok + 2).start()

    @pl.when(below)
    def _():
        w_copy(w_ref, tok, w_down.at[0], tok - 2).start()

    to_x.start()
    to_y.start()
    w_copy(w_ref, tok, w_core.at[tok], tok ^ 1).start()
    keep_x = pltpu.make_async_copy(x_ref, mine, own.at[0])
    keep_w = pltpu.make_async_copy(w_ref, block(tok), own.at[1])
    keep_x.start()
    keep_w.start()
    loads = [
        pltpu.make_async_copy(weight, to, own.at[2 + at])
        for at, (weight, to) in enumerate(zip(weights, held))
    ]
    for copy in loads:
        copy.start()
    for copy in loads:
        copy.wait()
    for (start, stop), out in zip(parts, joined):
        count = stop - start
        for at, source in enumerate(held):
            value = source[:, start:stop]
            if at < 2:
                value = (value.astype(F32) * gain_ref[...]).astype(BF16)
            out[:, at * count : (at + 1) * count] = value

    def relay(distance):
        low, high = tok - 2 * distance, tok + 2 * distance

        @pl.when(level >= distance)
        def _():
            w_copy(block(low), low, w_core.at[low], tok ^ 1).wait_recv()

            @pl.when(above)
            def _():
                w_copy(block(low), low, w_up.at[distance], tok + 2).start()

            w_copy(block(low), low, w_core.at[low], tok ^ 1).start()

        @pl.when(level + distance <= last)
        def _():
            w_copy(block(high), high, w_core.at[high], tok ^ 1).wait_recv()

            @pl.when(below)
            def _():
                w_copy(block(high), high, w_down.at[distance], tok - 2).start()

            w_copy(block(high), high, w_core.at[high], tok ^ 1).start()

    relay(1)
    stores = [
        pltpu.make_async_copy(out, to, own.at[5 + at])
        for at, (out, to) in enumerate(zip(joined, locals_ref))
    ]
    for copy in stores:
        copy.start()
    from_x = rows_ref.at[pl.ds(0, half), cols(me ^ 1)]
    from_y = rows_ref.at[pl.ds(half, half), cols(me ^ 2)]
    top, bottom = x_copy(from_x, from_x, 2, 2), x_copy(from_y, from_y, 3, 1)
    to_x.wait_recv()
    top.start()
    to_y.wait_recv()
    bottom.start()
    for distance in range(2, pairs):
        relay(distance)
    for copy in (keep_x, keep_w, *stores):
        copy.wait()
    for copy in (top, bottom):
        copy.wait_recv()
    for copy in (to_x, to_y, top, bottom):
        copy.wait_send()

    for distance in range(pairs):

        @pl.when((level >= distance) & above)
        def _(distance=distance):
            w_copy(block(tok), tok, w_up.at[distance], tok + 2).wait_send()

        @pl.when((level + distance <= last) & below)
        def _(distance=distance):
            w_copy(block(tok), tok, w_down.at[distance], tok - 2).wait_send()

        near, far = 2 * distance + tok % 2, 2 * distance + 1 - tok % 2
        w_copy(block(near), near, w_core.at[near], tok ^ 1).wait_send()
        w_copy(block(far), far, w_core.at[near], tok ^ 1).wait_recv()


def first_gather(inputs, weight, gain, weights, parts):
    tokens, width = inputs.shape
    shard, cols = weight.shape
    pairs = lax.axis_size("tok") // 2
    dma = pltpu.SemaphoreType.DMA
    locals_ff = [(shard, 3 * (stop - start)) for start, stop in parts]
    shapes = [(tokens, 4 * width), (2 * pairs * shard, cols), *locals_ff]
    *gathered, first, second = pl.pallas_call(
        functools.partial(first_kernel, parts),
        out_shape=[jax.ShapeDtypeStruct(shape, BF16) for shape in shapes],
        in_specs=[pl.BlockSpec(memory_space=pltpu.VMEM)] * 3
        + [pl.BlockSpec(memory_space=pl.ANY)] * 3,
        out_specs=[pl.BlockSpec(memory_space=pl.ANY)] * 4,
        scratch_shapes=[pltpu.VMEM(array.shape, BF16) for array in weights]
        + [pltpu.VMEM(shape, BF16) for shape in locals_ff]
        + [
            dma((7,)), dma((4,)), dma((4,)), dma((pairs,)), dma((pairs,)),
            dma((2 * pairs,)), dma((2 * pairs,)),
        ],
        compiler_params=pltpu.CompilerParams(
            collective_id=0, has_side_effects=True, vmem_limit_bytes=60 << 20
        ),
    )(inputs, weight, gain, *weights)
    return *gathered, (first, second)


def in_order(mebibytes):
    return pltpu.CompilerParams(
        dimension_semantics=(pltpu.ARBITRARY,), vmem_limit_bytes=mebibytes << 20
    )


def cost(flops, bytes_accessed, transcendentals=0):
    return pl.CostEstimate(
        flops=flops, bytes_accessed=bytes_accessed, transcendentals=transcendentals
    )


def turn(vector, cos, sin):
    half = HEAD // 2
    lower, upper = vector[:, :half], vector[:, half:]
    return jnp.concatenate([lower * cos - upper * sin, upper * cos + lower * sin], axis=1)


def unturn(vector, cos, sin):
    half = HEAD // 2
    lower, upper = vector[:, :half], vector[:, half:]
    return jnp.concatenate([lower * cos + upper * sin, upper * cos - lower * sin], axis=1)


def seen(first_ref, position_ref, queries, keys):
    row = lax.broadcasted_iota(jnp.int32, (queries, keys), 0) + first_ref[0]
    distance = row - lax.broadcasted_iota(jnp.int32, (queries, keys), 1)
    return (distance >= 0) & (distance <= position_ref[...])


def forward_kernel(
    first_ref, q_ref, kv_ref, cos_ref, sin_ref, pos_ref, scale_ref, out_ref, norm_ref
):
    query = turn(q_ref[...].astype(F32) * scale_ref[...], cos_ref[...], sin_ref[...])
    query = (query * HEAD ** (-0.5)).astype(BF16)
    keys, values = kv_ref[:, :HEAD], kv_ref[:, HEAD:]
    scores = nt(query, keys)
    scores = jnp.where(seen(first_ref, pos_ref, *scores.shape), scores, MASKED)
    top = jnp.max(scores, axis=1, keepdims=True)
    weights = jnp.exp(scores - top)
    total = jnp.sum(weights, axis=1, keepdims=True)
    out_ref[...] = (nn(weights.astype(BF16), values) / total).astype(BF16)
    norm_ref[0] = top + jnp.log(total)


def backward_kernel(
    first_ref, q_ref, kv_ref, cos_ref, sin_ref, pos_ref, scale_ref, att_ref, datt_ref, norm_ref,
    dq_ref, dkv_ref,
):
    head = pl.program_id(0)
    scale = HEAD ** (-0.5)
    cos, sin = cos_ref[...], sin_ref[...]
    query = (turn(q_ref[...].astype(F32) * scale_ref[...], cos, sin) * scale).astype(BF16)
    keys, values = kv_ref[:, :HEAD], kv_ref[:, HEAD:]
    scores = nt(query, keys)
    visible = seen(first_ref, pos_ref, *scores.shape)
    again = jnp.where(visible, jnp.exp(scores - norm_ref[0]), 0.0)
    d_att = datt_ref[...]
    delta = jnp.sum(d_att.astype(F32) * att_ref[...].astype(F32), axis=1, keepdims=True)
    d_scores = (again * (nt(d_att, values) - delta)).astype(BF16)
    d_query = nn(d_scores, keys) * scale
    dq_ref[...] = unturn(d_query, cos, sin).astype(BF16)

    @pl.when(head == 0)
    def _():
        dkv_ref[...] = jnp.zeros_like(dkv_ref)

    dkv_ref[:, :HEAD] += tn(d_scores, query)
    dkv_ref[:, HEAD:] += tn(again.astype(BF16), d_att)


def whole_spec(shape):
    return pl.BlockSpec(shape, lambda head: (0,) * len(shape))


def attention_forward(first, qkv, kv, cos, sin, pos, scale):
    rows, keys = qkv.shape[0], kv.shape[0]
    head_spec = pl.BlockSpec((rows, HEAD), lambda head: (0, head))
    return pl.pallas_call(
        forward_kernel,
        grid=(HEADS,),
        out_shape=(
            jax.ShapeDtypeStruct((rows, HEADS * HEAD), BF16),
            jax.ShapeDtypeStruct((HEADS, rows, 1), F32),
        ),
        in_specs=[
            pl.BlockSpec(memory_space=pltpu.SMEM),
            head_spec,
            whole_spec((keys, 2 * HEAD)),
            whole_spec((rows, HEAD // 2)),
            whole_spec((rows, HEAD // 2)),
            whole_spec((rows, 1)),
            whole_spec((rows, 1)),
        ],
        out_specs=(head_spec, pl.BlockSpec((1, rows, 1), lambda head: (head, 0, 0))),
        compiler_params=in_order(32),
        cost_estimate=cost(4 * rows * keys * HEADS * HEAD, 4 * rows * HEADS * HEAD + 4 * keys * HEAD, rows * keys * HEADS),
        name="att_f",
    )(first, qkv, kv, cos, sin, pos, scale)


def attention_backward(first, qkv, kv, cos, sin, pos, scale, att, d_att, norm):
    rows, keys = qkv.shape[0], kv.shape[0]
    head_spec = pl.BlockSpec((rows, HEAD), lambda head: (0, head))
    return pl.pallas_call(
        backward_kernel,
        grid=(HEADS,),
        out_shape=(
            jax.ShapeDtypeStruct((rows, HEADS * HEAD), BF16),
            jax.ShapeDtypeStruct((keys, 2 * HEAD), F32),
        ),
        in_specs=[
            pl.BlockSpec(memory_space=pltpu.SMEM),
            head_spec,
            whole_spec((keys, 2 * HEAD)),
            whole_spec((rows, HEAD // 2)),
            whole_spec((rows, HEAD // 2)),
            whole_spec((rows, 1)),
            whole_spec((rows, 1)),
            head_spec,
            head_spec,
            pl.BlockSpec((1, rows, 1), lambda head: (head, 0, 0)),
        ],
        out_specs=(head_spec, whole_spec((keys, 2 * HEAD))),
        compiler_params=in_order(60),
        cost_estimate=cost(10 * rows * keys * HEADS * HEAD, 8 * rows * HEADS * HEAD + 12 * keys * HEAD, rows * keys * HEADS),
        name="att_b",
    )(first, qkv, kv, cos, sin, pos, scale, att, d_att, norm)


def keep_half(core_ref, total, kept, sent):
    half = total.shape[0] // 2
    for core, (first, second) in enumerate(((kept, sent), (sent, kept))):

        @pl.when(core_ref[0] == core)
        def _(first=first, second=second):
            first[...] = total[:half]
            second[...] = total[half:]


def pair_kernel(core_ref, left_ref, right_ref, *refs):
    total = tn(left_ref[...], right_ref[...])
    if len(refs) == 4:
        weight = refs[0][:, : total.shape[1]].astype(F32)
        refs[3][...] = jnp.sum(total * weight, axis=1, keepdims=True)
    keep_half(core_ref, total.astype(BF16), *refs[-3:-1] if len(refs) == 4 else refs)


def split_pairs(total, pairs, core):
    rows, cols = total.shape
    total = total.reshape(pairs, 2, rows // pairs // 2, cols)
    return tuple(
        lax.dynamic_index_in_dim(total, index, 1, False).reshape(-1, cols)
        for index in (core, 1 - core)
    )


def core_index():
    return (lax.axis_index("tok") % 2).astype(jnp.int32).reshape(1)


def pair_grad(left, right, weight=None):
    tokens, rows = left.shape
    cols = right.shape[1]
    pairs = lax.axis_size("tok") // 2
    step = rows // pairs
    if step % 128 or cols % 128:
        total = tn(left, right)
        halves = split_pairs(total.astype(BF16), pairs, lax.axis_index("tok") % 2)
        if weight is None:
            return halves
        return *halves, jnp.sum(total * weight[:, :cols].astype(F32), axis=1, keepdims=True)
    out_shape = [jax.ShapeDtypeStruct((rows // 2, cols), BF16)] * 2
    out_specs = [pl.BlockSpec((step // 2, cols), lambda pair: (pair, 0))] * 2
    in_specs = [
        pl.BlockSpec(memory_space=pltpu.SMEM),
        pl.BlockSpec((tokens, step), lambda pair: (0, pair)),
        pl.BlockSpec((tokens, cols), lambda pair: (0, 0)),
    ]
    operands = [core_index(), left, right]
    if weight is not None:
        operands.append(weight)
        in_specs.append(pl.BlockSpec((step, weight.shape[1]), lambda pair: (pair, 0)))
        out_shape.append(jax.ShapeDtypeStruct((rows, 1), F32))
        out_specs.append(pl.BlockSpec((step, 1), lambda pair: (pair, 0)))
    return pl.pallas_call(
        pair_kernel,
        grid=(pairs,),
        out_shape=out_shape,
        in_specs=in_specs,
        out_specs=out_specs,
        compiler_params=in_order(48),
        cost_estimate=cost(2 * tokens * rows * cols, 2 * (tokens * (rows + cols) + rows * cols)),
    )(*operands)


def part_kernel(core_ref, rows_ref, above_ref, d_gate_ref, d_up_ref, hidden_ref, kept, sent):
    cols = hidden_ref.shape[1]
    for at, (left_ref, right_ref) in enumerate(
        ((rows_ref, d_gate_ref), (rows_ref, d_up_ref), (above_ref, hidden_ref))
    ):
        total = tn(left_ref[...], right_ref[...]).astype(BF16)
        window = (slice(None), pl.ds(at * cols, cols))
        keep_half(core_ref, total, kept.at[window], sent.at[window])


def part_grad(rows, above, d_gate, d_up, hidden):
    tokens, features = rows.shape
    cols = hidden.shape[1]
    pairs = lax.axis_size("tok") // 2
    step = features // pairs
    if step % 128 or cols % 128:
        total = [tn(rows, d_gate), tn(rows, d_up), tn(above, hidden)]
        total = jnp.concatenate(total, axis=1).astype(BF16)
        return split_pairs(total, pairs, lax.axis_index("tok") % 2)
    out = jax.ShapeDtypeStruct((features // 2, 3 * cols), BF16)
    left_spec = pl.BlockSpec((tokens, step), lambda pair: (0, pair))
    right_spec = pl.BlockSpec((tokens, cols), lambda pair: (0, 0))
    return pl.pallas_call(
        part_kernel,
        grid=(pairs,),
        out_shape=(out, out),
        in_specs=[pl.BlockSpec(memory_space=pltpu.SMEM)] + [left_spec] * 2 + [right_spec] * 3,
        out_specs=[pl.BlockSpec((step // 2, 3 * cols), lambda pair: (pair, 0))] * 2,
        compiler_params=in_order(48),
        cost_estimate=cost(
            6 * tokens * features * cols,
            2 * (2 * tokens * features + 3 * cols * (tokens + features)),
        ),
    )(core_index(), rows, above, d_gate, d_up, hidden)


def join_kernel(kept_ref, got_ref, right_ref, out_ref):
    cols = kept_ref.shape[1]
    out_ref[:, :cols] = (kept_ref[...].astype(F32) + got_ref[...].astype(F32)).astype(BF16)
    out_ref[:, cols:] = right_ref[...]


def join(kept, got, right):
    rows, cols = kept.shape
    width = cols + right.shape[1]
    if cols % 128:
        both = (kept.astype(F32) + got.astype(F32)).astype(BF16)
        return jnp.concatenate([both, right], axis=1)
    step = rows // 4
    left_spec = pl.BlockSpec((step, cols), lambda at: (at, 0))
    return pl.pallas_call(
        join_kernel,
        grid=(4,),
        out_shape=jax.ShapeDtypeStruct((rows, width), BF16),
        in_specs=[left_spec, left_spec, pl.BlockSpec((step, right.shape[1]), lambda at: (at, 0))],
        out_specs=pl.BlockSpec((step, width), lambda at: (at, 0)),
        compiler_params=in_order(32),
        cost_estimate=cost(rows * cols, 2 * rows * (2 * width + cols)),
    )(kept, got, right)


def pieces_grad_kernel(me_ref, core_ref, own, along_x, along_y, top, bottom, right_ref, kept, sent):
    at = pl.program_id(0)
    half = top.shape[0]
    for index, piece in enumerate((own, along_x, along_y)):

        @pl.when(at == index)
        def _(piece=piece):
            keep_half(core_ref, tn(piece[...], right_ref[...]).astype(BF16), kept, sent)

    @pl.when(at == 3)
    def _():
        total = tn(top[...], right_ref[:half]) + tn(bottom[...], right_ref[half:])
        keep_half(core_ref, total.astype(BF16), kept, sent)


def pieces_grad(pieces, right):
    tokens, step = pieces[0].shape
    cols = right.shape[1]
    me = lax.axis_index("mdl").astype(jnp.int32).reshape(1)
    out = jax.ShapeDtypeStruct((2 * step, cols), BF16)
    return pl.pallas_call(
        pieces_grad_kernel,
        grid_spec=pltpu.PrefetchScalarGridSpec(
            num_scalar_prefetch=2,
            grid=(4,),
            in_specs=[
                pl.BlockSpec(array.shape, lambda at, me_ref, core_ref: (0, 0))
                for array in (*pieces, right)
            ],
            out_specs=[
                pl.BlockSpec((step // 2, cols), lambda at, me_ref, core_ref: (me_ref[0] ^ at, 0))
            ]
            * 2,
        ),
        out_shape=(out, out),
        compiler_params=in_order(48),
        cost_estimate=cost(8 * tokens * step * cols, 2 * (4 * tokens * step + 5 * step * cols)),
    )(me, core_index(), *pieces, right)


def sum_kernel(starts, *refs):
    *lefts, weight_ref, out_ref = refs
    total = 0.0
    for left_ref, start in zip(lefts, starts):
        total += nt(left_ref[...], weight_ref[:, start : start + left_ref.shape[1]])
    out_ref[...] = total


def sum_products(lefts, weight, starts):
    tokens = lefts[0].shape[0]
    rows, cols = weight.shape
    if lefts[0].shape[1] % 128:
        return sum(
            nt(left, weight[:, start : start + left.shape[1]])
            for left, start in zip(lefts, starts)
        )
    step = 512
    depth = sum(left.shape[1] for left in lefts)
    return pl.pallas_call(
        functools.partial(sum_kernel, starts),
        grid=(rows // step,),
        out_shape=jax.ShapeDtypeStruct((tokens, rows), F32),
        in_specs=[pl.BlockSpec(left.shape, lambda row: (0, 0)) for left in lefts]
        + [pl.BlockSpec((step, cols), lambda row: (row, 0))],
        out_specs=pl.BlockSpec((tokens, step), lambda row: (0, row)),
        compiler_params=in_order(48),
        cost_estimate=cost(2 * tokens * rows * depth, 2 * rows * cols + 4 * tokens * rows),
    )(*lefts, weight)


def payload_kernel(starts, me_ref, *refs):
    lefts, weight_ref = refs[: len(starts)], refs[len(starts)]
    top_sent, bottom_sent, top_kept, bottom_kept = refs[-4:]
    total = refs[-5][...] if len(refs) == len(starts) + 6 else 0.0
    for left_ref, start in zip(lefts, starts):
        total += nt(left_ref[...], weight_ref[:, start : start + left_ref.shape[1]])
    total = total.astype(BF16)
    half = total.shape[0] // 2
    places = (
        ((top_kept, 0), (bottom_kept, 0)),
        ((top_sent, 0), (bottom_kept, 1)),
        ((top_kept, 1), (bottom_sent, 0)),
        ((top_sent, 1), (bottom_sent, 1)),
    )
    for distance, ((top, top_at), (bottom, bottom_at)) in enumerate(places):

        @pl.when(pl.program_id(0) == 3 - distance)
        def _(top=top, top_at=top_at, bottom=bottom, bottom_at=bottom_at):
            top[top_at] = total[:half]
            bottom[bottom_at] = total[half:]


def scatter_product(lefts, weight, starts, partial=()):
    tokens = lefts[0].shape[0]
    rows, cols = weight.shape
    step = rows // 4
    me = lax.axis_index("mdl").astype(jnp.int32).reshape(1)
    out = jax.ShapeDtypeStruct((2, tokens // 2, step), BF16)
    depth = sum(left.shape[1] for left in lefts)
    return pl.pallas_call(
        functools.partial(payload_kernel, starts),
        grid_spec=pltpu.PrefetchScalarGridSpec(
            num_scalar_prefetch=1,
            grid=(4,),
            in_specs=[pl.BlockSpec(left.shape, lambda at, me_ref: (0, 0)) for left in lefts]
            + [pl.BlockSpec((step, cols), lambda at, me_ref: (me_ref[0] ^ (3 - at), 0))]
            + [pl.BlockSpec((tokens, step), lambda at, me_ref: (0, me_ref[0] ^ (3 - at)))]
            * len(partial),
            out_specs=[pl.BlockSpec(out.shape, lambda at, me_ref: (0, 0, 0))] * 4,
        ),
        out_shape=(out,) * 4,
        compiler_params=in_order(48),
        cost_estimate=cost(2 * tokens * rows * depth, 2 * (tokens * depth + rows * cols + tokens * rows)),
    )(me, *lefts, weight, *partial)


def pieces_kernel(start, me_ref, own, along_x, along_y, top, bottom, weight_ref, out_ref, total):
    at = pl.program_id(0)
    width = out_ref.shape[1]
    half = top.shape[0]
    for index, piece in enumerate((own, along_x, along_y)):

        @pl.when(at == index)
        def _(index=index, piece=piece):
            part = nn(piece[...], weight_ref[:, start : start + width])
            if index:
                total[...] += part
            else:
                total[...] = part

    @pl.when(at == 3)
    def _():
        weight = weight_ref[:, start : start + width]
        out_ref[:half] = (total[:half] + nn(top[...], weight)).astype(BF16)
        out_ref[half:] = (total[half:] + nn(bottom[...], weight)).astype(BF16)


def pieces_product(pieces, weight, start, width):
    tokens, step = pieces[0].shape
    rows, cols = weight.shape
    me = lax.axis_index("mdl").astype(jnp.int32).reshape(1)
    return pl.pallas_call(
        functools.partial(pieces_kernel, start),
        grid_spec=pltpu.PrefetchScalarGridSpec(
            num_scalar_prefetch=1,
            grid=(4,),
            in_specs=[pl.BlockSpec(piece.shape, lambda at, me_ref: (0, 0)) for piece in pieces]
            + [pl.BlockSpec((step, cols), lambda at, me_ref: (me_ref[0] ^ at, 0))],
            out_specs=pl.BlockSpec((tokens, width), lambda at, me_ref: (0, 0)),
            scratch_shapes=[pltpu.VMEM((tokens, width), F32)],
        ),
        out_shape=jax.ShapeDtypeStruct((tokens, width), BF16),
        compiler_params=in_order(40),
        cost_estimate=cost(2 * tokens * rows * width, 2 * (tokens * rows + rows * cols + tokens * width)),
    )(me, *pieces, weight)


def product_to_mdl(lefts, weight, starts, partial=()):
    if lax.axis_size("mdl") == 4:
        payload = scatter_product(lefts, weight, starts, partial)
        return payload, lambda payload, *earlier: scatter_payload(payload, *earlier)
    part = sum((sum_products(lefts, weight, starts), *partial))
    return (part.astype(BF16),), lambda payload, *earlier: scatter_mdl(payload[0], 1)


def after(value, *earlier):
    return lax.optimization_barrier((value, *earlier))[0]


def row_scale(rows_b, axis=-1):
    rows = rows_b.astype(F32)
    return lax.rsqrt(jnp.mean(rows * rows, axis=axis, keepdims=True) + NORM_EPS)


def gelu_parts(value):
    root = math.sqrt(2.0 / math.pi)
    square = value * value
    tanh = jnp.tanh(root * (value + 0.044715 * value * square))
    cdf = 0.5 * (1.0 + tanh)
    slope = cdf + 0.5 * value * (1.0 - tanh * tanh) * root * (1.0 + 3 * 0.044715 * square)
    return value * cdf, slope


def scaled(weight, gain):
    return (weight.astype(F32) * gain.astype(F32)[:, None]).astype(BF16)


def on_device(
    inputs, positions, norm1_gain, qkv_weight, out_weight, norm2_gain, gate_weight,
    up_weight, down_weight, cotangent,
):
    me = lax.axis_index("mdl")
    size = lax.axis_size("mdl")
    head_cols = HEADS * HEAD
    width = inputs.shape[1]
    features = width * size

    def from_tok(weight, dim):
        return lax.all_gather(weight, "tok", axis=dim, tiled=True)

    def from_pair(sent):
        count = lax.axis_size("tok")
        return lax.ppermute(sent, "tok", [(i, i ^ 1) for i in range(count)])

    def pair_sum(local):
        kept, got = local[0], from_pair(local[1])
        return (kept.astype(F32) + got.astype(F32)).astype(BF16)

    def to_tok(both):
        count = lax.axis_size("tok")
        groups = [list(range(core, count, 2)) for core in range(2)]
        total = lax.psum_scatter(
            both, "tok", scatter_dimension=0, tiled=True, axis_index_groups=groups
        )
        return total.astype(F32)

    qkv_cols, ff_cols = qkv_weight.shape[1], gate_weight.shape[1]
    attn_local = jnp.concatenate([scaled(qkv_weight, norm1_gain), out_weight.T], axis=1)
    middle = ff_cols // 256 * 128
    parts = ((0, middle), (middle, ff_cols))
    if size == 4 and lax.axis_size("tok") == 8:
        rows_in, w_attn, locals_ff = first_gather(
            inputs,
            attn_local,
            norm2_gain.astype(F32)[:, None],
            (gate_weight, up_weight, down_weight.T),
            parts,
        )
    else:
        rows_in = gather_mdl(inputs, 1)
        w_attn = from_tok(attn_local, 0)
        scaled_gu = [scaled(weight, norm2_gain) for weight in (gate_weight, up_weight)]
        locals_ff = [
            jnp.concatenate([w[:, start:stop] for w in (*scaled_gu, down_weight.T)], axis=1)
            for start, stop in parts
        ]
    w_qkv = w_attn[:, :qkv_cols]
    w_parts = [from_tok(local, 0) for local in locals_ff]

    qkv = rows_to_cols(nn(rows_in, w_qkv).astype(BF16))
    count = qkv.shape[0]
    scale_own = row_scale(lax.dynamic_slice_in_dim(rows_in, me * count, count, 0))
    half = HEAD // 2
    frequency = jnp.exp(jnp.arange(half, dtype=F32) * (-2.0 * math.log(10000.0) / HEAD))
    angles = positions.astype(F32)[:, None] * frequency[None, :]
    cos, sin = jnp.cos(angles), jnp.sin(angles)
    kv_own = qkv[:, head_cols:].astype(F32) * scale_own
    key_rows = turn(kv_own[:, :HEAD], cos, sin)
    kv = gather_mdl(jnp.concatenate([key_rows, kv_own[:, HEAD:]], axis=1).astype(BF16), 0)
    first = (me * count).astype(jnp.int32).reshape(1)
    pos = positions[:, None]
    attended, log_norm = attention_forward(first, qkv, kv, cos, sin, pos, scale_own)
    head_block = cols_to_rows(attended)
    residual = inputs.astype(F32)
    payload, scatter = product_to_mdl((head_block,), w_attn, (qkv_cols,))
    mixed = residual + scatter(payload)

    rows_two = gather_mdl(mixed.astype(BF16), 1)
    scale_two = row_scale(rows_two)
    rows_hat = (rows_two.astype(F32) * scale_two).astype(BF16)
    rows, above, stat_two, partial, hiddens, sums = rows_hat, cotangent, 0.0, (), [], []
    for index, (weight, (start, stop)) in enumerate(zip(w_parts, parts)):
        cols = stop - start
        last = index == len(parts) - 1
        gate_in = nn(rows, weight[:, :cols])
        up_in = nn(rows, weight[:, cols : 2 * cols])
        d_hidden = nn(above, weight[:, 2 * cols :])
        gelu, slope = gelu_parts(gate_in)
        hidden = (gelu * up_in).astype(BF16)
        d_gate = d_hidden * up_in * slope
        d_up = d_hidden * gelu
        stat_two += jnp.sum(d_gate * gate_in + d_up * up_in, axis=1)
        d_gate, d_up = d_gate.astype(BF16), d_up.astype(BF16)
        hiddens.append(hidden)
        lefts, starts = (d_gate, d_up), (0, cols)
        if last:
            payload, scatter = product_to_mdl(lefts, weight, starts, partial)
            rows, above, _ = lax.optimization_barrier((rows, above, payload[0]))
        local = part_grad(rows, above, d_gate, d_up, hidden)
        if not last:
            d_gate = after(d_gate, local[0])
            partial = (sum_products((d_gate, d_up), weight, starts),)
            rows, above, _ = lax.optimization_barrier((rows, above, local[0]))
        sums.append(to_tok(pair_sum(local)))
    d_two = scatter(payload)
    stat_two = sum_mdl(stat_two.reshape(8, -1)).reshape(-1, 1) * (1.0 / features)
    scale_mixed = scale_two * mixed
    cotangent_own = lax.dynamic_slice_in_dim(cotangent, me * width, width, 1).astype(F32)
    d_mixed = cotangent_own + scale_two * (d_two - scale_mixed * stat_two)

    d_mixed_b = after(d_mixed.astype(BF16), local[0])
    down_starts = tuple(2 * (stop - start) for start, stop in parts)
    ffn = (sum_products((after(hiddens[0], d_mixed_b),), w_parts[0], down_starts[:1]),)
    ffn_payload, ffn_scatter = product_to_mdl(
        (after(hiddens[1], d_mixed_b),), w_parts[1], down_starts[1:], ffn
    )
    if size == 4 and lax.axis_size("tok") == 8:
        pieces = gather_pieces(d_mixed_b)
        scale_one = row_scale(after(rows_in, pieces[1]))
        d_head = pieces_product(pieces, w_attn, qkv_cols, head_block.shape[1])
        heads_later = after(head_block, d_head)
        out_local = pieces_grad(pieces, heads_later)
    else:
        scale_one = row_scale(rows_in)
        d_mixed_rows = gather_mdl(d_mixed_b, 1)
        d_head = nn(d_mixed_rows, w_attn[:, qkv_cols:]).astype(BF16)
        out_local = pair_grad(d_mixed_rows, head_block)
    out_both = pair_sum(out_local)
    d_attended = rows_to_cols(d_head)
    *ffn_payload, _ = lax.optimization_barrier((*ffn_payload, d_attended))
    d_query, d_kv = attention_backward(
        first, qkv, kv, cos, sin, pos, scale_own, attended, d_attended, log_norm
    )
    d_kv = scatter_mdl(d_kv.astype(BF16), 0)
    d_key = unturn(d_kv[:, :HEAD], cos, sin).astype(BF16)
    d_qkv = jnp.concatenate([d_query, d_key, d_kv[:, HEAD:].astype(BF16)], axis=1)
    stat_one = jnp.sum(d_qkv.astype(F32) * qkv.astype(F32), axis=1) * scale_own[:, 0]
    d_qkv_part = cols_to_rows(d_qkv)
    stat_rows = jnp.zeros((size, count), F32)
    stat_rows = sum_mdl(lax.dynamic_update_slice(stat_rows, stat_one[None], (me, 0)))
    stat_one = stat_rows.reshape(-1, 1) * (1.0 / features)
    d_scaled = (d_qkv_part.astype(F32) * scale_one).astype(BF16)
    kept, sent, gain_one = pair_grad(rows_in, d_scaled, w_attn)
    got = from_pair(sent)
    both = join(kept, got, out_both)
    attn_sum = to_tok(both)
    qkv_sum, out_grad = attn_sum[:, :qkv_cols], attn_sum[:, qkv_cols:].T
    payload, scatter = product_to_mdl((after(d_qkv_part, kept),), w_attn, (0,))
    d_one = scatter(payload)
    ffn_sum = ffn_scatter(ffn_payload, d_qkv_part)
    block_out = (mixed + ffn_sum).astype(BF16)
    input_grad = d_mixed + scale_one * (d_one - (scale_one * residual) * stat_one)

    norm1_late, norm2_late, gate_late, up_late, _ = lax.optimization_barrier(
        (norm1_gain, norm2_gain, gate_weight, up_weight, local[0])
    )

    def unfold(total, gain):
        return total * gain.astype(F32)[:, None]

    def joined(at):
        widths = [total.shape[1] // 3 for total in sums]
        pieces = [total[:, at * cols :][:, :cols] for total, cols in zip(sums, widths)]
        return jnp.concatenate(pieces, axis=1)

    gate_sum, up_sum, down_grad = joined(0), joined(1), joined(2).T
    gain_two = jnp.sum(
        gate_late.astype(F32) * gate_sum + up_late.astype(F32) * up_sum, axis=1
    )
    gate_grad, up_grad = unfold(gate_sum, norm2_late), unfold(up_sum, norm2_late)
    gain_two_grad = sum_mdl(gain_two)
    gain_one = sum_mdl(sum_tok(gain_one.reshape(8, -1))).reshape(-1)
    shard = norm1_gain.shape[0]
    gain_one = lax.dynamic_slice_in_dim(gain_one, lax.axis_index("tok") * shard, shard, 0)
    gain_one_grad = gain_one / norm1_late.astype(F32)
    return (
        block_out,
        input_grad,
        gain_one_grad,
        unfold(qkv_sum, norm1_late),
        out_grad,
        gain_two_grad,
        gate_grad,
        up_grad,
        down_grad,
    )


def solution(mesh):
    return jax.shard_map(
        on_device,
        mesh=mesh,
        in_specs=(
            P("tok", "mdl"),
            P(("tok", "mdl")),
            P("tok"),
            P("tok", "mdl"),
            P("mdl", "tok"),
            P("tok"),
            P("tok", "mdl"),
            P("tok", "mdl"),
            P("mdl", "tok"),
            P("tok", None),
        ),
        out_specs=(
            P("tok", "mdl"),
            P("tok", "mdl"),
            P("tok"),
            P("tok", "mdl"),
            P("mdl", "tok"),
            P("tok"),
            P("tok", "mdl"),
            P("tok", "mdl"),
            P("mdl", "tok"),
        ),
        check_vma=False,
    )
```

```python
import functools
import math

import jax
import jax.numpy as jnp
from jax import lax
from jax.experimental import pallas as pl
from jax.experimental.pallas import tpu as pltpu
from jax.sharding import PartitionSpec as P


HEADS = 10
HEAD = 256
NORM_EPS = 1e-06
F32 = jnp.float32
BF16 = jnp.bfloat16
MASKED = -1e30


def nt(left_op, right_op):
    return lax.dot_general(
        left_op, right_op, (((1,), (1,)), ((), ())), preferred_element_type=F32
    )


def tn(left_op, right_op):
    return lax.dot_general(
        left_op, right_op, (((0,), (0,)), ((), ())), preferred_element_type=F32
    )


def nn(left_op, right_op):
    return jnp.dot(left_op, right_op, preferred_element_type=F32)


def swap(block, distance):
    size = lax.axis_size("mdl")
    return lax.ppermute(block, "mdl", [(i, i ^ distance) for i in range(size)])


def gather_mdl(block, dim):
    size = lax.axis_size("mdl")
    if size != 4:
        return lax.all_gather(block, "mdl", axis=dim, tiled=True)
    me = lax.axis_index("mdl")
    half = block.shape[0] // 2
    along_x = swap(block, 1)
    along_y = swap(block, 2)
    top = swap(along_x[:half], 2)
    bottom = swap(along_y[half:], 1)
    width = block.shape[dim]
    shape = list(block.shape)
    shape[dim] = width * size
    whole = jnp.zeros(shape, block.dtype)

    def put(whole, piece, source, row):
        start = [0, 0]
        start[dim] = source * width
        start[0] = start[0] + row
        return lax.dynamic_update_slice(whole, piece, tuple(start))

    whole = put(whole, block, me, 0)
    whole = put(whole, along_x, me ^ 1, 0)
    whole = put(whole, along_y, me ^ 2, 0)
    whole = put(whole, top, me ^ 3, 0)
    whole = put(whole, bottom, me ^ 3, half)
    return whole


def scatter_mdl(part, dim):
    size = lax.axis_size("mdl")
    if size != 4:
        return lax.psum_scatter(part, "mdl", scatter_dimension=dim, tiled=True).astype(F32)
    me = lax.axis_index("mdl")
    shape = list(part.shape)
    shape[dim] //= size
    half = shape[0] // 2

    def piece(block, row):
        start = [0, 0]
        start[dim] = block * shape[dim]
        start[0] = start[0] + row
        return lax.dynamic_slice(part, tuple(start), (half, shape[1]))

    sums = []
    for row, first, second in ((0, 1, 2), (half, 2, 1)):
        sent = jnp.stack([piece(me ^ first, row), piece(me ^ 3, row)])
        sums.append((row, second, swap(sent, first)))
    partial = []
    for row, second, got in sums:
        other = piece(me ^ second, row).astype(F32) + got[1].astype(F32)
        partial.append((row, got[0], swap(other.astype(BF16), second)))
    return jnp.concatenate(
        [
            piece(me, row).astype(F32) + first.astype(F32) + second.astype(F32)
            for row, first, second in partial
        ],
        axis=0,
    )


def gather_pieces(block):
    half = block.shape[0] // 2
    along_x = swap(block, 1)
    along_y = swap(block, 2)
    top = swap(along_x[:half], 2)
    bottom = swap(along_y[half:], 1)
    return block, along_x, along_y, top, bottom


def scatter_payload(payload, *earlier):
    top_sent, bottom_sent, top_kept, bottom_kept = payload
    got_top = swap(top_sent, 1)
    got_bottom = swap(bottom_sent, 2)
    halves = []
    for kept, got, second in ((top_kept, got_top, 2), (bottom_kept, got_bottom, 1)):
        passed = (kept[1].astype(F32) + got[1].astype(F32)).astype(BF16)
        if earlier:
            passed = after(passed, *earlier)
        last = swap(passed, second)
        halves.append(kept[0].astype(F32) + got[0].astype(F32) + last.astype(F32))
    return jnp.concatenate(halves, axis=0)


def sum_mdl(value):
    size = lax.axis_size("mdl")
    distance = 1
    while distance < size:
        value = value + swap(value, distance)
        distance *= 2
    return value


def sum_tok(value):
    size = lax.axis_size("tok")
    distance = 1
    while distance < size:
        value = value + lax.ppermute(value, "tok", [(i, i ^ distance) for i in range(size)])
        distance *= 2
    return value


def rows_to_cols(block):
    return lax.all_to_all(block, "mdl", split_axis=0, concat_axis=1, tiled=True)


def cols_to_rows(block):
    return lax.all_to_all(block, "mdl", split_axis=1, concat_axis=0, tiled=True)


def first_kernel(
    parts, x_ref, w_ref, gain_ref, *refs
):
    weights, (rows_ref, weight_ref), locals_ref = refs[:3], refs[3:5], refs[5:7]
    held, joined = refs[7:10], refs[10:12]
    own, x_sent, x_got, w_up, w_down, w_core, w_got = refs[12:]
    me, tok = lax.axis_index("mdl"), lax.axis_index("tok")
    pairs = lax.axis_size("tok") // 2
    level, last = tok // 2, pairs - 1
    half, width, shard = x_ref.shape[0] // 2, x_ref.shape[1], w_ref.shape[0]
    below, above = level > 0, level < last

    barrier = pltpu.get_barrier_semaphore()
    pl.semaphore_signal(barrier, inc=1, device_id={"mdl": me ^ 1})
    pl.semaphore_signal(barrier, inc=1, device_id={"mdl": me ^ 2})
    pl.semaphore_signal(barrier, inc=1, device_id={"tok": tok ^ 1})

    @pl.when(below)
    def _():
        pl.semaphore_signal(barrier, inc=1, device_id={"tok": tok - 2})

    @pl.when(above)
    def _():
        pl.semaphore_signal(barrier, inc=1, device_id={"tok": tok + 2})

    pl.semaphore_wait(barrier, 3 + below.astype(jnp.int32) + above.astype(jnp.int32))

    def cols(block):
        return pl.ds(pl.multiple_of(block * width, 128), width)

    def block(index):
        return weight_ref.at[pl.ds(pl.multiple_of(index * shard, 16), shard)]

    def x_copy(source, target, at, to):
        return pltpu.make_async_remote_copy(
            source, target, x_sent.at[at], x_got.at[at], device_id={"mdl": me ^ to}
        )

    def w_copy(source, index, sent, to):
        return pltpu.make_async_remote_copy(
            source, block(index), sent, w_got.at[index], device_id={"tok": to}
        )

    mine = rows_ref.at[:, cols(me)]
    to_x, to_y = x_copy(x_ref, mine, 0, 1), x_copy(x_ref, mine, 1, 2)

    @pl.when(above)
    def _():
        w_copy(w_ref, tok, w_up.at[0], tok + 2).start()

    @pl.when(below)
    def _():
        w_copy(w_ref, tok, w_down.at[0], tok - 2).start()

    to_x.start()
    to_y.start()
    w_copy(w_ref, tok, w_core.at[tok], tok ^ 1).start()
    keep_x = pltpu.make_async_copy(x_ref, mine, own.at[0])
    keep_w = pltpu.make_async_copy(w_ref, block(tok), own.at[1])
    keep_x.start()
    keep_w.start()
    loads = [
        pltpu.make_async_copy(weight, to, own.at[2 + at])
        for at, (weight, to) in enumerate(zip(weights, held))
    ]
    for copy in loads:
        copy.start()
    for copy in loads:
        copy.wait()
    for (start, stop), out in zip(parts, joined):
        count = stop - start
        for at, source in enumerate(held):
            value = source[:, start:stop]
            if at < 2:
                value = (value.astype(F32) * gain_ref[...]).astype(BF16)
            out[:, at * count : (at + 1) * count] = value

    def relay(distance):
        low, high = tok - 2 * distance, tok + 2 * distance

        @pl.when(level >= distance)
        def _():
            w_copy(block(low), low, w_core.at[low], tok ^ 1).wait_recv()

            @pl.when(above)
            def _():
                w_copy(block(low), low, w_up.at[distance], tok + 2).start()

            w_copy(block(low), low, w_core.at[low], tok ^ 1).start()

        @pl.when(level + distance <= last)
        def _():
            w_copy(block(high), high, w_core.at[high], tok ^ 1).wait_recv()

            @pl.when(below)
            def _():
                w_copy(block(high), high, w_down.at[distance], tok - 2).start()

            w_copy(block(high), high, w_core.at[high], tok ^ 1).start()

    relay(1)
    stores = [
        pltpu.make_async_copy(out, to, own.at[5 + at])
        for at, (out, to) in enumerate(zip(joined, locals_ref))
    ]
    for copy in stores:
        copy.start()
    from_x = rows_ref.at[pl.ds(0, half), cols(me ^ 1)]
    from_y = rows_ref.at[pl.ds(half, half), cols(me ^ 2)]
    top, bottom = x_copy(from_x, from_x, 2, 2), x_copy(from_y, from_y, 3, 1)
    to_x.wait_recv()
    top.start()
    to_y.wait_recv()
    bottom.start()
    for distance in range(2, pairs):
        relay(distance)
    for copy in (keep_x, keep_w, *stores):
        copy.wait()
    for copy in (top, bottom):
        copy.wait_recv()
    for copy in (to_x, to_y, top, bottom):
        copy.wait_send()

    for distance in range(pairs):

        @pl.when((level >= distance) & above)
        def _(distance=distance):
            w_copy(block(tok), tok, w_up.at[distance], tok + 2).wait_send()

        @pl.when((level + distance <= last) & below)
        def _(distance=distance):
            w_copy(block(tok), tok, w_down.at[distance], tok - 2).wait_send()

        near, far = 2 * distance + tok % 2, 2 * distance + 1 - tok % 2
        w_copy(block(near), near, w_core.at[near], tok ^ 1).wait_send()
        w_copy(block(far), far, w_core.at[near], tok ^ 1).wait_recv()


def first_gather(inputs, weight, gain, weights, parts):
    tokens, width = inputs.shape
    shard, cols = weight.shape
    pairs = lax.axis_size("tok") // 2
    dma = pltpu.SemaphoreType.DMA
    locals_ff = [(shard, 3 * (stop - start)) for start, stop in parts]
    shapes = [(tokens, 4 * width), (2 * pairs * shard, cols), *locals_ff]
    *gathered, first, second = pl.pallas_call(
        functools.partial(first_kernel, parts),
        out_shape=[jax.ShapeDtypeStruct(shape, BF16) for shape in shapes],
        in_specs=[pl.BlockSpec(memory_space=pltpu.VMEM)] * 3
        + [pl.BlockSpec(memory_space=pl.ANY)] * 3,
        out_specs=[pl.BlockSpec(memory_space=pl.ANY)] * 4,
        scratch_shapes=[pltpu.VMEM(array.shape, BF16) for array in weights]
        + [pltpu.VMEM(shape, BF16) for shape in locals_ff]
        + [
            dma((7,)), dma((4,)), dma((4,)), dma((pairs,)), dma((pairs,)),
            dma((2 * pairs,)), dma((2 * pairs,)),
        ],
        compiler_params=pltpu.CompilerParams(
            collective_id=0, has_side_effects=True, vmem_limit_bytes=60 << 20
        ),
    )(inputs, weight, gain, *weights)
    return *gathered, (first, second)


def in_order(mebibytes):
    return pltpu.CompilerParams(
        dimension_semantics=(pltpu.ARBITRARY,), vmem_limit_bytes=mebibytes << 20
    )


def cost(flops, bytes_accessed, transcendentals=0):
    return pl.CostEstimate(
        flops=flops, bytes_accessed=bytes_accessed, transcendentals=transcendentals
    )


def turn(vector, cos, sin):
    half = HEAD // 2
    lower, upper = vector[:, :half], vector[:, half:]
    return jnp.concatenate([lower * cos - upper * sin, upper * cos + lower * sin], axis=1)


def unturn(vector, cos, sin):
    half = HEAD // 2
    lower, upper = vector[:, :half], vector[:, half:]
    return jnp.concatenate([lower * cos + upper * sin, upper * cos - lower * sin], axis=1)


def seen(first_ref, position_ref, queries, keys):
    row = lax.broadcasted_iota(jnp.int32, (queries, keys), 0) + first_ref[0]
    distance = row - lax.broadcasted_iota(jnp.int32, (queries, keys), 1)
    return (distance >= 0) & (distance <= position_ref[...])


def forward_kernel(
    first_ref, q_ref, kv_ref, cos_ref, sin_ref, pos_ref, scale_ref, out_ref, norm_ref
):
    query = turn(q_ref[...].astype(F32) * scale_ref[...], cos_ref[...], sin_ref[...])
    query = (query * HEAD ** (-0.5)).astype(BF16)
    keys, values = kv_ref[:, :HEAD], kv_ref[:, HEAD:]
    scores = nt(query, keys)
    scores = jnp.where(seen(first_ref, pos_ref, *scores.shape), scores, MASKED)
    top = jnp.max(scores, axis=1, keepdims=True)
    weights = jnp.exp(scores - top)
    total = jnp.sum(weights, axis=1, keepdims=True)
    out_ref[...] = (nn(weights.astype(BF16), values) / total).astype(BF16)
    norm_ref[0] = top + jnp.log(total)


def backward_kernel(
    first_ref, q_ref, kv_ref, cos_ref, sin_ref, pos_ref, scale_ref, att_ref, datt_ref, norm_ref,
    dq_ref, dkv_ref,
):
    head = pl.program_id(0)
    scale = HEAD ** (-0.5)
    cos, sin = cos_ref[...], sin_ref[...]
    query = (turn(q_ref[...].astype(F32) * scale_ref[...], cos, sin) * scale).astype(BF16)
    keys, values = kv_ref[:, :HEAD], kv_ref[:, HEAD:]
    scores = nt(query, keys)
    visible = seen(first_ref, pos_ref, *scores.shape)
    again = jnp.where(visible, jnp.exp(scores - norm_ref[0]), 0.0)
    d_att = datt_ref[...]
    delta = jnp.sum(d_att.astype(F32) * att_ref[...].astype(F32), axis=1, keepdims=True)
    d_scores = (again * (nt(d_att, values) - delta)).astype(BF16)
    d_query = nn(d_scores, keys) * scale
    dq_ref[...] = unturn(d_query, cos, sin).astype(BF16)

    @pl.when(head == 0)
    def _():
        dkv_ref[...] = jnp.zeros_like(dkv_ref)

    dkv_ref[:, :HEAD] += tn(d_scores, query)
    dkv_ref[:, HEAD:] += tn(again.astype(BF16), d_att)


def whole_spec(shape):
    return pl.BlockSpec(shape, lambda head: (0,) * len(shape))


def attention_forward(first, qkv, kv, cos, sin, pos, scale):
    rows, keys = qkv.shape[0], kv.shape[0]
    head_spec = pl.BlockSpec((rows, HEAD), lambda head: (0, head))
    return pl.pallas_call(
        forward_kernel,
        grid=(HEADS,),
        out_shape=(
            jax.ShapeDtypeStruct((rows, HEADS * HEAD), BF16),
            jax.ShapeDtypeStruct((HEADS, rows, 1), F32),
        ),
        in_specs=[
            pl.BlockSpec(memory_space=pltpu.SMEM),
            head_spec,
            whole_spec((keys, 2 * HEAD)),
            whole_spec((rows, HEAD // 2)),
            whole_spec((rows, HEAD // 2)),
            whole_spec((rows, 1)),
            whole_spec((rows, 1)),
        ],
        out_specs=(head_spec, pl.BlockSpec((1, rows, 1), lambda head: (head, 0, 0))),
        compiler_params=in_order(32),
        cost_estimate=cost(4 * rows * keys * HEADS * HEAD, 4 * rows * HEADS * HEAD + 4 * keys * HEAD, rows * keys * HEADS),
        name="att_f",
    )(first, qkv, kv, cos, sin, pos, scale)


def attention_backward(first, qkv, kv, cos, sin, pos, scale, att, d_att, norm):
    rows, keys = qkv.shape[0], kv.shape[0]
    head_spec = pl.BlockSpec((rows, HEAD), lambda head: (0, head))
    return pl.pallas_call(
        backward_kernel,
        grid=(HEADS,),
        out_shape=(
            jax.ShapeDtypeStruct((rows, HEADS * HEAD), BF16),
            jax.ShapeDtypeStruct((keys, 2 * HEAD), F32),
        ),
        in_specs=[
            pl.BlockSpec(memory_space=pltpu.SMEM),
            head_spec,
            whole_spec((keys, 2 * HEAD)),
            whole_spec((rows, HEAD // 2)),
            whole_spec((rows, HEAD // 2)),
            whole_spec((rows, 1)),
            whole_spec((rows, 1)),
            head_spec,
            head_spec,
            pl.BlockSpec((1, rows, 1), lambda head: (head, 0, 0)),
        ],
        out_specs=(head_spec, whole_spec((keys, 2 * HEAD))),
        compiler_params=in_order(40),
        cost_estimate=cost(10 * rows * keys * HEADS * HEAD, 8 * rows * HEADS * HEAD + 12 * keys * HEAD, rows * keys * HEADS),
        name="att_b",
    )(first, qkv, kv, cos, sin, pos, scale, att, d_att, norm)


def keep_half(core_ref, total, kept, sent):
    half = total.shape[0] // 2
    for core, (first, second) in enumerate(((kept, sent), (sent, kept))):

        @pl.when(core_ref[0] == core)
        def _(first=first, second=second):
            first[...] = total[:half]
            second[...] = total[half:]


def pair_kernel(core_ref, left_ref, right_ref, *refs):
    total = tn(left_ref[...], right_ref[...])
    if len(refs) == 4:
        weight = refs[0][:, : total.shape[1]].astype(F32)
        refs[3][...] = jnp.sum(total * weight, axis=1, keepdims=True)
    keep_half(core_ref, total.astype(BF16), *refs[-3:-1] if len(refs) == 4 else refs)


def split_pairs(total, pairs, core):
    rows, cols = total.shape
    total = total.reshape(pairs, 2, rows // pairs // 2, cols)
    return tuple(
        lax.dynamic_index_in_dim(total, index, 1, False).reshape(-1, cols)
        for index in (core, 1 - core)
    )


def core_index():
    return (lax.axis_index("tok") % 2).astype(jnp.int32).reshape(1)


def pair_grad(left, right, weight=None):
    tokens, rows = left.shape
    cols = right.shape[1]
    pairs = lax.axis_size("tok") // 2
    step = rows // pairs
    if step % 128 or cols % 128:
        total = tn(left, right)
        halves = split_pairs(total.astype(BF16), pairs, lax.axis_index("tok") % 2)
        if weight is None:
            return halves
        return *halves, jnp.sum(total * weight[:, :cols].astype(F32), axis=1, keepdims=True)
    out_shape = [jax.ShapeDtypeStruct((rows // 2, cols), BF16)] * 2
    out_specs = [pl.BlockSpec((step // 2, cols), lambda pair: (pair, 0))] * 2
    in_specs = [
        pl.BlockSpec(memory_space=pltpu.SMEM),
        pl.BlockSpec((tokens, step), lambda pair: (0, pair)),
        pl.BlockSpec((tokens, cols), lambda pair: (0, 0)),
    ]
    operands = [core_index(), left, right]
    if weight is not None:
        operands.append(weight)
        in_specs.append(pl.BlockSpec((step, weight.shape[1]), lambda pair: (pair, 0)))
        out_shape.append(jax.ShapeDtypeStruct((rows, 1), F32))
        out_specs.append(pl.BlockSpec((step, 1), lambda pair: (pair, 0)))
    return pl.pallas_call(
        pair_kernel,
        grid=(pairs,),
        out_shape=out_shape,
        in_specs=in_specs,
        out_specs=out_specs,
        compiler_params=in_order(48),
        cost_estimate=cost(2 * tokens * rows * cols, 2 * (tokens * (rows + cols) + rows * cols)),
    )(*operands)


def part_kernel(core_ref, rows_ref, above_ref, d_gate_ref, d_up_ref, hidden_ref, kept, sent):
    cols = hidden_ref.shape[1]
    for at, (left_ref, right_ref) in enumerate(
        ((rows_ref, d_gate_ref), (rows_ref, d_up_ref), (above_ref, hidden_ref))
    ):
        total = tn(left_ref[...], right_ref[...]).astype(BF16)
        window = (slice(None), pl.ds(at * cols, cols))
        keep_half(core_ref, total, kept.at[window], sent.at[window])


def part_grad(rows, above, d_gate, d_up, hidden):
    tokens, features = rows.shape
    cols = hidden.shape[1]
    pairs = lax.axis_size("tok") // 2
    step = features // pairs
    if step % 128 or cols % 128:
        total = [tn(rows, d_gate), tn(rows, d_up), tn(above, hidden)]
        total = jnp.concatenate(total, axis=1).astype(BF16)
        return split_pairs(total, pairs, lax.axis_index("tok") % 2)
    out = jax.ShapeDtypeStruct((features // 2, 3 * cols), BF16)
    left_spec = pl.BlockSpec((tokens, step), lambda pair: (0, pair))
    right_spec = pl.BlockSpec((tokens, cols), lambda pair: (0, 0))
    return pl.pallas_call(
        part_kernel,
        grid=(pairs,),
        out_shape=(out, out),
        in_specs=[pl.BlockSpec(memory_space=pltpu.SMEM)] + [left_spec] * 2 + [right_spec] * 3,
        out_specs=[pl.BlockSpec((step // 2, 3 * cols), lambda pair: (pair, 0))] * 2,
        compiler_params=in_order(48),
        cost_estimate=cost(
            6 * tokens * features * cols,
            2 * (2 * tokens * features + 3 * cols * (tokens + features)),
        ),
    )(core_index(), rows, above, d_gate, d_up, hidden)


def hold_piece(pieces, held):
    *blocks, top, bottom = pieces
    at = pl.program_id(0)
    for index, piece in enumerate(blocks):

        @pl.when(at == index)
        def _(piece=piece):
            held[...] = piece[...]

    @pl.when(at == len(blocks))
    def _():
        half = top.shape[0]
        held[:half] = top[...]
        held[half:] = bottom[...]


def pieces_grad_kernel(me_ref, core_ref, *refs):
    *pieces, right_ref, kept, sent, held = refs
    hold_piece(pieces, held)
    keep_half(core_ref, tn(held[...], right_ref[...]).astype(BF16), kept, sent)


def add_kernel(left_ref, right_ref, out_ref):
    out_ref[...] = (left_ref[...].astype(F32) + right_ref[...].astype(F32)).astype(BF16)


def add_pair(left, right):
    rows, cols = left.shape
    if rows % 256 or cols % 128:
        return (left.astype(F32) + right.astype(F32)).astype(BF16)
    steps = 10 if rows % 160 == 0 else 8
    spec = pl.BlockSpec((rows // steps, cols), lambda at: (at, 0))
    return pl.pallas_call(
        add_kernel,
        grid=(steps,),
        out_shape=jax.ShapeDtypeStruct(left.shape, BF16),
        in_specs=[spec, spec],
        out_specs=spec,
        compiler_params=in_order(16),
        cost_estimate=cost(rows * cols, 6 * rows * cols),
    )(left, right)


def pieces_grad(pieces, right):
    tokens, step = pieces[0].shape
    cols = right.shape[1]
    me = lax.axis_index("mdl").astype(jnp.int32).reshape(1)
    out = jax.ShapeDtypeStruct((2 * step, cols), BF16)
    return pl.pallas_call(
        pieces_grad_kernel,
        grid_spec=pltpu.PrefetchScalarGridSpec(
            num_scalar_prefetch=2,
            grid=(4,),
            in_specs=[
                pl.BlockSpec(array.shape, lambda at, me_ref, core_ref: (0, 0))
                for array in (*pieces, right)
            ],
            out_specs=[
                pl.BlockSpec((step // 2, cols), lambda at, me_ref, core_ref: (me_ref[0] ^ at, 0))
            ]
            * 2,
            scratch_shapes=[pltpu.VMEM((tokens, step), BF16)],
        ),
        out_shape=(out, out),
        compiler_params=in_order(48),
        cost_estimate=cost(8 * tokens * step * cols, 2 * (4 * tokens * step + 5 * step * cols)),
    )(me, core_index(), *pieces, right)


def sum_kernel(starts, *refs):
    *lefts, weight_ref, out_ref = refs
    total = 0.0
    for left_ref, start in zip(lefts, starts):
        total += nt(left_ref[...], weight_ref[:, start : start + left_ref.shape[1]])
    out_ref[...] = total


def sum_products(lefts, weight, starts):
    tokens = lefts[0].shape[0]
    rows, cols = weight.shape
    if lefts[0].shape[1] % 128:
        return sum(
            nt(left, weight[:, start : start + left.shape[1]])
            for left, start in zip(lefts, starts)
        )
    step = 512
    depth = sum(left.shape[1] for left in lefts)
    return pl.pallas_call(
        functools.partial(sum_kernel, starts),
        grid=(rows // step,),
        out_shape=jax.ShapeDtypeStruct((tokens, rows), F32),
        in_specs=[pl.BlockSpec(left.shape, lambda row: (0, 0)) for left in lefts]
        + [pl.BlockSpec((step, cols), lambda row: (row, 0))],
        out_specs=pl.BlockSpec((tokens, step), lambda row: (0, row)),
        compiler_params=in_order(48),
        cost_estimate=cost(2 * tokens * rows * depth, 2 * rows * cols + 4 * tokens * rows),
    )(*lefts, weight)


def payload_kernel(starts, me_ref, *refs):
    lefts, weight_ref = refs[: len(starts)], refs[len(starts)]
    top_sent, bottom_sent, top_kept, bottom_kept = refs[-4:]
    total = refs[-5][...] if len(refs) == len(starts) + 6 else 0.0
    for left_ref, start in zip(lefts, starts):
        total += nt(left_ref[...], weight_ref[:, start : start + left_ref.shape[1]])
    total = total.astype(BF16)
    half = total.shape[0] // 2
    places = (
        ((top_kept, 0), (bottom_kept, 0)),
        ((top_sent, 0), (bottom_kept, 1)),
        ((top_kept, 1), (bottom_sent, 0)),
        ((top_sent, 1), (bottom_sent, 1)),
    )
    for distance, ((top, top_at), (bottom, bottom_at)) in enumerate(places):

        @pl.when(pl.program_id(0) == 3 - distance)
        def _(top=top, top_at=top_at, bottom=bottom, bottom_at=bottom_at):
            top[top_at] = total[:half]
            bottom[bottom_at] = total[half:]


def scatter_product(lefts, weight, starts, partial=()):
    tokens = lefts[0].shape[0]
    rows, cols = weight.shape
    step = rows // 4
    me = lax.axis_index("mdl").astype(jnp.int32).reshape(1)
    out = jax.ShapeDtypeStruct((2, tokens // 2, step), BF16)
    depth = sum(left.shape[1] for left in lefts)
    return pl.pallas_call(
        functools.partial(payload_kernel, starts),
        grid_spec=pltpu.PrefetchScalarGridSpec(
            num_scalar_prefetch=1,
            grid=(4,),
            in_specs=[pl.BlockSpec(left.shape, lambda at, me_ref: (0, 0)) for left in lefts]
            + [pl.BlockSpec((step, cols), lambda at, me_ref: (me_ref[0] ^ (3 - at), 0))]
            + [pl.BlockSpec((tokens, step), lambda at, me_ref: (0, me_ref[0] ^ (3 - at)))]
            * len(partial),
            out_specs=[pl.BlockSpec(out.shape, lambda at, me_ref: (0, 0, 0))] * 4,
        ),
        out_shape=(out,) * 4,
        compiler_params=in_order(48),
        cost_estimate=cost(2 * tokens * rows * depth, 2 * (tokens * depth + rows * cols + tokens * rows)),
    )(me, *lefts, weight, *partial)


def pieces_kernel(start, me_ref, *refs):
    *pieces, weight_ref, out_ref, total, held = refs
    hold_piece(pieces, held)
    at = pl.program_id(0)
    part = nn(held[...], weight_ref[:, start : start + out_ref.shape[1]])
    part = part + jnp.where(at > 0, total[...], 0.0)
    total[...] = part

    @pl.when(at == 3)
    def _():
        out_ref[...] = part.astype(BF16)


def pieces_product(pieces, weight, start, width):
    tokens, step = pieces[0].shape
    rows, cols = weight.shape
    me = lax.axis_index("mdl").astype(jnp.int32).reshape(1)
    return pl.pallas_call(
        functools.partial(pieces_kernel, start),
        grid_spec=pltpu.PrefetchScalarGridSpec(
            num_scalar_prefetch=1,
            grid=(4,),
            in_specs=[pl.BlockSpec(piece.shape, lambda at, me_ref: (0, 0)) for piece in pieces]
            + [pl.BlockSpec((step, cols), lambda at, me_ref: (me_ref[0] ^ at, 0))],
            out_specs=pl.BlockSpec((tokens, width), lambda at, me_ref: (0, 0)),
            scratch_shapes=[pltpu.VMEM((tokens, width), F32), pltpu.VMEM((tokens, step), BF16)],
        ),
        out_shape=jax.ShapeDtypeStruct((tokens, width), BF16),
        compiler_params=in_order(40),
        cost_estimate=cost(2 * tokens * rows * width, 2 * (tokens * rows + rows * cols + tokens * width)),
    )(me, *pieces, weight)


def product_to_mdl(lefts, weight, starts, partial=()):
    if lax.axis_size("mdl") == 4:
        payload = scatter_product(lefts, weight, starts, partial)
        return payload, lambda payload, *earlier: scatter_payload(payload, *earlier)
    part = sum((sum_products(lefts, weight, starts), *partial))
    return (part.astype(BF16),), lambda payload, *earlier: scatter_mdl(payload[0], 1)


def after(value, *earlier):
    return lax.optimization_barrier((value, *earlier))[0]


def row_scale(rows_b, axis=-1):
    rows = rows_b.astype(F32)
    return lax.rsqrt(jnp.mean(rows * rows, axis=axis, keepdims=True) + NORM_EPS)


def gelu_parts(value):
    root = math.sqrt(2.0 / math.pi)
    square = value * value
    tanh = jnp.tanh(root * (value + 0.044715 * value * square))
    cdf = 0.5 * (1.0 + tanh)
    slope = cdf + 0.5 * value * (1.0 - tanh * tanh) * root * (1.0 + 3 * 0.044715 * square)
    return value * cdf, slope


def scaled(weight, gain):
    return (weight.astype(F32) * gain.astype(F32)[:, None]).astype(BF16)


def on_device(
    inputs, positions, norm1_gain, qkv_weight, out_weight, norm2_gain, gate_weight,
    up_weight, down_weight, cotangent,
):
    me = lax.axis_index("mdl")
    size = lax.axis_size("mdl")
    head_cols = HEADS * HEAD
    width = inputs.shape[1]
    features = width * size

    def from_tok(weight, dim):
        return lax.all_gather(weight, "tok", axis=dim, tiled=True)

    def pair_to_tok(local):
        kept, sent = local
        count = lax.axis_size("tok")
        got = lax.ppermute(sent, "tok", [(i, i ^ 1) for i in range(count)])
        both = add_pair(kept, got)
        groups = [list(range(core, count, 2)) for core in range(2)]
        total = lax.psum_scatter(
            both, "tok", scatter_dimension=0, tiled=True, axis_index_groups=groups
        )
        return total.astype(F32)

    qkv_cols, ff_cols = qkv_weight.shape[1], gate_weight.shape[1]
    attn_local = jnp.concatenate([scaled(qkv_weight, norm1_gain), out_weight.T], axis=1)
    middle = ff_cols // 256 * 128
    parts = ((0, middle), (middle, ff_cols))
    if size == 4 and lax.axis_size("tok") == 8:
        rows_in, w_attn, locals_ff = first_gather(
            inputs,
            attn_local,
            norm2_gain.astype(F32)[:, None],
            (gate_weight, up_weight, down_weight.T),
            parts,
        )
    else:
        rows_in = gather_mdl(inputs, 1)
        w_attn = from_tok(attn_local, 0)
        scaled_gu = [scaled(weight, norm2_gain) for weight in (gate_weight, up_weight)]
        locals_ff = [
            jnp.concatenate([w[:, start:stop] for w in (*scaled_gu, down_weight.T)], axis=1)
            for start, stop in parts
        ]
    w_qkv = w_attn[:, :qkv_cols]
    w_parts = [from_tok(local, 0) for local in locals_ff]

    qkv = rows_to_cols(nn(rows_in, w_qkv).astype(BF16))
    count = qkv.shape[0]
    scale_own = row_scale(lax.dynamic_slice_in_dim(rows_in, me * count, count, 0))
    scale_one = row_scale(after(rows_in, qkv))
    half = HEAD // 2
    frequency = jnp.exp(jnp.arange(half, dtype=F32) * (-2.0 * math.log(10000.0) / HEAD))
    angles = positions.astype(F32)[:, None] * frequency[None, :]
    cos, sin = jnp.cos(angles), jnp.sin(angles)
    kv_own = qkv[:, head_cols:].astype(F32) * scale_own
    key_rows = turn(kv_own[:, :HEAD], cos, sin)
    kv = gather_mdl(jnp.concatenate([key_rows, kv_own[:, HEAD:]], axis=1).astype(BF16), 0)
    first = (me * count).astype(jnp.int32).reshape(1)
    pos = positions[:, None]
    attended, log_norm = attention_forward(first, qkv, kv, cos, sin, pos, scale_own)
    head_block = cols_to_rows(attended)
    residual = inputs.astype(F32)
    payload, scatter = product_to_mdl((head_block,), w_attn, (qkv_cols,))
    mixed = residual + scatter(payload)

    rows_two = gather_mdl(mixed.astype(BF16), 1)
    scale_two = row_scale(rows_two)
    rows_hat = (rows_two.astype(F32) * scale_two).astype(BF16)
    rows, above, stat_two, partial, hiddens, sums = rows_hat, cotangent, 0.0, (), [], []
    for index, (weight, (start, stop)) in enumerate(zip(w_parts, parts)):
        cols = stop - start
        last = index == len(parts) - 1
        gate_in = nn(rows, weight[:, :cols])
        up_in = nn(rows, weight[:, cols : 2 * cols])
        d_hidden = nn(above, weight[:, 2 * cols :])
        gelu, slope = gelu_parts(gate_in)
        hidden = (gelu * up_in).astype(BF16)
        d_gate = d_hidden * up_in * slope
        d_up = d_hidden * gelu
        stat_two += jnp.sum(d_gate * gate_in + d_up * up_in, axis=1)
        d_gate, d_up = d_gate.astype(BF16), d_up.astype(BF16)
        hiddens.append(hidden)
        lefts, starts = (d_gate, d_up), (0, cols)
        if last:
            payload, scatter = product_to_mdl(lefts, weight, starts, partial)
            rows, above, _ = lax.optimization_barrier((rows, above, payload[0]))
        local = part_grad(rows, above, d_gate, d_up, hidden)
        if not last:
            d_gate = after(d_gate, local[0])
            partial = (sum_products((d_gate, d_up), weight, starts),)
            rows, above, _ = lax.optimization_barrier((rows, above, local[0]))
        sums.append(pair_to_tok(local))
    d_two = scatter(payload)
    stat_two = sum_mdl(stat_two.reshape(8, -1)).reshape(-1, 1) * (1.0 / features)
    scale_mixed = scale_two * mixed
    cotangent_own = lax.dynamic_slice_in_dim(cotangent, me * width, width, 1).astype(F32)
    d_mixed = cotangent_own + scale_two * (d_two - scale_mixed * stat_two)

    d_mixed_b = after(d_mixed.astype(BF16), local[0])
    down_starts = tuple(2 * (stop - start) for start, stop in parts)
    ffn = (sum_products((after(hiddens[0], d_mixed_b),), w_parts[0], down_starts[:1]),)
    ffn_payload, ffn_scatter = product_to_mdl(
        (after(hiddens[1], d_mixed_b),), w_parts[1], down_starts[1:], ffn
    )
    if size == 4 and lax.axis_size("tok") == 8:
        pieces = gather_pieces(d_mixed_b)
        d_head = pieces_product(pieces, w_attn, qkv_cols, head_block.shape[1])
        heads_later = after(head_block, d_head)
        out_local = pieces_grad(pieces, heads_later)
    else:
        d_mixed_rows = gather_mdl(d_mixed_b, 1)
        d_head = nn(d_mixed_rows, w_attn[:, qkv_cols:]).astype(BF16)
        out_local = pair_grad(d_mixed_rows, head_block)
    out_grad = pair_to_tok(out_local)
    d_attended = rows_to_cols(d_head)
    d_query, d_kv = attention_backward(
        first, qkv, kv, cos, sin, pos, scale_own, attended, d_attended, log_norm
    )
    d_kv = scatter_mdl(d_kv.astype(BF16), 0)
    d_key = unturn(d_kv[:, :HEAD], cos, sin).astype(BF16)
    d_qkv = jnp.concatenate([d_query, d_key, d_kv[:, HEAD:].astype(BF16)], axis=1)
    stat_one = jnp.sum(d_qkv.astype(F32) * qkv.astype(F32), axis=1) * scale_own[:, 0]
    d_qkv_part = cols_to_rows(d_qkv)
    stat_rows = jnp.zeros((size, count), F32)
    stat_rows = sum_mdl(lax.dynamic_update_slice(stat_rows, stat_one[None], (me, 0)))
    stat_one = stat_rows.reshape(-1, 1) * (1.0 / features)
    payload, scatter = product_to_mdl((d_qkv_part,), w_attn, (0,))
    d_scaled = (after(d_qkv_part, payload[0]).astype(F32) * scale_one).astype(BF16)
    *qkv_local, gain_one = pair_grad(rows_in, d_scaled, w_attn)
    qkv_sum = pair_to_tok(qkv_local)
    d_one = scatter(payload)
    ffn_sum = ffn_scatter(ffn_payload, d_qkv_part)
    block_out = (mixed + ffn_sum).astype(BF16)
    input_grad = d_mixed + scale_one * (d_one - (scale_one * residual) * stat_one)

    norm1_late, norm2_late, gate_late, up_late, _ = lax.optimization_barrier(
        (norm1_gain, norm2_gain, gate_weight, up_weight, local[0])
    )

    def unfold(total, gain):
        return total * gain.astype(F32)[:, None]

    def joined(at):
        widths = [total.shape[1] // 3 for total in sums]
        pieces = [total[:, at * cols :][:, :cols] for total, cols in zip(sums, widths)]
        return jnp.concatenate(pieces, axis=1)

    gate_sum, up_sum, down_grad = joined(0), joined(1), joined(2).T
    gain_two = jnp.sum(
        gate_late.astype(F32) * gate_sum + up_late.astype(F32) * up_sum, axis=1
    )
    gate_grad, up_grad = unfold(gate_sum, norm2_late), unfold(up_sum, norm2_late)
    out_grad = out_grad.T
    gain_two_grad = sum_mdl(gain_two)
    gain_one = sum_mdl(sum_tok(gain_one.reshape(8, -1))).reshape(-1)
    shard = norm1_gain.shape[0]
    gain_one = lax.dynamic_slice_in_dim(gain_one, lax.axis_index("tok") * shard, shard, 0)
    gain_one_grad = gain_one / norm1_late.astype(F32)
    return (
        block_out,
        input_grad,
        gain_one_grad,
        unfold(qkv_sum, norm1_late),
        out_grad,
        gain_two_grad,
        gate_grad,
        up_grad,
        down_grad,
    )


def solution(mesh):
    return jax.shard_map(
        on_device,
        mesh=mesh,
        in_specs=(
            P("tok", "mdl"),
            P(("tok", "mdl")),
            P("tok"),
            P("tok", "mdl"),
            P("mdl", "tok"),
            P("tok"),
            P("tok", "mdl"),
            P("tok", "mdl"),
            P("mdl", "tok"),
            P("tok", None),
        ),
        out_specs=(
            P("tok", "mdl"),
            P("tok", "mdl"),
            P("tok"),
            P("tok", "mdl"),
            P("mdl", "tok"),
            P("tok"),
            P("tok", "mdl"),
            P("tok", "mdl"),
            P("mdl", "tok"),
        ),
        check_vma=False,
    )
```

```python
import functools
import math

import jax
import jax.numpy as jnp
from jax import lax
from jax.experimental import pallas as pl
from jax.experimental.pallas import tpu as pltpu
from jax.sharding import PartitionSpec as P


HEADS = 10
HEAD = 256
NORM_EPS = 1e-06
F32 = jnp.float32
BF16 = jnp.bfloat16
MASKED = -1e30


def nt(left_op, right_op):
    return lax.dot_general(
        left_op, right_op, (((1,), (1,)), ((), ())), preferred_element_type=F32
    )


def tn(left_op, right_op):
    return lax.dot_general(
        left_op, right_op, (((0,), (0,)), ((), ())), preferred_element_type=F32
    )


def nn(left_op, right_op):
    return jnp.dot(left_op, right_op, preferred_element_type=F32)


def swap(block, distance):
    size = lax.axis_size("mdl")
    return lax.ppermute(block, "mdl", [(i, i ^ distance) for i in range(size)])


def gather_mdl(block, dim):
    size = lax.axis_size("mdl")
    if size != 4:
        return lax.all_gather(block, "mdl", axis=dim, tiled=True)
    me = lax.axis_index("mdl")
    half = block.shape[0] // 2
    along_x = swap(block, 1)
    along_y = swap(block, 2)
    top = swap(along_x[:half], 2)
    bottom = swap(along_y[half:], 1)
    width = block.shape[dim]
    shape = list(block.shape)
    shape[dim] = width * size
    whole = jnp.zeros(shape, block.dtype)

    def put(whole, piece, source, row):
        start = [0, 0]
        start[dim] = source * width
        start[0] = start[0] + row
        return lax.dynamic_update_slice(whole, piece, tuple(start))

    whole = put(whole, block, me, 0)
    whole = put(whole, along_x, me ^ 1, 0)
    whole = put(whole, along_y, me ^ 2, 0)
    whole = put(whole, top, me ^ 3, 0)
    whole = put(whole, bottom, me ^ 3, half)
    return whole


def scatter_mdl(part, dim):
    size = lax.axis_size("mdl")
    if size != 4:
        return lax.psum_scatter(part, "mdl", scatter_dimension=dim, tiled=True).astype(F32)
    me = lax.axis_index("mdl")
    shape = list(part.shape)
    shape[dim] //= size
    half = shape[0] // 2

    def piece(block, row):
        start = [0, 0]
        start[dim] = block * shape[dim]
        start[0] = start[0] + row
        return lax.dynamic_slice(part, tuple(start), (half, shape[1]))

    sums = []
    for row, first, second in ((0, 1, 2), (half, 2, 1)):
        sent = jnp.stack([piece(me ^ first, row), piece(me ^ 3, row)])
        sums.append((row, second, swap(sent, first)))
    partial = []
    for row, second, got in sums:
        other = piece(me ^ second, row).astype(F32) + got[1].astype(F32)
        partial.append((row, got[0], swap(other.astype(BF16), second)))
    return jnp.concatenate(
        [
            piece(me, row).astype(F32) + first.astype(F32) + second.astype(F32)
            for row, first, second in partial
        ],
        axis=0,
    )


def gather_pieces(block):
    half = block.shape[0] // 2
    along_x = swap(block, 1)
    along_y = swap(block, 2)
    top = swap(along_x[:half], 2)
    bottom = swap(along_y[half:], 1)
    return block, along_x, along_y, top, bottom


def scatter_payload(payload, *earlier):
    top_sent, bottom_sent, top_kept, bottom_kept = payload
    got_top = swap(top_sent, 1)
    got_bottom = swap(bottom_sent, 2)
    halves = []
    for kept, got, second in ((top_kept, got_top, 2), (bottom_kept, got_bottom, 1)):
        passed = (kept[1].astype(F32) + got[1].astype(F32)).astype(BF16)
        if earlier:
            passed = after(passed, *earlier)
        last = swap(passed, second)
        halves.append(kept[0].astype(F32) + got[0].astype(F32) + last.astype(F32))
    return jnp.concatenate(halves, axis=0)


def sum_mdl(value):
    size = lax.axis_size("mdl")
    distance = 1
    while distance < size:
        value = value + swap(value, distance)
        distance *= 2
    return value


def sum_tok(value):
    size = lax.axis_size("tok")
    distance = 1
    while distance < size:
        value = value + lax.ppermute(value, "tok", [(i, i ^ distance) for i in range(size)])
        distance *= 2
    return value


def rows_to_cols(block):
    return lax.all_to_all(block, "mdl", split_axis=0, concat_axis=1, tiled=True)


def cols_to_rows(block):
    return lax.all_to_all(block, "mdl", split_axis=1, concat_axis=0, tiled=True)


def first_kernel(parts, x_ref, w_ref, *refs):
    weights, (rows_ref, weight_ref), locals_ref = refs[:3], refs[3:5], refs[5:7]
    held, joined = refs[7:10], refs[10:12]
    own, x_sent, x_got, w_up, w_down, w_core, w_got = refs[12:]
    me, tok = lax.axis_index("mdl"), lax.axis_index("tok")
    pairs = lax.axis_size("tok") // 2
    level, last = tok // 2, pairs - 1
    half, width = x_ref.shape[0] // 2, x_ref.shape[1]
    shard, all_cols = w_ref.shape[0], weight_ref.shape[1]
    below, above = level > 0, level < last

    barrier = pltpu.get_barrier_semaphore()
    pl.semaphore_signal(barrier, inc=1, device_id={"mdl": me ^ 1})
    pl.semaphore_signal(barrier, inc=1, device_id={"mdl": me ^ 2})
    pl.semaphore_signal(barrier, inc=1, device_id={"tok": tok ^ 1})

    @pl.when(below)
    def _():
        pl.semaphore_signal(barrier, inc=1, device_id={"tok": tok - 2})

    @pl.when(above)
    def _():
        pl.semaphore_signal(barrier, inc=1, device_id={"tok": tok + 2})

    pl.semaphore_wait(barrier, 3 + below.astype(jnp.int32) + above.astype(jnp.int32))

    def cols(block):
        return pl.ds(pl.multiple_of(block * width, 128), width)

    piece = shard // 2

    def block(index, part):
        return weight_ref.at[pl.ds(pl.multiple_of(index * shard + part * piece, 16), piece)]

    def x_copy(source, target, at, to):
        return pltpu.make_async_remote_copy(
            source, target, x_sent.at[at], x_got.at[at], device_id={"mdl": me ^ to}
        )

    def w_copy(source, index, part, sent, to):
        return pltpu.make_async_remote_copy(
            source, block(index, part), sent, w_got.at[index, part], device_id={"tok": to}
        )

    mine = rows_ref.at[:, cols(me)]
    to_x, to_y = x_copy(x_ref, mine, 0, 1), x_copy(x_ref, mine, 1, 2)
    keeps = [pltpu.make_async_copy(x_ref, mine, own.at[0])]
    for part in range(2):
        source = w_ref.at[pl.ds(part * piece, piece), pl.ds(0, all_cols)]

        @pl.when(above)
        def _(source=source, part=part):
            w_copy(source, tok, part, w_up.at[0, part], tok + 2).start()

        @pl.when(below)
        def _(source=source, part=part):
            w_copy(source, tok, part, w_down.at[0, part], tok - 2).start()

        w_copy(source, tok, part, w_core.at[tok, part], tok ^ 1).start()
        keeps.append(pltpu.make_async_copy(source, block(tok, part), own.at[1 + part]))
        if part == 0:
            to_x.start()
            to_y.start()
    loads = [
        pltpu.make_async_copy(weight, to, own.at[3 + at])
        for at, (weight, to) in enumerate(zip(weights, held))
    ]
    for copy in (*keeps, *loads):
        copy.start()
    for copy in loads:
        copy.wait()
    gain = w_ref[:, all_cols : all_cols + 1].astype(F32)
    for (start, stop), out in zip(parts, joined):
        count = stop - start
        for at, source in enumerate(held):
            value = source[:, start:stop]
            if at < 2:
                value = (value.astype(F32) * gain).astype(BF16)
            out[:, at * count : (at + 1) * count] = value

    def relay(distance, part):
        low, high = tok - 2 * distance, tok + 2 * distance

        @pl.when(level >= distance)
        def _():
            source = block(low, part)
            w_copy(source, low, part, w_core.at[low, part], tok ^ 1).wait_recv()

            @pl.when(above)
            def _():
                w_copy(source, low, part, w_up.at[distance, part], tok + 2).start()

            w_copy(source, low, part, w_core.at[low, part], tok ^ 1).start()

        @pl.when(level + distance <= last)
        def _():
            source = block(high, part)
            w_copy(source, high, part, w_core.at[high, part], tok ^ 1).wait_recv()

            @pl.when(below)
            def _():
                w_copy(source, high, part, w_down.at[distance, part], tok - 2).start()

            w_copy(source, high, part, w_core.at[high, part], tok ^ 1).start()

    relay(1, 0)
    relay(1, 1)
    stores = [
        pltpu.make_async_copy(out, to, own.at[6 + at])
        for at, (out, to) in enumerate(zip(joined, locals_ref))
    ]
    for copy in stores:
        copy.start()
    from_x = rows_ref.at[pl.ds(0, half), cols(me ^ 1)]
    from_y = rows_ref.at[pl.ds(half, half), cols(me ^ 2)]
    top, bottom = x_copy(from_x, from_x, 2, 2), x_copy(from_y, from_y, 3, 1)
    to_x.wait_recv()
    top.start()
    to_y.wait_recv()
    bottom.start()
    for distance in range(2, pairs):
        relay(distance, 0)
        relay(distance, 1)
    for copy in (*keeps, *stores):
        copy.wait()
    for copy in (top, bottom):
        copy.wait_recv()
    for copy in (to_x, to_y, top, bottom):
        copy.wait_send()

    for distance in range(pairs):
        for part in range(2):
            mine = block(tok, part)

            @pl.when((level >= distance) & above)
            def _(mine=mine, distance=distance, part=part):
                w_copy(mine, tok, part, w_up.at[distance, part], tok + 2).wait_send()

            @pl.when((level + distance <= last) & below)
            def _(mine=mine, distance=distance, part=part):
                w_copy(mine, tok, part, w_down.at[distance, part], tok - 2).wait_send()

            near, far = 2 * distance + tok % 2, 2 * distance + 1 - tok % 2
            w_copy(block(near, part), near, part, w_core.at[near, part], tok ^ 1).wait_send()
            w_copy(block(far, part), far, part, w_core.at[near, part], tok ^ 1).wait_recv()


def first_gather(inputs, weight, weights, parts):
    tokens, width = inputs.shape
    shard, cols = weight.shape
    pairs = lax.axis_size("tok") // 2
    dma = pltpu.SemaphoreType.DMA
    locals_ff = [(shard, 3 * (stop - start)) for start, stop in parts]
    shapes = [(tokens, 4 * width), (2 * pairs * shard, cols - 128), *locals_ff]
    *gathered, first, second = pl.pallas_call(
        functools.partial(first_kernel, parts),
        out_shape=[jax.ShapeDtypeStruct(shape, BF16) for shape in shapes],
        in_specs=[pl.BlockSpec(memory_space=pltpu.VMEM)] * 2
        + [pl.BlockSpec(memory_space=pl.ANY)] * 3,
        out_specs=[pl.BlockSpec(memory_space=pl.ANY)] * 4,
        scratch_shapes=[pltpu.VMEM(array.shape, BF16) for array in weights]
        + [pltpu.VMEM(shape, BF16) for shape in locals_ff]
        + [
            dma((8,)), dma((4,)), dma((4,)), dma((pairs, 2)), dma((pairs, 2)),
            dma((2 * pairs, 2)), dma((2 * pairs, 2)),
        ],
        compiler_params=pltpu.CompilerParams(
            collective_id=0, has_side_effects=True, vmem_limit_bytes=60 << 20
        ),
    )(inputs, weight, *weights)
    return *gathered, (first, second)


def in_order(mebibytes):
    return pltpu.CompilerParams(
        dimension_semantics=(pltpu.ARBITRARY,), vmem_limit_bytes=mebibytes << 20
    )


def cost(flops, bytes_accessed, transcendentals=0):
    return pl.CostEstimate(
        flops=flops, bytes_accessed=bytes_accessed, transcendentals=transcendentals
    )


def turn(vector, cos, sin):
    half = HEAD // 2
    lower, upper = vector[:, :half], vector[:, half:]
    return jnp.concatenate([lower * cos - upper * sin, upper * cos + lower * sin], axis=1)


def unturn(vector, cos, sin):
    half = HEAD // 2
    lower, upper = vector[:, :half], vector[:, half:]
    return jnp.concatenate([lower * cos + upper * sin, upper * cos - lower * sin], axis=1)


def seen(first_ref, position_ref, queries, keys):
    row = lax.broadcasted_iota(jnp.int32, (queries, keys), 0) + first_ref[0]
    distance = row - lax.broadcasted_iota(jnp.int32, (queries, keys), 1)
    return (distance >= 0) & (distance <= position_ref[...])


def forward_kernel(
    first_ref, q_ref, kv_ref, cos_ref, sin_ref, pos_ref, scale_ref, out_ref, norm_ref
):
    query = turn(q_ref[...].astype(F32) * scale_ref[...], cos_ref[...], sin_ref[...])
    query = (query * HEAD ** (-0.5)).astype(BF16)
    keys, values = kv_ref[:, :HEAD], kv_ref[:, HEAD:]
    scores = nt(query, keys)
    scores = jnp.where(seen(first_ref, pos_ref, *scores.shape), scores, MASKED)
    top = jnp.max(scores, axis=1, keepdims=True)
    weights = jnp.exp(scores - top)
    total = jnp.sum(weights, axis=1, keepdims=True)
    out_ref[...] = (nn(weights.astype(BF16), values) / total).astype(BF16)
    norm_ref[0] = top + jnp.log(total)


def backward_kernel(
    first_ref, q_ref, kv_ref, cos_ref, sin_ref, pos_ref, scale_ref, att_ref, datt_ref, norm_ref,
    dq_ref, dkv_ref,
):
    head = pl.program_id(0)
    scale = HEAD ** (-0.5)
    cos, sin = cos_ref[...], sin_ref[...]
    query = (turn(q_ref[...].astype(F32) * scale_ref[...], cos, sin) * scale).astype(BF16)
    keys, values = kv_ref[:, :HEAD], kv_ref[:, HEAD:]
    scores = nt(query, keys)
    visible = seen(first_ref, pos_ref, *scores.shape)
    again = jnp.where(visible, jnp.exp(scores - norm_ref[0]), 0.0)
    d_att = datt_ref[...]
    delta = jnp.sum(d_att.astype(F32) * att_ref[...].astype(F32), axis=1, keepdims=True)
    d_scores = (again * (nt(d_att, values) - delta)).astype(BF16)
    d_query = nn(d_scores, keys) * scale
    dq_ref[...] = unturn(d_query, cos, sin).astype(BF16)

    @pl.when(head == 0)
    def _():
        dkv_ref[...] = jnp.zeros_like(dkv_ref)

    dkv_ref[:, :HEAD] += tn(d_scores, query)
    dkv_ref[:, HEAD:] += tn(again.astype(BF16), d_att)


def whole_spec(shape):
    return pl.BlockSpec(shape, lambda head: (0,) * len(shape))


def attention_forward(first, qkv, kv, cos, sin, pos, scale):
    rows, keys = qkv.shape[0], kv.shape[0]
    head_spec = pl.BlockSpec((rows, HEAD), lambda head: (0, head))
    return pl.pallas_call(
        forward_kernel,
        grid=(HEADS,),
        out_shape=(
            jax.ShapeDtypeStruct((rows, HEADS * HEAD), BF16),
            jax.ShapeDtypeStruct((HEADS, rows, 1), F32),
        ),
        in_specs=[
            pl.BlockSpec(memory_space=pltpu.SMEM),
            head_spec,
            whole_spec((keys, 2 * HEAD)),
            whole_spec((rows, HEAD // 2)),
            whole_spec((rows, HEAD // 2)),
            whole_spec((rows, 1)),
            whole_spec((rows, 1)),
        ],
        out_specs=(head_spec, pl.BlockSpec((1, rows, 1), lambda head: (head, 0, 0))),
        compiler_params=in_order(32),
        cost_estimate=cost(4 * rows * keys * HEADS * HEAD, 4 * rows * HEADS * HEAD + 4 * keys * HEAD, rows * keys * HEADS),
        name="att_f",
    )(first, qkv, kv, cos, sin, pos, scale)


def attention_backward(first, qkv, kv, cos, sin, pos, scale, att, d_att, norm):
    rows, keys = qkv.shape[0], kv.shape[0]
    head_spec = pl.BlockSpec((rows, HEAD), lambda head: (0, head))
    return pl.pallas_call(
        backward_kernel,
        grid=(HEADS,),
        out_shape=(
            jax.ShapeDtypeStruct((rows, HEADS * HEAD), BF16),
            jax.ShapeDtypeStruct((keys, 2 * HEAD), F32),
        ),
        in_specs=[
            pl.BlockSpec(memory_space=pltpu.SMEM),
            head_spec,
            whole_spec((keys, 2 * HEAD)),
            whole_spec((rows, HEAD // 2)),
            whole_spec((rows, HEAD // 2)),
            whole_spec((rows, 1)),
            whole_spec((rows, 1)),
            head_spec,
            head_spec,
            pl.BlockSpec((1, rows, 1), lambda head: (head, 0, 0)),
        ],
        out_specs=(head_spec, whole_spec((keys, 2 * HEAD))),
        compiler_params=in_order(40),
        cost_estimate=cost(10 * rows * keys * HEADS * HEAD, 8 * rows * HEADS * HEAD + 12 * keys * HEAD, rows * keys * HEADS),
        name="att_b",
    )(first, qkv, kv, cos, sin, pos, scale, att, d_att, norm)


def keep_half(core_ref, total, kept, sent):
    half = total.shape[0] // 2
    for core, (first, second) in enumerate(((kept, sent), (sent, kept))):

        @pl.when(core_ref[0] == core)
        def _(first=first, second=second):
            first[...] = total[:half]
            second[...] = total[half:]


def pair_kernel(core_ref, left_ref, right_ref, *refs):
    total = tn(left_ref[...], right_ref[...])
    if len(refs) == 4:
        weight = refs[0][:, : total.shape[1]].astype(F32)
        refs[3][...] = jnp.sum(total * weight, axis=1, keepdims=True)
    keep_half(core_ref, total.astype(BF16), *refs[-3:-1] if len(refs) == 4 else refs)


def split_pairs(total, pairs, core):
    rows, cols = total.shape
    total = total.reshape(pairs, 2, rows // pairs // 2, cols)
    return tuple(
        lax.dynamic_index_in_dim(total, index, 1, False).reshape(-1, cols)
        for index in (core, 1 - core)
    )


def core_index():
    return (lax.axis_index("tok") % 2).astype(jnp.int32).reshape(1)


def pair_grad(left, right, weight=None):
    tokens, rows = left.shape
    cols = right.shape[1]
    pairs = lax.axis_size("tok") // 2
    step = rows // pairs
    if step % 128 or cols % 128:
        total = tn(left, right)
        halves = split_pairs(total.astype(BF16), pairs, lax.axis_index("tok") % 2)
        if weight is None:
            return halves
        return *halves, jnp.sum(total * weight[:, :cols].astype(F32), axis=1, keepdims=True)
    out_shape = [jax.ShapeDtypeStruct((rows // 2, cols), BF16)] * 2
    out_specs = [pl.BlockSpec((step // 2, cols), lambda pair: (pair, 0))] * 2
    in_specs = [
        pl.BlockSpec(memory_space=pltpu.SMEM),
        pl.BlockSpec((tokens, step), lambda pair: (0, pair)),
        pl.BlockSpec((tokens, cols), lambda pair: (0, 0)),
    ]
    operands = [core_index(), left, right]
    if weight is not None:
        operands.append(weight)
        in_specs.append(pl.BlockSpec((step, weight.shape[1]), lambda pair: (pair, 0)))
        out_shape.append(jax.ShapeDtypeStruct((rows, 1), F32))
        out_specs.append(pl.BlockSpec((step, 1), lambda pair: (pair, 0)))
    return pl.pallas_call(
        pair_kernel,
        grid=(pairs,),
        out_shape=out_shape,
        in_specs=in_specs,
        out_specs=out_specs,
        compiler_params=in_order(48),
        cost_estimate=cost(2 * tokens * rows * cols, 2 * (tokens * (rows + cols) + rows * cols)),
    )(*operands)


def part_kernel(core_ref, rows_ref, above_ref, d_gate_ref, d_up_ref, hidden_ref, kept, sent):
    cols = hidden_ref.shape[1]
    for at, (left_ref, right_ref) in enumerate(
        ((rows_ref, d_gate_ref), (rows_ref, d_up_ref), (above_ref, hidden_ref))
    ):
        total = tn(left_ref[...], right_ref[...]).astype(BF16)
        window = (slice(None), pl.ds(at * cols, cols))
        keep_half(core_ref, total, kept.at[window], sent.at[window])


def part_grad(rows, above, d_gate, d_up, hidden):
    tokens, features = rows.shape
    cols = hidden.shape[1]
    pairs = lax.axis_size("tok") // 2
    step = features // pairs
    if step % 128 or cols % 128:
        total = [tn(rows, d_gate), tn(rows, d_up), tn(above, hidden)]
        total = jnp.concatenate(total, axis=1).astype(BF16)
        return split_pairs(total, pairs, lax.axis_index("tok") % 2)
    out = jax.ShapeDtypeStruct((features // 2, 3 * cols), BF16)
    left_spec = pl.BlockSpec((tokens, step), lambda pair: (0, pair))
    right_spec = pl.BlockSpec((tokens, cols), lambda pair: (0, 0))
    return pl.pallas_call(
        part_kernel,
        grid=(pairs,),
        out_shape=(out, out),
        in_specs=[pl.BlockSpec(memory_space=pltpu.SMEM)] + [left_spec] * 2 + [right_spec] * 3,
        out_specs=[pl.BlockSpec((step // 2, 3 * cols), lambda pair: (pair, 0))] * 2,
        compiler_params=in_order(48),
        cost_estimate=cost(
            6 * tokens * features * cols,
            2 * (2 * tokens * features + 3 * cols * (tokens + features)),
        ),
    )(core_index(), rows, above, d_gate, d_up, hidden)


def hold_piece(pieces, held):
    *blocks, top, bottom = pieces
    at = pl.program_id(0)
    for index, piece in enumerate(blocks):

        @pl.when(at == index)
        def _(piece=piece):
            held[...] = piece[...]

    @pl.when(at == len(blocks))
    def _():
        half = top.shape[0]
        held[:half] = top[...]
        held[half:] = bottom[...]


def pieces_grad_kernel(me_ref, core_ref, *refs):
    *pieces, right_ref, kept, sent, held = refs
    hold_piece(pieces, held)
    keep_half(core_ref, tn(held[...], right_ref[...]).astype(BF16), kept, sent)


def add_kernel(left_ref, right_ref, out_ref):
    out_ref[...] = (left_ref[...].astype(F32) + right_ref[...].astype(F32)).astype(BF16)


def add_pair(left, right):
    rows, cols = left.shape
    if rows % 256 or cols % 128:
        return (left.astype(F32) + right.astype(F32)).astype(BF16)
    steps = 10 if rows % 160 == 0 else 8
    spec = pl.BlockSpec((rows // steps, cols), lambda at: (at, 0))
    return pl.pallas_call(
        add_kernel,
        grid=(steps,),
        out_shape=jax.ShapeDtypeStruct(left.shape, BF16),
        in_specs=[spec, spec],
        out_specs=spec,
        compiler_params=in_order(16),
        cost_estimate=cost(rows * cols, 6 * rows * cols),
    )(left, right)


def pieces_grad(pieces, right):
    tokens, step = pieces[0].shape
    cols = right.shape[1]
    me = lax.axis_index("mdl").astype(jnp.int32).reshape(1)
    out = jax.ShapeDtypeStruct((2 * step, cols), BF16)
    return pl.pallas_call(
        pieces_grad_kernel,
        grid_spec=pltpu.PrefetchScalarGridSpec(
            num_scalar_prefetch=2,
            grid=(4,),
            in_specs=[
                pl.BlockSpec(array.shape, lambda at, me_ref, core_ref: (0, 0))
                for array in (*pieces, right)
            ],
            out_specs=[
                pl.BlockSpec((step // 2, cols), lambda at, me_ref, core_ref: (me_ref[0] ^ at, 0))
            ]
            * 2,
            scratch_shapes=[pltpu.VMEM((tokens, step), BF16)],
        ),
        out_shape=(out, out),
        compiler_params=in_order(48),
        cost_estimate=cost(8 * tokens * step * cols, 2 * (4 * tokens * step + 5 * step * cols)),
    )(me, core_index(), *pieces, right)


def sum_kernel(starts, *refs):
    *lefts, weight_ref, out_ref = refs
    total = 0.0
    for left_ref, start in zip(lefts, starts):
        total += nt(left_ref[...], weight_ref[:, start : start + left_ref.shape[1]])
    out_ref[...] = total


def sum_products(lefts, weight, starts):
    tokens = lefts[0].shape[0]
    rows, cols = weight.shape
    if lefts[0].shape[1] % 128:
        return sum(
            nt(left, weight[:, start : start + left.shape[1]])
            for left, start in zip(lefts, starts)
        )
    step = 512
    depth = sum(left.shape[1] for left in lefts)
    return pl.pallas_call(
        functools.partial(sum_kernel, starts),
        grid=(rows // step,),
        out_shape=jax.ShapeDtypeStruct((tokens, rows), F32),
        in_specs=[pl.BlockSpec(left.shape, lambda row: (0, 0)) for left in lefts]
        + [pl.BlockSpec((step, cols), lambda row: (row, 0))],
        out_specs=pl.BlockSpec((tokens, step), lambda row: (0, row)),
        compiler_params=in_order(48),
        cost_estimate=cost(2 * tokens * rows * depth, 2 * rows * cols + 4 * tokens * rows),
    )(*lefts, weight)


def payload_kernel(starts, me_ref, *refs):
    lefts, weight_ref = refs[: len(starts)], refs[len(starts)]
    top_sent, bottom_sent, top_kept, bottom_kept = refs[-4:]
    total = refs[-5][...] if len(refs) == len(starts) + 6 else 0.0
    for left_ref, start in zip(lefts, starts):
        total += nt(left_ref[...], weight_ref[:, start : start + left_ref.shape[1]])
    total = total.astype(BF16)
    half = total.shape[0] // 2
    places = (
        ((top_kept, 0), (bottom_kept, 0)),
        ((top_sent, 0), (bottom_kept, 1)),
        ((top_kept, 1), (bottom_sent, 0)),
        ((top_sent, 1), (bottom_sent, 1)),
    )
    for distance, ((top, top_at), (bottom, bottom_at)) in enumerate(places):

        @pl.when(pl.program_id(0) == 3 - distance)
        def _(top=top, top_at=top_at, bottom=bottom, bottom_at=bottom_at):
            top[top_at] = total[:half]
            bottom[bottom_at] = total[half:]


def scatter_product(lefts, weight, starts, partial=()):
    tokens = lefts[0].shape[0]
    rows, cols = weight.shape
    step = rows // 4
    me = lax.axis_index("mdl").astype(jnp.int32).reshape(1)
    out = jax.ShapeDtypeStruct((2, tokens // 2, step), BF16)
    depth = sum(left.shape[1] for left in lefts)
    return pl.pallas_call(
        functools.partial(payload_kernel, starts),
        grid_spec=pltpu.PrefetchScalarGridSpec(
            num_scalar_prefetch=1,
            grid=(4,),
            in_specs=[pl.BlockSpec(left.shape, lambda at, me_ref: (0, 0)) for left in lefts]
            + [pl.BlockSpec((step, cols), lambda at, me_ref: (me_ref[0] ^ (3 - at), 0))]
            + [pl.BlockSpec((tokens, step), lambda at, me_ref: (0, me_ref[0] ^ (3 - at)))]
            * len(partial),
            out_specs=[pl.BlockSpec(out.shape, lambda at, me_ref: (0, 0, 0))] * 4,
        ),
        out_shape=(out,) * 4,
        compiler_params=in_order(48),
        cost_estimate=cost(2 * tokens * rows * depth, 2 * (tokens * depth + rows * cols + tokens * rows)),
    )(me, *lefts, weight, *partial)


def pieces_kernel(start, me_ref, *refs):
    *pieces, weight_ref, out_ref, total, held = refs
    hold_piece(pieces, held)
    at = pl.program_id(0)
    part = nn(held[...], weight_ref[:, start : start + out_ref.shape[1]])
    part = part + jnp.where(at > 0, total[...], 0.0)
    total[...] = part

    @pl.when(at == 3)
    def _():
        out_ref[...] = part.astype(BF16)


def pieces_product(pieces, weight, start, width):
    tokens, step = pieces[0].shape
    rows, cols = weight.shape
    me = lax.axis_index("mdl").astype(jnp.int32).reshape(1)
    return pl.pallas_call(
        functools.partial(pieces_kernel, start),
        grid_spec=pltpu.PrefetchScalarGridSpec(
            num_scalar_prefetch=1,
            grid=(4,),
            in_specs=[pl.BlockSpec(piece.shape, lambda at, me_ref: (0, 0)) for piece in pieces]
            + [pl.BlockSpec((step, cols), lambda at, me_ref: (me_ref[0] ^ at, 0))],
            out_specs=pl.BlockSpec((tokens, width), lambda at, me_ref: (0, 0)),
            scratch_shapes=[pltpu.VMEM((tokens, width), F32), pltpu.VMEM((tokens, step), BF16)],
        ),
        out_shape=jax.ShapeDtypeStruct((tokens, width), BF16),
        compiler_params=in_order(40),
        cost_estimate=cost(2 * tokens * rows * width, 2 * (tokens * rows + rows * cols + tokens * width)),
    )(me, *pieces, weight)


def product_to_mdl(lefts, weight, starts, partial=()):
    if lax.axis_size("mdl") == 4:
        payload = scatter_product(lefts, weight, starts, partial)
        return payload, lambda payload, *earlier: scatter_payload(payload, *earlier)
    part = sum((sum_products(lefts, weight, starts), *partial))
    return (part.astype(BF16),), lambda payload, *earlier: scatter_mdl(payload[0], 1)


def after(value, *earlier):
    return lax.optimization_barrier((value, *earlier))[0]


def row_scale(rows_b, axis=-1):
    rows = rows_b.astype(F32)
    return lax.rsqrt(jnp.mean(rows * rows, axis=axis, keepdims=True) + NORM_EPS)


def gelu_parts(value):
    root = math.sqrt(2.0 / math.pi)
    square = value * value
    tanh = jnp.tanh(root * (value + 0.044715 * value * square))
    cdf = 0.5 * (1.0 + tanh)
    slope = cdf + 0.5 * value * (1.0 - tanh * tanh) * root * (1.0 + 3 * 0.044715 * square)
    return value * cdf, slope


def scaled(weight, gain):
    return (weight.astype(F32) * gain.astype(F32)[:, None]).astype(BF16)


def on_device(
    inputs, positions, norm1_gain, qkv_weight, out_weight, norm2_gain, gate_weight,
    up_weight, down_weight, cotangent,
):
    me = lax.axis_index("mdl")
    size = lax.axis_size("mdl")
    head_cols = HEADS * HEAD
    width = inputs.shape[1]
    features = width * size

    def from_tok(weight, dim):
        return lax.all_gather(weight, "tok", axis=dim, tiled=True)

    def pair_to_tok(local):
        kept, sent = local
        count = lax.axis_size("tok")
        got = lax.ppermute(sent, "tok", [(i, i ^ 1) for i in range(count)])
        both = add_pair(kept, got)
        groups = [list(range(core, count, 2)) for core in range(2)]
        total = lax.psum_scatter(
            both, "tok", scatter_dimension=0, tiled=True, axis_index_groups=groups
        )
        return total.astype(F32)

    qkv_cols, ff_cols = qkv_weight.shape[1], gate_weight.shape[1]
    attn_local = jnp.concatenate([scaled(qkv_weight, norm1_gain), out_weight.T], axis=1)
    middle = ff_cols // 256 * 128
    parts = ((0, middle), (middle, ff_cols))
    if size == 4 and lax.axis_size("tok") == 8:
        gain_cols = jnp.broadcast_to(norm2_gain[:, None], (norm2_gain.shape[0], 128))
        rows_in, w_attn, locals_ff = first_gather(
            inputs,
            jnp.concatenate([attn_local, gain_cols], axis=1),
            (gate_weight, up_weight, down_weight.T),
            parts,
        )
    else:
        rows_in = gather_mdl(inputs, 1)
        w_attn = from_tok(attn_local, 0)
        scaled_gu = [scaled(weight, norm2_gain) for weight in (gate_weight, up_weight)]
        locals_ff = [
            jnp.concatenate([w[:, start:stop] for w in (*scaled_gu, down_weight.T)], axis=1)
            for start, stop in parts
        ]
    w_qkv = w_attn[:, :qkv_cols]
    w_parts = [from_tok(local, 0) for local in locals_ff]

    qkv = rows_to_cols(nn(rows_in, w_qkv).astype(BF16))
    count = qkv.shape[0]
    scale_own = row_scale(lax.dynamic_slice_in_dim(rows_in, me * count, count, 0))
    scale_one = row_scale(after(rows_in, qkv))
    half = HEAD // 2
    frequency = jnp.exp(jnp.arange(half, dtype=F32) * (-2.0 * math.log(10000.0) / HEAD))
    angles = positions.astype(F32)[:, None] * frequency[None, :]
    cos, sin = jnp.cos(angles), jnp.sin(angles)
    kv_own = qkv[:, head_cols:].astype(F32) * scale_own
    key_rows = turn(kv_own[:, :HEAD], cos, sin)
    kv = gather_mdl(jnp.concatenate([key_rows, kv_own[:, HEAD:]], axis=1).astype(BF16), 0)
    first = (me * count).astype(jnp.int32).reshape(1)
    pos = positions[:, None]
    attended, log_norm = attention_forward(first, qkv, kv, cos, sin, pos, scale_own)
    head_block = cols_to_rows(attended)
    residual = inputs.astype(F32)
    payload, scatter = product_to_mdl((head_block,), w_attn, (qkv_cols,))
    mixed = residual + scatter(payload)

    rows_two = gather_mdl(mixed.astype(BF16), 1)
    scale_two = row_scale(rows_two)
    rows_hat = (rows_two.astype(F32) * scale_two).astype(BF16)
    rows, above, stat_two, partial, hiddens, sums = rows_hat, cotangent, 0.0, (), [], []
    for index, (weight, (start, stop)) in enumerate(zip(w_parts, parts)):
        cols = stop - start
        last = index == len(parts) - 1
        gate_in = nn(rows, weight[:, :cols])
        up_in = nn(rows, weight[:, cols : 2 * cols])
        d_hidden = nn(above, weight[:, 2 * cols :])
        gelu, slope = gelu_parts(gate_in)
        hidden = (gelu * up_in).astype(BF16)
        d_gate = d_hidden * up_in * slope
        d_up = d_hidden * gelu
        stat_two += jnp.sum(d_gate * gate_in + d_up * up_in, axis=1)
        d_gate, d_up = d_gate.astype(BF16), d_up.astype(BF16)
        hiddens.append(hidden)
        lefts, starts = (d_gate, d_up), (0, cols)
        if last:
            payload, scatter = product_to_mdl(lefts, weight, starts, partial)
            rows, above, _ = lax.optimization_barrier((rows, above, payload[0]))
        local = part_grad(rows, above, d_gate, d_up, hidden)
        if not last:
            d_gate = after(d_gate, local[0])
            partial = (sum_products((d_gate, d_up), weight, starts),)
            rows, above, _ = lax.optimization_barrier((rows, above, local[0]))
        sums.append(pair_to_tok(local))
    d_two = scatter(payload)
    stat_two = sum_mdl(stat_two.reshape(8, -1)).reshape(-1, 1) * (1.0 / features)
    scale_mixed = scale_two * mixed
    cotangent_own = lax.dynamic_slice_in_dim(cotangent, me * width, width, 1).astype(F32)
    d_mixed = cotangent_own + scale_two * (d_two - scale_mixed * stat_two)

    d_mixed_b = after(d_mixed.astype(BF16), local[0])
    down_starts = tuple(2 * (stop - start) for start, stop in parts)
    ffn = (sum_products((after(hiddens[0], d_mixed_b),), w_parts[0], down_starts[:1]),)
    ffn_payload, ffn_scatter = product_to_mdl(
        (after(hiddens[1], d_mixed_b),), w_parts[1], down_starts[1:], ffn
    )
    if size == 4 and lax.axis_size("tok") == 8:
        pieces = gather_pieces(d_mixed_b)
        d_head = pieces_product(pieces, w_attn, qkv_cols, head_block.shape[1])
        heads_later = after(head_block, d_head)
        out_local = pieces_grad(pieces, heads_later)
    else:
        d_mixed_rows = gather_mdl(d_mixed_b, 1)
        d_head = nn(d_mixed_rows, w_attn[:, qkv_cols:]).astype(BF16)
        out_local = pair_grad(d_mixed_rows, head_block)
    out_grad = pair_to_tok(out_local)
    d_attended = rows_to_cols(d_head)
    d_query, d_kv = attention_backward(
        first, qkv, kv, cos, sin, pos, scale_own, attended, d_attended, log_norm
    )
    d_kv = scatter_mdl(d_kv.astype(BF16), 0)
    d_key = unturn(d_kv[:, :HEAD], cos, sin).astype(BF16)
    d_qkv = jnp.concatenate([d_query, d_key, d_kv[:, HEAD:].astype(BF16)], axis=1)
    stat_one = jnp.sum(d_qkv.astype(F32) * qkv.astype(F32), axis=1) * scale_own[:, 0]
    d_qkv_part = cols_to_rows(d_qkv)
    stat_rows = jnp.zeros((size, count), F32)
    stat_rows = sum_mdl(lax.dynamic_update_slice(stat_rows, stat_one[None], (me, 0)))
    stat_one = stat_rows.reshape(-1, 1) * (1.0 / features)
    payload, scatter = product_to_mdl((d_qkv_part,), w_attn, (0,))
    d_scaled = (after(d_qkv_part, payload[0]).astype(F32) * scale_one).astype(BF16)
    *qkv_local, gain_one = pair_grad(rows_in, d_scaled, w_attn)
    qkv_sum = pair_to_tok(qkv_local)
    d_one = scatter(payload)
    ffn_sum = ffn_scatter(ffn_payload, d_qkv_part)
    block_out = (mixed + ffn_sum).astype(BF16)
    input_grad = d_mixed + scale_one * (d_one - (scale_one * residual) * stat_one)

    norm1_late, norm2_late, gate_late, up_late, _ = lax.optimization_barrier(
        (norm1_gain, norm2_gain, gate_weight, up_weight, local[0])
    )

    def unfold(total, gain):
        return total * gain.astype(F32)[:, None]

    def joined(at):
        widths = [total.shape[1] // 3 for total in sums]
        pieces = [total[:, at * cols :][:, :cols] for total, cols in zip(sums, widths)]
        return jnp.concatenate(pieces, axis=1)

    gate_sum, up_sum, down_grad = joined(0), joined(1), joined(2).T
    gain_two = jnp.sum(
        gate_late.astype(F32) * gate_sum + up_late.astype(F32) * up_sum, axis=1
    )
    gate_grad, up_grad = unfold(gate_sum, norm2_late), unfold(up_sum, norm2_late)
    out_grad = out_grad.T
    gain_two_grad = sum_mdl(gain_two)
    gain_one = sum_mdl(sum_tok(gain_one.reshape(8, -1))).reshape(-1)
    shard = norm1_gain.shape[0]
    gain_one = lax.dynamic_slice_in_dim(gain_one, lax.axis_index("tok") * shard, shard, 0)
    gain_one_grad = gain_one / norm1_late.astype(F32)
    return (
        block_out,
        input_grad,
        gain_one_grad,
        unfold(qkv_sum, norm1_late),
        out_grad,
        gain_two_grad,
        gate_grad,
        up_grad,
        down_grad,
    )


def solution(mesh):
    return jax.shard_map(
        on_device,
        mesh=mesh,
        in_specs=(
            P("tok", "mdl"),
            P(("tok", "mdl")),
            P("tok"),
            P("tok", "mdl"),
            P("mdl", "tok"),
            P("tok"),
            P("tok", "mdl"),
            P("tok", "mdl"),
            P("mdl", "tok"),
            P("tok", None),
        ),
        out_specs=(
            P("tok", "mdl"),
            P("tok", "mdl"),
            P("tok"),
            P("tok", "mdl"),
            P("mdl", "tok"),
            P("tok"),
            P("tok", "mdl"),
            P("tok", "mdl"),
            P("mdl", "tok"),
        ),
        check_vma=False,
    )
```

```python
import functools
import math

import jax
import jax.numpy as jnp
from jax import lax
from jax.experimental import pallas as pl
from jax.experimental.pallas import tpu as pltpu
from jax.sharding import PartitionSpec as P


HEADS = 10
HEAD = 256
NORM_EPS = 1e-06
F32 = jnp.float32
BF16 = jnp.bfloat16
MASKED = -1e30


def nt(left_op, right_op):
    return lax.dot_general(
        left_op, right_op, (((1,), (1,)), ((), ())), preferred_element_type=F32
    )


def tn(left_op, right_op):
    return lax.dot_general(
        left_op, right_op, (((0,), (0,)), ((), ())), preferred_element_type=F32
    )


def nn(left_op, right_op):
    return jnp.dot(left_op, right_op, preferred_element_type=F32)


def swap(block, distance):
    size = lax.axis_size("mdl")
    return lax.ppermute(block, "mdl", [(i, i ^ distance) for i in range(size)])


def gather_mdl(block, dim):
    size = lax.axis_size("mdl")
    if size != 4:
        return lax.all_gather(block, "mdl", axis=dim, tiled=True)
    me = lax.axis_index("mdl")
    half = block.shape[0] // 2
    along_x = swap(block, 1)
    along_y = swap(block, 2)
    top = swap(along_x[:half], 2)
    bottom = swap(along_y[half:], 1)
    width = block.shape[dim]
    shape = list(block.shape)
    shape[dim] = width * size
    whole = jnp.zeros(shape, block.dtype)

    def put(whole, piece, source, row):
        start = [0, 0]
        start[dim] = source * width
        start[0] = start[0] + row
        return lax.dynamic_update_slice(whole, piece, tuple(start))

    whole = put(whole, block, me, 0)
    whole = put(whole, along_x, me ^ 1, 0)
    whole = put(whole, along_y, me ^ 2, 0)
    whole = put(whole, top, me ^ 3, 0)
    whole = put(whole, bottom, me ^ 3, half)
    return whole


def scatter_mdl(part, dim):
    size = lax.axis_size("mdl")
    if size != 4:
        return lax.psum_scatter(part, "mdl", scatter_dimension=dim, tiled=True).astype(F32)
    me = lax.axis_index("mdl")
    shape = list(part.shape)
    shape[dim] //= size
    half = shape[0] // 2

    def piece(block, row):
        start = [0, 0]
        start[dim] = block * shape[dim]
        start[0] = start[0] + row
        return lax.dynamic_slice(part, tuple(start), (half, shape[1]))

    sums = []
    for row, first, second in ((0, 1, 2), (half, 2, 1)):
        sent = jnp.stack([piece(me ^ first, row), piece(me ^ 3, row)])
        sums.append((row, second, swap(sent, first)))
    partial = []
    for row, second, got in sums:
        other = piece(me ^ second, row).astype(F32) + got[1].astype(F32)
        partial.append((row, got[0], swap(other.astype(BF16), second)))
    return jnp.concatenate(
        [
            piece(me, row).astype(F32) + first.astype(F32) + second.astype(F32)
            for row, first, second in partial
        ],
        axis=0,
    )


def gather_pieces(block):
    half = block.shape[0] // 2
    along_x = swap(block, 1)
    along_y = swap(block, 2)
    top = swap(along_x[:half], 2)
    bottom = swap(along_y[half:], 1)
    return block, along_x, along_y, top, bottom


def scatter_payload(payload, *earlier):
    top_sent, bottom_sent, top_kept, bottom_kept = payload
    got_top = swap(top_sent, 1)
    got_bottom = swap(bottom_sent, 2)
    halves = []
    for kept, got, second in ((top_kept, got_top, 2), (bottom_kept, got_bottom, 1)):
        passed = (kept[1].astype(F32) + got[1].astype(F32)).astype(BF16)
        if earlier:
            passed = after(passed, *earlier)
        last = swap(passed, second)
        halves.append(kept[0].astype(F32) + got[0].astype(F32) + last.astype(F32))
    return jnp.concatenate(halves, axis=0)


def sum_mdl(value):
    size = lax.axis_size("mdl")
    distance = 1
    while distance < size:
        value = value + swap(value, distance)
        distance *= 2
    return value


def sum_tok(value):
    size = lax.axis_size("tok")
    distance = 1
    while distance < size:
        value = value + lax.ppermute(value, "tok", [(i, i ^ distance) for i in range(size)])
        distance *= 2
    return value


def rows_to_cols(block):
    return lax.all_to_all(block, "mdl", split_axis=0, concat_axis=1, tiled=True)


def cols_to_rows(block):
    return lax.all_to_all(block, "mdl", split_axis=1, concat_axis=0, tiled=True)


def first_kernel(parts, x_ref, gains_ref, right_ref, *refs):
    weights, (rows_ref, weight_ref), locals_ref = refs[:4], refs[4:6], refs[6:8]
    held, joined, left_ref = refs[8:12], refs[12:14], refs[14]
    own, x_sent, x_got, w_up, w_down, w_core, w_got = refs[15:]
    me, tok = lax.axis_index("mdl"), lax.axis_index("tok")
    pairs = lax.axis_size("tok") // 2
    level, last = tok // 2, pairs - 1
    half, width = x_ref.shape[0] // 2, x_ref.shape[1]
    shard, split, all_cols = *left_ref.shape, weight_ref.shape[1]
    below, above = level > 0, level < last

    barrier = pltpu.get_barrier_semaphore()
    pl.semaphore_signal(barrier, inc=1, device_id={"mdl": me ^ 1})
    pl.semaphore_signal(barrier, inc=1, device_id={"mdl": me ^ 2})
    pl.semaphore_signal(barrier, inc=1, device_id={"tok": tok ^ 1})

    @pl.when(below)
    def _():
        pl.semaphore_signal(barrier, inc=1, device_id={"tok": tok - 2})

    @pl.when(above)
    def _():
        pl.semaphore_signal(barrier, inc=1, device_id={"tok": tok + 2})

    pl.semaphore_wait(barrier, 3 + below.astype(jnp.int32) + above.astype(jnp.int32))

    def cols(block):
        return pl.ds(pl.multiple_of(block * width, 128), width)

    windows = (pl.ds(split, all_cols - split), pl.ds(0, split))

    def block(index, part):
        return weight_ref.at[pl.ds(pl.multiple_of(index * shard, 16), shard), windows[part]]

    def x_copy(source, target, at, to):
        return pltpu.make_async_remote_copy(
            source, target, x_sent.at[at], x_got.at[at], device_id={"mdl": me ^ to}
        )

    def w_copy(source, index, part, sent, to):
        return pltpu.make_async_remote_copy(
            source, block(index, part), sent, w_got.at[index, part], device_id={"tok": to}
        )

    mine = rows_ref.at[:, cols(me)]
    to_x, to_y = x_copy(x_ref, mine, 0, 1), x_copy(x_ref, mine, 1, 2)
    keeps = [pltpu.make_async_copy(x_ref, mine, own.at[0])]
    loads = [
        pltpu.make_async_copy(weight, to, own.at[3 + at])
        for at, (weight, to) in enumerate(zip(weights, held))
    ]

    def send_own(source, part):
        @pl.when(above)
        def _():
            w_copy(source, tok, part, w_up.at[0, part], tok + 2).start()

        @pl.when(below)
        def _():
            w_copy(source, tok, part, w_down.at[0, part], tok - 2).start()

        w_copy(source, tok, part, w_core.at[tok, part], tok ^ 1).start()
        keeps.append(pltpu.make_async_copy(source, block(tok, part), own.at[1 + part]))
        keeps[-1].start()

    send_own(right_ref, 0)
    for copy in (to_x, to_y, keeps[0], *loads):
        copy.start()
    loads[0].wait()
    gain_one, gain = gains_ref[:, :1].astype(F32), gains_ref[:, 64:65].astype(F32)
    left_ref[...] = (held[0][...].astype(F32) * gain_one).astype(BF16)
    held = held[1:]
    for copy in loads[1:]:
        copy.wait()
    for (start, stop), out in zip(parts, joined):
        count = stop - start
        for at, source in enumerate(held):
            value = source[:, start:stop]
            if at < 2:
                value = (value.astype(F32) * gain).astype(BF16)
            out[:, at * count : (at + 1) * count] = value
        if start == 0:
            send_own(left_ref, 1)

    def relay(distance, part):
        low, high = tok - 2 * distance, tok + 2 * distance

        @pl.when(level >= distance)
        def _():
            source = block(low, part)
            w_copy(source, low, part, w_core.at[low, part], tok ^ 1).wait_recv()

            @pl.when(above)
            def _():
                w_copy(source, low, part, w_up.at[distance, part], tok + 2).start()

            w_copy(source, low, part, w_core.at[low, part], tok ^ 1).start()

        @pl.when(level + distance <= last)
        def _():
            source = block(high, part)
            w_copy(source, high, part, w_core.at[high, part], tok ^ 1).wait_recv()

            @pl.when(below)
            def _():
                w_copy(source, high, part, w_down.at[distance, part], tok - 2).start()

            w_copy(source, high, part, w_core.at[high, part], tok ^ 1).start()

    relay(1, 0)
    relay(1, 1)
    stores = [
        pltpu.make_async_copy(out, to, own.at[7 + at])
        for at, (out, to) in enumerate(zip(joined, locals_ref))
    ]
    for copy in stores:
        copy.start()
    from_x = rows_ref.at[pl.ds(0, half), cols(me ^ 1)]
    from_y = rows_ref.at[pl.ds(half, half), cols(me ^ 2)]
    top, bottom = x_copy(from_x, from_x, 2, 2), x_copy(from_y, from_y, 3, 1)
    to_x.wait_recv()
    top.start()
    to_y.wait_recv()
    bottom.start()
    for distance in range(2, pairs):
        relay(distance, 0)
        relay(distance, 1)
    for copy in (*keeps, *stores):
        copy.wait()
    for copy in (top, bottom):
        copy.wait_recv()
    for copy in (to_x, to_y, top, bottom):
        copy.wait_send()

    for distance in range(pairs):
        for part in range(2):
            mine = block(tok, part)

            @pl.when((level >= distance) & above)
            def _(mine=mine, distance=distance, part=part):
                w_copy(mine, tok, part, w_up.at[distance, part], tok + 2).wait_send()

            @pl.when((level + distance <= last) & below)
            def _(mine=mine, distance=distance, part=part):
                w_copy(mine, tok, part, w_down.at[distance, part], tok - 2).wait_send()

            near, far = 2 * distance + tok % 2, 2 * distance + 1 - tok % 2
            w_copy(block(near, part), near, part, w_core.at[near, part], tok ^ 1).wait_send()
            w_copy(block(far, part), far, part, w_core.at[near, part], tok ^ 1).wait_recv()


def first_gather(inputs, gains, right, weights, parts):
    tokens, width = inputs.shape
    shard, left_cols = weights[0].shape
    cols = left_cols + right.shape[1]
    pairs = lax.axis_size("tok") // 2
    dma = pltpu.SemaphoreType.DMA
    locals_ff = [(shard, 3 * (stop - start)) for start, stop in parts]
    shapes = [(tokens, 4 * width), (2 * pairs * shard, cols), *locals_ff]
    *gathered, first, second = pl.pallas_call(
        functools.partial(first_kernel, parts),
        out_shape=[jax.ShapeDtypeStruct(shape, BF16) for shape in shapes],
        in_specs=[pl.BlockSpec(memory_space=pltpu.VMEM)] * 3
        + [pl.BlockSpec(memory_space=pl.ANY)] * 4,
        out_specs=[pl.BlockSpec(memory_space=pl.ANY)] * 4,
        scratch_shapes=[pltpu.VMEM(array.shape, BF16) for array in weights]
        + [pltpu.VMEM(shape, BF16) for shape in (*locals_ff, weights[0].shape)]
        + [
            dma((9,)), dma((4,)), dma((4,)), dma((pairs, 2)), dma((pairs, 2)),
            dma((2 * pairs, 2)), dma((2 * pairs, 2)),
        ],
        compiler_params=pltpu.CompilerParams(
            collective_id=0, has_side_effects=True, vmem_limit_bytes=60 << 20
        ),
    )(inputs, gains, right, *weights)
    return *gathered, (first, second)


def in_order(mebibytes):
    return pltpu.CompilerParams(
        dimension_semantics=(pltpu.ARBITRARY,), vmem_limit_bytes=mebibytes << 20
    )


def cost(flops, bytes_accessed, transcendentals=0):
    return pl.CostEstimate(
        flops=flops, bytes_accessed=bytes_accessed, transcendentals=transcendentals
    )


def turn(vector, cos, sin):
    half = HEAD // 2
    lower, upper = vector[:, :half], vector[:, half:]
    return jnp.concatenate([lower * cos - upper * sin, upper * cos + lower * sin], axis=1)


def unturn(vector, cos, sin):
    half = HEAD // 2
    lower, upper = vector[:, :half], vector[:, half:]
    return jnp.concatenate([lower * cos + upper * sin, upper * cos - lower * sin], axis=1)


def seen(first_ref, position_ref, queries, keys):
    row = lax.broadcasted_iota(jnp.int32, (queries, keys), 0) + first_ref[0]
    distance = row - lax.broadcasted_iota(jnp.int32, (queries, keys), 1)
    return (distance >= 0) & (distance <= position_ref[...])


def forward_kernel(
    first_ref, q_ref, kv_ref, cos_ref, sin_ref, pos_ref, scale_ref, out_ref, norm_ref
):
    query = turn(q_ref[...].astype(F32) * scale_ref[...], cos_ref[...], sin_ref[...])
    query = (query * HEAD ** (-0.5)).astype(BF16)
    keys, values = kv_ref[:, :HEAD], kv_ref[:, HEAD:]
    scores = nt(query, keys)
    scores = jnp.where(seen(first_ref, pos_ref, *scores.shape), scores, MASKED)
    top = jnp.max(scores, axis=1, keepdims=True)
    weights = jnp.exp(scores - top)
    total = jnp.sum(weights, axis=1, keepdims=True)
    out_ref[...] = (nn(weights.astype(BF16), values) / total).astype(BF16)
    norm_ref[0] = top + jnp.log(total)


def backward_kernel(
    first_ref, q_ref, kv_ref, cos_ref, sin_ref, pos_ref, scale_ref, att_ref, datt_ref, norm_ref,
    dq_ref, dkv_ref,
):
    head = pl.program_id(0)
    scale = HEAD ** (-0.5)
    cos, sin = cos_ref[...], sin_ref[...]
    query = (turn(q_ref[...].astype(F32) * scale_ref[...], cos, sin) * scale).astype(BF16)
    keys, values = kv_ref[:, :HEAD], kv_ref[:, HEAD:]
    scores = nt(query, keys)
    visible = seen(first_ref, pos_ref, *scores.shape)
    again = jnp.where(visible, jnp.exp(scores - norm_ref[0]), 0.0)
    d_att = datt_ref[...]
    delta = jnp.sum(d_att.astype(F32) * att_ref[...].astype(F32), axis=1, keepdims=True)
    d_scores = (again * (nt(d_att, values) - delta)).astype(BF16)
    d_query = nn(d_scores, keys) * scale
    dq_ref[...] = unturn(d_query, cos, sin).astype(BF16)

    @pl.when(head == 0)
    def _():
        dkv_ref[...] = jnp.zeros_like(dkv_ref)

    dkv_ref[:, :HEAD] += tn(d_scores, query)
    dkv_ref[:, HEAD:] += tn(again.astype(BF16), d_att)


def whole_spec(shape):
    return pl.BlockSpec(shape, lambda head: (0,) * len(shape))


def attention_forward(first, qkv, kv, cos, sin, pos, scale):
    rows, keys = qkv.shape[0], kv.shape[0]
    head_spec = pl.BlockSpec((rows, HEAD), lambda head: (0, head))
    return pl.pallas_call(
        forward_kernel,
        grid=(HEADS,),
        out_shape=(
            jax.ShapeDtypeStruct((rows, HEADS * HEAD), BF16),
            jax.ShapeDtypeStruct((HEADS, rows, 1), F32),
        ),
        in_specs=[
            pl.BlockSpec(memory_space=pltpu.SMEM),
            head_spec,
            whole_spec((keys, 2 * HEAD)),
            whole_spec((rows, HEAD // 2)),
            whole_spec((rows, HEAD // 2)),
            whole_spec((rows, 1)),
            whole_spec((rows, 1)),
        ],
        out_specs=(head_spec, pl.BlockSpec((1, rows, 1), lambda head: (head, 0, 0))),
        compiler_params=in_order(32),
        cost_estimate=cost(4 * rows * keys * HEADS * HEAD, 4 * rows * HEADS * HEAD + 4 * keys * HEAD, rows * keys * HEADS),
        name="att_f",
    )(first, qkv, kv, cos, sin, pos, scale)


def attention_backward(first, qkv, kv, cos, sin, pos, scale, att, d_att, norm):
    rows, keys = qkv.shape[0], kv.shape[0]
    head_spec = pl.BlockSpec((rows, HEAD), lambda head: (0, head))
    return pl.pallas_call(
        backward_kernel,
        grid=(HEADS,),
        out_shape=(
            jax.ShapeDtypeStruct((rows, HEADS * HEAD), BF16),
            jax.ShapeDtypeStruct((keys, 2 * HEAD), F32),
        ),
        in_specs=[
            pl.BlockSpec(memory_space=pltpu.SMEM),
            head_spec,
            whole_spec((keys, 2 * HEAD)),
            whole_spec((rows, HEAD // 2)),
            whole_spec((rows, HEAD // 2)),
            whole_spec((rows, 1)),
            whole_spec((rows, 1)),
            head_spec,
            head_spec,
            pl.BlockSpec((1, rows, 1), lambda head: (head, 0, 0)),
        ],
        out_specs=(head_spec, whole_spec((keys, 2 * HEAD))),
        compiler_params=in_order(40),
        cost_estimate=cost(10 * rows * keys * HEADS * HEAD, 8 * rows * HEADS * HEAD + 12 * keys * HEAD, rows * keys * HEADS),
        name="att_b",
    )(first, qkv, kv, cos, sin, pos, scale, att, d_att, norm)


def keep_half(core_ref, total, kept, sent):
    half = total.shape[0] // 2
    for core, (first, second) in enumerate(((kept, sent), (sent, kept))):

        @pl.when(core_ref[0] == core)
        def _(first=first, second=second):
            first[...] = total[:half]
            second[...] = total[half:]


def pair_kernel(core_ref, left_ref, right_ref, *refs):
    total = tn(left_ref[...], right_ref[...])
    if len(refs) == 4:
        weight = refs[0][:, : total.shape[1]].astype(F32)
        refs[3][...] = jnp.sum(total * weight, axis=1, keepdims=True)
    keep_half(core_ref, total.astype(BF16), *refs[-3:-1] if len(refs) == 4 else refs)


def split_pairs(total, pairs, core):
    rows, cols = total.shape
    total = total.reshape(pairs, 2, rows // pairs // 2, cols)
    return tuple(
        lax.dynamic_index_in_dim(total, index, 1, False).reshape(-1, cols)
        for index in (core, 1 - core)
    )


def core_index():
    return (lax.axis_index("tok") % 2).astype(jnp.int32).reshape(1)


def pair_grad(left, right, weight=None):
    tokens, rows = left.shape
    cols = right.shape[1]
    pairs = lax.axis_size("tok") // 2
    step = rows // pairs
    if step % 128 or cols % 128:
        total = tn(left, right)
        halves = split_pairs(total.astype(BF16), pairs, lax.axis_index("tok") % 2)
        if weight is None:
            return halves
        return *halves, jnp.sum(total * weight[:, :cols].astype(F32), axis=1, keepdims=True)
    out_shape = [jax.ShapeDtypeStruct((rows // 2, cols), BF16)] * 2
    out_specs = [pl.BlockSpec((step // 2, cols), lambda pair: (pair, 0))] * 2
    in_specs = [
        pl.BlockSpec(memory_space=pltpu.SMEM),
        pl.BlockSpec((tokens, step), lambda pair: (0, pair)),
        pl.BlockSpec((tokens, cols), lambda pair: (0, 0)),
    ]
    operands = [core_index(), left, right]
    if weight is not None:
        operands.append(weight)
        in_specs.append(pl.BlockSpec((step, weight.shape[1]), lambda pair: (pair, 0)))
        out_shape.append(jax.ShapeDtypeStruct((rows, 1), F32))
        out_specs.append(pl.BlockSpec((step, 1), lambda pair: (pair, 0)))
    return pl.pallas_call(
        pair_kernel,
        grid=(pairs,),
        out_shape=out_shape,
        in_specs=in_specs,
        out_specs=out_specs,
        compiler_params=in_order(48),
        cost_estimate=cost(2 * tokens * rows * cols, 2 * (tokens * (rows + cols) + rows * cols)),
    )(*operands)


def part_kernel(core_ref, rows_ref, above_ref, d_gate_ref, d_up_ref, hidden_ref, kept, sent):
    cols = hidden_ref.shape[1]
    for at, (left_ref, right_ref) in enumerate(
        ((rows_ref, d_gate_ref), (rows_ref, d_up_ref), (above_ref, hidden_ref))
    ):
        total = tn(left_ref[...], right_ref[...]).astype(BF16)
        window = (slice(None), pl.ds(at * cols, cols))
        keep_half(core_ref, total, kept.at[window], sent.at[window])


def part_grad(rows, above, d_gate, d_up, hidden):
    tokens, features = rows.shape
    cols = hidden.shape[1]
    pairs = lax.axis_size("tok") // 2
    step = features // pairs
    if step % 128 or cols % 128:
        total = [tn(rows, d_gate), tn(rows, d_up), tn(above, hidden)]
        total = jnp.concatenate(total, axis=1).astype(BF16)
        return split_pairs(total, pairs, lax.axis_index("tok") % 2)
    out = jax.ShapeDtypeStruct((features // 2, 3 * cols), BF16)
    left_spec = pl.BlockSpec((tokens, step), lambda pair: (0, pair))
    right_spec = pl.BlockSpec((tokens, cols), lambda pair: (0, 0))
    return pl.pallas_call(
        part_kernel,
        grid=(pairs,),
        out_shape=(out, out),
        in_specs=[pl.BlockSpec(memory_space=pltpu.SMEM)] + [left_spec] * 2 + [right_spec] * 3,
        out_specs=[pl.BlockSpec((step // 2, 3 * cols), lambda pair: (pair, 0))] * 2,
        compiler_params=in_order(48),
        cost_estimate=cost(
            6 * tokens * features * cols,
            2 * (2 * tokens * features + 3 * cols * (tokens + features)),
        ),
    )(core_index(), rows, above, d_gate, d_up, hidden)


def hold_piece(pieces, held):
    *blocks, top, bottom = pieces
    at = pl.program_id(0)
    for index, piece in enumerate(blocks):

        @pl.when(at == index)
        def _(piece=piece):
            held[...] = piece[...]

    @pl.when(at == len(blocks))
    def _():
        half = top.shape[0]
        held[:half] = top[...]
        held[half:] = bottom[...]


def pieces_grad_kernel(me_ref, core_ref, *refs):
    *pieces, right_ref, kept, sent, held = refs
    hold_piece(pieces, held)
    keep_half(core_ref, tn(held[...], right_ref[...]).astype(BF16), kept, sent)


def add_kernel(left_ref, right_ref, out_ref):
    out_ref[...] = (left_ref[...].astype(F32) + right_ref[...].astype(F32)).astype(BF16)


def add_pair(left, right):
    rows, cols = left.shape
    if rows % 256 or cols % 128:
        return (left.astype(F32) + right.astype(F32)).astype(BF16)
    steps = 10 if rows % 160 == 0 else 8
    spec = pl.BlockSpec((rows // steps, cols), lambda at: (at, 0))
    return pl.pallas_call(
        add_kernel,
        grid=(steps,),
        out_shape=jax.ShapeDtypeStruct(left.shape, BF16),
        in_specs=[spec, spec],
        out_specs=spec,
        compiler_params=in_order(16),
        cost_estimate=cost(rows * cols, 6 * rows * cols),
    )(left, right)


def pieces_grad(pieces, right):
    tokens, step = pieces[0].shape
    cols = right.shape[1]
    me = lax.axis_index("mdl").astype(jnp.int32).reshape(1)
    out = jax.ShapeDtypeStruct((2 * step, cols), BF16)
    return pl.pallas_call(
        pieces_grad_kernel,
        grid_spec=pltpu.PrefetchScalarGridSpec(
            num_scalar_prefetch=2,
            grid=(4,),
            in_specs=[
                pl.BlockSpec(array.shape, lambda at, me_ref, core_ref: (0, 0))
                for array in (*pieces, right)
            ],
            out_specs=[
                pl.BlockSpec((step // 2, cols), lambda at, me_ref, core_ref: (me_ref[0] ^ at, 0))
            ]
            * 2,
            scratch_shapes=[pltpu.VMEM((tokens, step), BF16)],
        ),
        out_shape=(out, out),
        compiler_params=in_order(48),
        cost_estimate=cost(8 * tokens * step * cols, 2 * (4 * tokens * step + 5 * step * cols)),
    )(me, core_index(), *pieces, right)


def sum_kernel(starts, *refs):
    *lefts, weight_ref, out_ref = refs
    total = 0.0
    for left_ref, start in zip(lefts, starts):
        total += nt(left_ref[...], weight_ref[:, start : start + left_ref.shape[1]])
    out_ref[...] = total


def sum_products(lefts, weight, starts):
    tokens = lefts[0].shape[0]
    rows, cols = weight.shape
    if lefts[0].shape[1] % 128:
        return sum(
            nt(left, weight[:, start : start + left.shape[1]])
            for left, start in zip(lefts, starts)
        )
    step = 512
    depth = sum(left.shape[1] for left in lefts)
    return pl.pallas_call(
        functools.partial(sum_kernel, starts),
        grid=(rows // step,),
        out_shape=jax.ShapeDtypeStruct((tokens, rows), F32),
        in_specs=[pl.BlockSpec(left.shape, lambda row: (0, 0)) for left in lefts]
        + [pl.BlockSpec((step, cols), lambda row: (row, 0))],
        out_specs=pl.BlockSpec((tokens, step), lambda row: (0, row)),
        compiler_params=in_order(48),
        cost_estimate=cost(2 * tokens * rows * depth, 2 * rows * cols + 4 * tokens * rows),
    )(*lefts, weight)


def payload_kernel(starts, me_ref, *refs):
    lefts, weight_ref = refs[: len(starts)], refs[len(starts)]
    top_sent, bottom_sent, top_kept, bottom_kept = refs[-4:]
    total = refs[-5][...] if len(refs) == len(starts) + 6 else 0.0
    for left_ref, start in zip(lefts, starts):
        total += nt(left_ref[...], weight_ref[:, start : start + left_ref.shape[1]])
    total = total.astype(BF16)
    half = total.shape[0] // 2
    places = (
        ((top_kept, 0), (bottom_kept, 0)),
        ((top_sent, 0), (bottom_kept, 1)),
        ((top_kept, 1), (bottom_sent, 0)),
        ((top_sent, 1), (bottom_sent, 1)),
    )
    for distance, ((top, top_at), (bottom, bottom_at)) in enumerate(places):

        @pl.when(pl.program_id(0) == 3 - distance)
        def _(top=top, top_at=top_at, bottom=bottom, bottom_at=bottom_at):
            top[top_at] = total[:half]
            bottom[bottom_at] = total[half:]


def scatter_product(lefts, weight, starts, partial=()):
    tokens = lefts[0].shape[0]
    rows, cols = weight.shape
    step = rows // 4
    me = lax.axis_index("mdl").astype(jnp.int32).reshape(1)
    out = jax.ShapeDtypeStruct((2, tokens // 2, step), BF16)
    depth = sum(left.shape[1] for left in lefts)
    return pl.pallas_call(
        functools.partial(payload_kernel, starts),
        grid_spec=pltpu.PrefetchScalarGridSpec(
            num_scalar_prefetch=1,
            grid=(4,),
            in_specs=[pl.BlockSpec(left.shape, lambda at, me_ref: (0, 0)) for left in lefts]
            + [pl.BlockSpec((step, cols), lambda at, me_ref: (me_ref[0] ^ (3 - at), 0))]
            + [pl.BlockSpec((tokens, step), lambda at, me_ref: (0, me_ref[0] ^ (3 - at)))]
            * len(partial),
            out_specs=[pl.BlockSpec(out.shape, lambda at, me_ref: (0, 0, 0))] * 4,
        ),
        out_shape=(out,) * 4,
        compiler_params=in_order(48),
        cost_estimate=cost(2 * tokens * rows * depth, 2 * (tokens * depth + rows * cols + tokens * rows)),
    )(me, *lefts, weight, *partial)


def pieces_kernel(start, me_ref, *refs):
    *pieces, weight_ref, out_ref, total, held = refs
    hold_piece(pieces, held)
    at = pl.program_id(0)
    part = nn(held[...], weight_ref[:, start : start + out_ref.shape[1]])
    part = part + jnp.where(at > 0, total[...], 0.0)
    total[...] = part

    @pl.when(at == 3)
    def _():
        out_ref[...] = part.astype(BF16)


def pieces_product(pieces, weight, start, width):
    tokens, step = pieces[0].shape
    rows, cols = weight.shape
    me = lax.axis_index("mdl").astype(jnp.int32).reshape(1)
    return pl.pallas_call(
        functools.partial(pieces_kernel, start),
        grid_spec=pltpu.PrefetchScalarGridSpec(
            num_scalar_prefetch=1,
            grid=(4,),
            in_specs=[pl.BlockSpec(piece.shape, lambda at, me_ref: (0, 0)) for piece in pieces]
            + [pl.BlockSpec((step, cols), lambda at, me_ref: (me_ref[0] ^ at, 0))],
            out_specs=pl.BlockSpec((tokens, width), lambda at, me_ref: (0, 0)),
            scratch_shapes=[pltpu.VMEM((tokens, width), F32), pltpu.VMEM((tokens, step), BF16)],
        ),
        out_shape=jax.ShapeDtypeStruct((tokens, width), BF16),
        compiler_params=in_order(40),
        cost_estimate=cost(2 * tokens * rows * width, 2 * (tokens * rows + rows * cols + tokens * width)),
    )(me, *pieces, weight)


def product_to_mdl(lefts, weight, starts, partial=()):
    if lax.axis_size("mdl") == 4:
        payload = scatter_product(lefts, weight, starts, partial)
        return payload, lambda payload, *earlier: scatter_payload(payload, *earlier)
    part = sum((sum_products(lefts, weight, starts), *partial))
    return (part.astype(BF16),), lambda payload, *earlier: scatter_mdl(payload[0], 1)


def after(value, *earlier):
    return lax.optimization_barrier((value, *earlier))[0]


def row_scale(rows_b, axis=-1):
    rows = rows_b.astype(F32)
    return lax.rsqrt(jnp.mean(rows * rows, axis=axis, keepdims=True) + NORM_EPS)


def gelu_parts(value):
    root = math.sqrt(2.0 / math.pi)
    square = value * value
    tanh = jnp.tanh(root * (value + 0.044715 * value * square))
    cdf = 0.5 * (1.0 + tanh)
    slope = cdf + 0.5 * value * (1.0 - tanh * tanh) * root * (1.0 + 3 * 0.044715 * square)
    return value * cdf, slope


def scaled(weight, gain):
    return (weight.astype(F32) * gain.astype(F32)[:, None]).astype(BF16)


def on_device(
    inputs, positions, norm1_gain, qkv_weight, out_weight, norm2_gain, gate_weight,
    up_weight, down_weight, cotangent,
):
    me = lax.axis_index("mdl")
    size = lax.axis_size("mdl")
    head_cols = HEADS * HEAD
    width = inputs.shape[1]
    features = width * size

    def from_tok(weight, dim):
        return lax.all_gather(weight, "tok", axis=dim, tiled=True)

    def pair_to_tok(local):
        kept, sent = local
        count = lax.axis_size("tok")
        got = lax.ppermute(sent, "tok", [(i, i ^ 1) for i in range(count)])
        both = add_pair(kept, got)
        groups = [list(range(core, count, 2)) for core in range(2)]
        total = lax.psum_scatter(
            both, "tok", scatter_dimension=0, tiled=True, axis_index_groups=groups
        )
        return total.astype(F32)

    qkv_cols, ff_cols = qkv_weight.shape[1], gate_weight.shape[1]
    middle = ff_cols // 256 * 128
    parts = ((0, middle), (middle, ff_cols))
    if size == 4 and lax.axis_size("tok") == 8:
        lane = lax.broadcasted_iota(jnp.int32, (norm1_gain.shape[0], 128), 1)
        rows_in, w_attn, locals_ff = first_gather(
            inputs,
            jnp.where(lane < 64, norm1_gain[:, None], norm2_gain[:, None]),
            out_weight.T,
            (qkv_weight, gate_weight, up_weight, down_weight.T),
            parts,
        )
    else:
        rows_in = gather_mdl(inputs, 1)
        attn_local = jnp.concatenate([scaled(qkv_weight, norm1_gain), out_weight.T], axis=1)
        w_attn = from_tok(attn_local, 0)
        scaled_gu = [scaled(weight, norm2_gain) for weight in (gate_weight, up_weight)]
        locals_ff = [
            jnp.concatenate([w[:, start:stop] for w in (*scaled_gu, down_weight.T)], axis=1)
            for start, stop in parts
        ]
    w_qkv = w_attn[:, :qkv_cols]
    w_parts = [from_tok(local, 0) for local in locals_ff]

    qkv = rows_to_cols(nn(rows_in, w_qkv).astype(BF16))
    count = qkv.shape[0]
    scale_own = row_scale(lax.dynamic_slice_in_dim(rows_in, me * count, count, 0))
    scale_one = row_scale(after(rows_in, qkv))
    half = HEAD // 2
    frequency = jnp.exp(jnp.arange(half, dtype=F32) * (-2.0 * math.log(10000.0) / HEAD))
    angles = positions.astype(F32)[:, None] * frequency[None, :]
    cos, sin = jnp.cos(angles), jnp.sin(angles)
    kv_own = qkv[:, head_cols:].astype(F32) * scale_own
    key_rows = turn(kv_own[:, :HEAD], cos, sin)
    kv = gather_mdl(jnp.concatenate([key_rows, kv_own[:, HEAD:]], axis=1).astype(BF16), 0)
    first = (me * count).astype(jnp.int32).reshape(1)
    pos = positions[:, None]
    attended, log_norm = attention_forward(first, qkv, kv, cos, sin, pos, scale_own)
    head_block = cols_to_rows(attended)
    residual = inputs.astype(F32)
    payload, scatter = product_to_mdl((head_block,), w_attn, (qkv_cols,))
    mixed = residual + scatter(payload)

    rows_two = gather_mdl(mixed.astype(BF16), 1)
    scale_two = row_scale(rows_two)
    rows_hat = (rows_two.astype(F32) * scale_two).astype(BF16)
    rows, above, stat_two, partial, hiddens, sums = rows_hat, cotangent, 0.0, (), [], []
    for index, (weight, (start, stop)) in enumerate(zip(w_parts, parts)):
        cols = stop - start
        last = index == len(parts) - 1
        gate_in = nn(rows, weight[:, :cols])
        up_in = nn(rows, weight[:, cols : 2 * cols])
        d_hidden = nn(above, weight[:, 2 * cols :])
        gelu, slope = gelu_parts(gate_in)
        hidden = (gelu * up_in).astype(BF16)
        d_gate = d_hidden * up_in * slope
        d_up = d_hidden * gelu
        stat_two += jnp.sum(d_gate * gate_in + d_up * up_in, axis=1)
        d_gate, d_up = d_gate.astype(BF16), d_up.astype(BF16)
        hiddens.append(hidden)
        lefts, starts = (d_gate, d_up), (0, cols)
        if last:
            payload, scatter = product_to_mdl(lefts, weight, starts, partial)
            rows, above, _ = lax.optimization_barrier((rows, above, payload[0]))
        local = part_grad(rows, above, d_gate, d_up, hidden)
        if not last:
            d_gate = after(d_gate, local[0])
            partial = (sum_products((d_gate, d_up), weight, starts),)
            rows, above, _ = lax.optimization_barrier((rows, above, local[0]))
        sums.append(pair_to_tok(local))
    d_two = scatter(payload)
    stat_two = sum_mdl(stat_two.reshape(8, -1)).reshape(-1, 1) * (1.0 / features)
    scale_mixed = scale_two * mixed
    cotangent_own = lax.dynamic_slice_in_dim(cotangent, me * width, width, 1).astype(F32)
    d_mixed = cotangent_own + scale_two * (d_two - scale_mixed * stat_two)

    d_mixed_b = after(d_mixed.astype(BF16), local[0])
    down_starts = tuple(2 * (stop - start) for start, stop in parts)
    ffn = (sum_products((after(hiddens[0], d_mixed_b),), w_parts[0], down_starts[:1]),)
    ffn_payload, ffn_scatter = product_to_mdl(
        (after(hiddens[1], d_mixed_b),), w_parts[1], down_starts[1:], ffn
    )
    if size == 4 and lax.axis_size("tok") == 8:
        pieces = gather_pieces(d_mixed_b)
        d_head = pieces_product(pieces, w_attn, qkv_cols, head_block.shape[1])
        heads_later = after(head_block, d_head)
        out_local = pieces_grad(pieces, heads_later)
    else:
        d_mixed_rows = gather_mdl(d_mixed_b, 1)
        d_head = nn(d_mixed_rows, w_attn[:, qkv_cols:]).astype(BF16)
        out_local = pair_grad(d_mixed_rows, head_block)
    out_grad = pair_to_tok(out_local)
    d_attended = rows_to_cols(d_head)
    d_query, d_kv = attention_backward(
        first, qkv, kv, cos, sin, pos, scale_own, attended, d_attended, log_norm
    )
    d_kv = scatter_mdl(d_kv.astype(BF16), 0)
    d_key = unturn(d_kv[:, :HEAD], cos, sin).astype(BF16)
    d_qkv = jnp.concatenate([d_query, d_key, d_kv[:, HEAD:].astype(BF16)], axis=1)
    stat_one = jnp.sum(d_qkv.astype(F32) * qkv.astype(F32), axis=1) * scale_own[:, 0]
    d_qkv_part = cols_to_rows(d_qkv)
    stat_rows = jnp.zeros((size, count), F32)
    stat_rows = sum_mdl(lax.dynamic_update_slice(stat_rows, stat_one[None], (me, 0)))
    stat_one = stat_rows.reshape(-1, 1) * (1.0 / features)
    payload, scatter = product_to_mdl((d_qkv_part,), w_attn, (0,))
    d_scaled = (after(d_qkv_part, payload[0]).astype(F32) * scale_one).astype(BF16)
    *qkv_local, gain_one = pair_grad(rows_in, d_scaled, w_attn)
    qkv_sum = pair_to_tok(qkv_local)
    d_one = scatter(payload)
    ffn_sum = ffn_scatter(ffn_payload, d_qkv_part)
    block_out = (mixed + ffn_sum).astype(BF16)
    input_grad = d_mixed + scale_one * (d_one - (scale_one * residual) * stat_one)

    norm1_late, norm2_late, gate_late, up_late, _ = lax.optimization_barrier(
        (norm1_gain, norm2_gain, gate_weight, up_weight, local[0])
    )

    def unfold(total, gain):
        return total * gain.astype(F32)[:, None]

    def joined(at):
        widths = [total.shape[1] // 3 for total in sums]
        pieces = [total[:, at * cols :][:, :cols] for total, cols in zip(sums, widths)]
        return jnp.concatenate(pieces, axis=1)

    gate_sum, up_sum, down_grad = joined(0), joined(1), joined(2).T
    gain_two = jnp.sum(
        gate_late.astype(F32) * gate_sum + up_late.astype(F32) * up_sum, axis=1
    )
    gate_grad, up_grad = unfold(gate_sum, norm2_late), unfold(up_sum, norm2_late)
    out_grad = out_grad.T
    gain_two_grad = sum_mdl(gain_two)
    gain_one = sum_mdl(sum_tok(gain_one.reshape(8, -1))).reshape(-1)
    shard = norm1_gain.shape[0]
    gain_one = lax.dynamic_slice_in_dim(gain_one, lax.axis_index("tok") * shard, shard, 0)
    gain_one_grad = gain_one / norm1_late.astype(F32)
    return (
        block_out,
        input_grad,
        gain_one_grad,
        unfold(qkv_sum, norm1_late),
        out_grad,
        gain_two_grad,
        gate_grad,
        up_grad,
        down_grad,
    )


def solution(mesh):
    return jax.shard_map(
        on_device,
        mesh=mesh,
        in_specs=(
            P("tok", "mdl"),
            P(("tok", "mdl")),
            P("tok"),
            P("tok", "mdl"),
            P("mdl", "tok"),
            P("tok"),
            P("tok", "mdl"),
            P("tok", "mdl"),
            P("mdl", "tok"),
            P("tok", None),
        ),
        out_specs=(
            P("tok", "mdl"),
            P("tok", "mdl"),
            P("tok"),
            P("tok", "mdl"),
            P("mdl", "tok"),
            P("tok"),
            P("tok", "mdl"),
            P("tok", "mdl"),
            P("mdl", "tok"),
        ),
        check_vma=False,
    )
```

```python
import functools
import math

import jax
import jax.numpy as jnp
from jax import lax
from jax.experimental import pallas as pl
from jax.experimental.pallas import tpu as pltpu
from jax.sharding import PartitionSpec as P


HEADS = 10
HEAD = 256
NORM_EPS = 1e-06
F32 = jnp.float32
BF16 = jnp.bfloat16
MASKED = -1e30


def nt(left_op, right_op):
    return lax.dot_general(
        left_op, right_op, (((1,), (1,)), ((), ())), preferred_element_type=F32
    )


def tn(left_op, right_op):
    return lax.dot_general(
        left_op, right_op, (((0,), (0,)), ((), ())), preferred_element_type=F32
    )


def nn(left_op, right_op):
    return jnp.dot(left_op, right_op, preferred_element_type=F32)


def swap(block, distance):
    size = lax.axis_size("mdl")
    return lax.ppermute(block, "mdl", [(i, i ^ distance) for i in range(size)])


def gather_mdl(block, dim):
    size = lax.axis_size("mdl")
    if size != 4:
        return lax.all_gather(block, "mdl", axis=dim, tiled=True)
    me = lax.axis_index("mdl")
    half = block.shape[0] // 2
    along_x = swap(block, 1)
    along_y = swap(block, 2)
    top = swap(along_x[:half], 2)
    bottom = swap(along_y[half:], 1)
    width = block.shape[dim]
    shape = list(block.shape)
    shape[dim] = width * size
    whole = jnp.zeros(shape, block.dtype)

    def put(whole, piece, source, row):
        start = [0, 0]
        start[dim] = source * width
        start[0] = start[0] + row
        return lax.dynamic_update_slice(whole, piece, tuple(start))

    whole = put(whole, block, me, 0)
    whole = put(whole, along_x, me ^ 1, 0)
    whole = put(whole, along_y, me ^ 2, 0)
    whole = put(whole, top, me ^ 3, 0)
    whole = put(whole, bottom, me ^ 3, half)
    return whole


def scatter_mdl(part, dim):
    size = lax.axis_size("mdl")
    if size != 4:
        return lax.psum_scatter(part, "mdl", scatter_dimension=dim, tiled=True).astype(F32)
    me = lax.axis_index("mdl")
    shape = list(part.shape)
    shape[dim] //= size
    half = shape[0] // 2

    def piece(block, row):
        start = [0, 0]
        start[dim] = block * shape[dim]
        start[0] = start[0] + row
        return lax.dynamic_slice(part, tuple(start), (half, shape[1]))

    sums = []
    for row, first, second in ((0, 1, 2), (half, 2, 1)):
        sent = jnp.stack([piece(me ^ first, row), piece(me ^ 3, row)])
        sums.append((row, second, swap(sent, first)))
    partial = []
    for row, second, got in sums:
        other = piece(me ^ second, row).astype(F32) + got[1].astype(F32)
        partial.append((row, got[0], swap(other.astype(BF16), second)))
    return jnp.concatenate(
        [
            piece(me, row).astype(F32) + first.astype(F32) + second.astype(F32)
            for row, first, second in partial
        ],
        axis=0,
    )


def gather_pieces(block):
    half = block.shape[0] // 2
    along_x = swap(block, 1)
    along_y = swap(block, 2)
    top = swap(along_x[:half], 2)
    bottom = swap(along_y[half:], 1)
    return block, along_x, along_y, top, bottom


def scatter_payload(payload, *earlier):
    top_sent, bottom_sent, top_kept, bottom_kept = payload
    got_top = swap(top_sent, 1)
    got_bottom = swap(bottom_sent, 2)
    halves = []
    for kept, got, second in ((top_kept, got_top, 2), (bottom_kept, got_bottom, 1)):
        passed = (kept[1].astype(F32) + got[1].astype(F32)).astype(BF16)
        if earlier:
            passed = after(passed, *earlier)
        last = swap(passed, second)
        halves.append(kept[0].astype(F32) + got[0].astype(F32) + last.astype(F32))
    return jnp.concatenate(halves, axis=0)


def sum_mdl(value):
    size = lax.axis_size("mdl")
    distance = 1
    while distance < size:
        value = value + swap(value, distance)
        distance *= 2
    return value


def sum_tok(value):
    size = lax.axis_size("tok")
    distance = 1
    while distance < size:
        value = value + lax.ppermute(value, "tok", [(i, i ^ distance) for i in range(size)])
        distance *= 2
    return value


def rows_to_cols(block):
    return lax.all_to_all(block, "mdl", split_axis=0, concat_axis=1, tiled=True)


def cols_to_rows(block):
    return lax.all_to_all(block, "mdl", split_axis=1, concat_axis=0, tiled=True)


def first_kernel(parts, x_ref, gains_ref, right_ref, *refs):
    weights, (rows_ref, weight_ref), locals_ref = refs[:4], refs[4:6], refs[6:8]
    held, joined, left_ref = refs[8:12], refs[12:14], refs[14]
    own, x_sent, x_got, w_up, w_down, w_core, w_got = refs[15:]
    me, tok = lax.axis_index("mdl"), lax.axis_index("tok")
    pairs = lax.axis_size("tok") // 2
    level, last = tok // 2, pairs - 1
    half, width = x_ref.shape[0] // 2, x_ref.shape[1]
    shard, split, all_cols = *left_ref.shape, weight_ref.shape[1]
    below, above = level > 0, level < last

    barrier = pltpu.get_barrier_semaphore()
    pl.semaphore_signal(barrier, inc=1, device_id={"mdl": me ^ 1})
    pl.semaphore_signal(barrier, inc=1, device_id={"mdl": me ^ 2})
    pl.semaphore_signal(barrier, inc=1, device_id={"tok": tok ^ 1})

    @pl.when(below)
    def _():
        pl.semaphore_signal(barrier, inc=1, device_id={"tok": tok - 2})

    @pl.when(above)
    def _():
        pl.semaphore_signal(barrier, inc=1, device_id={"tok": tok + 2})

    pl.semaphore_wait(barrier, 3 + below.astype(jnp.int32) + above.astype(jnp.int32))

    def cols(block):
        return pl.ds(pl.multiple_of(block * width, 128), width)

    near_cols = split // 256 * 128
    windows = (
        pl.ds(split, all_cols - split),
        pl.ds(0, near_cols),
        pl.ds(near_cols, split - near_cols),
    )

    def block(index, part):
        return weight_ref.at[pl.ds(pl.multiple_of(index * shard, 16), shard), windows[part]]

    def x_copy(source, target, at, to):
        return pltpu.make_async_remote_copy(
            source, target, x_sent.at[at], x_got.at[at], device_id={"mdl": me ^ to}
        )

    def w_copy(source, index, part, sent, to):
        return pltpu.make_async_remote_copy(
            source, block(index, part), sent, w_got.at[index, part], device_id={"tok": to}
        )

    mine = rows_ref.at[:, cols(me)]
    to_x, to_y = x_copy(x_ref, mine, 0, 1), x_copy(x_ref, mine, 1, 2)
    keeps = [pltpu.make_async_copy(x_ref, mine, own.at[0])]
    loads = [
        pltpu.make_async_copy(weight, to, own.at[4 + at])
        for at, (weight, to) in enumerate(zip(weights, held))
    ]

    def send_own(source, part):
        @pl.when(above)
        def _():
            w_copy(source, tok, part, w_up.at[0, part], tok + 2).start()

        @pl.when(below)
        def _():
            w_copy(source, tok, part, w_down.at[0, part], tok - 2).start()

        w_copy(source, tok, part, w_core.at[tok, part], tok ^ 1).start()
        keeps.append(pltpu.make_async_copy(source, block(tok, part), own.at[1 + part]))
        keeps[-1].start()

    send_own(right_ref, 0)
    for copy in (to_x, to_y, keeps[0], *loads):
        copy.start()
    loads[0].wait()
    gain_one, gain = gains_ref[:, :1].astype(F32), gains_ref[:, 64:65].astype(F32)
    left_ref[...] = (held[0][...].astype(F32) * gain_one).astype(BF16)
    held = held[1:]
    for copy in loads[1:]:
        copy.wait()
    for (start, stop), out in zip(parts, joined):
        count = stop - start
        for at, source in enumerate(held):
            value = source[:, start:stop]
            if at < 2:
                value = (value.astype(F32) * gain).astype(BF16)
            out[:, at * count : (at + 1) * count] = value
        if start == 0:
            for part in (1, 2):
                send_own(left_ref.at[:, windows[part]], part)

    def relay(distance, part):
        low, high = tok - 2 * distance, tok + 2 * distance

        @pl.when(level >= distance)
        def _():
            source = block(low, part)
            w_copy(source, low, part, w_core.at[low, part], tok ^ 1).wait_recv()

            @pl.when(above)
            def _():
                w_copy(source, low, part, w_up.at[distance, part], tok + 2).start()

            w_copy(source, low, part, w_core.at[low, part], tok ^ 1).start()

        @pl.when(level + distance <= last)
        def _():
            source = block(high, part)
            w_copy(source, high, part, w_core.at[high, part], tok ^ 1).wait_recv()

            @pl.when(below)
            def _():
                w_copy(source, high, part, w_down.at[distance, part], tok - 2).start()

            w_copy(source, high, part, w_core.at[high, part], tok ^ 1).start()

    for part in range(3):
        relay(1, part)
    stores = [
        pltpu.make_async_copy(out, to, own.at[8 + at])
        for at, (out, to) in enumerate(zip(joined, locals_ref))
    ]
    for copy in stores:
        copy.start()
    from_x = rows_ref.at[pl.ds(0, half), cols(me ^ 1)]
    from_y = rows_ref.at[pl.ds(half, half), cols(me ^ 2)]
    top, bottom = x_copy(from_x, from_x, 2, 2), x_copy(from_y, from_y, 3, 1)
    to_x.wait_recv()
    top.start()
    to_y.wait_recv()
    bottom.start()
    for distance in range(2, pairs):
        for part in range(3):
            relay(distance, part)
    for copy in (*keeps, *stores):
        copy.wait()
    for copy in (top, bottom):
        copy.wait_recv()
    for copy in (to_x, to_y, top, bottom):
        copy.wait_send()

    for distance in range(pairs):
        for part in range(3):
            mine = block(tok, part)

            @pl.when((level >= distance) & above)
            def _(mine=mine, distance=distance, part=part):
                w_copy(mine, tok, part, w_up.at[distance, part], tok + 2).wait_send()

            @pl.when((level + distance <= last) & below)
            def _(mine=mine, distance=distance, part=part):
                w_copy(mine, tok, part, w_down.at[distance, part], tok - 2).wait_send()

            near, far = 2 * distance + tok % 2, 2 * distance + 1 - tok % 2
            w_copy(block(near, part), near, part, w_core.at[near, part], tok ^ 1).wait_send()
            w_copy(block(far, part), far, part, w_core.at[near, part], tok ^ 1).wait_recv()


def first_gather(inputs, gains, right, weights, parts):
    tokens, width = inputs.shape
    shard, left_cols = weights[0].shape
    cols = left_cols + right.shape[1]
    pairs = lax.axis_size("tok") // 2
    dma = pltpu.SemaphoreType.DMA
    locals_ff = [(shard, 3 * (stop - start)) for start, stop in parts]
    shapes = [(tokens, 4 * width), (2 * pairs * shard, cols), *locals_ff]
    *gathered, first, second = pl.pallas_call(
        functools.partial(first_kernel, parts),
        out_shape=[jax.ShapeDtypeStruct(shape, BF16) for shape in shapes],
        in_specs=[pl.BlockSpec(memory_space=pltpu.VMEM)] * 3
        + [pl.BlockSpec(memory_space=pl.ANY)] * 4,
        out_specs=[pl.BlockSpec(memory_space=pl.ANY)] * 4,
        scratch_shapes=[pltpu.VMEM(array.shape, BF16) for array in weights]
        + [pltpu.VMEM(shape, BF16) for shape in (*locals_ff, weights[0].shape)]
        + [
            dma((10,)), dma((4,)), dma((4,)), dma((pairs, 3)), dma((pairs, 3)),
            dma((2 * pairs, 3)), dma((2 * pairs, 3)),
        ],
        compiler_params=pltpu.CompilerParams(
            collective_id=0, has_side_effects=True, vmem_limit_bytes=60 << 20
        ),
    )(inputs, gains, right, *weights)
    return *gathered, (first, second)


def in_order(mebibytes):
    return pltpu.CompilerParams(
        dimension_semantics=(pltpu.ARBITRARY,), vmem_limit_bytes=mebibytes << 20
    )


def cost(flops, bytes_accessed, transcendentals=0):
    return pl.CostEstimate(
        flops=flops, bytes_accessed=bytes_accessed, transcendentals=transcendentals
    )


def turn(vector, cos, sin):
    half = HEAD // 2
    lower, upper = vector[:, :half], vector[:, half:]
    return jnp.concatenate([lower * cos - upper * sin, upper * cos + lower * sin], axis=1)


def unturn(vector, cos, sin):
    half = HEAD // 2
    lower, upper = vector[:, :half], vector[:, half:]
    return jnp.concatenate([lower * cos + upper * sin, upper * cos - lower * sin], axis=1)


def seen(first_ref, position_ref, queries, keys):
    row = lax.broadcasted_iota(jnp.int32, (queries, keys), 0) + first_ref[0]
    distance = row - lax.broadcasted_iota(jnp.int32, (queries, keys), 1)
    return (distance >= 0) & (distance <= position_ref[...])


def forward_kernel(
    first_ref, q_ref, kv_ref, cos_ref, sin_ref, pos_ref, scale_ref, out_ref, norm_ref
):
    query = turn(q_ref[...].astype(F32) * scale_ref[...], cos_ref[...], sin_ref[...])
    query = (query * HEAD ** (-0.5)).astype(BF16)
    keys, values = kv_ref[:, :HEAD], kv_ref[:, HEAD:]
    scores = nt(query, keys)
    scores = jnp.where(seen(first_ref, pos_ref, *scores.shape), scores, MASKED)
    top = jnp.max(scores, axis=1, keepdims=True)
    weights = jnp.exp(scores - top)
    total = jnp.sum(weights, axis=1, keepdims=True)
    out_ref[...] = (nn(weights.astype(BF16), values) / total).astype(BF16)
    norm_ref[0] = top + jnp.log(total)


def backward_kernel(
    first_ref, q_ref, kv_ref, cos_ref, sin_ref, pos_ref, scale_ref, att_ref, datt_ref, norm_ref,
    dq_ref, dkv_ref,
):
    head = pl.program_id(0)
    scale = HEAD ** (-0.5)
    cos, sin = cos_ref[...], sin_ref[...]
    query = (turn(q_ref[...].astype(F32) * scale_ref[...], cos, sin) * scale).astype(BF16)
    keys, values = kv_ref[:, :HEAD], kv_ref[:, HEAD:]
    scores = nt(query, keys)
    visible = seen(first_ref, pos_ref, *scores.shape)
    again = jnp.where(visible, jnp.exp(scores - norm_ref[0]), 0.0)
    d_att = datt_ref[...]
    delta = jnp.sum(d_att.astype(F32) * att_ref[...].astype(F32), axis=1, keepdims=True)
    d_scores = (again * (nt(d_att, values) - delta)).astype(BF16)
    d_query = nn(d_scores, keys) * scale
    dq_ref[...] = unturn(d_query, cos, sin).astype(BF16)

    @pl.when(head == 0)
    def _():
        dkv_ref[...] = jnp.zeros_like(dkv_ref)

    dkv_ref[:, :HEAD] += tn(d_scores, query)
    dkv_ref[:, HEAD:] += tn(again.astype(BF16), d_att)


def whole_spec(shape):
    return pl.BlockSpec(shape, lambda head: (0,) * len(shape))


def attention_forward(first, qkv, kv, cos, sin, pos, scale):
    rows, keys = qkv.shape[0], kv.shape[0]
    head_spec = pl.BlockSpec((rows, HEAD), lambda head: (0, head))
    return pl.pallas_call(
        forward_kernel,
        grid=(HEADS,),
        out_shape=(
            jax.ShapeDtypeStruct((rows, HEADS * HEAD), BF16),
            jax.ShapeDtypeStruct((HEADS, rows, 1), F32),
        ),
        in_specs=[
            pl.BlockSpec(memory_space=pltpu.SMEM),
            head_spec,
            whole_spec((keys, 2 * HEAD)),
            whole_spec((rows, HEAD // 2)),
            whole_spec((rows, HEAD // 2)),
            whole_spec((rows, 1)),
            whole_spec((rows, 1)),
        ],
        out_specs=(head_spec, pl.BlockSpec((1, rows, 1), lambda head: (head, 0, 0))),
        compiler_params=in_order(32),
        cost_estimate=cost(4 * rows * keys * HEADS * HEAD, 4 * rows * HEADS * HEAD + 4 * keys * HEAD, rows * keys * HEADS),
        name="att_f",
    )(first, qkv, kv, cos, sin, pos, scale)


def attention_backward(first, qkv, kv, cos, sin, pos, scale, att, d_att, norm):
    rows, keys = qkv.shape[0], kv.shape[0]
    head_spec = pl.BlockSpec((rows, HEAD), lambda head: (0, head))
    return pl.pallas_call(
        backward_kernel,
        grid=(HEADS,),
        out_shape=(
            jax.ShapeDtypeStruct((rows, HEADS * HEAD), BF16),
            jax.ShapeDtypeStruct((keys, 2 * HEAD), F32),
        ),
        in_specs=[
            pl.BlockSpec(memory_space=pltpu.SMEM),
            head_spec,
            whole_spec((keys, 2 * HEAD)),
            whole_spec((rows, HEAD // 2)),
            whole_spec((rows, HEAD // 2)),
            whole_spec((rows, 1)),
            whole_spec((rows, 1)),
            head_spec,
            head_spec,
            pl.BlockSpec((1, rows, 1), lambda head: (head, 0, 0)),
        ],
        out_specs=(head_spec, whole_spec((keys, 2 * HEAD))),
        compiler_params=in_order(40),
        cost_estimate=cost(10 * rows * keys * HEADS * HEAD, 8 * rows * HEADS * HEAD + 12 * keys * HEAD, rows * keys * HEADS),
        name="att_b",
    )(first, qkv, kv, cos, sin, pos, scale, att, d_att, norm)


def keep_half(core_ref, total, kept, sent):
    half = total.shape[0] // 2
    for core, (first, second) in enumerate(((kept, sent), (sent, kept))):

        @pl.when(core_ref[0] == core)
        def _(first=first, second=second):
            first[...] = total[:half]
            second[...] = total[half:]


def pair_kernel(core_ref, left_ref, right_ref, *refs):
    total = tn(left_ref[...], right_ref[...])
    if len(refs) == 4:
        weight = refs[0][:, : total.shape[1]].astype(F32)
        refs[3][...] = jnp.sum(total * weight, axis=1, keepdims=True)
    keep_half(core_ref, total.astype(BF16), *refs[-3:-1] if len(refs) == 4 else refs)


def split_pairs(total, pairs, core):
    rows, cols = total.shape
    total = total.reshape(pairs, 2, rows // pairs // 2, cols)
    return tuple(
        lax.dynamic_index_in_dim(total, index, 1, False).reshape(-1, cols)
        for index in (core, 1 - core)
    )


def core_index():
    return (lax.axis_index("tok") % 2).astype(jnp.int32).reshape(1)


def pair_grad(left, right, weight=None):
    tokens, rows = left.shape
    cols = right.shape[1]
    pairs = lax.axis_size("tok") // 2
    step = rows // pairs
    if step % 128 or cols % 128:
        total = tn(left, right)
        halves = split_pairs(total.astype(BF16), pairs, lax.axis_index("tok") % 2)
        if weight is None:
            return halves
        return *halves, jnp.sum(total * weight[:, :cols].astype(F32), axis=1, keepdims=True)
    out_shape = [jax.ShapeDtypeStruct((rows // 2, cols), BF16)] * 2
    out_specs = [pl.BlockSpec((step // 2, cols), lambda pair: (pair, 0))] * 2
    in_specs = [
        pl.BlockSpec(memory_space=pltpu.SMEM),
        pl.BlockSpec((tokens, step), lambda pair: (0, pair)),
        pl.BlockSpec((tokens, cols), lambda pair: (0, 0)),
    ]
    operands = [core_index(), left, right]
    if weight is not None:
        operands.append(weight)
        in_specs.append(pl.BlockSpec((step, weight.shape[1]), lambda pair: (pair, 0)))
        out_shape.append(jax.ShapeDtypeStruct((rows, 1), F32))
        out_specs.append(pl.BlockSpec((step, 1), lambda pair: (pair, 0)))
    return pl.pallas_call(
        pair_kernel,
        grid=(pairs,),
        out_shape=out_shape,
        in_specs=in_specs,
        out_specs=out_specs,
        compiler_params=in_order(48),
        cost_estimate=cost(2 * tokens * rows * cols, 2 * (tokens * (rows + cols) + rows * cols)),
    )(*operands)


def part_kernel(core_ref, rows_ref, above_ref, d_gate_ref, d_up_ref, hidden_ref, kept, sent):
    cols = hidden_ref.shape[1]
    for at, (left_ref, right_ref) in enumerate(
        ((rows_ref, d_gate_ref), (rows_ref, d_up_ref), (above_ref, hidden_ref))
    ):
        total = tn(left_ref[...], right_ref[...]).astype(BF16)
        window = (slice(None), pl.ds(at * cols, cols))
        keep_half(core_ref, total, kept.at[window], sent.at[window])


def part_grad(rows, above, d_gate, d_up, hidden):
    tokens, features = rows.shape
    cols = hidden.shape[1]
    pairs = lax.axis_size("tok") // 2
    step = features // pairs
    if step % 128 or cols % 128:
        total = [tn(rows, d_gate), tn(rows, d_up), tn(above, hidden)]
        total = jnp.concatenate(total, axis=1).astype(BF16)
        return split_pairs(total, pairs, lax.axis_index("tok") % 2)
    out = jax.ShapeDtypeStruct((features // 2, 3 * cols), BF16)
    left_spec = pl.BlockSpec((tokens, step), lambda pair: (0, pair))
    right_spec = pl.BlockSpec((tokens, cols), lambda pair: (0, 0))
    return pl.pallas_call(
        part_kernel,
        grid=(pairs,),
        out_shape=(out, out),
        in_specs=[pl.BlockSpec(memory_space=pltpu.SMEM)] + [left_spec] * 2 + [right_spec] * 3,
        out_specs=[pl.BlockSpec((step // 2, 3 * cols), lambda pair: (pair, 0))] * 2,
        compiler_params=in_order(48),
        cost_estimate=cost(
            6 * tokens * features * cols,
            2 * (2 * tokens * features + 3 * cols * (tokens + features)),
        ),
    )(core_index(), rows, above, d_gate, d_up, hidden)


def hold_piece(pieces, held):
    *blocks, top, bottom = pieces
    at = pl.program_id(0)
    for index, piece in enumerate(blocks):

        @pl.when(at == index)
        def _(piece=piece):
            held[...] = piece[...]

    @pl.when(at == len(blocks))
    def _():
        half = top.shape[0]
        held[:half] = top[...]
        held[half:] = bottom[...]


def pieces_grad_kernel(me_ref, core_ref, *refs):
    *pieces, right_ref, kept, sent, held = refs
    hold_piece(pieces, held)
    keep_half(core_ref, tn(held[...], right_ref[...]).astype(BF16), kept, sent)


def add_kernel(left_ref, right_ref, out_ref):
    out_ref[...] = (left_ref[...].astype(F32) + right_ref[...].astype(F32)).astype(BF16)


def add_pair(left, right):
    rows, cols = left.shape
    if rows % 256 or cols % 128:
        return (left.astype(F32) + right.astype(F32)).astype(BF16)
    steps = 10 if rows % 160 == 0 else 8
    spec = pl.BlockSpec((rows // steps, cols), lambda at: (at, 0))
    return pl.pallas_call(
        add_kernel,
        grid=(steps,),
        out_shape=jax.ShapeDtypeStruct(left.shape, BF16),
        in_specs=[spec, spec],
        out_specs=spec,
        compiler_params=in_order(16),
        cost_estimate=cost(rows * cols, 6 * rows * cols),
    )(left, right)


def pieces_grad(pieces, right):
    tokens, step = pieces[0].shape
    cols = right.shape[1]
    me = lax.axis_index("mdl").astype(jnp.int32).reshape(1)
    out = jax.ShapeDtypeStruct((2 * step, cols), BF16)
    return pl.pallas_call(
        pieces_grad_kernel,
        grid_spec=pltpu.PrefetchScalarGridSpec(
            num_scalar_prefetch=2,
            grid=(4,),
            in_specs=[
                pl.BlockSpec(array.shape, lambda at, me_ref, core_ref: (0, 0))
                for array in (*pieces, right)
            ],
            out_specs=[
                pl.BlockSpec((step // 2, cols), lambda at, me_ref, core_ref: (me_ref[0] ^ at, 0))
            ]
            * 2,
            scratch_shapes=[pltpu.VMEM((tokens, step), BF16)],
        ),
        out_shape=(out, out),
        compiler_params=in_order(48),
        cost_estimate=cost(8 * tokens * step * cols, 2 * (4 * tokens * step + 5 * step * cols)),
    )(me, core_index(), *pieces, right)


def sum_kernel(starts, *refs):
    *lefts, weight_ref, out_ref = refs
    total = 0.0
    for left_ref, start in zip(lefts, starts):
        total += nt(left_ref[...], weight_ref[:, start : start + left_ref.shape[1]])
    out_ref[...] = total


def sum_products(lefts, weight, starts):
    tokens = lefts[0].shape[0]
    rows, cols = weight.shape
    if lefts[0].shape[1] % 128:
        return sum(
            nt(left, weight[:, start : start + left.shape[1]])
            for left, start in zip(lefts, starts)
        )
    step = 512
    depth = sum(left.shape[1] for left in lefts)
    return pl.pallas_call(
        functools.partial(sum_kernel, starts),
        grid=(rows // step,),
        out_shape=jax.ShapeDtypeStruct((tokens, rows), F32),
        in_specs=[pl.BlockSpec(left.shape, lambda row: (0, 0)) for left in lefts]
        + [pl.BlockSpec((step, cols), lambda row: (row, 0))],
        out_specs=pl.BlockSpec((tokens, step), lambda row: (0, row)),
        compiler_params=in_order(48),
        cost_estimate=cost(2 * tokens * rows * depth, 2 * rows * cols + 4 * tokens * rows),
    )(*lefts, weight)


def payload_kernel(starts, me_ref, *refs):
    lefts, weight_ref = refs[: len(starts)], refs[len(starts)]
    top_sent, bottom_sent, top_kept, bottom_kept = refs[-4:]
    total = refs[-5][...] if len(refs) == len(starts) + 6 else 0.0
    for left_ref, start in zip(lefts, starts):
        total += nt(left_ref[...], weight_ref[:, start : start + left_ref.shape[1]])
    total = total.astype(BF16)
    half = total.shape[0] // 2
    places = (
        ((top_kept, 0), (bottom_kept, 0)),
        ((top_sent, 0), (bottom_kept, 1)),
        ((top_kept, 1), (bottom_sent, 0)),
        ((top_sent, 1), (bottom_sent, 1)),
    )
    for distance, ((top, top_at), (bottom, bottom_at)) in enumerate(places):

        @pl.when(pl.program_id(0) == 3 - distance)
        def _(top=top, top_at=top_at, bottom=bottom, bottom_at=bottom_at):
            top[top_at] = total[:half]
            bottom[bottom_at] = total[half:]


def scatter_product(lefts, weight, starts, partial=()):
    tokens = lefts[0].shape[0]
    rows, cols = weight.shape
    step = rows // 4
    me = lax.axis_index("mdl").astype(jnp.int32).reshape(1)
    out = jax.ShapeDtypeStruct((2, tokens // 2, step), BF16)
    depth = sum(left.shape[1] for left in lefts)
    return pl.pallas_call(
        functools.partial(payload_kernel, starts),
        grid_spec=pltpu.PrefetchScalarGridSpec(
            num_scalar_prefetch=1,
            grid=(4,),
            in_specs=[pl.BlockSpec(left.shape, lambda at, me_ref: (0, 0)) for left in lefts]
            + [pl.BlockSpec((step, cols), lambda at, me_ref: (me_ref[0] ^ (3 - at), 0))]
            + [pl.BlockSpec((tokens, step), lambda at, me_ref: (0, me_ref[0] ^ (3 - at)))]
            * len(partial),
            out_specs=[pl.BlockSpec(out.shape, lambda at, me_ref: (0, 0, 0))] * 4,
        ),
        out_shape=(out,) * 4,
        compiler_params=in_order(48),
        cost_estimate=cost(2 * tokens * rows * depth, 2 * (tokens * depth + rows * cols + tokens * rows)),
    )(me, *lefts, weight, *partial)


def pieces_kernel(start, me_ref, *refs):
    *pieces, weight_ref, out_ref, total, held = refs
    hold_piece(pieces, held)
    at = pl.program_id(0)
    part = nn(held[...], weight_ref[:, start : start + out_ref.shape[1]])
    part = part + jnp.where(at > 0, total[...], 0.0)
    total[...] = part

    @pl.when(at == 3)
    def _():
        out_ref[...] = part.astype(BF16)


def pieces_product(pieces, weight, start, width):
    tokens, step = pieces[0].shape
    rows, cols = weight.shape
    me = lax.axis_index("mdl").astype(jnp.int32).reshape(1)
    return pl.pallas_call(
        functools.partial(pieces_kernel, start),
        grid_spec=pltpu.PrefetchScalarGridSpec(
            num_scalar_prefetch=1,
            grid=(4,),
            in_specs=[pl.BlockSpec(piece.shape, lambda at, me_ref: (0, 0)) for piece in pieces]
            + [pl.BlockSpec((step, cols), lambda at, me_ref: (me_ref[0] ^ at, 0))],
            out_specs=pl.BlockSpec((tokens, width), lambda at, me_ref: (0, 0)),
            scratch_shapes=[pltpu.VMEM((tokens, width), F32), pltpu.VMEM((tokens, step), BF16)],
        ),
        out_shape=jax.ShapeDtypeStruct((tokens, width), BF16),
        compiler_params=in_order(40),
        cost_estimate=cost(2 * tokens * rows * width, 2 * (tokens * rows + rows * cols + tokens * width)),
    )(me, *pieces, weight)


def product_to_mdl(lefts, weight, starts, partial=()):
    if lax.axis_size("mdl") == 4:
        payload = scatter_product(lefts, weight, starts, partial)
        return payload, lambda payload, *earlier: scatter_payload(payload, *earlier)
    part = sum((sum_products(lefts, weight, starts), *partial))
    return (part.astype(BF16),), lambda payload, *earlier: scatter_mdl(payload[0], 1)


def after(value, *earlier):
    return lax.optimization_barrier((value, *earlier))[0]


def row_scale(rows_b, axis=-1):
    rows = rows_b.astype(F32)
    return lax.rsqrt(jnp.mean(rows * rows, axis=axis, keepdims=True) + NORM_EPS)


def gelu_parts(value):
    root = math.sqrt(2.0 / math.pi)
    square = value * value
    tanh = jnp.tanh(root * (value + 0.044715 * value * square))
    cdf = 0.5 * (1.0 + tanh)
    slope = cdf + 0.5 * value * (1.0 - tanh * tanh) * root * (1.0 + 3 * 0.044715 * square)
    return value * cdf, slope


def scaled(weight, gain):
    return (weight.astype(F32) * gain.astype(F32)[:, None]).astype(BF16)


def on_device(
    inputs, positions, norm1_gain, qkv_weight, out_weight, norm2_gain, gate_weight,
    up_weight, down_weight, cotangent,
):
    me = lax.axis_index("mdl")
    size = lax.axis_size("mdl")
    head_cols = HEADS * HEAD
    width = inputs.shape[1]
    features = width * size

    def from_tok(weight, dim):
        return lax.all_gather(weight, "tok", axis=dim, tiled=True)

    def pair_to_tok(local):
        kept, sent = local
        count = lax.axis_size("tok")
        got = lax.ppermute(sent, "tok", [(i, i ^ 1) for i in range(count)])
        both = add_pair(kept, got)
        groups = [list(range(core, count, 2)) for core in range(2)]
        total = lax.psum_scatter(
            both, "tok", scatter_dimension=0, tiled=True, axis_index_groups=groups
        )
        return total.astype(F32)

    qkv_cols, ff_cols = qkv_weight.shape[1], gate_weight.shape[1]
    middle = ff_cols // 256 * 128
    parts = ((0, middle), (middle, ff_cols))
    if size == 4 and lax.axis_size("tok") == 8:
        lane = lax.broadcasted_iota(jnp.int32, (norm1_gain.shape[0], 128), 1)
        rows_in, w_attn, locals_ff = first_gather(
            inputs,
            jnp.where(lane < 64, norm1_gain[:, None], norm2_gain[:, None]),
            out_weight.T,
            (qkv_weight, gate_weight, up_weight, down_weight.T),
            parts,
        )
    else:
        rows_in = gather_mdl(inputs, 1)
        attn_local = jnp.concatenate([scaled(qkv_weight, norm1_gain), out_weight.T], axis=1)
        w_attn = from_tok(attn_local, 0)
        scaled_gu = [scaled(weight, norm2_gain) for weight in (gate_weight, up_weight)]
        locals_ff = [
            jnp.concatenate([w[:, start:stop] for w in (*scaled_gu, down_weight.T)], axis=1)
            for start, stop in parts
        ]
    w_qkv = w_attn[:, :qkv_cols]
    w_parts = [from_tok(local, 0) for local in locals_ff]

    qkv = rows_to_cols(nn(rows_in, w_qkv).astype(BF16))
    count = qkv.shape[0]
    scale_own = row_scale(lax.dynamic_slice_in_dim(rows_in, me * count, count, 0))
    scale_one = row_scale(after(rows_in, qkv))
    half = HEAD // 2
    frequency = jnp.exp(jnp.arange(half, dtype=F32) * (-2.0 * math.log(10000.0) / HEAD))
    angles = positions.astype(F32)[:, None] * frequency[None, :]
    cos, sin = jnp.cos(angles), jnp.sin(angles)
    kv_own = qkv[:, head_cols:].astype(F32) * scale_own
    key_rows = turn(kv_own[:, :HEAD], cos, sin)
    kv = gather_mdl(jnp.concatenate([key_rows, kv_own[:, HEAD:]], axis=1).astype(BF16), 0)
    first = (me * count).astype(jnp.int32).reshape(1)
    pos = positions[:, None]
    attended, log_norm = attention_forward(first, qkv, kv, cos, sin, pos, scale_own)
    head_block = cols_to_rows(attended)
    residual = inputs.astype(F32)
    payload, scatter = product_to_mdl((head_block,), w_attn, (qkv_cols,))
    mixed = residual + scatter(payload)

    rows_two = gather_mdl(mixed.astype(BF16), 1)
    scale_two = row_scale(rows_two)
    rows_hat = (rows_two.astype(F32) * scale_two).astype(BF16)
    rows, above, stat_two, partial, hiddens, sums = rows_hat, cotangent, 0.0, (), [], []
    for index, (weight, (start, stop)) in enumerate(zip(w_parts, parts)):
        cols = stop - start
        last = index == len(parts) - 1
        gate_in = nn(rows, weight[:, :cols])
        up_in = nn(rows, weight[:, cols : 2 * cols])
        d_hidden = nn(above, weight[:, 2 * cols :])
        gelu, slope = gelu_parts(gate_in)
        hidden = (gelu * up_in).astype(BF16)
        d_gate = d_hidden * up_in * slope
        d_up = d_hidden * gelu
        stat_two += jnp.sum(d_gate * gate_in + d_up * up_in, axis=1)
        d_gate, d_up = d_gate.astype(BF16), d_up.astype(BF16)
        hiddens.append(hidden)
        lefts, starts = (d_gate, d_up), (0, cols)
        if last:
            payload, scatter = product_to_mdl(lefts, weight, starts, partial)
            rows, above, _ = lax.optimization_barrier((rows, above, payload[0]))
        local = part_grad(rows, above, d_gate, d_up, hidden)
        if not last:
            d_gate = after(d_gate, local[0])
            partial = (sum_products((d_gate, d_up), weight, starts),)
            rows, above, _ = lax.optimization_barrier((rows, above, local[0]))
        sums.append(pair_to_tok(local))
    d_two = scatter(payload)
    stat_two = sum_mdl(stat_two.reshape(8, -1)).reshape(-1, 1) * (1.0 / features)
    scale_mixed = scale_two * mixed
    cotangent_own = lax.dynamic_slice_in_dim(cotangent, me * width, width, 1).astype(F32)
    d_mixed = cotangent_own + scale_two * (d_two - scale_mixed * stat_two)

    d_mixed_b = after(d_mixed.astype(BF16), local[0])
    down_starts = tuple(2 * (stop - start) for start, stop in parts)
    ffn = (sum_products((after(hiddens[0], d_mixed_b),), w_parts[0], down_starts[:1]),)
    ffn_payload, ffn_scatter = product_to_mdl(
        (after(hiddens[1], d_mixed_b),), w_parts[1], down_starts[1:], ffn
    )
    if size == 4 and lax.axis_size("tok") == 8:
        pieces = gather_pieces(d_mixed_b)
        d_head = pieces_product(pieces, w_attn, qkv_cols, head_block.shape[1])
        heads_later = after(head_block, d_head)
        out_local = pieces_grad(pieces, heads_later)
    else:
        d_mixed_rows = gather_mdl(d_mixed_b, 1)
        d_head = nn(d_mixed_rows, w_attn[:, qkv_cols:]).astype(BF16)
        out_local = pair_grad(d_mixed_rows, head_block)
    out_grad = pair_to_tok(out_local)
    d_attended = rows_to_cols(d_head)
    d_query, d_kv = attention_backward(
        first, qkv, kv, cos, sin, pos, scale_own, attended, d_attended, log_norm
    )
    d_kv = scatter_mdl(d_kv.astype(BF16), 0)
    d_key = unturn(d_kv[:, :HEAD], cos, sin).astype(BF16)
    d_qkv = jnp.concatenate([d_query, d_key, d_kv[:, HEAD:].astype(BF16)], axis=1)
    stat_one = jnp.sum(d_qkv.astype(F32) * qkv.astype(F32), axis=1) * scale_own[:, 0]
    d_qkv_part = cols_to_rows(d_qkv)
    stat_rows = jnp.zeros((size, count), F32)
    stat_rows = sum_mdl(lax.dynamic_update_slice(stat_rows, stat_one[None], (me, 0)))
    stat_one = stat_rows.reshape(-1, 1) * (1.0 / features)
    payload, scatter = product_to_mdl((d_qkv_part,), w_attn, (0,))
    d_scaled = (after(d_qkv_part, payload[0]).astype(F32) * scale_one).astype(BF16)
    *qkv_local, gain_one = pair_grad(rows_in, d_scaled, w_attn)
    qkv_sum = pair_to_tok(qkv_local)
    d_one = scatter(payload)
    ffn_sum = ffn_scatter(ffn_payload, d_qkv_part)
    block_out = (mixed + ffn_sum).astype(BF16)
    input_grad = d_mixed + scale_one * (d_one - (scale_one * residual) * stat_one)

    norm1_late, norm2_late, gate_late, up_late, _ = lax.optimization_barrier(
        (norm1_gain, norm2_gain, gate_weight, up_weight, local[0])
    )

    def unfold(total, gain):
        return total * gain.astype(F32)[:, None]

    def joined(at):
        widths = [total.shape[1] // 3 for total in sums]
        pieces = [total[:, at * cols :][:, :cols] for total, cols in zip(sums, widths)]
        return jnp.concatenate(pieces, axis=1)

    gate_sum, up_sum, down_grad = joined(0), joined(1), joined(2).T
    gain_two = jnp.sum(
        gate_late.astype(F32) * gate_sum + up_late.astype(F32) * up_sum, axis=1
    )
    gate_grad, up_grad = unfold(gate_sum, norm2_late), unfold(up_sum, norm2_late)
    out_grad = out_grad.T
    gain_two_grad = sum_mdl(gain_two)
    gain_one = sum_mdl(sum_tok(gain_one.reshape(8, -1))).reshape(-1)
    shard = norm1_gain.shape[0]
    gain_one = lax.dynamic_slice_in_dim(gain_one, lax.axis_index("tok") * shard, shard, 0)
    gain_one_grad = gain_one / norm1_late.astype(F32)
    return (
        block_out,
        input_grad,
        gain_one_grad,
        unfold(qkv_sum, norm1_late),
        out_grad,
        gain_two_grad,
        gate_grad,
        up_grad,
        down_grad,
    )


def solution(mesh):
    return jax.shard_map(
        on_device,
        mesh=mesh,
        in_specs=(
            P("tok", "mdl"),
            P(("tok", "mdl")),
            P("tok"),
            P("tok", "mdl"),
            P("mdl", "tok"),
            P("tok"),
            P("tok", "mdl"),
            P("tok", "mdl"),
            P("mdl", "tok"),
            P("tok", None),
        ),
        out_specs=(
            P("tok", "mdl"),
            P("tok", "mdl"),
            P("tok"),
            P("tok", "mdl"),
            P("mdl", "tok"),
            P("tok"),
            P("tok", "mdl"),
            P("tok", "mdl"),
            P("mdl", "tok"),
        ),
        check_vma=False,
    )
```
